32 devices in a mesh: section: 2 (over core), ctx: 4 (over y, x), shard: 4 (over z).
Axes of the slice: x: 2, y: 2, z: 4, core: 2. Of those that a mesh axis runs over, the one named last changes fastest.
Arguments:
- inputs: bfloat16 [4, 2, 512, 1088], P('shard', None, 'ctx'), may hold values from -6 to 6
- cotangent: bfloat16 [4, 2, 512, 1088], P('shard', None, 'ctx'), may hold values from -6 to 6
- qkv_weight: bfloat16 [2, 1088, 3264], P('section', 'shard'), may hold values from -0.1875 to 0.1875
- out_weight: bfloat16 [2, 1088, 1088], P('section', 'shard'), may hold values from -1.5 to 1.5
- up_weight: bfloat16 [2, 1088, 4352], P('section', 'shard'), may hold values from -0.1875 to 0.1875
- down_weight: bfloat16 [2, 4352, 1088], P('section', None, 'shard'), may hold values from -0.09375 to 0.09375
- norm_gain: bfloat16 [2, 2, 1088], P('section', None, 'shard'), may hold values from 0.5 to 1.5
- norm_bias: bfloat16 [2, 2, 1088], P('section', None, 'shard'), may hold values from -3 to 3
Outputs:
- layer_outputs: bfloat16 [2, 4, 2, 512, 1088], P('section', 'shard', None, 'ctx')
- input_grads: bfloat16 [2, 4, 2, 512, 1088], P('section', 'shard', None, 'ctx')
- qkv_grad: float32 [2, 1088, 3264], P('section', ('ctx', 'shard'))
- out_grad: float32 [2, 1088, 1088], P('section', ('ctx', 'shard'))
- up_grad: float32 [2, 1088, 4352], P('section', ('ctx', 'shard'))
- down_grad: float32 [2, 4352, 1088], P('section', None, ('ctx', 'shard'))
- gain_grad: float32 [2, 2, 1088], P('section', None, ('ctx', 'shard'))
- bias_grad: float32 [2, 2, 1088], P('section', None, ('ctx', 'shard'))
The draws below stay inside these ranges and needn't reach their ends.
All inputs are finite; a program needn't handle non-finite values.
Results may differ from the reference program's by a relative error of at most 0.02.
Values may be sent and summed in bfloat16 or wider, within the bound.
A program may use at most 320 MiB of HBM per device.

```python
import math
import jax
import jax.numpy as jnp
from jax import lax

D = 1088
HEADS = 17
HEAD = 64
FF = 4352
MB = 2
GROUP = 512
LENGTH = 1024
SEQS = 4


def block_scale(key, shape, pieces, low, top_value):
    def one(position, parts):
        draws = jax.random.uniform(jax.random.fold_in(jax.random.fold_in(key, 6), position), (parts,), jnp.float32, low / len(pieces), top_value / len(pieces))
        return jnp.repeat(jnp.exp(draws), shape[position] // parts).reshape((-1,) + (1,) * (len(shape) - position - 1))

    level = one(*pieces[0])
    for cut in pieces[1:]:
        level = level * one(*cut)
    return level


def noise(rng, extent, width, most, cuts=(), held_as=jnp.bfloat16):
    factor_of = block_scale(rng, extent, cuts, -0.22, 0.18) if cuts else 1.0
    result = jax.random.normal(rng, extent, jnp.float32) * width * factor_of
    return jnp.minimum(jnp.maximum(result, -most), most).astype(held_as)


def setup_inputs(seed: int = 0) -> dict:
    seeds = jax.random.split(jax.random.key(seed), 9)
    inputs = noise(seeds[0], (SEQS, MB, GROUP, D), 1.0, 6.0, ((0, 4), (2, 4)))
    cotangent = noise(seeds[1], (SEQS, MB, GROUP, D), 1.0, 6.0, ((0, 4), (2, 4)))
    qkv_weight = noise(seeds[2], (2, D, 3 * D), D ** -0.5, 0.1875, ((0, 2), (1, 4)))
    out_weight = noise(seeds[3], (2, D, D), (D // 64) ** -0.5, 1.5, ((0, 2), (1, 4)))
    up_weight = noise(seeds[4], (2, D, FF), D ** -0.5, 0.1875, ((0, 2), (1, 4)))
    down_weight = noise(seeds[5], (2, FF, D), FF ** -0.5, 0.09375, ((0, 2), (2, 4)))
    norm_gain = jnp.clip(1.0 + 0.1 * jax.random.normal(seeds[6], (2, 2, D), jnp.float32), 0.5, 1.5).astype(jnp.bfloat16)
    norm_bias = noise(seeds[7], (2, 2, D), 0.5, 3.0, ((0, 2), (2, 4)))
    return dict(inputs=inputs, cotangent=cotangent, qkv_weight=qkv_weight, out_weight=out_weight, up_weight=up_weight, down_weight=down_weight, norm_gain=norm_gain, norm_bias=norm_bias)


@jax.custom_vjp
def low(v):
    return lax.optimization_barrier(v.astype(jnp.bfloat16)).astype(jnp.float32)

@jax.custom_vjp
def low_back(v):
    return v

def low_keep(v):
    return (low(v), None)

def low_pass(kept, grad):
    return (grad,)

def back_keep(v):
    return (v, None)

def back_low(kept, grad):
    return (low(grad),)
low.defvjp(low_keep, low_pass)
low_back.defvjp(back_keep, back_low)
eps_norm = 1e-05
score_scale = 0.125
high = lax.Precision.HIGHEST

def layer_norm(values, gain, shift):
    mean = lax.optimization_barrier(jnp.mean(values, axis=-1, keepdims=True))
    centred = values - mean
    var = lax.optimization_barrier(jnp.mean(centred * centred, axis=-1, keepdims=True))
    return centred * lax.rsqrt(var + eps_norm) * gain + shift

def attend_block(query_blk, query_start, key_rows, value_rows):
    block_len = query_blk.shape[0]
    total = key_rows.shape[0]
    scores = jnp.einsum('qhe,khe->hqk', query_blk, key_rows, precision=high) * score_scale
    scores = low_back(scores)
    query_pos = query_start + jnp.arange(block_len, dtype=jnp.int32)
    key_pos = jnp.arange(total, dtype=jnp.int32)
    causal = key_pos[None, :] <= query_pos[:, None]
    scores = jnp.where(causal[None], scores, -1e+30)
    softmax_w = low(jax.nn.softmax(scores, axis=-1))
    return jnp.einsum('hqk,khe->qhe', softmax_w, value_rows, precision=high)

def layer(values, w_qkv, w_out, w_up, w_down, gains, biases):
    total = values.shape[0]
    normed = low(layer_norm(values, gains[0], biases[0]))
    mixed = low_back(low(jnp.dot(normed, w_qkv, precision=high)))
    queries = mixed[:, :D].reshape(total, HEADS, HEAD)
    key_rows = mixed[:, D:2 * D].reshape(total, HEADS, HEAD)
    value_rows = mixed[:, 2 * D:].reshape(total, HEADS, HEAD)
    block_len = math.gcd(512, total)
    count = total // block_len
    query_blocks = queries.reshape(count, block_len, HEADS, HEAD)
    starts = jnp.arange(count, dtype=jnp.int32) * block_len
    checked = jax.checkpoint(attend_block)
    attended = lax.map(lambda pair: checked(pair[0], pair[1], key_rows, value_rows), (query_blocks, starts))
    attended = low_back(low(attended.reshape(total, D)))
    middle = values + low_back(jnp.dot(attended, w_out, precision=high))
    normed2 = low(layer_norm(middle, gains[1], biases[1]))
    upper = low_back(jnp.dot(normed2, w_up, precision=high))
    hidden = low(jax.nn.gelu(upper, approximate=True))
    return middle + low_back(jnp.dot(hidden, w_down, precision=high))

def reference(inputs, cotangent, qkv_weight, out_weight, up_weight, down_weight, norm_gain, norm_bias):
    seq_total = inputs.shape[0]
    flat_in = inputs.astype(jnp.float32).reshape(seq_total, LENGTH, D)
    flat_cot = cotangent.astype(jnp.float32).reshape(seq_total, LENGTH, D)
    params = (qkv_weight.astype(jnp.float32), out_weight.astype(jnp.float32), up_weight.astype(jnp.float32), down_weight.astype(jnp.float32), norm_gain.astype(jnp.float32), norm_bias.astype(jnp.float32))
    first = tuple((p[0] for p in params))
    second = tuple((p[1] for p in params))

    def one_sequence(totals, pair):
        seq_in, seq_cot = pair
        first_out, first_back = jax.vjp(layer, seq_in, *first)
        sent = low(first_out)
        second_out, second_back = jax.vjp(layer, sent, *second)
        second_grads = second_back(seq_cot)
        passed = low(second_grads[0])
        first_grads = first_back(passed)
        totals = tuple((t + jnp.stack([a, b]) for t, a, b in zip(totals, first_grads[1:], second_grads[1:])))
        return (totals, (sent, second_out, first_grads[0], passed))
    zeros = tuple((jnp.zeros_like(p) for p in params))
    totals, outs = lax.scan(one_sequence, zeros, (flat_in, flat_cot))
    sent, second_out, first_dx, passed = outs
    shape = (seq_total, MB, GROUP, D)
    layer_outputs = jnp.stack([sent.reshape(shape), second_out.reshape(shape)]).astype(jnp.bfloat16)
    input_grads = jnp.stack([first_dx.reshape(shape), passed.reshape(shape)]).astype(jnp.bfloat16)
    return (layer_outputs, input_grads, totals[0], totals[1], totals[2], totals[3], totals[4], totals[5])
```

```python
import functools

import jax
import jax.numpy as jnp
from jax import lax
from jax.experimental import pallas as pl
from jax.experimental.pallas import tpu as pltpu
from jax.sharding import PartitionSpec as P

HEAD = 64
LANES = 128
ROWS = 8
NEG = -1e30

eps_norm = 1e-05
score_scale = 0.125
f32 = jnp.float32
bf16 = jnp.bfloat16


def up_to(width, step):
    return -(-width // step) * step


def dot(a, b, dims):
    return lax.dot_general(a, b, (dims, ((), ())), preferred_element_type=f32)


def mm(a, b):
    return dot(a, b, ((1,), (0,)))


def mm_t(a, b):
    return dot(a, b, ((1,), (1,)))


def t_mm(a, b):
    return dot(a, b, ((0,), (0,)))


def attention_masks(core, half):
    row = lax.broadcasted_iota(jnp.int32, (2 * half, 2 * half), 0)
    col = lax.broadcasted_iota(jnp.int32, (2 * half, 2 * half), 1)
    row_slice, col_slice = row // half, col // half
    own = (col_slice < row_slice) | ((col_slice == row_slice) & (col <= row))
    other = (col_slice < row_slice) | ((col_slice == row_slice) & (core == 1))
    return jnp.where(jnp.stack([own, other]), 0.0, NEG).astype(f32)


def attention_forward_kernel(half, mask_ref, q_ref, k0_ref, k1_ref, v0_ref, v1_ref, o_ref, ob_ref, lse_ref):
    pair = pl.program_id(0)
    tokens = q_ref.shape[0]
    block = 2 * half

    @pl.when(pair == 0)
    def _():
        lse_ref[...] = jnp.zeros_like(lse_ref)

    lane = lax.broadcasted_iota(jnp.int32, (block, LANES), 1)
    for u in range(tokens // block):
        rows = pl.ds(u * block, block)
        keys = (u + 1) * block
        outs = []
        for h in range(2):
            cols = pl.ds(h * HEAD, HEAD)
            q = q_ref[rows, cols]
            scores = []
            for part, k_ref in enumerate((k0_ref, k1_ref)):
                s = mm_t(q, k_ref[pl.ds(0, keys), cols])
                last = s[:, keys - block :] + mask_ref[part]
                scores.append(last if u == 0 else jnp.concatenate([s[:, : keys - block], last], axis=1))
            top = jnp.maximum(
                jnp.max(scores[0], axis=1, keepdims=True), jnp.max(scores[1], axis=1, keepdims=True)
            )
            total, acc = 0.0, 0.0
            for s, v_ref in zip(scores, (v0_ref, v1_ref)):
                p = jnp.exp(s - top)
                total = total + jnp.sum(p, axis=1, keepdims=True)
                acc = acc + mm(p.astype(bf16), v_ref[pl.ds(0, keys), cols])
            outs.append(acc / total)
            lse = top + jnp.log(total)
            lse_ref[rows, :] = jnp.where(lane == 2 * pair + h, lse, lse_ref[rows, :])
        out = jnp.concatenate(outs, axis=1)
        o_ref[rows, :] = out
        ob_ref[rows, :] = out.astype(bf16)


def attention_forward(mask, q, k0, k1, v0, v1, half):
    tokens, width = q.shape
    spec = pl.BlockSpec((tokens, LANES), lambda i: (0, i))
    return pl.pallas_call(
        functools.partial(attention_forward_kernel, half),
        grid=(width // LANES,),
        in_specs=[pl.BlockSpec(mask.shape, lambda i: (0, 0, 0))] + [spec] * 5,
        out_specs=[spec, spec, pl.BlockSpec((tokens, LANES), lambda i: (0, 0))],
        out_shape=[
            jax.ShapeDtypeStruct((tokens, width), f32),
            jax.ShapeDtypeStruct((tokens, width), bf16),
            jax.ShapeDtypeStruct((tokens, LANES), f32),
        ],
        name="attention_forward",
    )(mask, q, k0, k1, v0, v1)


def attention_backward_kernel(
    half, mask_ref, q_ref, k0_ref, k1_ref, v0_ref, v1_ref, da_ref, o_ref, lse_ref,
    dq_ref, dk0_ref, dk1_ref, dv0_ref, dv1_ref, acc_ref,
):
    pair = pl.program_id(0)
    tokens = q_ref.shape[0]
    block = 2 * half
    lane = lax.broadcasted_iota(jnp.int32, (block, LANES), 1)
    acc_ref[...] = jnp.zeros_like(acc_ref)
    for u in range(tokens // block):
        rows = pl.ds(u * block, block)
        keys = (u + 1) * block
        dqs = []
        for h in range(2):
            cols = pl.ds(h * HEAD, HEAD)
            q, da = q_ref[rows, cols], da_ref[rows, cols]
            q_t, da_t = q.T, da.T
            lse = jnp.sum(jnp.where(lane == 2 * pair + h, lse_ref[rows, :], 0.0), axis=1, keepdims=True)
            delta = jnp.sum(da.astype(f32) * o_ref[rows, cols], axis=1, keepdims=True)
            dq = 0.0
            for part, (k_ref, v_ref) in enumerate(((k0_ref, v0_ref), (k1_ref, v1_ref))):
                k, v = k_ref[pl.ds(0, keys), cols], v_ref[pl.ds(0, keys), cols]
                s = mm_t(q, k)
                last = s[:, keys - block :] + mask_ref[part]
                s = last if u == 0 else jnp.concatenate([s[:, : keys - block], last], axis=1)
                p = jnp.exp(s - lse)
                ds = (p * (mm_t(da, v) - delta)).astype(bf16)
                dq = dq + mm(ds, k)
                acc_ref[part, 0, h, :, pl.ds(0, keys)] += mm(q_t, ds)
                acc_ref[part, 1, h, :, pl.ds(0, keys)] += mm(da_t, p.astype(bf16))
            dqs.append(dq * score_scale)
        dq_ref[rows, :] = jnp.concatenate(dqs, axis=1).astype(bf16)
    for part, (dk_ref, dv_ref) in enumerate(((dk0_ref, dv0_ref), (dk1_ref, dv1_ref))):
        for which, ref in enumerate((dk_ref, dv_ref)):
            both = jnp.concatenate([acc_ref[part, which, 0], acc_ref[part, which, 1]], axis=0)
            ref[...] = both.T.astype(ref.dtype)


def attention_backward(mask, q, k0, k1, v0, v1, da, o, lse, half):
    tokens, width = q.shape
    spec = pl.BlockSpec((tokens, LANES), lambda i: (0, i))
    whole = pl.BlockSpec((tokens, LANES), lambda i: (0, 0))
    shape = lambda t: jax.ShapeDtypeStruct((tokens, width), t)
    return pl.pallas_call(
        functools.partial(attention_backward_kernel, half),
        grid=(width // LANES,),
        in_specs=[pl.BlockSpec(mask.shape, lambda i: (0, 0, 0))] + [spec] * 7 + [whole],
        out_specs=[spec] * 5,
        out_shape=[shape(bf16), shape(f32), shape(bf16), shape(f32), shape(bf16)],
        scratch_shapes=[pltpu.VMEM((2, 2, 2, HEAD, tokens), f32)],
        name="attention_backward",
    )(mask, q, k0, k1, v0, v1, da, o, lse)


def normalised(values):
    mean = jnp.mean(values, axis=-1, keepdims=True)
    centred = values - mean
    var = jnp.mean(centred * centred, axis=-1, keepdims=True)
    scale = lax.rsqrt(var + eps_norm)
    return centred * scale, scale


def norm_backward(hat, scale, gain, grad):
    scaled = grad * gain
    mean = jnp.mean(scaled, axis=-1, keepdims=True)
    along = jnp.mean(scaled * hat, axis=-1, keepdims=True)
    return scale * (scaled - mean - hat * along)


def swap_cores(value):
    return lax.ppermute(value, "section", [(0, 1), (1, 0)])


def hop(value, source, target):
    return lax.ppermute(value, "shard", [(source, target)])


def gather_weights(attn_piece, ff_piece):
    def bring(piece, kind):
        parts = []
        for j in range(2):
            moves = []
            for layer in range(2):
                for core in range(2):
                    moves.append((layer * 4 + 2 * core + j, core * 4 + 2 * layer + kind))
            parts.append(lax.ppermute(piece, ("section", "shard"), moves))
        both = jnp.stack(parts)
        quarters = lax.all_gather(both, "ctx", axis=0)
        full = lax.all_gather(quarters, "section", axis=1)
        return full.reshape(4, 4 * piece.shape[0], piece.shape[1])

    return bring(attn_piece, 0), bring(ff_piece, 1)


def scatter_grads(grads, kind, section, shard):
    columns = grads.shape[1]
    rows = grads.shape[0] // 16
    terms = grads.reshape(4, 2, 2, rows, columns)
    terms = lax.psum_scatter(terms, "section", scatter_dimension=1, tiled=False)
    terms = lax.psum_scatter(terms, "ctx", scatter_dimension=0, tiled=False)
    total = None
    for j in range(2):
        moves = []
        for layer in range(2):
            for core in range(2):
                moves.append((core * 4 + 2 * layer + kind, layer * 4 + 2 * core + j))
        came = lax.ppermute(terms[j], ("section", "shard"), moves)
        total = came if total is None else jnp.where(shard % 2 == j, came, total)
    return total


def chain(inputs, cotangent, qkv_weight, out_weight, up_weight, down_weight, norm_gain, norm_bias):
    section, ctx, shard = lax.axis_index("section"), lax.axis_index("ctx"), lax.axis_index("shard")
    seq_count, blocks, slice_len, width = inputs.shape
    half = slice_len // 2
    tokens = blocks * 4 * half
    share = width // 4
    group = share // 4
    group_pad = up_to(group, ROWS)
    wide = up_to(width, LANES)
    ff = up_weight.shape[2]
    is_attn = shard % 2 == 0

    pad = lambda w: jnp.pad(w, ((0, 0), (0, wide - width)))
    own_qkv, own_out = qkv_weight[0], out_weight[0]
    attn_src = jnp.stack([pad(own_qkv[:, i * width : (i + 1) * width]) for i in range(3)] + [pad(own_out)])
    down_t = down_weight[0].T
    up0 = up_weight[0]
    ff_src = jnp.stack([up0[:, : ff // 2], up0[:, ff // 2 :], down_t[:, : ff // 2], down_t[:, ff // 2 :]])
    w_attn, w_ff = gather_weights(
        lax.dynamic_index_in_dim(attn_src, ctx, 0, keepdims=False),
        lax.dynamic_index_in_dim(ff_src, ctx, 0, keepdims=False),
    )
    norms = jnp.stack([norm_gain[0], norm_bias[0]])
    norms = lax.all_gather(lax.all_gather(norms, "shard", axis=2, tiled=True), "section", axis=0)
    norms = lax.dynamic_index_in_dim(norms, shard // 2, 0, keepdims=False).astype(f32)
    gain1, gain2, bias1, bias2 = norms[0, 0], norms[0, 1], norms[1, 0], norms[1, 1]

    def bring_tokens(array):
        own = lax.dynamic_slice_in_dim(array[0], section * half, half, 1)
        every = lax.all_gather(own, "shard", axis=0)
        mine = lax.all_to_all(every, "ctx", 0, 0)
        return jnp.swapaxes(mine, 0, 1).reshape(tokens, width)

    x_first, g_last = bring_tokens(inputs), bring_tokens(cotangent)
    mask = attention_masks(section, half)
    feature = lax.broadcasted_iota(jnp.int32, (width, 16 * group_pad), 0)
    place = lax.broadcasted_iota(jnp.int32, (width, 16 * group_pad), 1)
    spread = (feature // group * group_pad + feature % group == place).astype(bf16)
    grouped = lambda v: mm(v, spread).astype(bf16)

    def attn_forward(x):
        x = x.astype(f32)
        hat, scale = normalised(x)
        normed = (hat * gain1 + bias1).astype(bf16)
        q = (mm(normed, w_attn[0]) * score_scale).astype(bf16)
        k = mm(normed, w_attn[1]).astype(bf16)
        v = mm(normed, w_attn[2]).astype(bf16)
        k1, v1 = swap_cores(k), swap_cores(v)
        o, ob, lse = attention_forward(mask, q, k, k1, v, v1, half)
        middle = x + mm(ob[:, :width], w_attn[3])[:, :width]
        return middle.astype(bf16), (hat, scale, normed, q, k, k1, v, v1, o, ob, lse)

    def ff_forward(middle):
        middle = middle.astype(f32)
        hat, scale = normalised(middle)
        normed = (hat * gain2 + bias2).astype(bf16)
        upper = [mm(normed, w_ff[i]) for i in range(2)]
        hidden = [jax.nn.gelu(u, approximate=True).astype(bf16) for u in upper]
        y = middle + mm_t(hidden[0], w_ff[2]) + mm_t(hidden[1], w_ff[3])
        return y.astype(bf16), (hat, scale, normed, upper, hidden)

    def ff_backward(g, state):
        hat, scale, normed, upper, hidden = state
        d_upper = []
        for i in range(2):
            d_hidden = mm(g, w_ff[2 + i])
            _, back = jax.vjp(lambda u: jax.nn.gelu(u, approximate=True), upper[i])
            d_upper.append(back(d_hidden)[0].astype(bf16))
        d_normed = mm_t(d_upper[0], w_ff[0]) + mm_t(d_upper[1], w_ff[1])
        d_middle = g.astype(f32) + norm_backward(hat, scale, gain2, d_normed)
        return d_middle.astype(bf16), d_upper, d_normed

    def attn_backward(d_middle, state):
        hat, scale, normed, q, k, k1, v, v1, o, ob, lse = state
        d_att = mm_t(jnp.pad(d_middle, ((0, 0), (0, wide - width))), w_attn[3]).astype(bf16)
        d_att = jnp.pad(d_att, ((0, 0), (0, wide - width)))
        dq, dk, dk_other, dv, dv_other = attention_backward(mask, q, k, k1, v, v1, d_att, o, lse, half)
        dk = (dk + swap_cores(dk_other).astype(f32)).astype(bf16)
        dv = (dv + swap_cores(dv_other).astype(f32)).astype(bf16)
        d_mixed = (dq, dk, dv)
        d_normed = mm_t(dq, w_attn[0]) + mm_t(dk, w_attn[1]) + mm_t(dv, w_attn[2])
        dx = d_middle.astype(f32) + norm_backward(hat, scale, gain1, d_normed)
        return dx.astype(bf16), d_mixed, d_normed

    middle, _ = attn_forward(x_first)
    middle0 = hop(middle, 0, 1)
    y, _ = ff_forward(middle0)
    x = jnp.where(shard == 0, x_first, hop(y, 1, 2))
    middle, attn_state = attn_forward(x)
    middle = jnp.where(shard == 1, middle0, hop(middle, 2, 3))
    y, ff_state = ff_forward(middle)

    d_middle, _, _ = ff_backward(g_last, ff_state)
    d_middle1 = hop(d_middle, 3, 2)
    dx, _, _ = attn_backward(d_middle1, attn_state)
    g = jnp.where(shard == 3, g_last, hop(dx, 2, 1))
    d_middle, d_upper, d_normed2 = ff_backward(g, ff_state)
    hat2, _, normed2, _, hidden = ff_state
    g_grouped, n2_grouped = grouped(g), grouped(normed2)
    ff_grads = [t_mm(n2_grouped, d_upper[0]), t_mm(n2_grouped, d_upper[1]), t_mm(g_grouped, hidden[0]), t_mm(g_grouped, hidden[1])]
    ff_sums = scatter_grads(jnp.concatenate([v.astype(bf16) for v in ff_grads], axis=1), 1, section, shard)
    d_middle = jnp.where(shard == 2, d_middle1, hop(d_middle, 1, 0))
    dx, d_mixed, d_normed1 = attn_backward(d_middle, attn_state)
    hat1, _, normed, _, _, _, _, _, _, ob, _ = attn_state
    n1_grouped, att_grouped = grouped(normed), grouped(ob[:, :width])
    attn_grads = [t_mm(n1_grouped, d) for d in d_mixed] + [t_mm(att_grouped, jnp.pad(d_middle, ((0, 0), (0, wide - width))))]
    attn_sums = scatter_grads(jnp.concatenate([v.astype(bf16) for v in attn_grads], axis=1), 0, section, shard)

    own_hat = jnp.where(is_attn, hat1, hat2)
    own_grad = jnp.where(is_attn, d_normed1, d_normed2)
    terms = jnp.stack([jnp.sum(own_grad * own_hat, axis=0), jnp.sum(own_grad, axis=0)])
    terms = jnp.where(jnp.arange(4)[:, None, None] == shard, terms[None], 0.0)
    totals = lax.psum(terms, ("section", "ctx", "shard")).reshape(2, 2, 2, width)
    totals = lax.dynamic_index_in_dim(totals, section, 0, keepdims=False)
    totals = lax.dynamic_slice_in_dim(totals, (ctx * 4 + shard) * group, group, 2)

    final = jnp.where(is_attn, dx, y).reshape(blocks, 4, half, width)
    final = lax.all_to_all(jnp.swapaxes(final, 0, 1), "ctx", 0, 0)
    final = lax.all_to_all(final, "shard", 0, 0).reshape(2, 2, blocks, half, width)
    final = lax.all_to_all(final, "section", 0, 0)
    final = jnp.moveaxis(final, 0, 2).reshape(2, blocks, slice_len, width)

    attn_sums = attn_sums[:group].astype(f32)
    ff_sums = ff_sums[:group].astype(f32)
    qkv = jnp.concatenate([attn_sums[:, i * wide : i * wide + width] for i in range(3)], axis=1)
    return (
        final[1][None, None],
        final[0][None, None],
        qkv[None],
        attn_sums[:, 3 * wide : 3 * wide + width][None],
        ff_sums[:, :ff][None],
        ff_sums[:, ff:].T[None],
        totals[:, 0][None],
        totals[:, 1][None],
    )


def passed_along(value, axis, steps):
    count = lax.axis_size(axis)
    initial, last = (max(0, -steps), min(count, count - steps))
    return lax.ppermute(value, axis, [(source, source + steps) for source in range(initial, last)])


def layer_norm(values, gain, shift):
    mean = jnp.mean(values, axis=-1, keepdims=True)
    centred = values - mean
    var = jnp.mean(centred * centred, axis=-1, keepdims=True)
    return centred * lax.rsqrt(var + eps_norm) * gain + shift


def gelu_tanh(values):
    return jax.nn.gelu(values, approximate=True)


def split_pair(key_value, head_count):
    block_len, seq_count, double = key_value.shape
    model_width = double // 2
    key_rows = key_value[..., :model_width].reshape(block_len, seq_count, head_count, HEAD)
    value_rows = key_value[..., model_width:].reshape(block_len, seq_count, head_count, HEAD)
    return (key_rows, value_rows)


def causal_mask(query_pos, key_pos):
    return (key_pos[None, :] <= query_pos[:, None])[None, :, None, :]


def forward_block(running, queries, query_pos, key_value, key_pos):
    row_max, row_sum, accum = running
    key_rows, value_rows = split_pair(key_value, queries.shape[2])
    scores = (
        jnp.einsum("sqhe,kshe->sqhk", queries, key_rows, preferred_element_type=jnp.float32)
        * score_scale
    )
    causal = causal_mask(query_pos, key_pos)
    new_max = jnp.maximum(row_max, jnp.max(jnp.where(causal, scores, -1e30), axis=-1))
    softmax_w = jnp.where(causal, jnp.exp(scores - new_max[..., None]), 0.0)
    factor = jnp.exp(row_max - new_max)
    row_sum = row_sum * factor + jnp.sum(softmax_w, axis=-1)
    accum = accum * factor[..., None] + jnp.einsum(
        "sqhk,kshe->sqhe",
        softmax_w.astype(jnp.bfloat16),
        value_rows,
        preferred_element_type=jnp.float32,
    )
    return (new_max, row_sum, accum)


def split_rows(whole):
    key_count = whole.shape[0]
    block_size = 512
    blocks = whole.reshape((key_count // block_size, block_size) + whole.shape[1:])
    offsets = jnp.arange(key_count // block_size, dtype=jnp.int32) * block_size
    return (blocks, offsets, block_size)


def fold_keys(running, piece, start, queries, query_pos, group_len):
    blocks, offsets, block_size = split_rows(piece)

    def fold_scan_step(inner, scan_item):
        block_rows, offset = scan_item
        for group_id in range(block_rows.shape[2]):
            key_pos = (
                group_id * group_len + start + offset + jnp.arange(block_size, dtype=jnp.int32)
            )
            inner = forward_block(inner, queries, query_pos, block_rows[:, :, group_id], key_pos)
        return (inner, None)

    result, _ = lax.scan(fold_scan_step, running, (blocks, offsets))
    return result


def pair_terms(d_scores, softmax_w, queries, d_attended, block_size):
    d_keys = (
        jnp.einsum("sqhk,sqhe->kshe", d_scores, queries, preferred_element_type=jnp.float32)
        * score_scale
    )
    d_values = jnp.einsum(
        "sqhk,sqhe->kshe",
        softmax_w.astype(jnp.bfloat16),
        d_attended,
        preferred_element_type=jnp.float32,
    )
    shape = (block_size, queries.shape[0], queries.shape[2] * queries.shape[3])
    return jnp.concatenate([d_keys.reshape(shape), d_values.reshape(shape)], axis=-1)


def score_grads(
    queries, query_pos, log_total, row_delta, d_attended, key_rows, value_rows, key_pos
):
    scores = (
        jnp.einsum("sqhe,kshe->sqhk", queries, key_rows, preferred_element_type=jnp.float32)
        * score_scale
    )
    causal = causal_mask(query_pos, key_pos)
    softmax_w = jnp.where(causal, jnp.exp(scores - log_total[..., None]), 0.0)
    d_probs = jnp.einsum(
        "sqhe,kshe->sqhk", d_attended, value_rows, preferred_element_type=jnp.float32
    )
    d_scores = (softmax_w * (d_probs - row_delta[..., None])).astype(jnp.bfloat16)
    return (softmax_w, d_scores)


def backward_keys(whole, queries, query_pos, log_total, row_delta, d_attended, group_len):
    blocks, offsets, block_size = split_rows(whole)

    def backward_scan_step(d_queries, scan_item):
        block_rows, offset = scan_item
        for group_id in range(block_rows.shape[2]):
            key_pos = group_id * group_len + offset + jnp.arange(block_size, dtype=jnp.int32)
            key_rows, value_rows = split_pair(block_rows[:, :, group_id], queries.shape[2])
            softmax_w, d_scores = score_grads(
                queries, query_pos, log_total, row_delta, d_attended, key_rows, value_rows, key_pos
            )
            d_queries = (
                d_queries
                + jnp.einsum(
                    "sqhk,kshe->sqhe", d_scores, key_rows, preferred_element_type=jnp.float32
                )
                * score_scale
            )
        return (d_queries, None)

    d_queries, terms = lax.scan(
        backward_scan_step, jnp.zeros(queries.shape, jnp.float32), (blocks, offsets)
    )
    return (d_queries, None)


def owner_terms(
    own_cache, all_queries, all_d_att, all_totals, all_deltas, micro_index, ctx_id, group_len
):
    block_len, seq_count, group_count, double = own_cache.shape
    head_count = all_queries.shape[2]
    query_rows = all_queries.shape[1]
    query_size = 512
    block_count = query_rows // query_size

    def loop_step(index, total):
        offset = index * query_size
        q_block = lax.dynamic_slice_in_dim(all_queries, offset, query_size, 1)
        d_block = lax.dynamic_slice_in_dim(all_d_att, offset, query_size, 1)
        t_block = lax.dynamic_slice_in_dim(all_totals, offset, query_size, 1)
        r_block = lax.dynamic_slice_in_dim(all_deltas, offset, query_size, 1)
        query_pos = micro_index * group_len + offset + jnp.arange(query_size, dtype=jnp.int32)
        pieces = []
        for group_id in range(group_count):
            key_pos = (
                group_id * group_len + ctx_id * block_len + jnp.arange(block_len, dtype=jnp.int32)
            )
            key_rows, value_rows = split_pair(own_cache[:, :, group_id], head_count)
            softmax_w, d_scores = score_grads(
                q_block, query_pos, t_block, r_block, d_block, key_rows, value_rows, key_pos
            )
            pieces.append(pair_terms(d_scores, softmax_w, q_block, d_block, block_len))
        return total + jnp.stack(pieces, axis=2)

    return lax.fori_loop(0, block_count, loop_step, jnp.zeros(own_cache.shape, jnp.float32))


def store_at(store, value, micro_index, active):
    updated = lax.dynamic_update_index_in_dim(store, value, micro_index, 0)
    return jnp.where(active, updated, store)


def shards(inputs, cotangent, qkv_weight, out_weight, up_weight, down_weight, norm_gain, norm_bias):
    section_id = lax.axis_index("section")
    ctx_count = lax.axis_size("ctx")
    ctx_id = lax.axis_index("ctx")
    seq_count, group_count, block_len, model_width = inputs.shape
    head_count = model_width // HEAD
    group_len = block_len * ctx_count
    row_count = seq_count * block_len
    w_qkv, w_out, w_up, w_down, gains, biases = (
        lax.all_gather(qkv_weight[0], "shard", axis=0, tiled=True),
        lax.all_gather(out_weight[0], "shard", axis=0, tiled=True),
        lax.all_gather(up_weight[0], "shard", axis=0, tiled=True),
        lax.all_gather(down_weight[0], "shard", axis=1, tiled=True),
        lax.all_gather(norm_gain[0], "shard", axis=1, tiled=True),
        lax.all_gather(norm_bias[0], "shard", axis=1, tiled=True),
    )
    gains = gains.astype(jnp.float32)
    biases = biases.astype(jnp.float32)
    ff_width = w_up.shape[1]
    cache = jnp.zeros((block_len, seq_count, group_count, 2 * model_width), jnp.bfloat16)
    in_store = jnp.zeros((group_count, seq_count, block_len, model_width), jnp.bfloat16)
    query_store = jnp.zeros((group_count, seq_count, block_len, head_count, HEAD), jnp.bfloat16)
    att_store = jnp.zeros((group_count, seq_count, block_len, head_count, HEAD), jnp.float32)
    total_store = jnp.zeros((group_count, seq_count, block_len, head_count), jnp.float32)
    middle_store = jnp.zeros((group_count, row_count, model_width), jnp.float32)
    upper_store = jnp.zeros((group_count, row_count, ff_width), jnp.float32)
    out_store = jnp.zeros((group_count, seq_count, block_len, model_width), jnp.bfloat16)
    received = jnp.zeros((seq_count, block_len, model_width), jnp.bfloat16)
    for tick_no in range(group_count + 1):
        micro = tick_no - section_id
        active = (micro >= 0) & (micro < group_count)
        micro_index = jnp.clip(micro, 0, group_count - 1)
        own_input = lax.dynamic_index_in_dim(inputs, micro_index, 1, keepdims=False)
        entering = jnp.where(section_id == 0, own_input, received)
        flat_rows = entering.reshape(row_count, model_width).astype(jnp.float32)
        normed = layer_norm(flat_rows, gains[0], biases[0]).astype(jnp.bfloat16)
        mixed = jnp.dot(normed, w_qkv, preferred_element_type=jnp.float32).astype(jnp.bfloat16)
        queries = mixed[:, :model_width].reshape(seq_count, block_len, head_count, HEAD)
        fresh = jnp.swapaxes(
            mixed[:, model_width:].reshape(seq_count, block_len, 2 * model_width), 0, 1
        )
        updated = lax.dynamic_update_index_in_dim(cache, fresh, micro_index, 2)
        cache = jnp.where(active, updated, cache)
        query_pos = (
            micro_index * group_len + ctx_id * block_len + jnp.arange(block_len, dtype=jnp.int32)
        )
        start_state = (
            jnp.full((seq_count, block_len, head_count), -1e30, jnp.float32),
            jnp.zeros((seq_count, block_len, head_count), jnp.float32),
            jnp.zeros((seq_count, block_len, head_count, HEAD), jnp.float32),
        )
        row_max, row_sum, accum = fold_keys(
            start_state,
            lax.all_gather(cache, "ctx", axis=0, tiled=True),
            jnp.int32(0),
            queries,
            query_pos,
            group_len,
        )
        attended = accum / row_sum[..., None]
        log_total = row_max + jnp.log(row_sum)
        att_low = attended.reshape(row_count, model_width).astype(jnp.bfloat16)
        middle = flat_rows + jnp.dot(att_low, w_out, preferred_element_type=jnp.float32)
        normed2 = layer_norm(middle, gains[1], biases[1]).astype(jnp.bfloat16)
        upper = jnp.dot(normed2, w_up, preferred_element_type=jnp.float32)
        hidden = gelu_tanh(upper).astype(jnp.bfloat16)
        leaving = (middle + jnp.dot(hidden, w_down, preferred_element_type=jnp.float32)).astype(
            jnp.bfloat16
        )
        leaving = leaving.reshape(seq_count, block_len, model_width)
        in_store = store_at(in_store, entering, micro_index, active)
        query_store = store_at(query_store, queries, micro_index, active)
        att_store = store_at(att_store, attended, micro_index, active)
        total_store = store_at(total_store, log_total, micro_index, active)
        middle_store = store_at(middle_store, middle, micro_index, active)
        upper_store = store_at(upper_store, upper, micro_index, active)
        out_store = store_at(out_store, leaving, micro_index, active)
        if tick_no < group_count:
            received = passed_along(leaving, "section", 1)
    key_acc = jnp.zeros((block_len, seq_count, group_count, 2 * model_width), jnp.float32)
    grad_qkv = jnp.zeros((model_width, 3 * model_width), jnp.float32)
    grad_out = jnp.zeros((model_width, model_width), jnp.float32)
    grad_up = jnp.zeros((model_width, ff_width), jnp.float32)
    grad_down = jnp.zeros((ff_width, model_width), jnp.float32)
    grad_gain = jnp.zeros((2, model_width), jnp.float32)
    grad_bias = jnp.zeros((2, model_width), jnp.float32)
    grad_store = jnp.zeros((group_count, seq_count, block_len, model_width), jnp.bfloat16)
    coming = jnp.zeros((seq_count, block_len, model_width), jnp.bfloat16)
    for tick_no in range(group_count + 1):
        micro = group_count - tick_no - section_id
        active = (micro >= 0) & (micro < group_count)
        active_weight = active.astype(jnp.float32)
        micro_index = jnp.clip(micro, 0, group_count - 1)
        own_cot = lax.dynamic_index_in_dim(cotangent, micro_index, 1, keepdims=False)
        d_out = (
            jnp.where(section_id == 1, own_cot, coming)
            .reshape(row_count, model_width)
            .astype(jnp.float32)
        )
        flat_rows = in_store[micro_index].reshape(row_count, model_width).astype(jnp.float32)
        queries = query_store[micro_index]
        attended = att_store[micro_index]
        log_total = total_store[micro_index]
        middle = middle_store[micro_index]
        upper = upper_store[micro_index]
        normed2_full, norm2_back = jax.vjp(
            lambda v, g, b: layer_norm(v, g, b), middle, gains[1], biases[1]
        )
        normed2 = normed2_full.astype(jnp.bfloat16)
        hidden_full, gelu_back = jax.vjp(gelu_tanh, upper)
        hidden = hidden_full.astype(jnp.bfloat16)
        d_branch = d_out.astype(jnp.bfloat16)
        grad_down = grad_down + active_weight * jnp.dot(
            hidden.T, d_branch, preferred_element_type=jnp.float32
        )
        d_hidden = jnp.dot(d_branch, w_down.T, preferred_element_type=jnp.float32)
        d_upper = gelu_back(d_hidden)[0].astype(jnp.bfloat16)
        grad_up = grad_up + active_weight * jnp.dot(
            normed2.T, d_upper, preferred_element_type=jnp.float32
        )
        d_normed2 = jnp.dot(d_upper, w_up.T, preferred_element_type=jnp.float32)
        d_mid_norm, d_gain2, d_bias2 = norm2_back(d_normed2)
        d_middle = d_out + d_mid_norm
        att_low = attended.reshape(row_count, model_width).astype(jnp.bfloat16)
        d_att = d_middle.astype(jnp.bfloat16)
        grad_out = grad_out + active_weight * jnp.dot(
            att_low.T, d_att, preferred_element_type=jnp.float32
        )
        d_attended = jnp.dot(d_att, w_out.T, preferred_element_type=jnp.float32).astype(
            jnp.bfloat16
        )
        d_attended = d_attended.reshape(seq_count, block_len, head_count, HEAD)
        row_delta = jnp.sum(d_attended.astype(jnp.float32) * attended, axis=-1)
        query_pos = (
            micro_index * group_len + ctx_id * block_len + jnp.arange(block_len, dtype=jnp.int32)
        )
        whole = lax.all_gather(cache, "ctx", axis=0, tiled=True)
        d_queries, unused = backward_keys(
            whole, queries, query_pos, log_total, row_delta, d_attended, group_len
        )
        all_queries, all_d_att = (
            lax.all_gather(queries, "ctx", axis=1, tiled=True),
            lax.all_gather(d_attended, "ctx", axis=1, tiled=True),
        )
        all_totals, all_deltas = (
            lax.all_gather(log_total, "ctx", axis=1, tiled=True),
            lax.all_gather(row_delta, "ctx", axis=1, tiled=True),
        )
        shares = owner_terms(
            cache, all_queries, all_d_att, all_totals, all_deltas, micro_index, ctx_id, group_len
        )
        key_acc = key_acc + active_weight * shares
        d_pair = jnp.swapaxes(
            lax.dynamic_index_in_dim(key_acc, micro_index, 2, keepdims=False), 0, 1
        )
        d_mixed = jnp.concatenate(
            [d_queries.reshape(row_count, model_width), d_pair.reshape(row_count, 2 * model_width)],
            axis=-1,
        ).astype(jnp.bfloat16)
        normed_full, norm1_back = jax.vjp(
            lambda v, g, b: layer_norm(v, g, b), flat_rows, gains[0], biases[0]
        )
        normed = normed_full.astype(jnp.bfloat16)
        grad_qkv = grad_qkv + active_weight * jnp.dot(
            normed.T, d_mixed, preferred_element_type=jnp.float32
        )
        d_normed = jnp.dot(d_mixed, w_qkv.T, preferred_element_type=jnp.float32)
        d_flat_norm, d_gain1, d_bias1 = norm1_back(d_normed)
        grad_gain = grad_gain + active_weight * jnp.stack([d_gain1, d_gain2])
        grad_bias = grad_bias + active_weight * jnp.stack([d_bias1, d_bias2])
        d_entering = (
            (d_middle + d_flat_norm).astype(jnp.bfloat16).reshape(seq_count, block_len, model_width)
        )
        grad_store = store_at(grad_store, d_entering, micro_index, active)
        if tick_no < group_count:
            coming = passed_along(d_entering, "section", -1)
    sums = (
        lax.psum_scatter(grad_qkv, ("ctx", "shard"), scatter_dimension=0, tiled=True),
        lax.psum_scatter(grad_out, ("ctx", "shard"), scatter_dimension=0, tiled=True),
        lax.psum_scatter(grad_up, ("ctx", "shard"), scatter_dimension=0, tiled=True),
        lax.psum_scatter(grad_down, ("ctx", "shard"), scatter_dimension=1, tiled=True),
        lax.psum_scatter(grad_gain, ("ctx", "shard"), scatter_dimension=1, tiled=True),
        lax.psum_scatter(grad_bias, ("ctx", "shard"), scatter_dimension=1, tiled=True),
    )
    layer_outputs = jnp.swapaxes(out_store, 0, 1)[None]
    input_grads = jnp.swapaxes(grad_store, 0, 1)[None]
    return (
        layer_outputs,
        input_grads,
        sums[0][None],
        sums[1][None],
        sums[2][None],
        sums[3][None],
        sums[4][None],
        sums[5][None],
    )


def solution(mesh):
    in_specs = (
        P("shard", None, "ctx", None),
        P("shard", None, "ctx", None),
        P("section", "shard", None),
        P("section", "shard", None),
        P("section", "shard", None),
        P("section", None, "shard"),
        P("section", None, "shard"),
        P("section", None, "shard"),
    )
    out_specs = (
        P("section", "shard", None, "ctx", None),
        P("section", "shard", None, "ctx", None),
        P("section", ("ctx", "shard"), None),
        P("section", ("ctx", "shard"), None),
        P("section", ("ctx", "shard"), None),
        P("section", None, ("ctx", "shard")),
        P("section", None, ("ctx", "shard")),
        P("section", None, ("ctx", "shard")),
    )
    relay = mesh.shape["section"] == 2 and mesh.shape["shard"] == 4 and mesh.shape["ctx"] == 4
    return jax.shard_map(chain if relay else shards, mesh=mesh, in_specs=in_specs, out_specs=out_specs, check_vma=False)
```

```python
import functools

import jax
import jax.numpy as jnp
from jax import lax
from jax.experimental import pallas as pl
from jax.experimental.pallas import tpu as pltpu
from jax.sharding import PartitionSpec as P

HEAD = 64
LANES = 128
ROWS = 8
NEG = -1e30

eps_norm = 1e-05
score_scale = 0.125
f32 = jnp.float32
bf16 = jnp.bfloat16


def up_to(width, step):
    return -(-width // step) * step


def dot(a, b, dims):
    return lax.dot_general(a, b, (dims, ((), ())), preferred_element_type=f32)


def mm(a, b):
    return dot(a, b, ((1,), (0,)))


def mm_t(a, b):
    return dot(a, b, ((1,), (1,)))


def t_mm(a, b):
    return dot(a, b, ((0,), (0,)))


def attention_masks(core, half):
    row = lax.broadcasted_iota(jnp.int32, (2 * half, 2 * half), 0)
    col = lax.broadcasted_iota(jnp.int32, (2 * half, 2 * half), 1)
    row_slice, col_slice = row // half, col // half
    own = (col_slice < row_slice) | ((col_slice == row_slice) & (col <= row))
    other = (col_slice < row_slice) | ((col_slice == row_slice) & (core == 1))
    return jnp.where(jnp.stack([own, other]), 0.0, NEG).astype(f32)


def attention_forward_kernel(half, mask_ref, q_ref, k0_ref, k1_ref, v0_ref, v1_ref, o_ref, ob_ref, lse_ref):
    pair = pl.program_id(0)
    tokens = q_ref.shape[0]
    block = 2 * half

    @pl.when(pair == 0)
    def _():
        lse_ref[...] = jnp.zeros_like(lse_ref)

    lane = lax.broadcasted_iota(jnp.int32, (block, LANES), 1)
    for u in range(tokens // block):
        rows = pl.ds(u * block, block)
        keys = (u + 1) * block
        outs = []
        for h in range(2):
            cols = pl.ds(h * HEAD, HEAD)
            q = q_ref[rows, cols]
            scores = []
            for part, k_ref in enumerate((k0_ref, k1_ref)):
                s = mm_t(q, k_ref[pl.ds(0, keys), cols])
                last = s[:, keys - block :] + mask_ref[part]
                scores.append(last if u == 0 else jnp.concatenate([s[:, : keys - block], last], axis=1))
            top = jnp.maximum(
                jnp.max(scores[0], axis=1, keepdims=True), jnp.max(scores[1], axis=1, keepdims=True)
            )
            total, acc = 0.0, 0.0
            for s, v_ref in zip(scores, (v0_ref, v1_ref)):
                p = jnp.exp(s - top)
                total = total + jnp.sum(p, axis=1, keepdims=True)
                acc = acc + mm(p.astype(bf16), v_ref[pl.ds(0, keys), cols])
            outs.append(acc / total)
            lse = top + jnp.log(total)
            lse_ref[rows, :] = jnp.where(lane == 2 * pair + h, lse, lse_ref[rows, :])
        out = jnp.concatenate(outs, axis=1)
        o_ref[rows, :] = out
        ob_ref[rows, :] = out.astype(bf16)


def attention_forward(mask, q, k0, k1, v0, v1, half):
    tokens, width = q.shape
    spec = pl.BlockSpec((tokens, LANES), lambda i: (0, i))
    return pl.pallas_call(
        functools.partial(attention_forward_kernel, half),
        grid=(width // LANES,),
        in_specs=[pl.BlockSpec(mask.shape, lambda i: (0, 0, 0))] + [spec] * 5,
        out_specs=[spec, spec, pl.BlockSpec((tokens, LANES), lambda i: (0, 0))],
        out_shape=[
            jax.ShapeDtypeStruct((tokens, width), f32),
            jax.ShapeDtypeStruct((tokens, width), bf16),
            jax.ShapeDtypeStruct((tokens, LANES), f32),
        ],
        name="attention_forward",
    )(mask, q, k0, k1, v0, v1)


def attention_backward_kernel(
    half, mask_ref, q_ref, k0_ref, k1_ref, v0_ref, v1_ref, da_ref, o_ref, lse_ref,
    dq_ref, dk0_ref, dk1_ref, dv0_ref, dv1_ref, acc_ref,
):
    pair = pl.program_id(0)
    tokens = q_ref.shape[0]
    block = 2 * half
    lane = lax.broadcasted_iota(jnp.int32, (block, LANES), 1)
    acc_ref[...] = jnp.zeros_like(acc_ref)
    for u in range(tokens // block):
        rows = pl.ds(u * block, block)
        keys = (u + 1) * block
        dqs = []
        for h in range(2):
            cols = pl.ds(h * HEAD, HEAD)
            q, da = q_ref[rows, cols], da_ref[rows, cols]
            q_t, da_t = q.T, da.T
            lse = jnp.sum(jnp.where(lane == 2 * pair + h, lse_ref[rows, :], 0.0), axis=1, keepdims=True)
            delta = jnp.sum(da.astype(f32) * o_ref[rows, cols], axis=1, keepdims=True)
            dq = 0.0
            for part, (k_ref, v_ref) in enumerate(((k0_ref, v0_ref), (k1_ref, v1_ref))):
                k, v = k_ref[pl.ds(0, keys), cols], v_ref[pl.ds(0, keys), cols]
                s = mm_t(q, k)
                last = s[:, keys - block :] + mask_ref[part]
                s = last if u == 0 else jnp.concatenate([s[:, : keys - block], last], axis=1)
                p = jnp.exp(s - lse)
                ds = (p * (mm_t(da, v) - delta)).astype(bf16)
                dq = dq + mm(ds, k)
                acc_ref[part, 0, h, :, pl.ds(0, keys)] += mm(q_t, ds)
                acc_ref[part, 1, h, :, pl.ds(0, keys)] += mm(da_t, p.astype(bf16))
            dqs.append(dq * score_scale)
        dq_ref[rows, :] = jnp.concatenate(dqs, axis=1).astype(bf16)
    for part, (dk_ref, dv_ref) in enumerate(((dk0_ref, dv0_ref), (dk1_ref, dv1_ref))):
        for which, ref in enumerate((dk_ref, dv_ref)):
            both = jnp.concatenate([acc_ref[part, which, 0], acc_ref[part, which, 1]], axis=0)
            ref[...] = both.T.astype(ref.dtype)


def attention_backward(mask, q, k0, k1, v0, v1, da, o, lse, half):
    tokens, width = q.shape
    spec = pl.BlockSpec((tokens, LANES), lambda i: (0, i))
    whole = pl.BlockSpec((tokens, LANES), lambda i: (0, 0))
    shape = lambda t: jax.ShapeDtypeStruct((tokens, width), t)
    return pl.pallas_call(
        functools.partial(attention_backward_kernel, half),
        grid=(width // LANES,),
        in_specs=[pl.BlockSpec(mask.shape, lambda i: (0, 0, 0))] + [spec] * 7 + [whole],
        out_specs=[spec] * 5,
        out_shape=[shape(bf16), shape(f32), shape(bf16), shape(f32), shape(bf16)],
        scratch_shapes=[pltpu.VMEM((2, 2, 2, HEAD, tokens), f32)],
        name="attention_backward",
    )(mask, q, k0, k1, v0, v1, da, o, lse)


def normalised(values):
    mean = jnp.mean(values, axis=-1, keepdims=True)
    centred = values - mean
    var = jnp.mean(centred * centred, axis=-1, keepdims=True)
    scale = lax.rsqrt(var + eps_norm)
    return centred * scale, scale


def norm_backward(hat, scale, gain, grad):
    scaled = grad * gain
    mean = jnp.mean(scaled, axis=-1, keepdims=True)
    along = jnp.mean(scaled * hat, axis=-1, keepdims=True)
    return scale * (scaled - mean - hat * along)


def swap_cores(value):
    return lax.ppermute(value, "section", [(0, 1), (1, 0)])


def hop(value, source, target):
    return lax.ppermute(value, "shard", [(source, target)])


ANY = pl.BlockSpec(memory_space=pl.ANY)


def remote(src, dst, send, recv, section, ctx, shard):
    return pltpu.make_async_remote_copy(
        src_ref=src,
        dst_ref=dst,
        send_sem=send,
        recv_sem=recv,
        device_id=(section, ctx, shard),
        device_id_type=pl.DeviceIdType.MESH,
    )


def gather_kernel(
    attn_ref, ff_ref, x_ref, g_ref, norm_ref,
    w_attn_ref, w_ff_ref, x_all_ref, g_all_ref, norm_all_ref,
    send, recv, token_send, token_recv, norm_send, norm_recv, far_send, far_recv,
):
    section, ctx, shard = lax.axis_index("section"), lax.axis_index("ctx"), lax.axis_index("shard")
    kind = lax.rem(shard, 2)
    x_near, y_near = 1, 2
    near = lambda c, step: c + step - 2 * step * lax.rem(c // step, 2)
    far_core = 1 - shard // 2

    x_copy = remote(x_ref, x_all_ref.at[ctx], token_send.at[0], token_recv.at[ctx], section, shard, 0)
    g_copy = remote(g_ref, g_all_ref.at[ctx], token_send.at[1], token_recv.at[ctx], section, shard, 3)
    x_stays = (shard == 0) & (ctx == 0)
    g_stays = (shard == 3) & (ctx == 3)
    attn_copy = remote(
        attn_ref, w_attn_ref.at[ctx, shard], far_send.at[0], recv.at[ctx, shard], far_core, ctx, 2 * section
    )
    ff_copy = remote(
        ff_ref, w_ff_ref.at[ctx, shard], far_send.at[1], recv.at[ctx, shard], far_core, ctx, 2 * section + 1
    )

    @pl.when(jnp.logical_not(x_stays))
    def _():
        x_copy.start()

    attn_copy.start()
    norm_copies = []
    for core in range(2):
        for stage in range(2):
            index = core * 2 + stage
            copy = remote(
                norm_ref, norm_all_ref.at[shard], norm_send.at[index], norm_recv.at[shard],
                core, ctx, 2 * section + stage,
            )
            stays = (section == core) & (shard == 2 * section + stage)
            norm_copies.append((copy, stays))

            @pl.when(jnp.logical_not(stays))
            def _():
                copy.start()

    ff_copy.start()

    @pl.when(jnp.logical_not(g_stays))
    def _():
        g_copy.start()

    def spread(out_ref):
        def piece(c, s, which, core, to_ctx):
            return remote(
                out_ref.at[c, s], out_ref.at[c, s], send.at[which], recv.at[c, s], core, to_ctx, shard
            )

        mine = [2 * (1 - section) + j for j in range(2)]
        x_ctx, y_ctx = near(ctx, x_near), near(ctx, y_near)
        d_ctx = near(x_ctx, y_near)
        started = []

        def go(c, s, core, to_ctx):
            copy = piece(c, s, len(started), core, to_ctx)
            copy.start()
            started.append(copy)

        def arrived(c, s):
            piece(c, s, 0, section, ctx).wait_recv()

        for s in mine:
            arrived(ctx, s)
            go(ctx, s, section, x_ctx)
            go(ctx, s, section, y_ctx)
            go(ctx, s, 1 - section, ctx)
        arrived(x_ctx, mine[0])
        go(x_ctx, mine[0], section, y_ctx)
        go(x_ctx, mine[0], 1 - section, ctx)
        arrived(y_ctx, mine[0])
        go(y_ctx, mine[0], 1 - section, ctx)
        arrived(y_ctx, mine[1])
        go(y_ctx, mine[1], section, x_ctx)
        go(y_ctx, mine[1], 1 - section, ctx)
        arrived(x_ctx, mine[1])
        go(x_ctx, mine[1], 1 - section, ctx)
        for s in mine:
            arrived(d_ctx, s)
            go(d_ctx, s, 1 - section, ctx)
        for c in (ctx, x_ctx, y_ctx, d_ctx):
            for j in range(2):
                arrived(c, 2 * section + j)
        for copy in started:
            copy.wait_send()

    @pl.when(kind == 0)
    def _():
        spread(w_attn_ref)

    @pl.when(kind == 1)
    def _():
        spread(w_ff_ref)

    for s in range(4):

        @pl.when(jnp.logical_not((section == shard // 2) & (shard == s)))
        def _():
            remote(norm_ref, norm_all_ref.at[s], norm_send.at[0], norm_recv.at[s], section, ctx, shard).wait_recv()

    for c in range(4):

        @pl.when((shard == 0) & jnp.logical_not((ctx == 0) & (c == 0)))
        def _():
            remote(x_ref, x_all_ref.at[c], token_send.at[0], token_recv.at[c], section, ctx, shard).wait_recv()

        @pl.when((shard == 3) & jnp.logical_not((ctx == 3) & (c == 3)))
        def _():
            remote(g_ref, g_all_ref.at[c], token_send.at[1], token_recv.at[c], section, ctx, shard).wait_recv()

    @pl.when(jnp.logical_not(x_stays))
    def _():
        x_copy.wait_send()

    @pl.when(jnp.logical_not(g_stays))
    def _():
        g_copy.wait_send()

    attn_copy.wait_send()
    ff_copy.wait_send()
    for copy, stays in norm_copies:

        @pl.when(jnp.logical_not(stays))
        def _():
            copy.wait_send()


def gather_all(attn_piece, ff_piece, x_own, g_own, norm_own):
    like = lambda lead, v: jax.ShapeDtypeStruct(lead + v.shape, v.dtype)
    dma = pltpu.SemaphoreType.DMA
    return pl.pallas_call(
        gather_kernel,
        in_specs=[ANY] * 5,
        out_specs=[ANY] * 5,
        out_shape=[
            like((4, 4), attn_piece), like((4, 4), ff_piece), like((4,), x_own), like((4,), g_own), like((4,), norm_own),
        ],
        scratch_shapes=[dma((14,)), dma((4, 4)), dma((2,)), dma((4,)), dma((4,)), dma((4,)), dma((2,)), dma((2,))],
        compiler_params=pltpu.CompilerParams(has_side_effects=True),
        name="gather_all",
    )(attn_piece, ff_piece, x_own, g_own, norm_own)


def add_into(total, term):
    total[...] = (total[...].astype(f32) + term[...].astype(f32)).astype(bf16)


def reduce_kernel(*refs):
    attn_terms, ff_terms = refs[0:4], refs[4:8]
    attn_out, ff_out = refs[8:10]
    held, first, second, third = refs[10:14]
    load, first_send, first_recv, second_send, second_recv, third_send, third_recv, last_send, last_recv = refs[14:]
    section, ctx, shard = lax.axis_index("section"), lax.axis_index("ctx"), lax.axis_index("shard")
    kind = lax.rem(shard, 2)
    near = lambda c, step: c + step - 2 * step * lax.rem(c // step, 2)
    x_ctx, y_ctx = near(ctx, 1), near(ctx, 2)
    d_ctx = near(x_ctx, 2)
    count = len(attn_terms)

    def reduce(terms, out_ref, which):
        width = terms[0].shape[-1]
        cols = pl.ds(0, width)
        own = lambda i, c, j: held.at[i, c, j, :, cols]

        def give(i):
            return remote(
                terms[i].at[:, section], first.at[i, :, :, :, cols], first_send.at[i], first_recv.at[i],
                1 - section, ctx, shard,
            )

        def take(i):
            return pltpu.make_async_copy(terms[i].at[:, 1 - section], held.at[i, :, :, :, cols], load.at[i])

        def second_copy(i, j, part):
            to = (x_ctx, y_ctx)[j]
            return remote(
                own(i, (to, d_ctx)[part], j), second.at[i, j, part, :, cols],
                second_send.at[i, j, part], second_recv.at[i, j, part], section, to, shard,
            )

        def third_copy(i, j):
            to = (y_ctx, x_ctx)[j]
            return remote(
                own(i, to, j), third.at[i, j, :, cols], third_send.at[i, j], third_recv.at[i, j], section, to, shard
            )

        def last_copy(i, j):
            return remote(
                own(i, ctx, j), out_ref.at[i], last_send.at[i, j], last_recv.at[which, i],
                shard // 2, ctx, 2 * (1 - section) + j,
            )

        for i in range(count):
            give(i).start()
            take(i).start()
        for step in range(count + 2):
            i = step
            if i < count:
                take(i).wait()
                give(i).wait_recv()

                @pl.loop(0, 4)
                def _(c):
                    for j in range(2):
                        add_into(own(i, c, j), first.at[i, c, j, :, cols])

                for part in (1, 0):
                    for j in range(2):
                        second_copy(i, j, part).start()
            i = step - 1
            if 0 <= i < count:
                for j in range(2):
                    second_copy(i, j, 1).wait_recv()
                    add_into(own(i, (y_ctx, x_ctx)[j], j), second.at[i, j, 1, :, cols])
                    third_copy(i, j).start()
                for j in range(2):
                    second_copy(i, j, 0).wait_recv()
                    add_into(own(i, ctx, j), second.at[i, j, 0, :, cols])
            i = step - 2
            if 0 <= i < count:
                for j in range(2):
                    third_copy(i, j).wait_recv()
                    add_into(own(i, ctx, j), third.at[i, j, :, cols])
                    last_copy(i, j).start()
        for i in range(count):
            give(i).wait_send()
            for j in range(2):
                for part in range(2):
                    second_copy(i, j, part).wait_send()
                third_copy(i, j).wait_send()
                last_copy(i, j).wait_send()

    @pl.when(kind == 0)
    def _():
        reduce(attn_terms, attn_out, 0)

    @pl.when(kind == 1)
    def _():
        reduce(ff_terms, ff_out, 1)

    for i in range(count):
        for which, out_ref in enumerate((attn_out, ff_out)):
            remote(
                out_ref.at[i], out_ref.at[i], last_send.at[i, 0], last_recv.at[which, i], section, ctx, shard
            ).wait_recv()


def reduce_all(attn_terms, ff_terms):
    rows = attn_terms[0].shape[0] // 16
    count = len(attn_terms)
    split = lambda v: v.reshape(4, 2, 2, rows, v.shape[1])
    width = ff_terms[0].shape[1]
    dma = pltpu.SemaphoreType.DMA
    return pl.pallas_call(
        reduce_kernel,
        in_specs=[ANY] * (2 * count),
        out_specs=[ANY] * 2,
        out_shape=[
            jax.ShapeDtypeStruct((count, rows, attn_terms[0].shape[1]), bf16),
            jax.ShapeDtypeStruct((count, rows, width), bf16),
        ],
        scratch_shapes=[
            pltpu.VMEM((count, 4, 2, rows, width), bf16),
            pltpu.VMEM((count, 4, 2, rows, width), bf16),
            pltpu.VMEM((count, 2, 2, rows, width), bf16),
            pltpu.VMEM((count, 2, rows, width), bf16),
            dma((count,)), dma((count,)), dma((count,)),
            dma((count, 2, 2)), dma((count, 2, 2)),
            dma((count, 2)), dma((count, 2)),
            dma((count, 2)), dma((2, count)),
        ],
        compiler_params=pltpu.CompilerParams(has_side_effects=True, vmem_limit_bytes=48 * 2**20),
        name="reduce_all",
    )(*[split(v) for v in attn_terms], *[split(v) for v in ff_terms])


def chain(inputs, cotangent, qkv_weight, out_weight, up_weight, down_weight, norm_gain, norm_bias):
    section, ctx, shard = lax.axis_index("section"), lax.axis_index("ctx"), lax.axis_index("shard")
    seq_count, blocks, slice_len, width = inputs.shape
    half = slice_len // 2
    tokens = blocks * 4 * half
    share = width // 4
    group = share // 4
    group_pad = up_to(group, ROWS)
    wide = up_to(width, LANES)
    ff = up_weight.shape[2]
    is_attn = shard % 2 == 0

    pad = lambda w: jnp.pad(w, ((0, 0), (0, wide - width)))
    own_qkv, own_out = qkv_weight[0], out_weight[0]
    attn_src = jnp.stack([pad(own_qkv[:, i * width : (i + 1) * width]) for i in range(3)] + [pad(own_out)])
    down_t = down_weight[0].T
    up0 = up_weight[0]
    ff_src = jnp.stack([up0[:, : ff // 2], up0[:, ff // 2 :], down_t[:, : ff // 2], down_t[:, ff // 2 :]])
    norm_own = jnp.concatenate([norm_gain[0], norm_bias[0], jnp.zeros((4, share), bf16)], axis=0)
    x_own = lax.dynamic_slice_in_dim(inputs[0], section * half, half, 1)
    g_own = lax.dynamic_slice_in_dim(cotangent[0], section * half, half, 1)
    w_attn, w_ff, x_all, g_all, norm_all = gather_all(
        lax.dynamic_index_in_dim(attn_src, ctx, 0, keepdims=False),
        lax.dynamic_index_in_dim(ff_src, ctx, 0, keepdims=False),
        x_own, g_own, norm_own,
    )
    w_attn = w_attn.reshape(4, width, wide)
    w_ff = w_ff.reshape(4, width, ff // 2)
    own_place = jnp.arange(4)[:, None, None]
    norm_all = jnp.where((own_place == shard) & (section == shard // 2), norm_own, norm_all)
    norms = jnp.swapaxes(norm_all[:, :4], 0, 1).reshape(4, width).astype(f32)
    gain1, gain2, bias1, bias2 = norms[0], norms[1], norms[2], norms[3]

    def bring_tokens(every, own):
        mine = jnp.where((own_place[..., None] == ctx) & (shard == ctx), own, every)
        return jnp.swapaxes(mine, 0, 1).reshape(tokens, width)

    x_first, g_last = bring_tokens(x_all, x_own), bring_tokens(g_all, g_own)
    mask = attention_masks(section, half)
    feature = lax.broadcasted_iota(jnp.int32, (width, 16 * group_pad), 0)
    place = lax.broadcasted_iota(jnp.int32, (width, 16 * group_pad), 1)
    spread = (feature // group * group_pad + feature % group == place).astype(bf16)
    grouped = lambda v: mm(v, spread).astype(bf16)

    def attn_forward(x):
        x = x.astype(f32)
        hat, scale = normalised(x)
        normed = (hat * gain1 + bias1).astype(bf16)
        q = (mm(normed, w_attn[0]) * score_scale).astype(bf16)
        k = mm(normed, w_attn[1]).astype(bf16)
        v = mm(normed, w_attn[2]).astype(bf16)
        k1, v1 = swap_cores(k), swap_cores(v)
        o, ob, lse = attention_forward(mask, q, k, k1, v, v1, half)
        middle = x + mm(ob[:, :width], w_attn[3])[:, :width]
        return middle.astype(bf16), (hat, scale, normed, q, k, k1, v, v1, o, ob, lse)

    def ff_forward(middle):
        middle = middle.astype(f32)
        hat, scale = normalised(middle)
        normed = (hat * gain2 + bias2).astype(bf16)
        upper = [mm(normed, w_ff[i]) for i in range(2)]
        hidden = [jax.nn.gelu(u, approximate=True).astype(bf16) for u in upper]
        y = middle + mm_t(hidden[0], w_ff[2]) + mm_t(hidden[1], w_ff[3])
        return y.astype(bf16), (hat, scale, normed, upper, hidden)

    def ff_backward(g, state):
        hat, scale, normed, upper, hidden = state
        d_upper = []
        for i in range(2):
            d_hidden = mm(g, w_ff[2 + i])
            _, back = jax.vjp(lambda u: jax.nn.gelu(u, approximate=True), upper[i])
            d_upper.append(back(d_hidden)[0].astype(bf16))
        d_normed = mm_t(d_upper[0], w_ff[0]) + mm_t(d_upper[1], w_ff[1])
        d_middle = g.astype(f32) + norm_backward(hat, scale, gain2, d_normed)
        return d_middle.astype(bf16), d_upper, d_normed

    def attn_backward(d_middle, state):
        hat, scale, normed, q, k, k1, v, v1, o, ob, lse = state
        d_att = mm_t(jnp.pad(d_middle, ((0, 0), (0, wide - width))), w_attn[3]).astype(bf16)
        d_att = jnp.pad(d_att, ((0, 0), (0, wide - width)))
        dq, dk, dk_other, dv, dv_other = attention_backward(mask, q, k, k1, v, v1, d_att, o, lse, half)
        dk = (dk + swap_cores(dk_other).astype(f32)).astype(bf16)
        dv = (dv + swap_cores(dv_other).astype(f32)).astype(bf16)
        d_mixed = (dq, dk, dv)
        d_normed = mm_t(dq, w_attn[0]) + mm_t(dk, w_attn[1]) + mm_t(dv, w_attn[2])
        dx = d_middle.astype(f32) + norm_backward(hat, scale, gain1, d_normed)
        return dx.astype(bf16), d_mixed, d_normed

    middle, _ = attn_forward(x_first)
    middle0 = hop(middle, 0, 1)
    y, _ = ff_forward(middle0)
    x = jnp.where(shard == 0, x_first, hop(y, 1, 2))
    middle, attn_state = attn_forward(x)
    middle = jnp.where(shard == 1, middle0, hop(middle, 2, 3))
    y, ff_state = ff_forward(middle)

    d_middle, _, _ = ff_backward(g_last, ff_state)
    d_middle1 = hop(d_middle, 3, 2)
    dx, _, _ = attn_backward(d_middle1, attn_state)
    g = jnp.where(shard == 3, g_last, hop(dx, 2, 1))
    d_middle, d_upper, d_normed2 = ff_backward(g, ff_state)
    hat2, _, normed2, _, hidden = ff_state
    g_grouped, n2_grouped = grouped(g), grouped(normed2)
    ff_grads = [t_mm(n2_grouped, d_upper[0]), t_mm(n2_grouped, d_upper[1]), t_mm(g_grouped, hidden[0]), t_mm(g_grouped, hidden[1])]
    d_middle = jnp.where(shard == 2, d_middle1, hop(d_middle, 1, 0))
    dx, d_mixed, d_normed1 = attn_backward(d_middle, attn_state)
    hat1, _, normed, _, _, _, _, _, _, ob, _ = attn_state
    n1_grouped, att_grouped = grouped(normed), grouped(ob[:, :width])
    attn_grads = [t_mm(n1_grouped, d) for d in d_mixed] + [t_mm(att_grouped, jnp.pad(d_middle, ((0, 0), (0, wide - width))))]
    attn_sums, ff_sums = reduce_all([v.astype(bf16) for v in attn_grads], [v.astype(bf16) for v in ff_grads])

    own_hat = jnp.where(is_attn, hat1, hat2)
    own_grad = jnp.where(is_attn, d_normed1, d_normed2)
    terms = jnp.stack([jnp.sum(own_grad * own_hat, axis=0), jnp.sum(own_grad, axis=0)])
    terms = jnp.where(jnp.arange(4)[:, None, None] == shard, terms[None], 0.0)
    totals = lax.psum(terms, ("section", "ctx", "shard")).reshape(2, 2, 2, width)
    totals = lax.dynamic_index_in_dim(totals, section, 0, keepdims=False)
    totals = lax.dynamic_slice_in_dim(totals, (ctx * 4 + shard) * group, group, 2)

    final = jnp.where(is_attn, dx, y).reshape(blocks, 4, half, width)
    final = lax.all_to_all(jnp.swapaxes(final, 0, 1), "ctx", 0, 0)
    final = lax.all_to_all(final, "shard", 0, 0).reshape(2, 2, blocks, half, width)
    final = lax.all_to_all(final, "section", 0, 0)
    final = jnp.moveaxis(final, 0, 2).reshape(2, blocks, slice_len, width)

    attn_sums = attn_sums[:, :group, :width].astype(f32)
    ff_sums = ff_sums[:, :group].astype(f32)
    return (
        final[1][None, None],
        final[0][None, None],
        jnp.concatenate([attn_sums[0], attn_sums[1], attn_sums[2]], axis=1)[None],
        attn_sums[3][None],
        jnp.concatenate([ff_sums[0], ff_sums[1]], axis=1)[None],
        jnp.concatenate([ff_sums[2].T, ff_sums[3].T], axis=0)[None],
        totals[:, 0][None],
        totals[:, 1][None],
    )


def passed_along(value, axis, steps):
    count = lax.axis_size(axis)
    initial, last = (max(0, -steps), min(count, count - steps))
    return lax.ppermute(value, axis, [(source, source + steps) for source in range(initial, last)])


def layer_norm(values, gain, shift):
    mean = jnp.mean(values, axis=-1, keepdims=True)
    centred = values - mean
    var = jnp.mean(centred * centred, axis=-1, keepdims=True)
    return centred * lax.rsqrt(var + eps_norm) * gain + shift


def gelu_tanh(values):
    return jax.nn.gelu(values, approximate=True)


def split_pair(key_value, head_count):
    block_len, seq_count, double = key_value.shape
    model_width = double // 2
    key_rows = key_value[..., :model_width].reshape(block_len, seq_count, head_count, HEAD)
    value_rows = key_value[..., model_width:].reshape(block_len, seq_count, head_count, HEAD)
    return (key_rows, value_rows)


def causal_mask(query_pos, key_pos):
    return (key_pos[None, :] <= query_pos[:, None])[None, :, None, :]


def forward_block(running, queries, query_pos, key_value, key_pos):
    row_max, row_sum, accum = running
    key_rows, value_rows = split_pair(key_value, queries.shape[2])
    scores = (
        jnp.einsum("sqhe,kshe->sqhk", queries, key_rows, preferred_element_type=jnp.float32)
        * score_scale
    )
    causal = causal_mask(query_pos, key_pos)
    new_max = jnp.maximum(row_max, jnp.max(jnp.where(causal, scores, -1e30), axis=-1))
    softmax_w = jnp.where(causal, jnp.exp(scores - new_max[..., None]), 0.0)
    factor = jnp.exp(row_max - new_max)
    row_sum = row_sum * factor + jnp.sum(softmax_w, axis=-1)
    accum = accum * factor[..., None] + jnp.einsum(
        "sqhk,kshe->sqhe",
        softmax_w.astype(jnp.bfloat16),
        value_rows,
        preferred_element_type=jnp.float32,
    )
    return (new_max, row_sum, accum)


def split_rows(whole):
    key_count = whole.shape[0]
    block_size = 512
    blocks = whole.reshape((key_count // block_size, block_size) + whole.shape[1:])
    offsets = jnp.arange(key_count // block_size, dtype=jnp.int32) * block_size
    return (blocks, offsets, block_size)


def fold_keys(running, piece, start, queries, query_pos, group_len):
    blocks, offsets, block_size = split_rows(piece)

    def fold_scan_step(inner, scan_item):
        block_rows, offset = scan_item
        for group_id in range(block_rows.shape[2]):
            key_pos = (
                group_id * group_len + start + offset + jnp.arange(block_size, dtype=jnp.int32)
            )
            inner = forward_block(inner, queries, query_pos, block_rows[:, :, group_id], key_pos)
        return (inner, None)

    result, _ = lax.scan(fold_scan_step, running, (blocks, offsets))
    return result


def pair_terms(d_scores, softmax_w, queries, d_attended, block_size):
    d_keys = (
        jnp.einsum("sqhk,sqhe->kshe", d_scores, queries, preferred_element_type=jnp.float32)
        * score_scale
    )
    d_values = jnp.einsum(
        "sqhk,sqhe->kshe",
        softmax_w.astype(jnp.bfloat16),
        d_attended,
        preferred_element_type=jnp.float32,
    )
    shape = (block_size, queries.shape[0], queries.shape[2] * queries.shape[3])
    return jnp.concatenate([d_keys.reshape(shape), d_values.reshape(shape)], axis=-1)


def score_grads(
    queries, query_pos, log_total, row_delta, d_attended, key_rows, value_rows, key_pos
):
    scores = (
        jnp.einsum("sqhe,kshe->sqhk", queries, key_rows, preferred_element_type=jnp.float32)
        * score_scale
    )
    causal = causal_mask(query_pos, key_pos)
    softmax_w = jnp.where(causal, jnp.exp(scores - log_total[..., None]), 0.0)
    d_probs = jnp.einsum(
        "sqhe,kshe->sqhk", d_attended, value_rows, preferred_element_type=jnp.float32
    )
    d_scores = (softmax_w * (d_probs - row_delta[..., None])).astype(jnp.bfloat16)
    return (softmax_w, d_scores)


def backward_keys(whole, queries, query_pos, log_total, row_delta, d_attended, group_len):
    blocks, offsets, block_size = split_rows(whole)

    def backward_scan_step(d_queries, scan_item):
        block_rows, offset = scan_item
        for group_id in range(block_rows.shape[2]):
            key_pos = group_id * group_len + offset + jnp.arange(block_size, dtype=jnp.int32)
            key_rows, value_rows = split_pair(block_rows[:, :, group_id], queries.shape[2])
            softmax_w, d_scores = score_grads(
                queries, query_pos, log_total, row_delta, d_attended, key_rows, value_rows, key_pos
            )
            d_queries = (
                d_queries
                + jnp.einsum(
                    "sqhk,kshe->sqhe", d_scores, key_rows, preferred_element_type=jnp.float32
                )
                * score_scale
            )
        return (d_queries, None)

    d_queries, terms = lax.scan(
        backward_scan_step, jnp.zeros(queries.shape, jnp.float32), (blocks, offsets)
    )
    return (d_queries, None)


def owner_terms(
    own_cache, all_queries, all_d_att, all_totals, all_deltas, micro_index, ctx_id, group_len
):
    block_len, seq_count, group_count, double = own_cache.shape
    head_count = all_queries.shape[2]
    query_rows = all_queries.shape[1]
    query_size = 512
    block_count = query_rows // query_size

    def loop_step(index, total):
        offset = index * query_size
        q_block = lax.dynamic_slice_in_dim(all_queries, offset, query_size, 1)
        d_block = lax.dynamic_slice_in_dim(all_d_att, offset, query_size, 1)
        t_block = lax.dynamic_slice_in_dim(all_totals, offset, query_size, 1)
        r_block = lax.dynamic_slice_in_dim(all_deltas, offset, query_size, 1)
        query_pos = micro_index * group_len + offset + jnp.arange(query_size, dtype=jnp.int32)
        pieces = []
        for group_id in range(group_count):
            key_pos = (
                group_id * group_len + ctx_id * block_len + jnp.arange(block_len, dtype=jnp.int32)
            )
            key_rows, value_rows = split_pair(own_cache[:, :, group_id], head_count)
            softmax_w, d_scores = score_grads(
                q_block, query_pos, t_block, r_block, d_block, key_rows, value_rows, key_pos
            )
            pieces.append(pair_terms(d_scores, softmax_w, q_block, d_block, block_len))
        return total + jnp.stack(pieces, axis=2)

    return lax.fori_loop(0, block_count, loop_step, jnp.zeros(own_cache.shape, jnp.float32))


def store_at(store, value, micro_index, active):
    updated = lax.dynamic_update_index_in_dim(store, value, micro_index, 0)
    return jnp.where(active, updated, store)


def shards(inputs, cotangent, qkv_weight, out_weight, up_weight, down_weight, norm_gain, norm_bias):
    section_id = lax.axis_index("section")
    ctx_count = lax.axis_size("ctx")
    ctx_id = lax.axis_index("ctx")
    seq_count, group_count, block_len, model_width = inputs.shape
    head_count = model_width // HEAD
    group_len = block_len * ctx_count
    row_count = seq_count * block_len
    w_qkv, w_out, w_up, w_down, gains, biases = (
        lax.all_gather(qkv_weight[0], "shard", axis=0, tiled=True),
        lax.all_gather(out_weight[0], "shard", axis=0, tiled=True),
        lax.all_gather(up_weight[0], "shard", axis=0, tiled=True),
        lax.all_gather(down_weight[0], "shard", axis=1, tiled=True),
        lax.all_gather(norm_gain[0], "shard", axis=1, tiled=True),
        lax.all_gather(norm_bias[0], "shard", axis=1, tiled=True),
    )
    gains = gains.astype(jnp.float32)
    biases = biases.astype(jnp.float32)
    ff_width = w_up.shape[1]
    cache = jnp.zeros((block_len, seq_count, group_count, 2 * model_width), jnp.bfloat16)
    in_store = jnp.zeros((group_count, seq_count, block_len, model_width), jnp.bfloat16)
    query_store = jnp.zeros((group_count, seq_count, block_len, head_count, HEAD), jnp.bfloat16)
    att_store = jnp.zeros((group_count, seq_count, block_len, head_count, HEAD), jnp.float32)
    total_store = jnp.zeros((group_count, seq_count, block_len, head_count), jnp.float32)
    middle_store = jnp.zeros((group_count, row_count, model_width), jnp.float32)
    upper_store = jnp.zeros((group_count, row_count, ff_width), jnp.float32)
    out_store = jnp.zeros((group_count, seq_count, block_len, model_width), jnp.bfloat16)
    received = jnp.zeros((seq_count, block_len, model_width), jnp.bfloat16)
    for tick_no in range(group_count + 1):
        micro = tick_no - section_id
        active = (micro >= 0) & (micro < group_count)
        micro_index = jnp.clip(micro, 0, group_count - 1)
        own_input = lax.dynamic_index_in_dim(inputs, micro_index, 1, keepdims=False)
        entering = jnp.where(section_id == 0, own_input, received)
        flat_rows = entering.reshape(row_count, model_width).astype(jnp.float32)
        normed = layer_norm(flat_rows, gains[0], biases[0]).astype(jnp.bfloat16)
        mixed = jnp.dot(normed, w_qkv, preferred_element_type=jnp.float32).astype(jnp.bfloat16)
        queries = mixed[:, :model_width].reshape(seq_count, block_len, head_count, HEAD)
        fresh = jnp.swapaxes(
            mixed[:, model_width:].reshape(seq_count, block_len, 2 * model_width), 0, 1
        )
        updated = lax.dynamic_update_index_in_dim(cache, fresh, micro_index, 2)
        cache = jnp.where(active, updated, cache)
        query_pos = (
            micro_index * group_len + ctx_id * block_len + jnp.arange(block_len, dtype=jnp.int32)
        )
        start_state = (
            jnp.full((seq_count, block_len, head_count), -1e30, jnp.float32),
            jnp.zeros((seq_count, block_len, head_count), jnp.float32),
            jnp.zeros((seq_count, block_len, head_count, HEAD), jnp.float32),
        )
        row_max, row_sum, accum = fold_keys(
            start_state,
            lax.all_gather(cache, "ctx", axis=0, tiled=True),
            jnp.int32(0),
            queries,
            query_pos,
            group_len,
        )
        attended = accum / row_sum[..., None]
        log_total = row_max + jnp.log(row_sum)
        att_low = attended.reshape(row_count, model_width).astype(jnp.bfloat16)
        middle = flat_rows + jnp.dot(att_low, w_out, preferred_element_type=jnp.float32)
        normed2 = layer_norm(middle, gains[1], biases[1]).astype(jnp.bfloat16)
        upper = jnp.dot(normed2, w_up, preferred_element_type=jnp.float32)
        hidden = gelu_tanh(upper).astype(jnp.bfloat16)
        leaving = (middle + jnp.dot(hidden, w_down, preferred_element_type=jnp.float32)).astype(
            jnp.bfloat16
        )
        leaving = leaving.reshape(seq_count, block_len, model_width)
        in_store = store_at(in_store, entering, micro_index, active)
        query_store = store_at(query_store, queries, micro_index, active)
        att_store = store_at(att_store, attended, micro_index, active)
        total_store = store_at(total_store, log_total, micro_index, active)
        middle_store = store_at(middle_store, middle, micro_index, active)
        upper_store = store_at(upper_store, upper, micro_index, active)
        out_store = store_at(out_store, leaving, micro_index, active)
        if tick_no < group_count:
            received = passed_along(leaving, "section", 1)
    key_acc = jnp.zeros((block_len, seq_count, group_count, 2 * model_width), jnp.float32)
    grad_qkv = jnp.zeros((model_width, 3 * model_width), jnp.float32)
    grad_out = jnp.zeros((model_width, model_width), jnp.float32)
    grad_up = jnp.zeros((model_width, ff_width), jnp.float32)
    grad_down = jnp.zeros((ff_width, model_width), jnp.float32)
    grad_gain = jnp.zeros((2, model_width), jnp.float32)
    grad_bias = jnp.zeros((2, model_width), jnp.float32)
    grad_store = jnp.zeros((group_count, seq_count, block_len, model_width), jnp.bfloat16)
    coming = jnp.zeros((seq_count, block_len, model_width), jnp.bfloat16)
    for tick_no in range(group_count + 1):
        micro = group_count - tick_no - section_id
        active = (micro >= 0) & (micro < group_count)
        active_weight = active.astype(jnp.float32)
        micro_index = jnp.clip(micro, 0, group_count - 1)
        own_cot = lax.dynamic_index_in_dim(cotangent, micro_index, 1, keepdims=False)
        d_out = (
            jnp.where(section_id == 1, own_cot, coming)
            .reshape(row_count, model_width)
            .astype(jnp.float32)
        )
        flat_rows = in_store[micro_index].reshape(row_count, model_width).astype(jnp.float32)
        queries = query_store[micro_index]
        attended = att_store[micro_index]
        log_total = total_store[micro_index]
        middle = middle_store[micro_index]
        upper = upper_store[micro_index]
        normed2_full, norm2_back = jax.vjp(
            lambda v, g, b: layer_norm(v, g, b), middle, gains[1], biases[1]
        )
        normed2 = normed2_full.astype(jnp.bfloat16)
        hidden_full, gelu_back = jax.vjp(gelu_tanh, upper)
        hidden = hidden_full.astype(jnp.bfloat16)
        d_branch = d_out.astype(jnp.bfloat16)
        grad_down = grad_down + active_weight * jnp.dot(
            hidden.T, d_branch, preferred_element_type=jnp.float32
        )
        d_hidden = jnp.dot(d_branch, w_down.T, preferred_element_type=jnp.float32)
        d_upper = gelu_back(d_hidden)[0].astype(jnp.bfloat16)
        grad_up = grad_up + active_weight * jnp.dot(
            normed2.T, d_upper, preferred_element_type=jnp.float32
        )
        d_normed2 = jnp.dot(d_upper, w_up.T, preferred_element_type=jnp.float32)
        d_mid_norm, d_gain2, d_bias2 = norm2_back(d_normed2)
        d_middle = d_out + d_mid_norm
        att_low = attended.reshape(row_count, model_width).astype(jnp.bfloat16)
        d_att = d_middle.astype(jnp.bfloat16)
        grad_out = grad_out + active_weight * jnp.dot(
            att_low.T, d_att, preferred_element_type=jnp.float32
        )
        d_attended = jnp.dot(d_att, w_out.T, preferred_element_type=jnp.float32).astype(
            jnp.bfloat16
        )
        d_attended = d_attended.reshape(seq_count, block_len, head_count, HEAD)
        row_delta = jnp.sum(d_attended.astype(jnp.float32) * attended, axis=-1)
        query_pos = (
            micro_index * group_len + ctx_id * block_len + jnp.arange(block_len, dtype=jnp.int32)
        )
        whole = lax.all_gather(cache, "ctx", axis=0, tiled=True)
        d_queries, unused = backward_keys(
            whole, queries, query_pos, log_total, row_delta, d_attended, group_len
        )
        all_queries, all_d_att = (
            lax.all_gather(queries, "ctx", axis=1, tiled=True),
            lax.all_gather(d_attended, "ctx", axis=1, tiled=True),
        )
        all_totals, all_deltas = (
            lax.all_gather(log_total, "ctx", axis=1, tiled=True),
            lax.all_gather(row_delta, "ctx", axis=1, tiled=True),
        )
        shares = owner_terms(
            cache, all_queries, all_d_att, all_totals, all_deltas, micro_index, ctx_id, group_len
        )
        key_acc = key_acc + active_weight * shares
        d_pair = jnp.swapaxes(
            lax.dynamic_index_in_dim(key_acc, micro_index, 2, keepdims=False), 0, 1
        )
        d_mixed = jnp.concatenate(
            [d_queries.reshape(row_count, model_width), d_pair.reshape(row_count, 2 * model_width)],
            axis=-1,
        ).astype(jnp.bfloat16)
        normed_full, norm1_back = jax.vjp(
            lambda v, g, b: layer_norm(v, g, b), flat_rows, gains[0], biases[0]
        )
        normed = normed_full.astype(jnp.bfloat16)
        grad_qkv = grad_qkv + active_weight * jnp.dot(
            normed.T, d_mixed, preferred_element_type=jnp.float32
        )
        d_normed = jnp.dot(d_mixed, w_qkv.T, preferred_element_type=jnp.float32)
        d_flat_norm, d_gain1, d_bias1 = norm1_back(d_normed)
        grad_gain = grad_gain + active_weight * jnp.stack([d_gain1, d_gain2])
        grad_bias = grad_bias + active_weight * jnp.stack([d_bias1, d_bias2])
        d_entering = (
            (d_middle + d_flat_norm).astype(jnp.bfloat16).reshape(seq_count, block_len, model_width)
        )
        grad_store = store_at(grad_store, d_entering, micro_index, active)
        if tick_no < group_count:
            coming = passed_along(d_entering, "section", -1)
    sums = (
        lax.psum_scatter(grad_qkv, ("ctx", "shard"), scatter_dimension=0, tiled=True),
        lax.psum_scatter(grad_out, ("ctx", "shard"), scatter_dimension=0, tiled=True),
        lax.psum_scatter(grad_up, ("ctx", "shard"), scatter_dimension=0, tiled=True),
        lax.psum_scatter(grad_down, ("ctx", "shard"), scatter_dimension=1, tiled=True),
        lax.psum_scatter(grad_gain, ("ctx", "shard"), scatter_dimension=1, tiled=True),
        lax.psum_scatter(grad_bias, ("ctx", "shard"), scatter_dimension=1, tiled=True),
    )
    layer_outputs = jnp.swapaxes(out_store, 0, 1)[None]
    input_grads = jnp.swapaxes(grad_store, 0, 1)[None]
    return (
        layer_outputs,
        input_grads,
        sums[0][None],
        sums[1][None],
        sums[2][None],
        sums[3][None],
        sums[4][None],
        sums[5][None],
    )


def solution(mesh):
    in_specs = (
        P("shard", None, "ctx", None),
        P("shard", None, "ctx", None),
        P("section", "shard", None),
        P("section", "shard", None),
        P("section", "shard", None),
        P("section", None, "shard"),
        P("section", None, "shard"),
        P("section", None, "shard"),
    )
    out_specs = (
        P("section", "shard", None, "ctx", None),
        P("section", "shard", None, "ctx", None),
        P("section", ("ctx", "shard"), None),
        P("section", ("ctx", "shard"), None),
        P("section", ("ctx", "shard"), None),
        P("section", None, ("ctx", "shard")),
        P("section", None, ("ctx", "shard")),
        P("section", None, ("ctx", "shard")),
    )
    relay = mesh.shape["section"] == 2 and mesh.shape["shard"] == 4 and mesh.shape["ctx"] == 4
    return jax.shard_map(chain if relay else shards, mesh=mesh, in_specs=in_specs, out_specs=out_specs, check_vma=False)
```

```python
import functools

import jax
import jax.numpy as jnp
from jax import lax
from jax.experimental import pallas as pl
from jax.experimental.pallas import tpu as pltpu
from jax.sharding import PartitionSpec as P

HEAD = 64
LANES = 128
ROWS = 8
NEG = -1e30

eps_norm = 1e-05
score_scale = 0.125
f32 = jnp.float32
bf16 = jnp.bfloat16


def up_to(width, step):
    return -(-width // step) * step


def dot(a, b, dims):
    return lax.dot_general(a, b, (dims, ((), ())), preferred_element_type=f32)


def mm(a, b):
    return dot(a, b, ((1,), (0,)))


def mm_t(a, b):
    return dot(a, b, ((1,), (1,)))


def t_mm(a, b):
    return dot(a, b, ((0,), (0,)))


def attention_masks(core, half):
    row = lax.broadcasted_iota(jnp.int32, (2 * half, 2 * half), 0)
    col = lax.broadcasted_iota(jnp.int32, (2 * half, 2 * half), 1)
    row_slice, col_slice = row // half, col // half
    own = (col_slice < row_slice) | ((col_slice == row_slice) & (col <= row))
    other = (col_slice < row_slice) | ((col_slice == row_slice) & (core == 1))
    return jnp.where(jnp.stack([own, other]), 0.0, NEG).astype(f32)


def attention_forward_kernel(half, mask_ref, q_ref, k0_ref, k1_ref, v0_ref, v1_ref, o_ref, ob_ref, lse_ref):
    pair = pl.program_id(0)
    tokens = q_ref.shape[0]
    block = 2 * half

    @pl.when(pair == 0)
    def _():
        lse_ref[...] = jnp.zeros_like(lse_ref)

    lane = lax.broadcasted_iota(jnp.int32, (block, LANES), 1)
    for u in range(tokens // block):
        rows = pl.ds(u * block, block)
        keys = (u + 1) * block
        outs = []
        for h in range(2):
            cols = pl.ds(h * HEAD, HEAD)
            q = q_ref[rows, cols]
            scores = []
            for part, k_ref in enumerate((k0_ref, k1_ref)):
                s = mm_t(q, k_ref[pl.ds(0, keys), cols])
                last = s[:, keys - block :] + mask_ref[part]
                scores.append(last if u == 0 else jnp.concatenate([s[:, : keys - block], last], axis=1))
            top = jnp.maximum(
                jnp.max(scores[0], axis=1, keepdims=True), jnp.max(scores[1], axis=1, keepdims=True)
            )
            total, acc = 0.0, 0.0
            for s, v_ref in zip(scores, (v0_ref, v1_ref)):
                p = jnp.exp(s - top)
                total = total + jnp.sum(p, axis=1, keepdims=True)
                acc = acc + mm(p.astype(bf16), v_ref[pl.ds(0, keys), cols])
            outs.append(acc / total)
            lse = top + jnp.log(total)
            lse_ref[rows, :] = jnp.where(lane == 2 * pair + h, lse, lse_ref[rows, :])
        out = jnp.concatenate(outs, axis=1)
        o_ref[rows, :] = out
        ob_ref[rows, :] = out.astype(bf16)


def attention_forward(mask, q, k0, k1, v0, v1, half):
    tokens, width = q.shape
    spec = pl.BlockSpec((tokens, LANES), lambda i: (0, i))
    return pl.pallas_call(
        functools.partial(attention_forward_kernel, half),
        grid=(width // LANES,),
        in_specs=[pl.BlockSpec(mask.shape, lambda i: (0, 0, 0))] + [spec] * 5,
        out_specs=[spec, spec, pl.BlockSpec((tokens, LANES), lambda i: (0, 0))],
        out_shape=[
            jax.ShapeDtypeStruct((tokens, width), f32),
            jax.ShapeDtypeStruct((tokens, width), bf16),
            jax.ShapeDtypeStruct((tokens, LANES), f32),
        ],
        name="attention_forward",
    )(mask, q, k0, k1, v0, v1)


def attention_backward_kernel(
    half, mask_ref, q_ref, k0_ref, k1_ref, v0_ref, v1_ref, da_ref, o_ref, lse_ref,
    dq_ref, dk0_ref, dk1_ref, dv0_ref, dv1_ref, acc_ref,
):
    pair = pl.program_id(0)
    tokens = q_ref.shape[0]
    block = 2 * half
    lane = lax.broadcasted_iota(jnp.int32, (block, LANES), 1)
    acc_ref[...] = jnp.zeros_like(acc_ref)
    for u in range(tokens // block):
        rows = pl.ds(u * block, block)
        keys = (u + 1) * block
        dqs = []
        for h in range(2):
            cols = pl.ds(h * HEAD, HEAD)
            q, da = q_ref[rows, cols], da_ref[rows, cols]
            q_t, da_t = q.T, da.T
            lse = jnp.sum(jnp.where(lane == 2 * pair + h, lse_ref[rows, :], 0.0), axis=1, keepdims=True)
            delta = jnp.sum(da.astype(f32) * o_ref[rows, cols], axis=1, keepdims=True)
            dq = 0.0
            for part, (k_ref, v_ref) in enumerate(((k0_ref, v0_ref), (k1_ref, v1_ref))):
                k, v = k_ref[pl.ds(0, keys), cols], v_ref[pl.ds(0, keys), cols]
                s = mm_t(q, k)
                last = s[:, keys - block :] + mask_ref[part]
                s = last if u == 0 else jnp.concatenate([s[:, : keys - block], last], axis=1)
                p = jnp.exp(s - lse)
                ds = (p * (mm_t(da, v) - delta)).astype(bf16)
                dq = dq + mm(ds, k)
                acc_ref[part, 0, h, :, pl.ds(0, keys)] += mm(q_t, ds)
                acc_ref[part, 1, h, :, pl.ds(0, keys)] += mm(da_t, p.astype(bf16))
            dqs.append(dq * score_scale)
        dq_ref[rows, :] = jnp.concatenate(dqs, axis=1).astype(bf16)
    for part, (dk_ref, dv_ref) in enumerate(((dk0_ref, dv0_ref), (dk1_ref, dv1_ref))):
        for which, ref in enumerate((dk_ref, dv_ref)):
            both = jnp.concatenate([acc_ref[part, which, 0], acc_ref[part, which, 1]], axis=0)
            ref[...] = both.T.astype(ref.dtype)


def attention_backward(mask, q, k0, k1, v0, v1, da, o, lse, half):
    tokens, width = q.shape
    spec = pl.BlockSpec((tokens, LANES), lambda i: (0, i))
    whole = pl.BlockSpec((tokens, LANES), lambda i: (0, 0))
    shape = lambda t: jax.ShapeDtypeStruct((tokens, width), t)
    return pl.pallas_call(
        functools.partial(attention_backward_kernel, half),
        grid=(width // LANES,),
        in_specs=[pl.BlockSpec(mask.shape, lambda i: (0, 0, 0))] + [spec] * 7 + [whole],
        out_specs=[spec] * 5,
        out_shape=[shape(bf16), shape(f32), shape(bf16), shape(f32), shape(bf16)],
        scratch_shapes=[pltpu.VMEM((2, 2, 2, HEAD, tokens), f32)],
        name="attention_backward",
    )(mask, q, k0, k1, v0, v1, da, o, lse)


def norm_backward(hat, scale, gain, grad):
    scaled = grad * gain
    mean = jnp.mean(scaled, axis=-1, keepdims=True)
    along = jnp.mean(scaled * hat, axis=-1, keepdims=True)
    return scale * (scaled - mean - hat * along)


def swap_cores(value):
    return lax.ppermute(value, "section", [(0, 1), (1, 0)])


def hop(value, source, target):
    return lax.ppermute(value, "shard", [(source, target)])


ANY = pl.BlockSpec(memory_space=pl.ANY)


def remote(src, dst, send, recv, section, ctx, shard):
    return pltpu.make_async_remote_copy(
        src_ref=src,
        dst_ref=dst,
        send_sem=send,
        recv_sem=recv,
        device_id=(section, ctx, shard),
        device_id_type=pl.DeviceIdType.MESH,
    )


def normalised(values):
    mean = jnp.mean(values, axis=-1, keepdims=True)
    centred = values - mean
    var = jnp.mean(centred * centred, axis=-1, keepdims=True)
    scale = lax.rsqrt(var + eps_norm)
    return centred * scale, scale


def stack_heads(value, low):
    zero = jnp.zeros_like(value)
    return jnp.concatenate([jnp.where(low, value, zero), jnp.where(low, zero, value)], axis=0)


def unstack_heads(value, low):
    rows = value.shape[0] // 2
    return jnp.where(low, value[:rows], value[rows:])


def mask_last(scores, mask):
    width = mask.shape[1]
    last = scores[:, scores.shape[1] - width :] + mask
    if scores.shape[1] == width:
        return last
    return jnp.concatenate([scores[:, : scores.shape[1] - width], last], axis=1)


def attend_chunk(u, rows, mask_ref, q, k, k1, v, v1, o, lse):
    size = rows.size
    keys = pl.ds(0, (u + 1) * size)
    lane = lax.broadcasted_iota(jnp.int32, (size, LANES), 1)
    low = lane < HEAD

    @pl.loop(0, q.shape[1] // LANES)
    def _(pair):
        cols = pl.ds(pl.multiple_of(pair * LANES, LANES), LANES)
        q2 = stack_heads(q[rows, cols], low)
        scores = [mask_last(mm_t(q2, ref[keys, cols]), mask_ref[part]) for part, ref in enumerate((k, k1))]
        top = jnp.maximum(
            jnp.max(scores[0], axis=1, keepdims=True), jnp.max(scores[1], axis=1, keepdims=True)
        )
        total, acc = 0.0, 0.0
        for s, ref in zip(scores, (v, v1)):
            p = jnp.exp(s - top)
            total = total + jnp.sum(p, axis=1, keepdims=True)
            acc = acc + mm(p.astype(bf16), ref[keys, cols])
        o[rows, cols] = unstack_heads(acc / total, low)
        level = top + jnp.log(total)
        lse[rows, :] = jnp.where(
            lane == 2 * pair, level[:size], jnp.where(lane == 2 * pair + 1, level[size:], lse[rows, :])
        )


def near_ctx(c, step):
    return c + step - 2 * step * lax.rem(c // step, 2)


def forward_kernel(
    attn_ref, ff_ref, x_ref, g_ref, norm_ref, mask_ref,
    w_attn_out, w_ff_out, g_all_ref, norm_out,
    ent_out, nrm_out, q_out, k_out, k1_out, v_out, v1_out, o_out, lse_out, up_out, hid_out, lea_out,
    w, x_all, norm_all, norms, ent, nrm, q, k, k1, v, v1, o, lse, up, hid, lea,
    send, recv, token_send, token_recv, norm_send, norm_recv, far_send,
    hop_send, hop_recv, swap_send, swap_recv, save, keep,
):
    section, ctx, shard = lax.axis_index("section"), lax.axis_index("ctx"), lax.axis_index("shard")
    kind = lax.rem(shard, 2)
    far_core = 1 - shard // 2
    x_ctx, y_ctx = near_ctx(ctx, 1), near_ctx(ctx, 2)
    d_ctx = near_ctx(x_ctx, 2)
    width = ent.shape[1]
    wide = q.shape[1]
    size = 2 * x_ref.shape[1]
    chunks = ent.shape[0] // size
    attn_cols = pl.ds(0, attn_ref.shape[1])
    ff_cols = pl.ds(0, ff_ref.shape[1])

    x_copy = remote(x_ref, x_all.at[ctx], token_send.at[0], token_recv.at[ctx], section, shard, 0)
    g_copy = remote(g_ref, g_all_ref.at[ctx], token_send.at[1], token_recv.at[ctx], section, shard, 3)
    x_stays = (shard == 0) & (ctx == 0)
    g_stays = (shard == 3) & (ctx == 3)
    attn_copy = remote(
        attn_ref, w.at[ctx, shard, :, attn_cols], far_send.at[0], recv.at[ctx, shard], far_core, ctx, 2 * section
    )
    ff_copy = remote(
        ff_ref, w.at[ctx, shard, :, ff_cols], far_send.at[1], recv.at[ctx, shard], far_core, ctx, 2 * section + 1
    )
    x_local = pltpu.make_async_copy(x_ref, x_all.at[ctx], token_recv.at[ctx])
    norm_local = pltpu.make_async_copy(norm_ref, norm_all.at[shard], norm_recv.at[shard])

    @pl.when(x_stays)
    def _():
        x_local.start()

    @pl.when(jnp.logical_not(x_stays))
    def _():
        x_copy.start()

    attn_copy.start()
    norm_copies = []
    for core in range(2):
        for stage in range(2):
            copy = remote(
                norm_ref, norm_all.at[shard], norm_send.at[core * 2 + stage], norm_recv.at[shard],
                core, ctx, 2 * section + stage,
            )
            stays = (section == core) & (shard == 2 * section + stage)
            norm_copies.append((copy, stays))

            @pl.when(stays)
            def _():
                norm_local.start()

            @pl.when(jnp.logical_not(stays))
            def _():
                copy.start()

    ff_copy.start()

    @pl.when(jnp.logical_not(g_stays))
    def _():
        g_copy.start()

    def piece(cols, c, s, which, core, to_ctx):
        ref = w.at[c, s, :, cols]
        return remote(ref, ref, send.at[which], recv.at[c, s], core, to_ctx, shard)

    def collect(cols):
        mine = [2 * (1 - section) + j for j in range(2)]
        started = []

        def go(c, s, core, to_ctx):
            copy = piece(cols, c, s, len(started), core, to_ctx)
            copy.start()
            started.append(copy)

        def arrived(c, s):
            piece(cols, c, s, 0, section, ctx).wait_recv()

        for s in mine:
            arrived(ctx, s)
            go(ctx, s, section, x_ctx)
            go(ctx, s, section, y_ctx)
            go(ctx, s, 1 - section, ctx)
        arrived(x_ctx, mine[0])
        go(x_ctx, mine[0], section, y_ctx)
        go(x_ctx, mine[0], 1 - section, ctx)
        arrived(y_ctx, mine[0])
        go(y_ctx, mine[0], 1 - section, ctx)
        arrived(y_ctx, mine[1])
        go(y_ctx, mine[1], section, x_ctx)
        go(y_ctx, mine[1], 1 - section, ctx)
        arrived(x_ctx, mine[1])
        go(x_ctx, mine[1], 1 - section, ctx)
        for s in mine:
            arrived(d_ctx, s)
            go(d_ctx, s, 1 - section, ctx)
        for c in (ctx, x_ctx, y_ctx, d_ctx):
            for j in range(2):
                arrived(c, 2 * section + j)
        for s in range(4):
            pltpu.make_async_copy(norm_ref, norm_all.at[s], norm_recv.at[s]).wait()
        norms[...] = (norm_all[0] + norm_all[1]) + (norm_all[2] + norm_all[3])
        return started

    def hop_copy(u):
        rows = pl.ds(u * size, size)
        return remote(lea.at[rows], ent.at[rows], hop_send.at[u], hop_recv.at[u], section, ctx, shard + 1)

    def hop_wait(u):
        rows = pl.ds(u * size, size)
        remote(lea.at[rows], ent.at[rows], hop_send.at[u], hop_recv.at[u], section, ctx, shard).wait_recv()

    def weight(c, columns):
        value = w[c, :, :, pl.ds(0, columns)]
        return value.reshape(value.shape[0] * value.shape[1], columns)

    def saves(u, pairs):
        rows = pl.ds(u * size, size)
        copies = []
        for index, (src, dst) in enumerate(pairs):
            if len(src.shape) == 3:
                copies.append(pltpu.make_async_copy(src.at[:, rows], dst.at[:, rows], save.at[index, u]))
            else:
                copies.append(pltpu.make_async_copy(src.at[rows], dst.at[rows], save.at[index, u]))
        return copies

    norm_save = pltpu.make_async_copy(norms, norm_out, keep.at[1])

    @pl.when(kind == 0)
    def _():
        started = collect(attn_cols)
        norm_save.start()
        w_save = pltpu.make_async_copy(w.at[:, :, :, attn_cols], w_attn_out, keep.at[0])
        w_save.start()

        @pl.when(shard == 0)
        def _():
            for c in range(4):
                pltpu.make_async_copy(x_ref, x_all.at[c], token_recv.at[c]).wait()

        lse[...] = jnp.zeros_like(lse)
        gain, bias = norms[0:1, :width], norms[2:3, :width]
        pairs = ((ent, ent_out), (nrm, nrm_out), (q, q_out), (k, k_out), (k1, k1_out), (v, v_out), (v1, v1_out), (o, o_out), (lse, lse_out))
        for u in range(chunks):
            rows = pl.ds(u * size, size)

            @pl.when(shard == 0)
            def _():
                first = 2 * (u % 2)
                ent[rows] = x_all[first : first + 2, u // 2].reshape(size, width)

            @pl.when(shard > 0)
            def _():
                hop_wait(u)

            hat, _ = normalised(ent[rows].astype(f32))
            normed = (hat * gain + bias).astype(bf16)
            nrm[rows] = normed
            k[rows] = mm(normed, weight(1, wide)).astype(bf16)
            v[rows] = mm(normed, weight(2, wide)).astype(bf16)
            swaps = [
                remote(src.at[rows], dst.at[rows], swap_send.at[which, u], swap_recv.at[which, u], 1 - section, ctx, shard)
                for which, (src, dst) in enumerate(((k, k1), (v, v1)))
            ]
            for copy in swaps:
                copy.start()
            q[rows] = (mm(normed, weight(0, wide)) * score_scale).astype(bf16)
            for copy in swaps:
                copy.wait_recv()
            attend_chunk(u, rows, mask_ref, q, k, k1, v, v1, o, lse)
            out = mm(o[rows, :width].astype(bf16), weight(3, wide))[:, :width]
            lea[rows] = (ent[rows].astype(f32) + out).astype(bf16)
            hop_copy(u).start()
            for copy in saves(u, pairs):
                copy.start()
        for u in range(chunks):
            rows = pl.ds(u * size, size)
            for which, (src, dst) in enumerate(((k, k1), (v, v1))):
                remote(
                    src.at[rows], dst.at[rows], swap_send.at[which, u], swap_recv.at[which, u], 1 - section, ctx, shard
                ).wait_send()
            hop_copy(u).wait_send()
            for copy in saves(u, pairs):
                copy.wait()
        w_save.wait()
        norm_save.wait()
        for copy in started:
            copy.wait_send()

    @pl.when(kind == 1)
    def _():
        started = collect(ff_cols)
        norm_save.start()
        w_save = pltpu.make_async_copy(w, w_ff_out, keep.at[0])
        w_save.start()
        gain, bias = norms[1:2, :width], norms[3:4, :width]
        pairs = ((ent, ent_out), (nrm, nrm_out), (lea, lea_out), (up, up_out), (hid, hid_out))
        for u in range(chunks):
            rows = pl.ds(u * size, size)
            hop_wait(u)
            hat, _ = normalised(ent[rows].astype(f32))
            normed = (hat * gain + bias).astype(bf16)
            nrm[rows] = normed
            total = ent[rows].astype(f32)
            for i in range(2):
                upper = mm(normed, weight(i, ff_ref.shape[1]))
                up[i, rows] = upper
                hidden = jax.nn.gelu(upper, approximate=True).astype(bf16)
                hid[i, rows] = hidden
                total = total + mm_t(hidden, weight(2 + i, ff_ref.shape[1]))
            lea[rows] = total.astype(bf16)

            @pl.when(shard < 3)
            def _():
                hop_copy(u).start()

            for copy in saves(u, pairs):
                copy.start()
        for u in range(chunks):

            @pl.when(shard < 3)
            def _():
                hop_copy(u).wait_send()

            for copy in saves(u, pairs):
                copy.wait()
        w_save.wait()
        norm_save.wait()
        for copy in started:
            copy.wait_send()

    for c in range(4):

        @pl.when((shard == 3) & jnp.logical_not((ctx == 3) & (c == 3)))
        def _():
            remote(g_ref, g_all_ref.at[c], token_send.at[1], token_recv.at[c], section, ctx, shard).wait_recv()

    @pl.when(jnp.logical_not(x_stays))
    def _():
        x_copy.wait_send()

    @pl.when(jnp.logical_not(g_stays))
    def _():
        g_copy.wait_send()

    attn_copy.wait_send()
    ff_copy.wait_send()
    for copy, stays in norm_copies:

        @pl.when(jnp.logical_not(stays))
        def _():
            copy.wait_send()


def forward_relay(attn_piece, ff_piece, x_own, g_own, norm_own, mask):
    share, ff_half = ff_piece.shape
    wide = attn_piece.shape[1]
    blocks, half, width = x_own.shape
    tokens = blocks * 4 * half
    chunks = tokens // (2 * half)
    dma = pltpu.SemaphoreType.DMA
    vmem = pl.BlockSpec(memory_space=pltpu.VMEM)
    state = [
        ((tokens, width), bf16), ((tokens, width), bf16),
        ((tokens, wide), bf16), ((tokens, wide), bf16), ((tokens, wide), bf16), ((tokens, wide), bf16), ((tokens, wide), bf16),
        ((tokens, wide), f32), ((tokens, LANES), f32),
        ((2, tokens, ff_half), f32), ((2, tokens, ff_half), bf16), ((tokens, width), bf16),
    ]
    outs = [
        ((4, 4, share, wide), bf16), ((4, 4, share, ff_half), bf16), ((4,) + g_own.shape, bf16), (norm_own.shape, f32),
    ] + state
    return pl.pallas_call(
        forward_kernel,
        in_specs=[ANY] * 5 + [vmem],
        out_specs=[ANY] * len(outs),
        out_shape=[jax.ShapeDtypeStruct(s, t) for s, t in outs],
        scratch_shapes=[
            pltpu.VMEM((4, 4, share, ff_half), bf16),
            pltpu.VMEM((4,) + x_own.shape, bf16),
            pltpu.VMEM((4,) + norm_own.shape, f32),
            pltpu.VMEM(norm_own.shape, f32),
        ]
        + [pltpu.VMEM(s, t) for s, t in state]
        + [
            dma((14,)), dma((4, 4)), dma((2,)), dma((4,)), dma((4,)), dma((4,)), dma((2,)),
            dma((chunks,)), dma((chunks,)), dma((2, chunks)), dma((2, chunks)), dma((9, chunks)), dma((2,)),
        ],
        compiler_params=pltpu.CompilerParams(has_side_effects=True, vmem_limit_bytes=62 * 2**20),
        name="forward_relay",
    )(attn_piece, ff_piece, x_own, g_own, norm_own, mask)


def add_into(total, term):
    total[...] = (total[...].astype(f32) + term[...].astype(f32)).astype(bf16)


def reduce_kernel(*refs):
    attn_terms, ff_terms = refs[0:4], refs[4:8]
    attn_out, ff_out = refs[8:10]
    held, first, second, third = refs[10:14]
    load, first_send, first_recv, second_send, second_recv, third_send, third_recv, last_send, last_recv = refs[14:]
    section, ctx, shard = lax.axis_index("section"), lax.axis_index("ctx"), lax.axis_index("shard")
    kind = lax.rem(shard, 2)
    near = lambda c, step: c + step - 2 * step * lax.rem(c // step, 2)
    x_ctx, y_ctx = near(ctx, 1), near(ctx, 2)
    d_ctx = near(x_ctx, 2)
    count = len(attn_terms)

    def reduce(terms, out_ref, which):
        width = terms[0].shape[-1]
        cols = pl.ds(0, width)
        own = lambda i, c, j: held.at[i, c, j, :, cols]

        def give(i):
            return remote(
                terms[i].at[:, section], first.at[i, :, :, :, cols], first_send.at[i], first_recv.at[i],
                1 - section, ctx, shard,
            )

        def take(i):
            return pltpu.make_async_copy(terms[i].at[:, 1 - section], held.at[i, :, :, :, cols], load.at[i])

        def second_copy(i, j, part):
            to = (x_ctx, y_ctx)[j]
            return remote(
                own(i, (to, d_ctx)[part], j), second.at[i, j, part, :, cols],
                second_send.at[i, j, part], second_recv.at[i, j, part], section, to, shard,
            )

        def third_copy(i, j):
            to = (y_ctx, x_ctx)[j]
            return remote(
                own(i, to, j), third.at[i, j, :, cols], third_send.at[i, j], third_recv.at[i, j], section, to, shard
            )

        def last_copy(i, j):
            return remote(
                own(i, ctx, j), out_ref.at[i], last_send.at[i, j], last_recv.at[which, i],
                shard // 2, ctx, 2 * (1 - section) + j,
            )

        for i in range(count):
            give(i).start()
            take(i).start()
        for step in range(count + 2):
            i = step
            if i < count:
                take(i).wait()
                give(i).wait_recv()

                @pl.loop(0, 4)
                def _(c):
                    for j in range(2):
                        add_into(own(i, c, j), first.at[i, c, j, :, cols])

                for part in (1, 0):
                    for j in range(2):
                        second_copy(i, j, part).start()
            i = step - 1
            if 0 <= i < count:
                for j in range(2):
                    second_copy(i, j, 1).wait_recv()
                    add_into(own(i, (y_ctx, x_ctx)[j], j), second.at[i, j, 1, :, cols])
                    third_copy(i, j).start()
                for j in range(2):
                    second_copy(i, j, 0).wait_recv()
                    add_into(own(i, ctx, j), second.at[i, j, 0, :, cols])
            i = step - 2
            if 0 <= i < count:
                for j in range(2):
                    third_copy(i, j).wait_recv()
                    add_into(own(i, ctx, j), third.at[i, j, :, cols])
                    last_copy(i, j).start()
        for i in range(count):
            give(i).wait_send()
            for j in range(2):
                for part in range(2):
                    second_copy(i, j, part).wait_send()
                third_copy(i, j).wait_send()
                last_copy(i, j).wait_send()

    @pl.when(kind == 0)
    def _():
        reduce(attn_terms, attn_out, 0)

    @pl.when(kind == 1)
    def _():
        reduce(ff_terms, ff_out, 1)

    for i in range(count):
        for which, out_ref in enumerate((attn_out, ff_out)):
            remote(
                out_ref.at[i], out_ref.at[i], last_send.at[i, 0], last_recv.at[which, i], section, ctx, shard
            ).wait_recv()


def reduce_all(attn_terms, ff_terms):
    rows = attn_terms[0].shape[0] // 16
    count = len(attn_terms)
    split = lambda v: v.reshape(4, 2, 2, rows, v.shape[1])
    width = ff_terms[0].shape[1]
    dma = pltpu.SemaphoreType.DMA
    return pl.pallas_call(
        reduce_kernel,
        in_specs=[ANY] * (2 * count),
        out_specs=[ANY] * 2,
        out_shape=[
            jax.ShapeDtypeStruct((count, rows, attn_terms[0].shape[1]), bf16),
            jax.ShapeDtypeStruct((count, rows, width), bf16),
        ],
        scratch_shapes=[
            pltpu.VMEM((count, 4, 2, rows, width), bf16),
            pltpu.VMEM((count, 4, 2, rows, width), bf16),
            pltpu.VMEM((count, 2, 2, rows, width), bf16),
            pltpu.VMEM((count, 2, rows, width), bf16),
            dma((count,)), dma((count,)), dma((count,)),
            dma((count, 2, 2)), dma((count, 2, 2)),
            dma((count, 2)), dma((count, 2)),
            dma((count, 2)), dma((2, count)),
        ],
        compiler_params=pltpu.CompilerParams(has_side_effects=True, vmem_limit_bytes=48 * 2**20),
        name="reduce_all",
    )(*[split(v) for v in attn_terms], *[split(v) for v in ff_terms])


def chain(inputs, cotangent, qkv_weight, out_weight, up_weight, down_weight, norm_gain, norm_bias):
    section, ctx, shard = lax.axis_index("section"), lax.axis_index("ctx"), lax.axis_index("shard")
    seq_count, blocks, slice_len, width = inputs.shape
    half = slice_len // 2
    tokens = blocks * 4 * half
    share = width // 4
    group = share // 4
    group_pad = up_to(group, ROWS)
    wide = up_to(width, LANES)
    ff = up_weight.shape[2]
    is_attn = shard % 2 == 0

    pad = lambda w: jnp.pad(w, ((0, 0), (0, wide - width)))
    own_qkv, own_out = qkv_weight[0], out_weight[0]
    attn_src = jnp.stack([pad(own_qkv[:, i * width : (i + 1) * width]) for i in range(3)] + [pad(own_out)])
    down_t = down_weight[0].T
    up0 = up_weight[0]
    ff_src = jnp.stack([up0[:, : ff // 2], up0[:, ff // 2 :], down_t[:, : ff // 2], down_t[:, ff // 2 :]])
    norm_own = jnp.concatenate([norm_gain[0], norm_bias[0]], axis=0).astype(f32)
    norm_own = lax.dynamic_update_slice(
        jnp.zeros((ROWS, wide), f32), jnp.pad(norm_own, ((0, ROWS - 4), (0, 0))), (0, shard * share)
    )
    x_own = lax.dynamic_slice_in_dim(inputs[0], section * half, half, 1)
    g_own = lax.dynamic_slice_in_dim(cotangent[0], section * half, half, 1)
    mask = attention_masks(section, half)
    w_attn, w_ff, g_all, norms, ent, nrm, q, k, k1, v, v1, o, lse, up, hid, y = forward_relay(
        lax.dynamic_index_in_dim(attn_src, ctx, 0, keepdims=False),
        lax.dynamic_index_in_dim(ff_src, ctx, 0, keepdims=False),
        x_own, g_own, norm_own, jnp.concatenate([mask, mask], axis=1),
    )
    w_attn = w_attn.reshape(4, width, wide)
    w_ff = w_ff.reshape(4, width, ff // 2)
    own_place = jnp.arange(4)[:, None, None]
    gain1, gain2 = norms[0, :width], norms[1, :width]

    def bring_tokens(every, own):
        mine = jnp.where((own_place[..., None] == ctx) & (shard == ctx), own, every)
        return jnp.swapaxes(mine, 0, 1).reshape(tokens, width)

    g_last = bring_tokens(g_all, g_own)
    feature = lax.broadcasted_iota(jnp.int32, (width, 16 * group_pad), 0)
    place = lax.broadcasted_iota(jnp.int32, (width, 16 * group_pad), 1)
    spread = (feature // group * group_pad + feature % group == place).astype(bf16)
    grouped = lambda v: mm(v, spread).astype(bf16)

    def ff_backward(g, state):
        hat, scale, normed, upper, hidden = state
        d_upper = []
        for i in range(2):
            d_hidden = mm(g, w_ff[2 + i])
            _, back = jax.vjp(lambda u: jax.nn.gelu(u, approximate=True), upper[i])
            d_upper.append(back(d_hidden)[0].astype(bf16))
        d_normed = mm_t(d_upper[0], w_ff[0]) + mm_t(d_upper[1], w_ff[1])
        d_middle = g.astype(f32) + norm_backward(hat, scale, gain2, d_normed)
        return d_middle.astype(bf16), d_upper, d_normed

    def attn_backward(d_middle, state):
        hat, scale, normed, q, k, k1, v, v1, o, ob, lse = state
        d_att = mm_t(jnp.pad(d_middle, ((0, 0), (0, wide - width))), w_attn[3]).astype(bf16)
        d_att = jnp.pad(d_att, ((0, 0), (0, wide - width)))
        dq, dk, dk_other, dv, dv_other = attention_backward(mask, q, k, k1, v, v1, d_att, o, lse, half)
        dk = (dk + swap_cores(dk_other).astype(f32)).astype(bf16)
        dv = (dv + swap_cores(dv_other).astype(f32)).astype(bf16)
        d_mixed = (dq, dk, dv)
        d_normed = mm_t(dq, w_attn[0]) + mm_t(dk, w_attn[1]) + mm_t(dv, w_attn[2])
        dx = d_middle.astype(f32) + norm_backward(hat, scale, gain1, d_normed)
        return dx.astype(bf16), d_mixed, d_normed

    hat, scale = normalised(ent.astype(f32))
    attn_state = (hat, scale, nrm, q, k, k1, v, v1, o, o.astype(bf16), lse)
    ff_state = (hat, scale, nrm, (up[0], up[1]), (hid[0], hid[1]))

    d_middle, _, _ = ff_backward(g_last, ff_state)
    d_middle1 = hop(d_middle, 3, 2)
    dx, _, _ = attn_backward(d_middle1, attn_state)
    g = jnp.where(shard == 3, g_last, hop(dx, 2, 1))
    d_middle, d_upper, d_normed2 = ff_backward(g, ff_state)
    hat2, _, normed2, _, hidden = ff_state
    g_grouped, n2_grouped = grouped(g), grouped(normed2)
    ff_grads = [t_mm(n2_grouped, d_upper[0]), t_mm(n2_grouped, d_upper[1]), t_mm(g_grouped, hidden[0]), t_mm(g_grouped, hidden[1])]
    d_middle = jnp.where(shard == 2, d_middle1, hop(d_middle, 1, 0))
    dx, d_mixed, d_normed1 = attn_backward(d_middle, attn_state)
    hat1, _, normed, _, _, _, _, _, _, ob, _ = attn_state
    n1_grouped, att_grouped = grouped(normed), grouped(ob[:, :width])
    attn_grads = [t_mm(n1_grouped, d) for d in d_mixed] + [t_mm(att_grouped, jnp.pad(d_middle, ((0, 0), (0, wide - width))))]
    attn_sums, ff_sums = reduce_all([v.astype(bf16) for v in attn_grads], [v.astype(bf16) for v in ff_grads])

    own_hat = jnp.where(is_attn, hat1, hat2)
    own_grad = jnp.where(is_attn, d_normed1, d_normed2)
    terms = jnp.stack([jnp.sum(own_grad * own_hat, axis=0), jnp.sum(own_grad, axis=0)])
    terms = jnp.where(jnp.arange(4)[:, None, None] == shard, terms[None], 0.0)
    totals = lax.psum(terms, ("section", "ctx", "shard")).reshape(2, 2, 2, width)
    totals = lax.dynamic_index_in_dim(totals, section, 0, keepdims=False)
    totals = lax.dynamic_slice_in_dim(totals, (ctx * 4 + shard) * group, group, 2)

    final = jnp.where(is_attn, dx, y).reshape(blocks, 4, half, width)
    final = lax.all_to_all(jnp.swapaxes(final, 0, 1), "ctx", 0, 0)
    final = lax.all_to_all(final, "shard", 0, 0).reshape(2, 2, blocks, half, width)
    final = lax.all_to_all(final, "section", 0, 0)
    final = jnp.moveaxis(final, 0, 2).reshape(2, blocks, slice_len, width)

    attn_sums = attn_sums[:, :group, :width].astype(f32)
    ff_sums = ff_sums[:, :group].astype(f32)
    return (
        final[1][None, None],
        final[0][None, None],
        jnp.concatenate([attn_sums[0], attn_sums[1], attn_sums[2]], axis=1)[None],
        attn_sums[3][None],
        jnp.concatenate([ff_sums[0], ff_sums[1]], axis=1)[None],
        jnp.concatenate([ff_sums[2].T, ff_sums[3].T], axis=0)[None],
        totals[:, 0][None],
        totals[:, 1][None],
    )


def passed_along(value, axis, steps):
    count = lax.axis_size(axis)
    initial, last = (max(0, -steps), min(count, count - steps))
    return lax.ppermute(value, axis, [(source, source + steps) for source in range(initial, last)])


def layer_norm(values, gain, shift):
    mean = jnp.mean(values, axis=-1, keepdims=True)
    centred = values - mean
    var = jnp.mean(centred * centred, axis=-1, keepdims=True)
    return centred * lax.rsqrt(var + eps_norm) * gain + shift


def gelu_tanh(values):
    return jax.nn.gelu(values, approximate=True)


def split_pair(key_value, head_count):
    block_len, seq_count, double = key_value.shape
    model_width = double // 2
    key_rows = key_value[..., :model_width].reshape(block_len, seq_count, head_count, HEAD)
    value_rows = key_value[..., model_width:].reshape(block_len, seq_count, head_count, HEAD)
    return (key_rows, value_rows)


def causal_mask(query_pos, key_pos):
    return (key_pos[None, :] <= query_pos[:, None])[None, :, None, :]


def forward_block(running, queries, query_pos, key_value, key_pos):
    row_max, row_sum, accum = running
    key_rows, value_rows = split_pair(key_value, queries.shape[2])
    scores = (
        jnp.einsum("sqhe,kshe->sqhk", queries, key_rows, preferred_element_type=jnp.float32)
        * score_scale
    )
    causal = causal_mask(query_pos, key_pos)
    new_max = jnp.maximum(row_max, jnp.max(jnp.where(causal, scores, -1e30), axis=-1))
    softmax_w = jnp.where(causal, jnp.exp(scores - new_max[..., None]), 0.0)
    factor = jnp.exp(row_max - new_max)
    row_sum = row_sum * factor + jnp.sum(softmax_w, axis=-1)
    accum = accum * factor[..., None] + jnp.einsum(
        "sqhk,kshe->sqhe",
        softmax_w.astype(jnp.bfloat16),
        value_rows,
        preferred_element_type=jnp.float32,
    )
    return (new_max, row_sum, accum)


def split_rows(whole):
    key_count = whole.shape[0]
    block_size = 512
    blocks = whole.reshape((key_count // block_size, block_size) + whole.shape[1:])
    offsets = jnp.arange(key_count // block_size, dtype=jnp.int32) * block_size
    return (blocks, offsets, block_size)


def fold_keys(running, piece, start, queries, query_pos, group_len):
    blocks, offsets, block_size = split_rows(piece)

    def fold_scan_step(inner, scan_item):
        block_rows, offset = scan_item
        for group_id in range(block_rows.shape[2]):
            key_pos = (
                group_id * group_len + start + offset + jnp.arange(block_size, dtype=jnp.int32)
            )
            inner = forward_block(inner, queries, query_pos, block_rows[:, :, group_id], key_pos)
        return (inner, None)

    result, _ = lax.scan(fold_scan_step, running, (blocks, offsets))
    return result


def pair_terms(d_scores, softmax_w, queries, d_attended, block_size):
    d_keys = (
        jnp.einsum("sqhk,sqhe->kshe", d_scores, queries, preferred_element_type=jnp.float32)
        * score_scale
    )
    d_values = jnp.einsum(
        "sqhk,sqhe->kshe",
        softmax_w.astype(jnp.bfloat16),
        d_attended,
        preferred_element_type=jnp.float32,
    )
    shape = (block_size, queries.shape[0], queries.shape[2] * queries.shape[3])
    return jnp.concatenate([d_keys.reshape(shape), d_values.reshape(shape)], axis=-1)


def score_grads(
    queries, query_pos, log_total, row_delta, d_attended, key_rows, value_rows, key_pos
):
    scores = (
        jnp.einsum("sqhe,kshe->sqhk", queries, key_rows, preferred_element_type=jnp.float32)
        * score_scale
    )
    causal = causal_mask(query_pos, key_pos)
    softmax_w = jnp.where(causal, jnp.exp(scores - log_total[..., None]), 0.0)
    d_probs = jnp.einsum(
        "sqhe,kshe->sqhk", d_attended, value_rows, preferred_element_type=jnp.float32
    )
    d_scores = (softmax_w * (d_probs - row_delta[..., None])).astype(jnp.bfloat16)
    return (softmax_w, d_scores)


def backward_keys(whole, queries, query_pos, log_total, row_delta, d_attended, group_len):
    blocks, offsets, block_size = split_rows(whole)

    def backward_scan_step(d_queries, scan_item):
        block_rows, offset = scan_item
        for group_id in range(block_rows.shape[2]):
            key_pos = group_id * group_len + offset + jnp.arange(block_size, dtype=jnp.int32)
            key_rows, value_rows = split_pair(block_rows[:, :, group_id], queries.shape[2])
            softmax_w, d_scores = score_grads(
                queries, query_pos, log_total, row_delta, d_attended, key_rows, value_rows, key_pos
            )
            d_queries = (
                d_queries
                + jnp.einsum(
                    "sqhk,kshe->sqhe", d_scores, key_rows, preferred_element_type=jnp.float32
                )
                * score_scale
            )
        return (d_queries, None)

    d_queries, terms = lax.scan(
        backward_scan_step, jnp.zeros(queries.shape, jnp.float32), (blocks, offsets)
    )
    return (d_queries, None)


def owner_terms(
    own_cache, all_queries, all_d_att, all_totals, all_deltas, micro_index, ctx_id, group_len
):
    block_len, seq_count, group_count, double = own_cache.shape
    head_count = all_queries.shape[2]
    query_rows = all_queries.shape[1]
    query_size = 512
    block_count = query_rows // query_size

    def loop_step(index, total):
        offset = index * query_size
        q_block = lax.dynamic_slice_in_dim(all_queries, offset, query_size, 1)
        d_block = lax.dynamic_slice_in_dim(all_d_att, offset, query_size, 1)
        t_block = lax.dynamic_slice_in_dim(all_totals, offset, query_size, 1)
        r_block = lax.dynamic_slice_in_dim(all_deltas, offset, query_size, 1)
        query_pos = micro_index * group_len + offset + jnp.arange(query_size, dtype=jnp.int32)
        pieces = []
        for group_id in range(group_count):
            key_pos = (
                group_id * group_len + ctx_id * block_len + jnp.arange(block_len, dtype=jnp.int32)
            )
            key_rows, value_rows = split_pair(own_cache[:, :, group_id], head_count)
            softmax_w, d_scores = score_grads(
                q_block, query_pos, t_block, r_block, d_block, key_rows, value_rows, key_pos
            )
            pieces.append(pair_terms(d_scores, softmax_w, q_block, d_block, block_len))
        return total + jnp.stack(pieces, axis=2)

    return lax.fori_loop(0, block_count, loop_step, jnp.zeros(own_cache.shape, jnp.float32))


def store_at(store, value, micro_index, active):
    updated = lax.dynamic_update_index_in_dim(store, value, micro_index, 0)
    return jnp.where(active, updated, store)


def shards(inputs, cotangent, qkv_weight, out_weight, up_weight, down_weight, norm_gain, norm_bias):
    section_id = lax.axis_index("section")
    ctx_count = lax.axis_size("ctx")
    ctx_id = lax.axis_index("ctx")
    seq_count, group_count, block_len, model_width = inputs.shape
    head_count = model_width // HEAD
    group_len = block_len * ctx_count
    row_count = seq_count * block_len
    w_qkv, w_out, w_up, w_down, gains, biases = (
        lax.all_gather(qkv_weight[0], "shard", axis=0, tiled=True),
        lax.all_gather(out_weight[0], "shard", axis=0, tiled=True),
        lax.all_gather(up_weight[0], "shard", axis=0, tiled=True),
        lax.all_gather(down_weight[0], "shard", axis=1, tiled=True),
        lax.all_gather(norm_gain[0], "shard", axis=1, tiled=True),
        lax.all_gather(norm_bias[0], "shard", axis=1, tiled=True),
    )
    gains = gains.astype(jnp.float32)
    biases = biases.astype(jnp.float32)
    ff_width = w_up.shape[1]
    cache = jnp.zeros((block_len, seq_count, group_count, 2 * model_width), jnp.bfloat16)
    in_store = jnp.zeros((group_count, seq_count, block_len, model_width), jnp.bfloat16)
    query_store = jnp.zeros((group_count, seq_count, block_len, head_count, HEAD), jnp.bfloat16)
    att_store = jnp.zeros((group_count, seq_count, block_len, head_count, HEAD), jnp.float32)
    total_store = jnp.zeros((group_count, seq_count, block_len, head_count), jnp.float32)
    middle_store = jnp.zeros((group_count, row_count, model_width), jnp.float32)
    upper_store = jnp.zeros((group_count, row_count, ff_width), jnp.float32)
    out_store = jnp.zeros((group_count, seq_count, block_len, model_width), jnp.bfloat16)
    received = jnp.zeros((seq_count, block_len, model_width), jnp.bfloat16)
    for tick_no in range(group_count + 1):
        micro = tick_no - section_id
        active = (micro >= 0) & (micro < group_count)
        micro_index = jnp.clip(micro, 0, group_count - 1)
        own_input = lax.dynamic_index_in_dim(inputs, micro_index, 1, keepdims=False)
        entering = jnp.where(section_id == 0, own_input, received)
        flat_rows = entering.reshape(row_count, model_width).astype(jnp.float32)
        normed = layer_norm(flat_rows, gains[0], biases[0]).astype(jnp.bfloat16)
        mixed = jnp.dot(normed, w_qkv, preferred_element_type=jnp.float32).astype(jnp.bfloat16)
        queries = mixed[:, :model_width].reshape(seq_count, block_len, head_count, HEAD)
        fresh = jnp.swapaxes(
            mixed[:, model_width:].reshape(seq_count, block_len, 2 * model_width), 0, 1
        )
        updated = lax.dynamic_update_index_in_dim(cache, fresh, micro_index, 2)
        cache = jnp.where(active, updated, cache)
        query_pos = (
            micro_index * group_len + ctx_id * block_len + jnp.arange(block_len, dtype=jnp.int32)
        )
        start_state = (
            jnp.full((seq_count, block_len, head_count), -1e30, jnp.float32),
            jnp.zeros((seq_count, block_len, head_count), jnp.float32),
            jnp.zeros((seq_count, block_len, head_count, HEAD), jnp.float32),
        )
        row_max, row_sum, accum = fold_keys(
            start_state,
            lax.all_gather(cache, "ctx", axis=0, tiled=True),
            jnp.int32(0),
            queries,
            query_pos,
            group_len,
        )
        attended = accum / row_sum[..., None]
        log_total = row_max + jnp.log(row_sum)
        att_low = attended.reshape(row_count, model_width).astype(jnp.bfloat16)
        middle = flat_rows + jnp.dot(att_low, w_out, preferred_element_type=jnp.float32)
        normed2 = layer_norm(middle, gains[1], biases[1]).astype(jnp.bfloat16)
        upper = jnp.dot(normed2, w_up, preferred_element_type=jnp.float32)
        hidden = gelu_tanh(upper).astype(jnp.bfloat16)
        leaving = (middle + jnp.dot(hidden, w_down, preferred_element_type=jnp.float32)).astype(
            jnp.bfloat16
        )
        leaving = leaving.reshape(seq_count, block_len, model_width)
        in_store = store_at(in_store, entering, micro_index, active)
        query_store = store_at(query_store, queries, micro_index, active)
        att_store = store_at(att_store, attended, micro_index, active)
        total_store = store_at(total_store, log_total, micro_index, active)
        middle_store = store_at(middle_store, middle, micro_index, active)
        upper_store = store_at(upper_store, upper, micro_index, active)
        out_store = store_at(out_store, leaving, micro_index, active)
        if tick_no < group_count:
            received = passed_along(leaving, "section", 1)
    key_acc = jnp.zeros((block_len, seq_count, group_count, 2 * model_width), jnp.float32)
    grad_qkv = jnp.zeros((model_width, 3 * model_width), jnp.float32)
    grad_out = jnp.zeros((model_width, model_width), jnp.float32)
    grad_up = jnp.zeros((model_width, ff_width), jnp.float32)
    grad_down = jnp.zeros((ff_width, model_width), jnp.float32)
    grad_gain = jnp.zeros((2, model_width), jnp.float32)
    grad_bias = jnp.zeros((2, model_width), jnp.float32)
    grad_store = jnp.zeros((group_count, seq_count, block_len, model_width), jnp.bfloat16)
    coming = jnp.zeros((seq_count, block_len, model_width), jnp.bfloat16)
    for tick_no in range(group_count + 1):
        micro = group_count - tick_no - section_id
        active = (micro >= 0) & (micro < group_count)
        active_weight = active.astype(jnp.float32)
        micro_index = jnp.clip(micro, 0, group_count - 1)
        own_cot = lax.dynamic_index_in_dim(cotangent, micro_index, 1, keepdims=False)
        d_out = (
            jnp.where(section_id == 1, own_cot, coming)
            .reshape(row_count, model_width)
            .astype(jnp.float32)
        )
        flat_rows = in_store[micro_index].reshape(row_count, model_width).astype(jnp.float32)
        queries = query_store[micro_index]
        attended = att_store[micro_index]
        log_total = total_store[micro_index]
        middle = middle_store[micro_index]
        upper = upper_store[micro_index]
        normed2_full, norm2_back = jax.vjp(
            lambda v, g, b: layer_norm(v, g, b), middle, gains[1], biases[1]
        )
        normed2 = normed2_full.astype(jnp.bfloat16)
        hidden_full, gelu_back = jax.vjp(gelu_tanh, upper)
        hidden = hidden_full.astype(jnp.bfloat16)
        d_branch = d_out.astype(jnp.bfloat16)
        grad_down = grad_down + active_weight * jnp.dot(
            hidden.T, d_branch, preferred_element_type=jnp.float32
        )
        d_hidden = jnp.dot(d_branch, w_down.T, preferred_element_type=jnp.float32)
        d_upper = gelu_back(d_hidden)[0].astype(jnp.bfloat16)
        grad_up = grad_up + active_weight * jnp.dot(
            normed2.T, d_upper, preferred_element_type=jnp.float32
        )
        d_normed2 = jnp.dot(d_upper, w_up.T, preferred_element_type=jnp.float32)
        d_mid_norm, d_gain2, d_bias2 = norm2_back(d_normed2)
        d_middle = d_out + d_mid_norm
        att_low = attended.reshape(row_count, model_width).astype(jnp.bfloat16)
        d_att = d_middle.astype(jnp.bfloat16)
        grad_out = grad_out + active_weight * jnp.dot(
            att_low.T, d_att, preferred_element_type=jnp.float32
        )
        d_attended = jnp.dot(d_att, w_out.T, preferred_element_type=jnp.float32).astype(
            jnp.bfloat16
        )
        d_attended = d_attended.reshape(seq_count, block_len, head_count, HEAD)
        row_delta = jnp.sum(d_attended.astype(jnp.float32) * attended, axis=-1)
        query_pos = (
            micro_index * group_len + ctx_id * block_len + jnp.arange(block_len, dtype=jnp.int32)
        )
        whole = lax.all_gather(cache, "ctx", axis=0, tiled=True)
        d_queries, unused = backward_keys(
            whole, queries, query_pos, log_total, row_delta, d_attended, group_len
        )
        all_queries, all_d_att = (
            lax.all_gather(queries, "ctx", axis=1, tiled=True),
            lax.all_gather(d_attended, "ctx", axis=1, tiled=True),
        )
        all_totals, all_deltas = (
            lax.all_gather(log_total, "ctx", axis=1, tiled=True),
            lax.all_gather(row_delta, "ctx", axis=1, tiled=True),
        )
        shares = owner_terms(
            cache, all_queries, all_d_att, all_totals, all_deltas, micro_index, ctx_id, group_len
        )
        key_acc = key_acc + active_weight * shares
        d_pair = jnp.swapaxes(
            lax.dynamic_index_in_dim(key_acc, micro_index, 2, keepdims=False), 0, 1
        )
        d_mixed = jnp.concatenate(
            [d_queries.reshape(row_count, model_width), d_pair.reshape(row_count, 2 * model_width)],
            axis=-1,
        ).astype(jnp.bfloat16)
        normed_full, norm1_back = jax.vjp(
            lambda v, g, b: layer_norm(v, g, b), flat_rows, gains[0], biases[0]
        )
        normed = normed_full.astype(jnp.bfloat16)
        grad_qkv = grad_qkv + active_weight * jnp.dot(
            normed.T, d_mixed, preferred_element_type=jnp.float32
        )
        d_normed = jnp.dot(d_mixed, w_qkv.T, preferred_element_type=jnp.float32)
        d_flat_norm, d_gain1, d_bias1 = norm1_back(d_normed)
        grad_gain = grad_gain + active_weight * jnp.stack([d_gain1, d_gain2])
        grad_bias = grad_bias + active_weight * jnp.stack([d_bias1, d_bias2])
        d_entering = (
            (d_middle + d_flat_norm).astype(jnp.bfloat16).reshape(seq_count, block_len, model_width)
        )
        grad_store = store_at(grad_store, d_entering, micro_index, active)
        if tick_no < group_count:
            coming = passed_along(d_entering, "section", -1)
    sums = (
        lax.psum_scatter(grad_qkv, ("ctx", "shard"), scatter_dimension=0, tiled=True),
        lax.psum_scatter(grad_out, ("ctx", "shard"), scatter_dimension=0, tiled=True),
        lax.psum_scatter(grad_up, ("ctx", "shard"), scatter_dimension=0, tiled=True),
        lax.psum_scatter(grad_down, ("ctx", "shard"), scatter_dimension=1, tiled=True),
        lax.psum_scatter(grad_gain, ("ctx", "shard"), scatter_dimension=1, tiled=True),
        lax.psum_scatter(grad_bias, ("ctx", "shard"), scatter_dimension=1, tiled=True),
    )
    layer_outputs = jnp.swapaxes(out_store, 0, 1)[None]
    input_grads = jnp.swapaxes(grad_store, 0, 1)[None]
    return (
        layer_outputs,
        input_grads,
        sums[0][None],
        sums[1][None],
        sums[2][None],
        sums[3][None],
        sums[4][None],
        sums[5][None],
    )


def solution(mesh):
    in_specs = (
        P("shard", None, "ctx", None),
        P("shard", None, "ctx", None),
        P("section", "shard", None),
        P("section", "shard", None),
        P("section", "shard", None),
        P("section", None, "shard"),
        P("section", None, "shard"),
        P("section", None, "shard"),
    )
    out_specs = (
        P("section", "shard", None, "ctx", None),
        P("section", "shard", None, "ctx", None),
        P("section", ("ctx", "shard"), None),
        P("section", ("ctx", "shard"), None),
        P("section", ("ctx", "shard"), None),
        P("section", None, ("ctx", "shard")),
        P("section", None, ("ctx", "shard")),
        P("section", None, ("ctx", "shard")),
    )
    relay = mesh.shape["section"] == 2 and mesh.shape["shard"] == 4 and mesh.shape["ctx"] == 4
    return jax.shard_map(chain if relay else shards, mesh=mesh, in_specs=in_specs, out_specs=out_specs, check_vma=False)
```

```python
import functools

import jax
import jax.numpy as jnp
from jax import lax
from jax.experimental import pallas as pl
from jax.experimental.pallas import tpu as pltpu
from jax.sharding import PartitionSpec as P

HEAD = 64
LANES = 128
ROWS = 8
NEG = -1e30

eps_norm = 1e-05
score_scale = 0.125
f32 = jnp.float32
bf16 = jnp.bfloat16


def up_to(width, step):
    return -(-width // step) * step


def dot(a, b, dims):
    return lax.dot_general(a, b, (dims, ((), ())), preferred_element_type=f32)


def mm(a, b):
    return dot(a, b, ((1,), (0,)))


def mm_t(a, b):
    return dot(a, b, ((1,), (1,)))


def t_mm(a, b):
    return dot(a, b, ((0,), (0,)))


def attention_masks(core, half):
    row = lax.broadcasted_iota(jnp.int32, (2 * half, 2 * half), 0)
    col = lax.broadcasted_iota(jnp.int32, (2 * half, 2 * half), 1)
    row_slice, col_slice = row // half, col // half
    own = (col_slice < row_slice) | ((col_slice == row_slice) & (col <= row))
    other = (col_slice < row_slice) | ((col_slice == row_slice) & (core == 1))
    return jnp.where(jnp.stack([own, other]), 0.0, NEG).astype(f32)


def norm_backward(hat, scale, gain, grad):
    scaled = grad * gain
    mean = jnp.mean(scaled, axis=-1, keepdims=True)
    along = jnp.mean(scaled * hat, axis=-1, keepdims=True)
    return scale * (scaled - mean - hat * along)


ANY = pl.BlockSpec(memory_space=pl.ANY)


def remote(src, dst, send, recv, section, ctx, shard):
    return pltpu.make_async_remote_copy(
        src_ref=src,
        dst_ref=dst,
        send_sem=send,
        recv_sem=recv,
        device_id=(section, ctx, shard),
        device_id_type=pl.DeviceIdType.MESH,
    )


def normalised(values):
    mean = jnp.mean(values, axis=-1, keepdims=True)
    centred = values - mean
    var = jnp.mean(centred * centred, axis=-1, keepdims=True)
    scale = lax.rsqrt(var + eps_norm)
    return centred * scale, scale


def stack_heads(value, low):
    zero = jnp.zeros_like(value)
    return jnp.concatenate([jnp.where(low, value, zero), jnp.where(low, zero, value)], axis=0)


def unstack_heads(value, low):
    rows = value.shape[0] // 2
    return jnp.where(low, value[:rows], value[rows:])


def mask_last(scores, mask):
    width = mask.shape[1]
    last = scores[:, scores.shape[1] - width :] + mask
    if scores.shape[1] == width:
        return last
    return jnp.concatenate([scores[:, : scores.shape[1] - width], last], axis=1)


def attend_chunk(u, rows, mask_ref, q, k, k1, v, v1, o, lse):
    size = rows.size
    keys = pl.ds(0, (u + 1) * size)
    lane = lax.broadcasted_iota(jnp.int32, (size, LANES), 1)
    low = lane < HEAD

    @pl.loop(0, q.shape[1] // LANES)
    def _(pair):
        cols = pl.ds(pl.multiple_of(pair * LANES, LANES), LANES)
        q2 = stack_heads(q[rows, cols], low)
        scores = [mask_last(mm_t(q2, ref[keys, cols]), mask_ref[part]) for part, ref in enumerate((k, k1))]
        top = jnp.maximum(
            jnp.max(scores[0], axis=1, keepdims=True), jnp.max(scores[1], axis=1, keepdims=True)
        )
        total, acc = 0.0, 0.0
        for s, ref in zip(scores, (v, v1)):
            p = jnp.exp(s - top)
            total = total + jnp.sum(p, axis=1, keepdims=True)
            acc = acc + mm(p.astype(bf16), ref[keys, cols])
        o[rows, cols] = unstack_heads(acc / total, low)
        level = top + jnp.log(total)
        lse[rows, :] = jnp.where(
            lane == 2 * pair, level[:size], jnp.where(lane == 2 * pair + 1, level[size:], lse[rows, :])
        )


def near_ctx(c, step):
    return c + step - 2 * step * lax.rem(c // step, 2)


def forward_kernel(
    attn_ref, ff_ref, x_ref, g_ref, norm_ref, mask_ref,
    w_attn_out, w_ff_out, g_all_ref, norm_out,
    ent_out, nrm_out, q_out, k_out, k1_out, v_out, v1_out, o_out, lse_out, up_out, hid_out, lea_out,
    w, x_all, norm_all, norms, ent, nrm, q, k, k1, v, v1, o, lse, up, hid, lea,
    send, recv, token_send, token_recv, norm_send, norm_recv, far_send,
    hop_send, hop_recv, swap_send, swap_recv, save, keep,
):
    section, ctx, shard = lax.axis_index("section"), lax.axis_index("ctx"), lax.axis_index("shard")
    kind = lax.rem(shard, 2)
    far_core = 1 - shard // 2
    x_ctx, y_ctx = near_ctx(ctx, 1), near_ctx(ctx, 2)
    d_ctx = near_ctx(x_ctx, 2)
    width = ent.shape[1]
    wide = q.shape[1]
    size = 2 * x_ref.shape[1]
    chunks = ent.shape[0] // size
    attn_cols = pl.ds(0, attn_ref.shape[1])
    ff_cols = pl.ds(0, ff_ref.shape[1])

    x_copy = remote(x_ref, x_all.at[ctx], token_send.at[0], token_recv.at[ctx], section, shard, 0)
    g_copy = remote(g_ref, g_all_ref.at[ctx], token_send.at[1], token_recv.at[ctx], section, shard, 3)
    x_stays = (shard == 0) & (ctx == 0)
    g_stays = (shard == 3) & (ctx == 3)
    attn_copy = remote(
        attn_ref, w.at[ctx, shard, :, attn_cols], far_send.at[0], recv.at[ctx, shard], far_core, ctx, 2 * section
    )
    ff_copy = remote(
        ff_ref, w.at[ctx, shard, :, ff_cols], far_send.at[1], recv.at[ctx, shard], far_core, ctx, 2 * section + 1
    )
    x_local = pltpu.make_async_copy(x_ref, x_all.at[ctx], token_recv.at[ctx])
    norm_local = pltpu.make_async_copy(norm_ref, norm_all.at[shard], norm_recv.at[shard])

    @pl.when(x_stays)
    def _():
        x_local.start()

    @pl.when(jnp.logical_not(x_stays))
    def _():
        x_copy.start()

    attn_copy.start()
    norm_copies = []
    for core in range(2):
        for stage in range(2):
            copy = remote(
                norm_ref, norm_all.at[shard], norm_send.at[core * 2 + stage], norm_recv.at[shard],
                core, ctx, 2 * section + stage,
            )
            stays = (section == core) & (shard == 2 * section + stage)
            norm_copies.append((copy, stays))

            @pl.when(stays)
            def _():
                norm_local.start()

            @pl.when(jnp.logical_not(stays))
            def _():
                copy.start()

    ff_copy.start()

    @pl.when(jnp.logical_not(g_stays))
    def _():
        g_copy.start()

    def piece(cols, c, s, which, core, to_ctx):
        ref = w.at[c, s, :, cols]
        return remote(ref, ref, send.at[which], recv.at[c, s], core, to_ctx, shard)

    def collect(cols):
        mine = [2 * (1 - section) + j for j in range(2)]
        started = []

        def go(c, s, core, to_ctx):
            copy = piece(cols, c, s, len(started), core, to_ctx)
            copy.start()
            started.append(copy)

        def arrived(c, s):
            piece(cols, c, s, 0, section, ctx).wait_recv()

        for s in mine:
            arrived(ctx, s)
            go(ctx, s, section, x_ctx)
            go(ctx, s, section, y_ctx)
            go(ctx, s, 1 - section, ctx)
        arrived(x_ctx, mine[0])
        go(x_ctx, mine[0], section, y_ctx)
        go(x_ctx, mine[0], 1 - section, ctx)
        arrived(y_ctx, mine[0])
        go(y_ctx, mine[0], 1 - section, ctx)
        arrived(y_ctx, mine[1])
        go(y_ctx, mine[1], section, x_ctx)
        go(y_ctx, mine[1], 1 - section, ctx)
        arrived(x_ctx, mine[1])
        go(x_ctx, mine[1], 1 - section, ctx)
        for s in mine:
            arrived(d_ctx, s)
            go(d_ctx, s, 1 - section, ctx)
        for c in (ctx, x_ctx, y_ctx, d_ctx):
            for j in range(2):
                arrived(c, 2 * section + j)
        for s in range(4):
            pltpu.make_async_copy(norm_ref, norm_all.at[s], norm_recv.at[s]).wait()
        norms[...] = (norm_all[0] + norm_all[1]) + (norm_all[2] + norm_all[3])
        return started

    def hop_copy(u):
        rows = pl.ds(u * size, size)
        return remote(lea.at[rows], ent.at[rows], hop_send.at[u], hop_recv.at[u], section, ctx, shard + 1)

    def hop_wait(u):
        rows = pl.ds(u * size, size)
        remote(lea.at[rows], ent.at[rows], hop_send.at[u], hop_recv.at[u], section, ctx, shard).wait_recv()

    def weight(c, columns):
        value = w[c, :, :, pl.ds(0, columns)]
        return value.reshape(value.shape[0] * value.shape[1], columns)

    def saves(u, pairs):
        rows = pl.ds(u * size, size)
        copies = []
        for index, (src, dst) in enumerate(pairs):
            if len(src.shape) == 3:
                copies.append(pltpu.make_async_copy(src.at[:, rows], dst.at[:, rows], save.at[index, u]))
            else:
                copies.append(pltpu.make_async_copy(src.at[rows], dst.at[rows], save.at[index, u]))
        return copies

    norm_save = pltpu.make_async_copy(norms, norm_out, keep.at[1])

    @pl.when(kind == 0)
    def _():
        started = collect(attn_cols)
        norm_save.start()
        w_save = pltpu.make_async_copy(w.at[:, :, :, attn_cols], w_attn_out, keep.at[0])
        w_save.start()

        @pl.when(shard == 0)
        def _():
            for c in range(4):
                pltpu.make_async_copy(x_ref, x_all.at[c], token_recv.at[c]).wait()

        lse[...] = jnp.zeros_like(lse)
        gain, bias = norms[0:1, :width], norms[2:3, :width]
        pairs = ((ent, ent_out), (nrm, nrm_out), (q, q_out), (k, k_out), (k1, k1_out), (v, v_out), (v1, v1_out), (o, o_out), (lse, lse_out))
        for u in range(chunks):
            rows = pl.ds(u * size, size)

            @pl.when(shard == 0)
            def _():
                first = 2 * (u % 2)
                ent[rows] = x_all[first : first + 2, u // 2].reshape(size, width)

            @pl.when(shard > 0)
            def _():
                hop_wait(u)

            hat, _ = normalised(ent[rows].astype(f32))
            normed = (hat * gain + bias).astype(bf16)
            nrm[rows] = normed
            k[rows] = mm(normed, weight(1, wide)).astype(bf16)
            v[rows] = mm(normed, weight(2, wide)).astype(bf16)
            swaps = [
                remote(src.at[rows], dst.at[rows], swap_send.at[which, u], swap_recv.at[which, u], 1 - section, ctx, shard)
                for which, (src, dst) in enumerate(((k, k1), (v, v1)))
            ]
            for copy in swaps:
                copy.start()
            q[rows] = (mm(normed, weight(0, wide)) * score_scale).astype(bf16)
            for copy in swaps:
                copy.wait_recv()
            attend_chunk(u, rows, mask_ref, q, k, k1, v, v1, o, lse)
            out = mm(o[rows, :width].astype(bf16), weight(3, wide))[:, :width]
            lea[rows] = (ent[rows].astype(f32) + out).astype(bf16)
            hop_copy(u).start()
            for copy in saves(u, pairs):
                copy.start()
        for u in range(chunks):
            rows = pl.ds(u * size, size)
            for which, (src, dst) in enumerate(((k, k1), (v, v1))):
                remote(
                    src.at[rows], dst.at[rows], swap_send.at[which, u], swap_recv.at[which, u], 1 - section, ctx, shard
                ).wait_send()
            hop_copy(u).wait_send()
            for copy in saves(u, pairs):
                copy.wait()
        w_save.wait()
        norm_save.wait()
        for copy in started:
            copy.wait_send()

    @pl.when(kind == 1)
    def _():
        started = collect(ff_cols)
        norm_save.start()
        w_save = pltpu.make_async_copy(w, w_ff_out, keep.at[0])
        w_save.start()
        gain, bias = norms[1:2, :width], norms[3:4, :width]
        pairs = ((ent, ent_out), (nrm, nrm_out), (lea, lea_out), (up, up_out), (hid, hid_out))
        for u in range(chunks):
            rows = pl.ds(u * size, size)
            hop_wait(u)
            hat, _ = normalised(ent[rows].astype(f32))
            normed = (hat * gain + bias).astype(bf16)
            nrm[rows] = normed
            total = ent[rows].astype(f32)
            for i in range(2):
                upper = mm(normed, weight(i, ff_ref.shape[1]))
                up[i, rows] = upper
                hidden = jax.nn.gelu(upper, approximate=True).astype(bf16)
                hid[i, rows] = hidden
                total = total + mm_t(hidden, weight(2 + i, ff_ref.shape[1]))
            lea[rows] = total.astype(bf16)

            @pl.when(shard < 3)
            def _():
                hop_copy(u).start()

            for copy in saves(u, pairs):
                copy.start()
        for u in range(chunks):

            @pl.when(shard < 3)
            def _():
                hop_copy(u).wait_send()

            for copy in saves(u, pairs):
                copy.wait()
        w_save.wait()
        norm_save.wait()
        for copy in started:
            copy.wait_send()

    for c in range(4):

        @pl.when((shard == 3) & jnp.logical_not((ctx == 3) & (c == 3)))
        def _():
            remote(g_ref, g_all_ref.at[c], token_send.at[1], token_recv.at[c], section, ctx, shard).wait_recv()

    @pl.when(jnp.logical_not(x_stays))
    def _():
        x_copy.wait_send()

    @pl.when(jnp.logical_not(g_stays))
    def _():
        g_copy.wait_send()

    attn_copy.wait_send()
    ff_copy.wait_send()
    for copy, stays in norm_copies:

        @pl.when(jnp.logical_not(stays))
        def _():
            copy.wait_send()


def forward_relay(attn_piece, ff_piece, x_own, g_own, norm_own, mask):
    share, ff_half = ff_piece.shape
    wide = attn_piece.shape[1]
    blocks, half, width = x_own.shape
    tokens = blocks * 4 * half
    chunks = tokens // (2 * half)
    dma = pltpu.SemaphoreType.DMA
    vmem = pl.BlockSpec(memory_space=pltpu.VMEM)
    state = [
        ((tokens, width), bf16), ((tokens, width), bf16),
        ((tokens, wide), bf16), ((tokens, wide), bf16), ((tokens, wide), bf16), ((tokens, wide), bf16), ((tokens, wide), bf16),
        ((tokens, wide), f32), ((tokens, LANES), f32),
        ((2, tokens, ff_half), f32), ((2, tokens, ff_half), bf16), ((tokens, width), bf16),
    ]
    outs = [
        ((4, 4, share, wide), bf16), ((4, 4, share, ff_half), bf16), ((4,) + g_own.shape, bf16), (norm_own.shape, f32),
    ] + state
    return pl.pallas_call(
        forward_kernel,
        in_specs=[ANY] * 5 + [vmem],
        out_specs=[ANY] * len(outs),
        out_shape=[jax.ShapeDtypeStruct(s, t) for s, t in outs],
        scratch_shapes=[
            pltpu.VMEM((4, 4, share, ff_half), bf16),
            pltpu.VMEM((4,) + x_own.shape, bf16),
            pltpu.VMEM((4,) + norm_own.shape, f32),
            pltpu.VMEM(norm_own.shape, f32),
        ]
        + [pltpu.VMEM(s, t) for s, t in state]
        + [
            dma((14,)), dma((4, 4)), dma((2,)), dma((4,)), dma((4,)), dma((4,)), dma((2,)),
            dma((chunks,)), dma((chunks,)), dma((2, chunks)), dma((2, chunks)), dma((9, chunks)), dma((2,)),
        ],
        compiler_params=pltpu.CompilerParams(has_side_effects=True, vmem_limit_bytes=62 * 2**20),
        name="forward_relay",
    )(attn_piece, ff_piece, x_own, g_own, norm_own, mask)


def backward_kernel(
    w_attn_ref, w_ff_ref, g_ref, norm_ref, mask_ref,
    ent_ref, q_ref, k_ref, k1_ref, v_ref, v1_ref, o_ref, lse_ref, up_ref,
    coming_out, leaving_out, dq_out, dk_out, dv_out, d_up_out, sums_out,
    w, coming, leaving, ent, slots, o, lse, da, dq, dk, dv, give, take, big, sums,
    load, hop_send, hop_recv, swap_send, swap_recv, save, keep,
):
    section, ctx, shard = lax.axis_index("section"), lax.axis_index("ctx"), lax.axis_index("shard")
    kind = lax.rem(shard, 2)
    width = ent.shape[1]
    wide = dq.shape[1]
    size = da.shape[0]
    chunks = ent.shape[0] // size
    ff_half = w_ff_ref.shape[3]
    parts = ((0, wide), (wide, ff_half - wide))
    order = range(chunks - 1, -1, -1)

    def weight(c, start, columns):
        value = w[c, :, :, pl.ds(start, columns)]
        return value.reshape(value.shape[0] * value.shape[1], columns)

    def hop_copy(u):
        rows = pl.ds(u * size, size)
        return remote(leaving.at[rows], coming.at[rows], hop_send.at[u], hop_recv.at[u], section, ctx, shard - 1)

    def hop_wait(u):
        rows = pl.ds(u * size, size)
        remote(leaving.at[rows], coming.at[rows], hop_send.at[u], hop_recv.at[u], section, ctx, shard).wait_recv()

    def saves(u, pairs):
        rows = pl.ds(u * size, size)
        return [
            pltpu.make_async_copy(src.at[rows], dst.at[rows], save.at[index, u])
            for index, (src, dst) in enumerate(pairs)
        ]

    def finish_chunk(rows, d_normed, gain):
        hat, scale = normalised(ent[rows].astype(f32))
        sums[0:1, :width] += jnp.sum(d_normed * hat, axis=0, keepdims=True)
        sums[1:2, :width] += jnp.sum(d_normed, axis=0, keepdims=True)
        total = coming[rows].astype(f32) + norm_backward(hat, scale, gain, d_normed)
        leaving[rows] = total.astype(bf16)

    sums[...] = jnp.zeros_like(sums)
    ent_load = pltpu.make_async_copy(ent_ref, ent, load.at[0])
    ent_load.start()

    @pl.when(kind == 0)
    def _():
        loads = [pltpu.make_async_copy(w_attn_ref, w.at[:, :, :, pl.ds(0, wide)], load.at[1])]
        for i, ref in enumerate((q_ref, k_ref, k1_ref, v_ref, v1_ref)):
            loads.append(pltpu.make_async_copy(ref, slots.at[i], load.at[2 + i]))
        loads.append(pltpu.make_async_copy(o_ref, o, load.at[7]))
        loads.append(pltpu.make_async_copy(lse_ref, lse, load.at[8]))
        for copy in loads:
            copy.start()
        for copy in loads:
            copy.wait()
        ent_load.wait()
        gain = norm_ref[0:1, :width]
        lane = lax.broadcasted_iota(jnp.int32, (size, LANES), 1)
        low = lane < HEAD
        da[...] = jnp.zeros_like(da)
        pairs = ((coming, coming_out), (leaving, leaving_out), (dq, dq_out), (dk, dk_out), (dv, dv_out))

        def swap_copy(which, u):
            rows = pl.ds(u * size, size)
            return remote(
                give.at[which, rows], take.at[which, rows], swap_send.at[which, u], swap_recv.at[which, u],
                1 - section, ctx, shard,
            )

        for u in order:
            rows = pl.ds(u * size, size)
            keys = pl.ds(0, (u + 1) * size)
            hop_wait(u)
            da[:, :width] = mm_t(coming[rows], weight(3, 0, width)).astype(bf16)

            @pl.loop(0, wide // LANES)
            def _(pair):
                cols = pl.ds(pl.multiple_of(pair * LANES, LANES), LANES)
                q2 = stack_heads(slots[0, rows, cols], low)
                grad = da[:, cols]
                a2 = stack_heads(grad, low)
                level = lse[rows, :]
                product = grad.astype(f32) * o[rows, cols]
                column = lambda which: jnp.sum(jnp.where(lane == 2 * pair + which, level, 0.0), axis=1, keepdims=True)
                level2 = jnp.concatenate([column(0), column(1)], axis=0)
                delta2 = jnp.concatenate(
                    [
                        jnp.sum(jnp.where(low, product, 0.0), axis=1, keepdims=True),
                        jnp.sum(jnp.where(low, 0.0, product), axis=1, keepdims=True),
                    ],
                    axis=0,
                )
                dq2 = 0.0
                for part in range(2):
                    keys_now, values_now = slots[1 + part, keys, cols], slots[3 + part, keys, cols]
                    p = jnp.exp(mask_last(mm_t(q2, keys_now), mask_ref[part]) - level2)
                    ds = (p * (mm_t(a2, values_now) - delta2)).astype(bf16)
                    dq2 = dq2 + mm(ds, keys_now)
                    d_keys, d_values = t_mm(ds, q2), t_mm(p.astype(bf16), a2)
                    if u == chunks - 1:
                        big[2 * part, keys, cols] = d_keys
                        big[2 * part + 1, keys, cols] = d_values
                    else:
                        big[2 * part, keys, cols] += d_keys
                        big[2 * part + 1, keys, cols] += d_values
                dq[rows, cols] = (unstack_heads(dq2, low) * score_scale).astype(bf16)

            for which in range(2):
                give[which, rows] = big[2 + which, rows].astype(bf16)
                swap_copy(which, u).start()
            d_normed = mm_t(dq[rows], weight(0, 0, wide))
            for which, ref in enumerate((dk, dv)):
                swap_copy(which, u).wait_recv()
                ref[rows] = (big[which, rows] + take[which, rows].astype(f32)).astype(bf16)
                d_normed = d_normed + mm_t(ref[rows], weight(1 + which, 0, wide))
            finish_chunk(rows, d_normed, gain)

            @pl.when(shard > 0)
            def _():
                hop_copy(u).start()

            for copy in saves(u, pairs):
                copy.start()
        for u in order:
            for which in range(2):
                swap_copy(which, u).wait_send()

            @pl.when(shard > 0)
            def _():
                hop_copy(u).wait_send()

            for copy in saves(u, pairs):
                copy.wait()

    @pl.when(kind == 1)
    def _():
        loads = [pltpu.make_async_copy(w_ff_ref, w, load.at[1])]
        for i in range(2):
            for part, (start, columns) in enumerate(parts):
                loads.append(
                    pltpu.make_async_copy(
                        up_ref.at[i, :, pl.ds(start, columns)], big.at[2 * i + part, :, pl.ds(0, columns)], load.at[2 + 2 * i + part]
                    )
                )
        g_load = pltpu.make_async_copy(g_ref, coming, load.at[6])

        @pl.when(shard == 3)
        def _():
            g_load.start()

        for copy in loads:
            copy.start()
        for copy in loads:
            copy.wait()

        @pl.when(shard == 3)
        def _():
            g_load.wait()

        ent_load.wait()
        gain = norm_ref[1:2, :width]
        pairs = [(coming, coming_out), (leaving, leaving_out)]
        for i in range(2):
            for part, (start, columns) in enumerate(parts):
                pairs.append((slots.at[2 * i + part, :, pl.ds(0, columns)], d_up_out.at[i, :, pl.ds(start, columns)]))

        for u in order:
            rows = pl.ds(u * size, size)

            @pl.when(shard < 3)
            def _():
                hop_wait(u)

            grad = coming[rows]
            d_normed = 0.0
            for i in range(2):
                for part, (start, columns) in enumerate(parts):
                    cols = pl.ds(0, columns)
                    d_hidden = mm(grad, weight(2 + i, start, columns))
                    _, back = jax.vjp(lambda value: jax.nn.gelu(value, approximate=True), big[2 * i + part, rows, cols])
                    d_upper = back(d_hidden)[0].astype(bf16)
                    slots[2 * i + part, rows, cols] = d_upper
                    d_normed = d_normed + mm_t(d_upper, weight(i, start, columns))
            finish_chunk(rows, d_normed, gain)
            hop_copy(u).start()
            for copy in saves(u, pairs):
                copy.start()
        for u in order:
            hop_copy(u).wait_send()
            for copy in saves(u, pairs):
                copy.wait()

    sums_save = pltpu.make_async_copy(sums, sums_out, keep.at[0])
    sums_save.start()
    sums_save.wait()


def backward_relay(w_attn, w_ff, g, norms, mask, ent, q, k, k1, v, v1, o, lse, up):
    tokens, width = ent.shape
    wide = q.shape[1]
    size = mask.shape[2]
    chunks = tokens // size
    dma = pltpu.SemaphoreType.DMA
    vmem = pl.BlockSpec(memory_space=pltpu.VMEM)
    narrow, broad = ((tokens, width), bf16), ((tokens, wide), bf16)
    outs = [narrow, narrow, broad, broad, broad, (up.shape, bf16), (norms.shape, f32)]
    scratch = [
        ((4,) + w_ff.shape[1:], bf16), narrow, narrow, narrow, ((5, tokens, wide), bf16),
        (o.shape, f32), (lse.shape, f32), ((size, wide), bf16), broad, broad, broad,
        ((2, tokens, wide), bf16), ((2, tokens, wide), bf16), ((4, tokens, wide), f32), (norms.shape, f32),
    ]
    return pl.pallas_call(
        backward_kernel,
        in_specs=[ANY] * 3 + [vmem] * 2 + [ANY] * 9,
        out_specs=[ANY] * len(outs),
        out_shape=[jax.ShapeDtypeStruct(s, t) for s, t in outs],
        scratch_shapes=[pltpu.VMEM(s, t) for s, t in scratch]
        + [
            dma((9,)), dma((chunks,)), dma((chunks,)), dma((2, chunks)), dma((2, chunks)), dma((6, chunks)), dma((1,)),
        ],
        compiler_params=pltpu.CompilerParams(has_side_effects=True, vmem_limit_bytes=62 * 2**20),
        name="backward_relay",
    )(w_attn, w_ff, g, norms, mask, ent, q, k, k1, v, v1, o, lse, up)


def add_into(total, term):
    total[...] = (total[...].astype(f32) + term[...].astype(f32)).astype(bf16)


def reduce_kernel(*refs):
    attn_terms, ff_terms = refs[0:4], refs[4:8]
    attn_out, ff_out = refs[8:10]
    held, first, second, third = refs[10:14]
    load, first_send, first_recv, second_send, second_recv, third_send, third_recv, last_send, last_recv = refs[14:]
    section, ctx, shard = lax.axis_index("section"), lax.axis_index("ctx"), lax.axis_index("shard")
    kind = lax.rem(shard, 2)
    near = lambda c, step: c + step - 2 * step * lax.rem(c // step, 2)
    x_ctx, y_ctx = near(ctx, 1), near(ctx, 2)
    d_ctx = near(x_ctx, 2)
    count = len(attn_terms)

    def reduce(terms, out_ref, which):
        width = terms[0].shape[-1]
        cols = pl.ds(0, width)
        own = lambda i, c, j: held.at[i, c, j, :, cols]

        def give(i):
            return remote(
                terms[i].at[:, section], first.at[i, :, :, :, cols], first_send.at[i], first_recv.at[i],
                1 - section, ctx, shard,
            )

        def take(i):
            return pltpu.make_async_copy(terms[i].at[:, 1 - section], held.at[i, :, :, :, cols], load.at[i])

        def second_copy(i, j, part):
            to = (x_ctx, y_ctx)[j]
            return remote(
                own(i, (to, d_ctx)[part], j), second.at[i, j, part, :, cols],
                second_send.at[i, j, part], second_recv.at[i, j, part], section, to, shard,
            )

        def third_copy(i, j):
            to = (y_ctx, x_ctx)[j]
            return remote(
                own(i, to, j), third.at[i, j, :, cols], third_send.at[i, j], third_recv.at[i, j], section, to, shard
            )

        def last_copy(i, j):
            return remote(
                own(i, ctx, j), out_ref.at[i], last_send.at[i, j], last_recv.at[which, i],
                shard // 2, ctx, 2 * (1 - section) + j,
            )

        for i in range(count):
            give(i).start()
            take(i).start()
        for step in range(count + 2):
            i = step
            if i < count:
                take(i).wait()
                give(i).wait_recv()

                @pl.loop(0, 4)
                def _(c):
                    for j in range(2):
                        add_into(own(i, c, j), first.at[i, c, j, :, cols])

                for part in (1, 0):
                    for j in range(2):
                        second_copy(i, j, part).start()
            i = step - 1
            if 0 <= i < count:
                for j in range(2):
                    second_copy(i, j, 1).wait_recv()
                    add_into(own(i, (y_ctx, x_ctx)[j], j), second.at[i, j, 1, :, cols])
                    third_copy(i, j).start()
                for j in range(2):
                    second_copy(i, j, 0).wait_recv()
                    add_into(own(i, ctx, j), second.at[i, j, 0, :, cols])
            i = step - 2
            if 0 <= i < count:
                for j in range(2):
                    third_copy(i, j).wait_recv()
                    add_into(own(i, ctx, j), third.at[i, j, :, cols])
                    last_copy(i, j).start()
        for i in range(count):
            give(i).wait_send()
            for j in range(2):
                for part in range(2):
                    second_copy(i, j, part).wait_send()
                third_copy(i, j).wait_send()
                last_copy(i, j).wait_send()

    @pl.when(kind == 0)
    def _():
        reduce(attn_terms, attn_out, 0)

    @pl.when(kind == 1)
    def _():
        reduce(ff_terms, ff_out, 1)

    for i in range(count):
        for which, out_ref in enumerate((attn_out, ff_out)):
            remote(
                out_ref.at[i], out_ref.at[i], last_send.at[i, 0], last_recv.at[which, i], section, ctx, shard
            ).wait_recv()


def reduce_all(attn_terms, ff_terms):
    rows = attn_terms[0].shape[0] // 16
    count = len(attn_terms)
    split = lambda v: v.reshape(4, 2, 2, rows, v.shape[1])
    width = ff_terms[0].shape[1]
    dma = pltpu.SemaphoreType.DMA
    return pl.pallas_call(
        reduce_kernel,
        in_specs=[ANY] * (2 * count),
        out_specs=[ANY] * 2,
        out_shape=[
            jax.ShapeDtypeStruct((count, rows, attn_terms[0].shape[1]), bf16),
            jax.ShapeDtypeStruct((count, rows, width), bf16),
        ],
        scratch_shapes=[
            pltpu.VMEM((count, 4, 2, rows, width), bf16),
            pltpu.VMEM((count, 4, 2, rows, width), bf16),
            pltpu.VMEM((count, 2, 2, rows, width), bf16),
            pltpu.VMEM((count, 2, rows, width), bf16),
            dma((count,)), dma((count,)), dma((count,)),
            dma((count, 2, 2)), dma((count, 2, 2)),
            dma((count, 2)), dma((count, 2)),
            dma((count, 2)), dma((2, count)),
        ],
        compiler_params=pltpu.CompilerParams(has_side_effects=True, vmem_limit_bytes=48 * 2**20),
        name="reduce_all",
    )(*[split(v) for v in attn_terms], *[split(v) for v in ff_terms])


def chain(inputs, cotangent, qkv_weight, out_weight, up_weight, down_weight, norm_gain, norm_bias):
    section, ctx, shard = lax.axis_index("section"), lax.axis_index("ctx"), lax.axis_index("shard")
    seq_count, blocks, slice_len, width = inputs.shape
    half = slice_len // 2
    tokens = blocks * 4 * half
    share = width // 4
    group = share // 4
    group_pad = up_to(group, ROWS)
    wide = up_to(width, LANES)
    ff = up_weight.shape[2]
    is_attn = shard % 2 == 0

    pad = lambda w: jnp.pad(w, ((0, 0), (0, wide - width)))
    own_qkv, own_out = qkv_weight[0], out_weight[0]
    attn_src = jnp.stack([pad(own_qkv[:, i * width : (i + 1) * width]) for i in range(3)] + [pad(own_out)])
    down_t = down_weight[0].T
    up0 = up_weight[0]
    ff_src = jnp.stack([up0[:, : ff // 2], up0[:, ff // 2 :], down_t[:, : ff // 2], down_t[:, ff // 2 :]])
    norm_own = jnp.concatenate([norm_gain[0], norm_bias[0]], axis=0).astype(f32)
    norm_own = lax.dynamic_update_slice(
        jnp.zeros((ROWS, wide), f32), jnp.pad(norm_own, ((0, ROWS - 4), (0, 0))), (0, shard * share)
    )
    x_own = lax.dynamic_slice_in_dim(inputs[0], section * half, half, 1)
    g_own = lax.dynamic_slice_in_dim(cotangent[0], section * half, half, 1)
    mask = attention_masks(section, half)
    mask = jnp.concatenate([mask, mask], axis=1)
    w_attn, w_ff, g_all, norms, ent, nrm, q, k, k1, v, v1, o, lse, up, hid, y = forward_relay(
        lax.dynamic_index_in_dim(attn_src, ctx, 0, keepdims=False),
        lax.dynamic_index_in_dim(ff_src, ctx, 0, keepdims=False),
        x_own, g_own, norm_own, mask,
    )
    own_place = jnp.arange(4)[:, None, None]

    def bring_tokens(every, own):
        mine = jnp.where((own_place[..., None] == ctx) & (shard == ctx), own, every)
        return jnp.swapaxes(mine, 0, 1).reshape(tokens, width)

    g_last = bring_tokens(g_all, g_own)
    feature = lax.broadcasted_iota(jnp.int32, (width, 16 * group_pad), 0)
    place = lax.broadcasted_iota(jnp.int32, (width, 16 * group_pad), 1)
    spread = (feature // group * group_pad + feature % group == place).astype(bf16)
    grouped = lambda v: mm(v, spread).astype(bf16)

    coming, leaving, dq, dk, dv, d_up, sums = backward_relay(
        w_attn, w_ff, g_last, norms, mask, ent, q, k, k1, v, v1, o, lse, up
    )
    nrm_grouped, coming_grouped = grouped(nrm), grouped(coming)
    ff_grads = [t_mm(nrm_grouped, d_up[i]) for i in range(2)] + [t_mm(coming_grouped, hid[i]) for i in range(2)]
    o_grouped = grouped(o[:, :width].astype(bf16))
    attn_grads = [t_mm(nrm_grouped, d) for d in (dq, dk, dv)]
    attn_grads.append(t_mm(o_grouped, jnp.pad(coming, ((0, 0), (0, wide - width)))))
    attn_sums, ff_sums = reduce_all([v.astype(bf16) for v in attn_grads], [v.astype(bf16) for v in ff_grads])

    terms = sums[:2, :width]
    terms = jnp.where(jnp.arange(4)[:, None, None] == shard, terms[None], 0.0)
    totals = lax.psum(terms, ("section", "ctx", "shard")).reshape(2, 2, 2, width)
    totals = lax.dynamic_index_in_dim(totals, section, 0, keepdims=False)
    totals = lax.dynamic_slice_in_dim(totals, (ctx * 4 + shard) * group, group, 2)

    final = jnp.where(is_attn, leaving, y).reshape(blocks, 4, half, width)
    final = lax.all_to_all(jnp.swapaxes(final, 0, 1), "ctx", 0, 0)
    final = lax.all_to_all(final, "shard", 0, 0).reshape(2, 2, blocks, half, width)
    final = lax.all_to_all(final, "section", 0, 0)
    final = jnp.moveaxis(final, 0, 2).reshape(2, blocks, slice_len, width)

    attn_sums = attn_sums[:, :group, :width].astype(f32)
    ff_sums = ff_sums[:, :group].astype(f32)
    return (
        final[1][None, None],
        final[0][None, None],
        jnp.concatenate([attn_sums[0], attn_sums[1], attn_sums[2]], axis=1)[None],
        attn_sums[3][None],
        jnp.concatenate([ff_sums[0], ff_sums[1]], axis=1)[None],
        jnp.concatenate([ff_sums[2].T, ff_sums[3].T], axis=0)[None],
        totals[:, 0][None],
        totals[:, 1][None],
    )


def passed_along(value, axis, steps):
    count = lax.axis_size(axis)
    initial, last = (max(0, -steps), min(count, count - steps))
    return lax.ppermute(value, axis, [(source, source + steps) for source in range(initial, last)])


def layer_norm(values, gain, shift):
    mean = jnp.mean(values, axis=-1, keepdims=True)
    centred = values - mean
    var = jnp.mean(centred * centred, axis=-1, keepdims=True)
    return centred * lax.rsqrt(var + eps_norm) * gain + shift


def gelu_tanh(values):
    return jax.nn.gelu(values, approximate=True)


def split_pair(key_value, head_count):
    block_len, seq_count, double = key_value.shape
    model_width = double // 2
    key_rows = key_value[..., :model_width].reshape(block_len, seq_count, head_count, HEAD)
    value_rows = key_value[..., model_width:].reshape(block_len, seq_count, head_count, HEAD)
    return (key_rows, value_rows)


def causal_mask(query_pos, key_pos):
    return (key_pos[None, :] <= query_pos[:, None])[None, :, None, :]


def forward_block(running, queries, query_pos, key_value, key_pos):
    row_max, row_sum, accum = running
    key_rows, value_rows = split_pair(key_value, queries.shape[2])
    scores = (
        jnp.einsum("sqhe,kshe->sqhk", queries, key_rows, preferred_element_type=jnp.float32)
        * score_scale
    )
    causal = causal_mask(query_pos, key_pos)
    new_max = jnp.maximum(row_max, jnp.max(jnp.where(causal, scores, -1e30), axis=-1))
    softmax_w = jnp.where(causal, jnp.exp(scores - new_max[..., None]), 0.0)
    factor = jnp.exp(row_max - new_max)
    row_sum = row_sum * factor + jnp.sum(softmax_w, axis=-1)
    accum = accum * factor[..., None] + jnp.einsum(
        "sqhk,kshe->sqhe",
        softmax_w.astype(jnp.bfloat16),
        value_rows,
        preferred_element_type=jnp.float32,
    )
    return (new_max, row_sum, accum)


def split_rows(whole):
    key_count = whole.shape[0]
    block_size = 512
    blocks = whole.reshape((key_count // block_size, block_size) + whole.shape[1:])
    offsets = jnp.arange(key_count // block_size, dtype=jnp.int32) * block_size
    return (blocks, offsets, block_size)


def fold_keys(running, piece, start, queries, query_pos, group_len):
    blocks, offsets, block_size = split_rows(piece)

    def fold_scan_step(inner, scan_item):
        block_rows, offset = scan_item
        for group_id in range(block_rows.shape[2]):
            key_pos = (
                group_id * group_len + start + offset + jnp.arange(block_size, dtype=jnp.int32)
            )
            inner = forward_block(inner, queries, query_pos, block_rows[:, :, group_id], key_pos)
        return (inner, None)

    result, _ = lax.scan(fold_scan_step, running, (blocks, offsets))
    return result


def pair_terms(d_scores, softmax_w, queries, d_attended, block_size):
    d_keys = (
        jnp.einsum("sqhk,sqhe->kshe", d_scores, queries, preferred_element_type=jnp.float32)
        * score_scale
    )
    d_values = jnp.einsum(
        "sqhk,sqhe->kshe",
        softmax_w.astype(jnp.bfloat16),
        d_attended,
        preferred_element_type=jnp.float32,
    )
    shape = (block_size, queries.shape[0], queries.shape[2] * queries.shape[3])
    return jnp.concatenate([d_keys.reshape(shape), d_values.reshape(shape)], axis=-1)


def score_grads(
    queries, query_pos, log_total, row_delta, d_attended, key_rows, value_rows, key_pos
):
    scores = (
        jnp.einsum("sqhe,kshe->sqhk", queries, key_rows, preferred_element_type=jnp.float32)
        * score_scale
    )
    causal = causal_mask(query_pos, key_pos)
    softmax_w = jnp.where(causal, jnp.exp(scores - log_total[..., None]), 0.0)
    d_probs = jnp.einsum(
        "sqhe,kshe->sqhk", d_attended, value_rows, preferred_element_type=jnp.float32
    )
    d_scores = (softmax_w * (d_probs - row_delta[..., None])).astype(jnp.bfloat16)
    return (softmax_w, d_scores)


def backward_keys(whole, queries, query_pos, log_total, row_delta, d_attended, group_len):
    blocks, offsets, block_size = split_rows(whole)

    def backward_scan_step(d_queries, scan_item):
        block_rows, offset = scan_item
        for group_id in range(block_rows.shape[2]):
            key_pos = group_id * group_len + offset + jnp.arange(block_size, dtype=jnp.int32)
            key_rows, value_rows = split_pair(block_rows[:, :, group_id], queries.shape[2])
            softmax_w, d_scores = score_grads(
                queries, query_pos, log_total, row_delta, d_attended, key_rows, value_rows, key_pos
            )
            d_queries = (
                d_queries
                + jnp.einsum(
                    "sqhk,kshe->sqhe", d_scores, key_rows, preferred_element_type=jnp.float32
                )
                * score_scale
            )
        return (d_queries, None)

    d_queries, terms = lax.scan(
        backward_scan_step, jnp.zeros(queries.shape, jnp.float32), (blocks, offsets)
    )
    return (d_queries, None)


def owner_terms(
    own_cache, all_queries, all_d_att, all_totals, all_deltas, micro_index, ctx_id, group_len
):
    block_len, seq_count, group_count, double = own_cache.shape
    head_count = all_queries.shape[2]
    query_rows = all_queries.shape[1]
    query_size = 512
    block_count = query_rows // query_size

    def loop_step(index, total):
        offset = index * query_size
        q_block = lax.dynamic_slice_in_dim(all_queries, offset, query_size, 1)
        d_block = lax.dynamic_slice_in_dim(all_d_att, offset, query_size, 1)
        t_block = lax.dynamic_slice_in_dim(all_totals, offset, query_size, 1)
        r_block = lax.dynamic_slice_in_dim(all_deltas, offset, query_size, 1)
        query_pos = micro_index * group_len + offset + jnp.arange(query_size, dtype=jnp.int32)
        pieces = []
        for group_id in range(group_count):
            key_pos = (
                group_id * group_len + ctx_id * block_len + jnp.arange(block_len, dtype=jnp.int32)
            )
            key_rows, value_rows = split_pair(own_cache[:, :, group_id], head_count)
            softmax_w, d_scores = score_grads(
                q_block, query_pos, t_block, r_block, d_block, key_rows, value_rows, key_pos
            )
            pieces.append(pair_terms(d_scores, softmax_w, q_block, d_block, block_len))
        return total + jnp.stack(pieces, axis=2)

    return lax.fori_loop(0, block_count, loop_step, jnp.zeros(own_cache.shape, jnp.float32))


def store_at(store, value, micro_index, active):
    updated = lax.dynamic_update_index_in_dim(store, value, micro_index, 0)
    return jnp.where(active, updated, store)


def shards(inputs, cotangent, qkv_weight, out_weight, up_weight, down_weight, norm_gain, norm_bias):
    section_id = lax.axis_index("section")
    ctx_count = lax.axis_size("ctx")
    ctx_id = lax.axis_index("ctx")
    seq_count, group_count, block_len, model_width = inputs.shape
    head_count = model_width // HEAD
    group_len = block_len * ctx_count
    row_count = seq_count * block_len
    w_qkv, w_out, w_up, w_down, gains, biases = (
        lax.all_gather(qkv_weight[0], "shard", axis=0, tiled=True),
        lax.all_gather(out_weight[0], "shard", axis=0, tiled=True),
        lax.all_gather(up_weight[0], "shard", axis=0, tiled=True),
        lax.all_gather(down_weight[0], "shard", axis=1, tiled=True),
        lax.all_gather(norm_gain[0], "shard", axis=1, tiled=True),
        lax.all_gather(norm_bias[0], "shard", axis=1, tiled=True),
    )
    gains = gains.astype(jnp.float32)
    biases = biases.astype(jnp.float32)
    ff_width = w_up.shape[1]
    cache = jnp.zeros((block_len, seq_count, group_count, 2 * model_width), jnp.bfloat16)
    in_store = jnp.zeros((group_count, seq_count, block_len, model_width), jnp.bfloat16)
    query_store = jnp.zeros((group_count, seq_count, block_len, head_count, HEAD), jnp.bfloat16)
    att_store = jnp.zeros((group_count, seq_count, block_len, head_count, HEAD), jnp.float32)
    total_store = jnp.zeros((group_count, seq_count, block_len, head_count), jnp.float32)
    middle_store = jnp.zeros((group_count, row_count, model_width), jnp.float32)
    upper_store = jnp.zeros((group_count, row_count, ff_width), jnp.float32)
    out_store = jnp.zeros((group_count, seq_count, block_len, model_width), jnp.bfloat16)
    received = jnp.zeros((seq_count, block_len, model_width), jnp.bfloat16)
    for tick_no in range(group_count + 1):
        micro = tick_no - section_id
        active = (micro >= 0) & (micro < group_count)
        micro_index = jnp.clip(micro, 0, group_count - 1)
        own_input = lax.dynamic_index_in_dim(inputs, micro_index, 1, keepdims=False)
        entering = jnp.where(section_id == 0, own_input, received)
        flat_rows = entering.reshape(row_count, model_width).astype(jnp.float32)
        normed = layer_norm(flat_rows, gains[0], biases[0]).astype(jnp.bfloat16)
        mixed = jnp.dot(normed, w_qkv, preferred_element_type=jnp.float32).astype(jnp.bfloat16)
        queries = mixed[:, :model_width].reshape(seq_count, block_len, head_count, HEAD)
        fresh = jnp.swapaxes(
            mixed[:, model_width:].reshape(seq_count, block_len, 2 * model_width), 0, 1
        )
        updated = lax.dynamic_update_index_in_dim(cache, fresh, micro_index, 2)
        cache = jnp.where(active, updated, cache)
        query_pos = (
            micro_index * group_len + ctx_id * block_len + jnp.arange(block_len, dtype=jnp.int32)
        )
        start_state = (
            jnp.full((seq_count, block_len, head_count), -1e30, jnp.float32),
            jnp.zeros((seq_count, block_len, head_count), jnp.float32),
            jnp.zeros((seq_count, block_len, head_count, HEAD), jnp.float32),
        )
        row_max, row_sum, accum = fold_keys(
            start_state,
            lax.all_gather(cache, "ctx", axis=0, tiled=True),
            jnp.int32(0),
            queries,
            query_pos,
            group_len,
        )
        attended = accum / row_sum[..., None]
        log_total = row_max + jnp.log(row_sum)
        att_low = attended.reshape(row_count, model_width).astype(jnp.bfloat16)
        middle = flat_rows + jnp.dot(att_low, w_out, preferred_element_type=jnp.float32)
        normed2 = layer_norm(middle, gains[1], biases[1]).astype(jnp.bfloat16)
        upper = jnp.dot(normed2, w_up, preferred_element_type=jnp.float32)
        hidden = gelu_tanh(upper).astype(jnp.bfloat16)
        leaving = (middle + jnp.dot(hidden, w_down, preferred_element_type=jnp.float32)).astype(
            jnp.bfloat16
        )
        leaving = leaving.reshape(seq_count, block_len, model_width)
        in_store = store_at(in_store, entering, micro_index, active)
        query_store = store_at(query_store, queries, micro_index, active)
        att_store = store_at(att_store, attended, micro_index, active)
        total_store = store_at(total_store, log_total, micro_index, active)
        middle_store = store_at(middle_store, middle, micro_index, active)
        upper_store = store_at(upper_store, upper, micro_index, active)
        out_store = store_at(out_store, leaving, micro_index, active)
        if tick_no < group_count:
            received = passed_along(leaving, "section", 1)
    key_acc = jnp.zeros((block_len, seq_count, group_count, 2 * model_width), jnp.float32)
    grad_qkv = jnp.zeros((model_width, 3 * model_width), jnp.float32)
    grad_out = jnp.zeros((model_width, model_width), jnp.float32)
    grad_up = jnp.zeros((model_width, ff_width), jnp.float32)
    grad_down = jnp.zeros((ff_width, model_width), jnp.float32)
    grad_gain = jnp.zeros((2, model_width), jnp.float32)
    grad_bias = jnp.zeros((2, model_width), jnp.float32)
    grad_store = jnp.zeros((group_count, seq_count, block_len, model_width), jnp.bfloat16)
    coming = jnp.zeros((seq_count, block_len, model_width), jnp.bfloat16)
    for tick_no in range(group_count + 1):
        micro = group_count - tick_no - section_id
        active = (micro >= 0) & (micro < group_count)
        active_weight = active.astype(jnp.float32)
        micro_index = jnp.clip(micro, 0, group_count - 1)
        own_cot = lax.dynamic_index_in_dim(cotangent, micro_index, 1, keepdims=False)
        d_out = (
            jnp.where(section_id == 1, own_cot, coming)
            .reshape(row_count, model_width)
            .astype(jnp.float32)
        )
        flat_rows = in_store[micro_index].reshape(row_count, model_width).astype(jnp.float32)
        queries = query_store[micro_index]
        attended = att_store[micro_index]
        log_total = total_store[micro_index]
        middle = middle_store[micro_index]
        upper = upper_store[micro_index]
        normed2_full, norm2_back = jax.vjp(
            lambda v, g, b: layer_norm(v, g, b), middle, gains[1], biases[1]
        )
        normed2 = normed2_full.astype(jnp.bfloat16)
        hidden_full, gelu_back = jax.vjp(gelu_tanh, upper)
        hidden = hidden_full.astype(jnp.bfloat16)
        d_branch = d_out.astype(jnp.bfloat16)
        grad_down = grad_down + active_weight * jnp.dot(
            hidden.T, d_branch, preferred_element_type=jnp.float32
        )
        d_hidden = jnp.dot(d_branch, w_down.T, preferred_element_type=jnp.float32)
        d_upper = gelu_back(d_hidden)[0].astype(jnp.bfloat16)
        grad_up = grad_up + active_weight * jnp.dot(
            normed2.T, d_upper, preferred_element_type=jnp.float32
        )
        d_normed2 = jnp.dot(d_upper, w_up.T, preferred_element_type=jnp.float32)
        d_mid_norm, d_gain2, d_bias2 = norm2_back(d_normed2)
        d_middle = d_out + d_mid_norm
        att_low = attended.reshape(row_count, model_width).astype(jnp.bfloat16)
        d_att = d_middle.astype(jnp.bfloat16)
        grad_out = grad_out + active_weight * jnp.dot(
            att_low.T, d_att, preferred_element_type=jnp.float32
        )
        d_attended = jnp.dot(d_att, w_out.T, preferred_element_type=jnp.float32).astype(
            jnp.bfloat16
        )
        d_attended = d_attended.reshape(seq_count, block_len, head_count, HEAD)
        row_delta = jnp.sum(d_attended.astype(jnp.float32) * attended, axis=-1)
        query_pos = (
            micro_index * group_len + ctx_id * block_len + jnp.arange(block_len, dtype=jnp.int32)
        )
        whole = lax.all_gather(cache, "ctx", axis=0, tiled=True)
        d_queries, unused = backward_keys(
            whole, queries, query_pos, log_total, row_delta, d_attended, group_len
        )
        all_queries, all_d_att = (
            lax.all_gather(queries, "ctx", axis=1, tiled=True),
            lax.all_gather(d_attended, "ctx", axis=1, tiled=True),
        )
        all_totals, all_deltas = (
            lax.all_gather(log_total, "ctx", axis=1, tiled=True),
            lax.all_gather(row_delta, "ctx", axis=1, tiled=True),
        )
        shares = owner_terms(
            cache, all_queries, all_d_att, all_totals, all_deltas, micro_index, ctx_id, group_len
        )
        key_acc = key_acc + active_weight * shares
        d_pair = jnp.swapaxes(
            lax.dynamic_index_in_dim(key_acc, micro_index, 2, keepdims=False), 0, 1
        )
        d_mixed = jnp.concatenate(
            [d_queries.reshape(row_count, model_width), d_pair.reshape(row_count, 2 * model_width)],
            axis=-1,
        ).astype(jnp.bfloat16)
        normed_full, norm1_back = jax.vjp(
            lambda v, g, b: layer_norm(v, g, b), flat_rows, gains[0], biases[0]
        )
        normed = normed_full.astype(jnp.bfloat16)
        grad_qkv = grad_qkv + active_weight * jnp.dot(
            normed.T, d_mixed, preferred_element_type=jnp.float32
        )
        d_normed = jnp.dot(d_mixed, w_qkv.T, preferred_element_type=jnp.float32)
        d_flat_norm, d_gain1, d_bias1 = norm1_back(d_normed)
        grad_gain = grad_gain + active_weight * jnp.stack([d_gain1, d_gain2])
        grad_bias = grad_bias + active_weight * jnp.stack([d_bias1, d_bias2])
        d_entering = (
            (d_middle + d_flat_norm).astype(jnp.bfloat16).reshape(seq_count, block_len, model_width)
        )
        grad_store = store_at(grad_store, d_entering, micro_index, active)
        if tick_no < group_count:
            coming = passed_along(d_entering, "section", -1)
    sums = (
        lax.psum_scatter(grad_qkv, ("ctx", "shard"), scatter_dimension=0, tiled=True),
        lax.psum_scatter(grad_out, ("ctx", "shard"), scatter_dimension=0, tiled=True),
        lax.psum_scatter(grad_up, ("ctx", "shard"), scatter_dimension=0, tiled=True),
        lax.psum_scatter(grad_down, ("ctx", "shard"), scatter_dimension=1, tiled=True),
        lax.psum_scatter(grad_gain, ("ctx", "shard"), scatter_dimension=1, tiled=True),
        lax.psum_scatter(grad_bias, ("ctx", "shard"), scatter_dimension=1, tiled=True),
    )
    layer_outputs = jnp.swapaxes(out_store, 0, 1)[None]
    input_grads = jnp.swapaxes(grad_store, 0, 1)[None]
    return (
        layer_outputs,
        input_grads,
        sums[0][None],
        sums[1][None],
        sums[2][None],
        sums[3][None],
        sums[4][None],
        sums[5][None],
    )


def solution(mesh):
    in_specs = (
        P("shard", None, "ctx", None),
        P("shard", None, "ctx", None),
        P("section", "shard", None),
        P("section", "shard", None),
        P("section", "shard", None),
        P("section", None, "shard"),
        P("section", None, "shard"),
        P("section", None, "shard"),
    )
    out_specs = (
        P("section", "shard", None, "ctx", None),
        P("section", "shard", None, "ctx", None),
        P("section", ("ctx", "shard"), None),
        P("section", ("ctx", "shard"), None),
        P("section", ("ctx", "shard"), None),
        P("section", None, ("ctx", "shard")),
        P("section", None, ("ctx", "shard")),
        P("section", None, ("ctx", "shard")),
    )
    relay = mesh.shape["section"] == 2 and mesh.shape["shard"] == 4 and mesh.shape["ctx"] == 4
    return jax.shard_map(chain if relay else shards, mesh=mesh, in_specs=in_specs, out_specs=out_specs, check_vma=False)
```

```python
import functools

import jax
import jax.numpy as jnp
from jax import lax
from jax.experimental import pallas as pl
from jax.experimental.pallas import tpu as pltpu
from jax.sharding import PartitionSpec as P

HEAD = 64
LANES = 128
ROWS = 8
NEG = -1e30

eps_norm = 1e-05
score_scale = 0.125
f32 = jnp.float32
bf16 = jnp.bfloat16


def up_to(width, step):
    return -(-width // step) * step


def dot(a, b, dims):
    return lax.dot_general(a, b, (dims, ((), ())), preferred_element_type=f32)


def mm(a, b):
    return dot(a, b, ((1,), (0,)))


def mm_t(a, b):
    return dot(a, b, ((1,), (1,)))


def t_mm(a, b):
    return dot(a, b, ((0,), (0,)))


def attention_masks(core, half):
    row = lax.broadcasted_iota(jnp.int32, (2 * half, 2 * half), 0)
    col = lax.broadcasted_iota(jnp.int32, (2 * half, 2 * half), 1)
    row_slice, col_slice = row // half, col // half
    own = (col_slice < row_slice) | ((col_slice == row_slice) & (col <= row))
    other = (col_slice < row_slice) | ((col_slice == row_slice) & (core == 1))
    return jnp.where(jnp.stack([own, other]), 0.0, NEG).astype(f32)


def norm_backward(hat, scale, gain, grad):
    scaled = grad * gain
    mean = jnp.mean(scaled, axis=-1, keepdims=True)
    along = jnp.mean(scaled * hat, axis=-1, keepdims=True)
    return scale * (scaled - mean - hat * along)


ANY = pl.BlockSpec(memory_space=pl.ANY)


def remote(src, dst, send, recv, section, ctx, shard):
    return pltpu.make_async_remote_copy(
        src_ref=src,
        dst_ref=dst,
        send_sem=send,
        recv_sem=recv,
        device_id=(section, ctx, shard),
        device_id_type=pl.DeviceIdType.MESH,
    )


def normalised(values):
    mean = jnp.mean(values, axis=-1, keepdims=True)
    centred = values - mean
    var = jnp.mean(centred * centred, axis=-1, keepdims=True)
    scale = lax.rsqrt(var + eps_norm)
    return centred * scale, scale


def stack_heads(value, low):
    zero = jnp.zeros_like(value)
    return jnp.concatenate([jnp.where(low, value, zero), jnp.where(low, zero, value)], axis=0)


def unstack_heads(value, low):
    rows = value.shape[0] // 2
    return jnp.where(low, value[:rows], value[rows:])


def mask_last(scores, mask):
    width = mask.shape[1]
    last = scores[:, scores.shape[1] - width :] + mask
    if scores.shape[1] == width:
        return last
    return jnp.concatenate([scores[:, : scores.shape[1] - width], last], axis=1)


def attend_chunk(u, rows, mask_ref, q, k, k1, v, v1, o, lse):
    size = rows.size
    keys = pl.ds(0, (u + 1) * size)
    lane = lax.broadcasted_iota(jnp.int32, (size, LANES), 1)
    low = lane < HEAD

    @pl.loop(0, q.shape[1] // LANES)
    def _(pair):
        cols = pl.ds(pl.multiple_of(pair * LANES, LANES), LANES)
        q2 = stack_heads(q[rows, cols], low)
        scores = [mask_last(mm_t(q2, ref[keys, cols]), mask_ref[part]) for part, ref in enumerate((k, k1))]
        top = jnp.maximum(
            jnp.max(scores[0], axis=1, keepdims=True), jnp.max(scores[1], axis=1, keepdims=True)
        )
        total, acc = 0.0, 0.0
        for s, ref in zip(scores, (v, v1)):
            p = jnp.exp(s - top)
            total = total + jnp.sum(p, axis=1, keepdims=True)
            acc = acc + mm(p.astype(bf16), ref[keys, cols])
        o[rows, cols] = unstack_heads(acc / total, low)
        level = top + jnp.log(total)
        lse[rows, :] = jnp.where(
            lane == 2 * pair, level[:size], jnp.where(lane == 2 * pair + 1, level[size:], lse[rows, :])
        )


def near_ctx(c, step):
    return c + step - 2 * step * lax.rem(c // step, 2)


def forward_kernel(
    attn_ref, ff_ref, x_ref, g_ref, norm_ref, mask_ref,
    w_attn_out, w_ff_out, g_all_ref, norm_out,
    ent_out, nrm_out, q_out, k_out, k1_out, v_out, v1_out, o_out, lse_out, up_out, hid_out, lea_out,
    w, x_all, norm_all, norms, ent, nrm, q, k, k1, v, v1, o, lse, up, hid, lea,
    send, recv, token_send, token_recv, norm_send, norm_recv, far_send,
    hop_send, hop_recv, swap_send, swap_recv, save, keep,
):
    section, ctx, shard = lax.axis_index("section"), lax.axis_index("ctx"), lax.axis_index("shard")
    kind = lax.rem(shard, 2)
    far_core = 1 - shard // 2
    x_ctx, y_ctx = near_ctx(ctx, 1), near_ctx(ctx, 2)
    d_ctx = near_ctx(x_ctx, 2)
    width = ent.shape[1]
    wide = q.shape[1]
    size = 2 * x_ref.shape[1]
    chunks = ent.shape[0] // size
    attn_cols = pl.ds(0, attn_ref.shape[1])
    ff_cols = pl.ds(0, ff_ref.shape[1])

    x_copy = remote(x_ref, x_all.at[ctx], token_send.at[0], token_recv.at[ctx], section, shard, 0)
    g_copy = remote(g_ref, g_all_ref.at[ctx], token_send.at[1], token_recv.at[ctx], section, shard, 3)
    x_stays = (shard == 0) & (ctx == 0)
    g_stays = (shard == 3) & (ctx == 3)
    attn_copy = remote(
        attn_ref, w.at[ctx, shard, :, attn_cols], far_send.at[0], recv.at[ctx, shard], far_core, ctx, 2 * section
    )
    ff_copy = remote(
        ff_ref, w.at[ctx, shard, :, ff_cols], far_send.at[1], recv.at[ctx, shard], far_core, ctx, 2 * section + 1
    )
    x_local = pltpu.make_async_copy(x_ref, x_all.at[ctx], token_recv.at[ctx])
    norm_local = pltpu.make_async_copy(norm_ref, norm_all.at[shard], norm_recv.at[shard])

    @pl.when(x_stays)
    def _():
        x_local.start()

    @pl.when(jnp.logical_not(x_stays))
    def _():
        x_copy.start()

    attn_copy.start()
    norm_copies = []
    for core in range(2):
        for stage in range(2):
            copy = remote(
                norm_ref, norm_all.at[shard], norm_send.at[core * 2 + stage], norm_recv.at[shard],
                core, ctx, 2 * section + stage,
            )
            stays = (section == core) & (shard == 2 * section + stage)
            norm_copies.append((copy, stays))

            @pl.when(stays)
            def _():
                norm_local.start()

            @pl.when(jnp.logical_not(stays))
            def _():
                copy.start()

    ff_copy.start()

    @pl.when(jnp.logical_not(g_stays))
    def _():
        g_copy.start()

    def piece(cols, c, s, which, core, to_ctx):
        ref = w.at[c, s, :, cols]
        return remote(ref, ref, send.at[which], recv.at[c, s], core, to_ctx, shard)

    def collect(cols):
        mine = [2 * (1 - section) + j for j in range(2)]
        started = []

        def go(c, s, core, to_ctx):
            copy = piece(cols, c, s, len(started), core, to_ctx)
            copy.start()
            started.append(copy)

        def arrived(c, s):
            piece(cols, c, s, 0, section, ctx).wait_recv()

        for s in mine:
            arrived(ctx, s)
            go(ctx, s, section, x_ctx)
            go(ctx, s, section, y_ctx)
            go(ctx, s, 1 - section, ctx)
        arrived(x_ctx, mine[0])
        go(x_ctx, mine[0], section, y_ctx)
        go(x_ctx, mine[0], 1 - section, ctx)
        arrived(y_ctx, mine[0])
        go(y_ctx, mine[0], 1 - section, ctx)
        arrived(y_ctx, mine[1])
        go(y_ctx, mine[1], section, x_ctx)
        go(y_ctx, mine[1], 1 - section, ctx)
        arrived(x_ctx, mine[1])
        go(x_ctx, mine[1], 1 - section, ctx)
        for s in mine:
            arrived(d_ctx, s)
            go(d_ctx, s, 1 - section, ctx)
        for c in (ctx, x_ctx, y_ctx, d_ctx):
            for j in range(2):
                arrived(c, 2 * section + j)
        for s in range(4):
            pltpu.make_async_copy(norm_ref, norm_all.at[s], norm_recv.at[s]).wait()
        norms[...] = (norm_all[0] + norm_all[1]) + (norm_all[2] + norm_all[3])
        return started

    def hop_copy(u):
        rows = pl.ds(u * size, size)
        return remote(lea.at[rows], ent.at[rows], hop_send.at[u], hop_recv.at[u], section, ctx, shard + 1)

    def hop_wait(u):
        rows = pl.ds(u * size, size)
        remote(lea.at[rows], ent.at[rows], hop_send.at[u], hop_recv.at[u], section, ctx, shard).wait_recv()

    def weight(c, columns):
        value = w[c, :, :, pl.ds(0, columns)]
        return value.reshape(value.shape[0] * value.shape[1], columns)

    def saves(u, pairs):
        rows = pl.ds(u * size, size)
        copies = []
        for index, (src, dst) in enumerate(pairs):
            if len(src.shape) == 3:
                copies.append(pltpu.make_async_copy(src.at[:, rows], dst.at[:, rows], save.at[index, u]))
            else:
                copies.append(pltpu.make_async_copy(src.at[rows], dst.at[rows], save.at[index, u]))
        return copies

    norm_save = pltpu.make_async_copy(norms, norm_out, keep.at[1])

    @pl.when(kind == 0)
    def _():
        started = collect(attn_cols)
        norm_save.start()
        w_save = pltpu.make_async_copy(w.at[:, :, :, attn_cols], w_attn_out, keep.at[0])
        w_save.start()

        @pl.when(shard == 0)
        def _():
            for c in range(4):
                pltpu.make_async_copy(x_ref, x_all.at[c], token_recv.at[c]).wait()

        lse[...] = jnp.zeros_like(lse)
        gain, bias = norms[0:1, :width], norms[2:3, :width]
        pairs = ((ent, ent_out), (nrm, nrm_out), (q, q_out), (k, k_out), (k1, k1_out), (v, v_out), (v1, v1_out), (o, o_out), (lse, lse_out))
        for u in range(chunks):
            rows = pl.ds(u * size, size)

            @pl.when(shard == 0)
            def _():
                first = 2 * (u % 2)
                ent[rows] = x_all[first : first + 2, u // 2].reshape(size, width)

            @pl.when(shard > 0)
            def _():
                hop_wait(u)

            hat, _ = normalised(ent[rows].astype(f32))
            normed = (hat * gain + bias).astype(bf16)
            nrm[rows] = normed
            k[rows] = mm(normed, weight(1, wide)).astype(bf16)
            v[rows] = mm(normed, weight(2, wide)).astype(bf16)
            swaps = [
                remote(src.at[rows], dst.at[rows], swap_send.at[which, u], swap_recv.at[which, u], 1 - section, ctx, shard)
                for which, (src, dst) in enumerate(((k, k1), (v, v1)))
            ]
            for copy in swaps:
                copy.start()
            q[rows] = (mm(normed, weight(0, wide)) * score_scale).astype(bf16)
            for copy in swaps:
                copy.wait_recv()
            attend_chunk(u, rows, mask_ref, q, k, k1, v, v1, o, lse)
            out = mm(o[rows, :width].astype(bf16), weight(3, wide))[:, :width]
            lea[rows] = (ent[rows].astype(f32) + out).astype(bf16)
            hop_copy(u).start()
            for copy in saves(u, pairs):
                copy.start()
        for u in range(chunks):
            rows = pl.ds(u * size, size)
            for which, (src, dst) in enumerate(((k, k1), (v, v1))):
                remote(
                    src.at[rows], dst.at[rows], swap_send.at[which, u], swap_recv.at[which, u], 1 - section, ctx, shard
                ).wait_send()
            hop_copy(u).wait_send()
            for copy in saves(u, pairs):
                copy.wait()
        w_save.wait()
        norm_save.wait()
        for copy in started:
            copy.wait_send()

    @pl.when(kind == 1)
    def _():
        started = collect(ff_cols)
        norm_save.start()
        w_save = pltpu.make_async_copy(w, w_ff_out, keep.at[0])
        w_save.start()
        gain, bias = norms[1:2, :width], norms[3:4, :width]
        pairs = ((ent, ent_out), (nrm, nrm_out), (lea, lea_out), (up, up_out), (hid, hid_out))
        for u in range(chunks):
            rows = pl.ds(u * size, size)
            hop_wait(u)
            hat, _ = normalised(ent[rows].astype(f32))
            normed = (hat * gain + bias).astype(bf16)
            nrm[rows] = normed
            total = ent[rows].astype(f32)
            for i in range(2):
                upper = mm(normed, weight(i, ff_ref.shape[1]))
                up[i, rows] = upper
                hidden = jax.nn.gelu(upper, approximate=True).astype(bf16)
                hid[i, rows] = hidden
                total = total + mm_t(hidden, weight(2 + i, ff_ref.shape[1]))
            lea[rows] = total.astype(bf16)

            @pl.when(shard < 3)
            def _():
                hop_copy(u).start()

            for copy in saves(u, pairs):
                copy.start()
        for u in range(chunks):

            @pl.when(shard < 3)
            def _():
                hop_copy(u).wait_send()

            for copy in saves(u, pairs):
                copy.wait()
        w_save.wait()
        norm_save.wait()
        for copy in started:
            copy.wait_send()

    for c in range(4):

        @pl.when((shard == 3) & jnp.logical_not((ctx == 3) & (c == 3)))
        def _():
            remote(g_ref, g_all_ref.at[c], token_send.at[1], token_recv.at[c], section, ctx, shard).wait_recv()

    @pl.when(jnp.logical_not(x_stays))
    def _():
        x_copy.wait_send()

    @pl.when(jnp.logical_not(g_stays))
    def _():
        g_copy.wait_send()

    attn_copy.wait_send()
    ff_copy.wait_send()
    for copy, stays in norm_copies:

        @pl.when(jnp.logical_not(stays))
        def _():
            copy.wait_send()


def forward_relay(attn_piece, ff_piece, x_own, g_own, norm_own, mask):
    share, ff_half = ff_piece.shape
    wide = attn_piece.shape[1]
    blocks, half, width = x_own.shape
    tokens = blocks * 4 * half
    chunks = tokens // (2 * half)
    dma = pltpu.SemaphoreType.DMA
    vmem = pl.BlockSpec(memory_space=pltpu.VMEM)
    state = [
        ((tokens, width), bf16), ((tokens, width), bf16),
        ((tokens, wide), bf16), ((tokens, wide), bf16), ((tokens, wide), bf16), ((tokens, wide), bf16), ((tokens, wide), bf16),
        ((tokens, wide), f32), ((tokens, LANES), f32),
        ((2, tokens, ff_half), f32), ((2, tokens, ff_half), bf16), ((tokens, width), bf16),
    ]
    outs = [
        ((4, 4, share, wide), bf16), ((4, 4, share, ff_half), bf16), ((4,) + g_own.shape, bf16), (norm_own.shape, f32),
    ] + state
    return pl.pallas_call(
        forward_kernel,
        in_specs=[ANY] * 5 + [vmem],
        out_specs=[ANY] * len(outs),
        out_shape=[jax.ShapeDtypeStruct(s, t) for s, t in outs],
        scratch_shapes=[
            pltpu.VMEM((4, 4, share, ff_half), bf16),
            pltpu.VMEM((4,) + x_own.shape, bf16),
            pltpu.VMEM((4,) + norm_own.shape, f32),
            pltpu.VMEM(norm_own.shape, f32),
        ]
        + [pltpu.VMEM(s, t) for s, t in state]
        + [
            dma((14,)), dma((4, 4)), dma((2,)), dma((4,)), dma((4,)), dma((4,)), dma((2,)),
            dma((chunks,)), dma((chunks,)), dma((2, chunks)), dma((2, chunks)), dma((9, chunks)), dma((2,)),
        ],
        compiler_params=pltpu.CompilerParams(has_side_effects=True, vmem_limit_bytes=62 * 2**20),
        name="forward_relay",
    )(attn_piece, ff_piece, x_own, g_own, norm_own, mask)


def add_into(total, term):
    total[...] = (total[...].astype(f32) + term[...].astype(f32)).astype(bf16)


def backward_kernel(
    w_attn_ref, w_ff_ref, g_ref, norm_ref, mask_ref, place_ref,
    ent_ref, nrm_ref, q_ref, k_ref, k1_ref, v_ref, v1_ref, o_ref, lse_ref, up_ref, hid_ref, y_ref,
    attn_out, ff_out, rows_out, sums_out,
    w, coming, leaving, ent, slots, o, lse, da, take, big, sums, sums_in, spread, first, second, third,
    load, hop_send, hop_recv, swap_send, swap_recv, rows_send, rows_recv, free,
    sums_send, sums_recv, first_send, first_recv, second_send, second_recv, third_send, third_recv, last_send, last_recv,
):
    section, ctx, shard = lax.axis_index("section"), lax.axis_index("ctx"), lax.axis_index("shard")
    kind = lax.rem(shard, 2)
    width = ent.shape[1]
    wide = da.shape[1]
    half = da.shape[0] // 2
    x_ctx, y_ctx = near_ctx(ctx, 1), near_ctx(ctx, 2)
    d_ctx = near_ctx(x_ctx, 2)
    size = da.shape[0]
    chunks = ent.shape[0] // size
    ff_half = w_ff_ref.shape[3]
    parts = ((0, wide), (wide, ff_half - wide))
    order = range(chunks - 1, -1, -1)

    def weight(c, start, columns):
        value = w[c, :, :, pl.ds(start, columns)]
        return value.reshape(value.shape[0] * value.shape[1], columns)

    def hop_copy(u):
        rows = pl.ds(u * size, size)
        return remote(leaving.at[rows], coming.at[rows], hop_send.at[u], hop_recv.at[u], section, ctx, shard - 1)

    def hop_wait(u):
        rows = pl.ds(u * size, size)
        remote(leaving.at[rows], coming.at[rows], hop_send.at[u], hop_recv.at[u], section, ctx, shard).wait_recv()

    def rows_copy(src, t, local):
        block, c = t // 4, t % 4
        src = src.at[pl.ds(t * half, half)]
        dst = rows_out.at[kind, block, pl.ds(pl.multiple_of(section * half, half), half)]
        recv = rows_recv.at[kind, section, block]
        if local:
            return pltpu.make_async_copy(src, dst, recv)
        return remote(src, dst, rows_send.at[t], recv, shard // 2, c, ctx)

    def rows_stay(t):
        return (section == shard // 2) & (ctx == t % 4) & (ctx == shard)

    def rows_start(src, t):
        @pl.when(rows_stay(t))
        def _():
            rows_copy(src, t, True).start()

        @pl.when(jnp.logical_not(rows_stay(t)))
        def _():
            rows_copy(src, t, False).start()

    def rows_finish(src):
        for t in range(2 * chunks):

            @pl.when(jnp.logical_not(rows_stay(t)))
            def _():
                rows_copy(src, t, False).wait_send()

    def finish_chunk(rows, d_normed, gain):
        hat, scale = normalised(ent[rows].astype(f32))
        sums[0:1, :width] += jnp.sum(d_normed * hat, axis=0, keepdims=True)
        sums[1:2, :width] += jnp.sum(d_normed, axis=0, keepdims=True)
        total = coming[rows].astype(f32) + norm_backward(hat, scale, gain, d_normed)
        leaving[rows] = total.astype(bf16)

    sums[...] = jnp.zeros_like(sums)
    ent_load = pltpu.make_async_copy(ent_ref, ent, load.at[0])
    ent_load.start()

    nrm_load = pltpu.make_async_copy(nrm_ref, ent, load.at[9])

    def group_columns(index, value):
        columns = spread.shape[3]
        feature = lax.broadcasted_iota(jnp.int32, (width, LANES), 0)
        for side in range(2):
            for start in range(0, columns, LANES):
                chosen = feature == place_ref[side, 0:1, start : start + LANES]
                value_now = mm(value, jnp.where(chosen, 1.0, 0.0).astype(bf16))
                spread[index, side, :, start : start + LANES] = value_now.astype(bf16)

    def reduce(arrays, columns_all, out_ref, which, later_loads):
        rows = first.shape[3]
        cols_all = pl.ds(0, columns_all)
        count = len(arrays)
        gap = up_to(rows, 16)
        own = lambda i, c, j: w.at[i, c, pl.ds(gap * j, rows), cols_all]

        def terms(i, side):
            _, index, pieces = arrays[i]
            grouped = spread.at[index, side, :, pl.ds(0, 8 * rows)]

            def store(value, cols):
                for n in range(8):
                    part = value[n * rows : (n + 1) * rows].astype(bf16)
                    if side == 0:
                        w[2 * (i % 2) + n % 2, n // 2, pl.ds(2 * gap, rows), cols] = part
                    else:
                        w[i, n // 2, pl.ds(gap * (n % 2), rows), cols] = part

            for ref, columns, start in pieces:
                step = 2 * LANES

                @pl.loop(0, columns // step)
                def _(b):
                    at = pl.multiple_of(b * step, step)
                    store(t_mm(grouped[...], ref[:, pl.ds(at, step)]), pl.ds(pl.multiple_of(start + at, LANES), step))

                rest = columns % step
                if rest:
                    at = columns - rest
                    store(t_mm(grouped[...], ref[:, pl.ds(at, rest)]), pl.ds(start + at, rest))

        def first_copy(i, j):
            return remote(
                w.at[2 * (i % 2) + j, :, pl.ds(2 * gap, rows), cols_all], first.at[i % 2, j, :, :, cols_all],
                first_send.at[i, j], first_recv.at[i, j], 1 - section, ctx, shard,
            )

        def second_copy(i, j, part):
            to = (x_ctx, y_ctx)[j]
            return remote(
                own(i, (to, d_ctx)[part], j), second.at[i, j, part, :, cols_all],
                second_send.at[i, j, part], second_recv.at[i, j, part], section, to, shard,
            )

        def third_copy(i, j):
            to = (y_ctx, x_ctx)[j]
            return remote(
                own(i, to, j), third.at[i, j, :, cols_all], third_send.at[i, j], third_recv.at[i, j], section, to, shard
            )

        def last_copy(i, j):
            return remote(
                own(i, ctx, j), out_ref.at[arrays[i][0]], last_send.at[i, j], last_recv.at[which, arrays[i][0]],
                shard // 2, ctx, 2 * (1 - section) + j,
            )

        def sums_copy(step):
            to_core, to_ctx = ((1 - section, ctx), (section, x_ctx), (section, y_ctx))[step]
            return remote(sums, sums_in.at[step], sums_send.at[step], sums_recv.at[step], to_core, to_ctx, shard)

        def sums_last(j):
            return remote(
                sums, sums_out.at[which], sums_send.at[3 + j], sums_recv.at[3 + which],
                shard // 2, ctx, 2 * (1 - section) + j,
            )

        sums_copy(0).start()
        for step in range(count + 2):
            i = step
            if i < count:
                if i >= 2:
                    for j in range(2):
                        first_copy(i - 2, j).wait_send()
                if later_loads is not None and i == count - 1:
                    for copy in later_loads:
                        copy.wait()
                terms(i, 0)
                if i >= 2:
                    pl.semaphore_wait(free, 1)
                for j in range(2):
                    first_copy(i, j).start()
                terms(i, 1)
                if later_loads is not None and i == 0:
                    for copy in later_loads:
                        copy.start()
                for j in range(2):
                    first_copy(i, j).wait_recv()

                    @pl.loop(0, 4)
                    def _(c):
                        add_into(own(i, c, j), first.at[i % 2, j, c, :, cols_all])

                if i + 2 < count:
                    pl.semaphore_signal(
                        free, inc=1, device_id=(1 - section, ctx, shard), device_id_type=pl.DeviceIdType.MESH
                    )
                for part in (1, 0):
                    for j in range(2):
                        second_copy(i, j, part).start()
            i = step - 1
            if 0 <= i < count:
                for j in range(2):
                    second_copy(i, j, 1).wait_recv()
                    add_into(own(i, (y_ctx, x_ctx)[j], j), second.at[i, j, 1, :, cols_all])
                    third_copy(i, j).start()
                for j in range(2):
                    second_copy(i, j, 0).wait_recv()
                    add_into(own(i, ctx, j), second.at[i, j, 0, :, cols_all])
            i = step - 2
            if 0 <= i < count:
                for j in range(2):
                    third_copy(i, j).wait_recv()
                    add_into(own(i, ctx, j), third.at[i, j, :, cols_all])
                    last_copy(i, j).start()
            if step < 3:
                sums_copy(step).wait()
                sums[...] += sums_in[step]
                if step < 2:
                    sums_copy(step + 1).start()
                else:
                    for j in range(2):
                        sums_last(j).start()
        for i in range(count):
            for j in range(2):
                if i >= count - 2:
                    first_copy(i, j).wait_send()
                for part in range(2):
                    second_copy(i, j, part).wait_send()
                third_copy(i, j).wait_send()
                last_copy(i, j).wait_send()
        for j in range(2):
            sums_last(j).wait_send()

    @pl.when(kind == 0)
    def _():
        loads = [pltpu.make_async_copy(w_attn_ref, w.at[:, :, :, pl.ds(0, wide)], load.at[1])]
        for i, ref in enumerate((q_ref, k_ref, k1_ref, v_ref, v1_ref)):
            loads.append(pltpu.make_async_copy(ref, slots.at[i], load.at[2 + i]))
        loads.append(pltpu.make_async_copy(o_ref, o, load.at[7]))
        loads.append(pltpu.make_async_copy(lse_ref, lse, load.at[8]))
        for copy in loads:
            copy.start()
        for copy in loads:
            copy.wait()
        ent_load.wait()
        gain = norm_ref[0:1, :width]
        lane = lax.broadcasted_iota(jnp.int32, (size, LANES), 1)
        low = lane < HEAD
        da[...] = jnp.zeros_like(da)

        def swap_copy(which, u):
            rows = pl.ds(u * size, size)
            return remote(
                slots.at[2 + 2 * which, rows], take.at[which, rows], swap_send.at[which, u], swap_recv.at[which, u],
                1 - section, ctx, shard,
            )

        for u in order:
            rows = pl.ds(u * size, size)
            keys = pl.ds(0, (u + 1) * size)
            hop_wait(u)
            da[:, :width] = mm_t(coming[rows], weight(3, 0, width)).astype(bf16)

            @pl.loop(0, wide // LANES)
            def _(pair):
                cols = pl.ds(pl.multiple_of(pair * LANES, LANES), LANES)
                q2 = stack_heads(slots[0, rows, cols], low)
                grad = da[:, cols]
                a2 = stack_heads(grad, low)
                level = lse[rows, :]
                product = grad.astype(f32) * o[rows, cols]
                column = lambda which: jnp.sum(jnp.where(lane == 2 * pair + which, level, 0.0), axis=1, keepdims=True)
                level2 = jnp.concatenate([column(0), column(1)], axis=0)
                delta2 = jnp.concatenate(
                    [
                        jnp.sum(jnp.where(low, product, 0.0), axis=1, keepdims=True),
                        jnp.sum(jnp.where(low, 0.0, product), axis=1, keepdims=True),
                    ],
                    axis=0,
                )
                dq2 = 0.0
                for part in range(2):
                    keys_now, values_now = slots[1 + part, keys, cols], slots[3 + part, keys, cols]
                    p = jnp.exp(mask_last(mm_t(q2, keys_now), mask_ref[part]) - level2)
                    ds = (p * (mm_t(a2, values_now) - delta2)).astype(bf16)
                    dq2 = dq2 + mm(ds, keys_now)
                    d_keys, d_values = t_mm(ds, q2), t_mm(p.astype(bf16), a2)
                    if u == chunks - 1:
                        big[2 * part, keys, cols] = d_keys
                        big[2 * part + 1, keys, cols] = d_values
                    else:
                        big[2 * part, keys, cols] += d_keys
                        big[2 * part + 1, keys, cols] += d_values
                slots[0, rows, cols] = (unstack_heads(dq2, low) * score_scale).astype(bf16)

            for which in range(2):
                slots[2 + 2 * which, rows] = big[2 + which, rows].astype(bf16)
                swap_copy(which, u).start()
            d_normed = mm_t(slots[0, rows], weight(0, 0, wide))
            for which, index in enumerate((1, 3)):
                swap_copy(which, u).wait_recv()
                slots[index, rows] = (big[which, rows] + take[which, rows].astype(f32)).astype(bf16)
                d_normed = d_normed + mm_t(slots[index, rows], weight(1 + which, 0, wide))
            finish_chunk(rows, d_normed, gain)

            @pl.when(shard > 0)
            def _():
                hop_copy(u).start()

            for t in (2 * u, 2 * u + 1):
                rows_start(leaving, t)
        for u in order:
            for which in range(2):
                swap_copy(which, u).wait_send()
        nrm_load.start()
        group_columns(1, o[:, :width].astype(bf16))
        nrm_load.wait()
        group_columns(0, ent[...])
        whole = lambda index: ((slots.at[index], wide, 0),)
        reduce(
            ((3, 1, ((coming, width, 0),)), (0, 0, whole(0)), (1, 0, whole(1)), (2, 0, whole(3))), wide, attn_out, 0, None
        )
        rows_finish(leaving)
        for u in order:

            @pl.when(shard > 0)
            def _():
                hop_copy(u).wait_send()

    @pl.when(kind == 1)
    def _():
        loads = [pltpu.make_async_copy(w_ff_ref, w, load.at[1])]
        for i in range(2):
            for part, (start, columns) in enumerate(parts):
                loads.append(
                    pltpu.make_async_copy(
                        up_ref.at[i, :, pl.ds(start, columns)], big.at[2 * i + part, :, pl.ds(0, columns)], load.at[2 + 2 * i + part]
                    )
                )
        g_load = pltpu.make_async_copy(g_ref, coming, load.at[6])

        def hidden_loads(i):
            return [
                pltpu.make_async_copy(
                    hid_ref.at[i, :, pl.ds(start, columns)], take.at[part, :, pl.ds(0, columns)], load.at[7 + part]
                )
                for part, (start, columns) in enumerate(parts)
            ]

        for t in range(2 * chunks):
            rows_start(y_ref, t)

        @pl.when(shard == 3)
        def _():
            g_load.start()

        for copy in loads + hidden_loads(0):
            copy.start()
        for copy in loads:
            copy.wait()

        @pl.when(shard == 3)
        def _():
            g_load.wait()

        ent_load.wait()
        gain = norm_ref[1:2, :width]
        for u in order:
            rows = pl.ds(u * size, size)

            @pl.when(shard < 3)
            def _():
                hop_wait(u)

            grad = coming[rows]
            d_normed = 0.0
            for i in range(2):
                for part, (start, columns) in enumerate(parts):
                    cols = pl.ds(0, columns)
                    d_hidden = mm(grad, weight(2 + i, start, columns))
                    _, back = jax.vjp(lambda value: jax.nn.gelu(value, approximate=True), big[2 * i + part, rows, cols])
                    d_upper = back(d_hidden)[0].astype(bf16)
                    slots[2 * i + part, rows, cols] = d_upper
                    d_normed = d_normed + mm_t(d_upper, weight(i, start, columns))
            finish_chunk(rows, d_normed, gain)
            hop_copy(u).start()
        nrm_load.start()
        group_columns(1, coming[...])
        nrm_load.wait()
        group_columns(0, ent[...])
        for copy in hidden_loads(0):
            copy.wait()
        upper = lambda i: tuple((slots.at[2 * i + p], columns, start) for p, (start, columns) in enumerate(parts))
        hidden = tuple((take.at[p], columns, start) for p, (start, columns) in enumerate(parts))
        reduce(((2, 1, hidden), (0, 0, upper(0)), (1, 0, upper(1)), (3, 1, hidden)), ff_half, ff_out, 1, hidden_loads(1))
        rows_finish(y_ref)
        for u in order:
            hop_copy(u).wait_send()

    for index in range(attn_out.shape[0]):
        for which, ref in enumerate((attn_out, ff_out)):
            remote(
                ref.at[index], ref.at[index], last_send.at[index, 0], last_recv.at[which, index], section, ctx, shard
            ).wait_recv()
    for which in range(2):
        remote(sums, sums_out.at[which], sums_send.at[3], sums_recv.at[3 + which], section, ctx, shard).wait_recv()
        for core in range(2):
            for block in range(2):
                ref = rows_out.at[which, block, pl.ds(core * half, half)]
                pltpu.make_async_copy(ref, ref, rows_recv.at[which, core, block]).wait()


def backward_relay(w_attn, w_ff, g, norms, mask, place, ent, nrm, q, k, k1, v, v1, o, lse, up, hid, y, group_pad):
    tokens, width = ent.shape
    wide = q.shape[1]
    size = mask.shape[2]
    chunks = tokens // size
    ff_half = up.shape[2]
    dma = pltpu.SemaphoreType.DMA
    vmem = pl.BlockSpec(memory_space=pltpu.VMEM)
    narrow = ((tokens, width), bf16)
    outs = [
        ((4, group_pad, wide), bf16), ((4, group_pad, ff_half), bf16), ((2, 2, size, width), bf16), ((2,) + norms.shape, f32),
    ]
    scratch = [
        ((4,) + w_ff.shape[1:], bf16), narrow, narrow, narrow, ((5, tokens, wide), bf16),
        (o.shape, f32), (lse.shape, f32), ((size, wide), bf16), ((2, tokens, wide), bf16), ((4, tokens, wide), f32),
        (norms.shape, f32), ((3,) + norms.shape, f32), ((2, 2, tokens, place.shape[2]), bf16),
        ((2, 2, 4, group_pad, ff_half), bf16), ((4, 2, 2, group_pad, ff_half), bf16), ((4, 2, group_pad, ff_half), bf16),
    ]
    return pl.pallas_call(
        backward_kernel,
        in_specs=[ANY] * 3 + [vmem] * 3 + [ANY] * 12,
        out_specs=[ANY] * len(outs),
        out_shape=[jax.ShapeDtypeStruct(s, t) for s, t in outs],
        scratch_shapes=[pltpu.VMEM(s, t) for s, t in scratch]
        + [
            dma((10,)), dma((chunks,)), dma((chunks,)), dma((2, chunks)), dma((2, chunks)),
            dma((2 * chunks,)), dma((2, 2, 2)), pltpu.SemaphoreType.REGULAR,
            dma((5,)), dma((5,)), dma((4, 2)), dma((4, 2)), dma((4, 2, 2)), dma((4, 2, 2)), dma((4, 2)), dma((4, 2)),
            dma((4, 2)), dma((2, 4)),
        ],
        compiler_params=pltpu.CompilerParams(has_side_effects=True, vmem_limit_bytes=62 * 2**20),
        name="backward_relay",
    )(w_attn, w_ff, g, norms, mask, place, ent, nrm, q, k, k1, v, v1, o, lse, up, hid, y)


def chain(inputs, cotangent, qkv_weight, out_weight, up_weight, down_weight, norm_gain, norm_bias):
    section, ctx, shard = lax.axis_index("section"), lax.axis_index("ctx"), lax.axis_index("shard")
    seq_count, blocks, slice_len, width = inputs.shape
    half = slice_len // 2
    tokens = blocks * 4 * half
    share = width // 4
    group = share // 4
    group_pad = up_to(group, ROWS)
    wide = up_to(width, LANES)
    ff = up_weight.shape[2]
    is_attn = shard % 2 == 0

    pad = lambda w: jnp.pad(w, ((0, 0), (0, wide - width)))
    own_qkv, own_out = qkv_weight[0], out_weight[0]
    attn_src = jnp.stack([pad(own_qkv[:, i * width : (i + 1) * width]) for i in range(3)] + [pad(own_out)])
    down_t = down_weight[0].T
    up0 = up_weight[0]
    ff_src = jnp.stack([up0[:, : ff // 2], up0[:, ff // 2 :], down_t[:, : ff // 2], down_t[:, ff // 2 :]])
    norm_own = jnp.concatenate([norm_gain[0], norm_bias[0]], axis=0).astype(f32)
    norm_own = lax.dynamic_update_slice(
        jnp.zeros((ROWS, wide), f32), jnp.pad(norm_own, ((0, ROWS - 4), (0, 0))), (0, shard * share)
    )
    x_own = lax.dynamic_slice_in_dim(inputs[0], section * half, half, 1)
    g_own = lax.dynamic_slice_in_dim(cotangent[0], section * half, half, 1)
    mask = attention_masks(section, half)
    mask = jnp.concatenate([mask, mask], axis=1)
    w_attn, w_ff, g_all, norms, ent, nrm, q, k, k1, v, v1, o, lse, up, hid, y = forward_relay(
        lax.dynamic_index_in_dim(attn_src, ctx, 0, keepdims=False),
        lax.dynamic_index_in_dim(ff_src, ctx, 0, keepdims=False),
        x_own, g_own, norm_own, mask,
    )
    own_place = jnp.arange(4)[:, None, None]

    def bring_tokens(every, own):
        mine = jnp.where((own_place[..., None] == ctx) & (shard == ctx), own, every)
        return jnp.swapaxes(mine, 0, 1).reshape(tokens, width)

    g_last = bring_tokens(g_all, g_own)
    slot = jnp.arange(up_to(8 * group_pad, LANES))
    row = slot % group_pad
    place = []
    for side in (section, 1 - section):
        owner = (slot // (2 * group_pad)) * 4 + 2 * side + (slot // group_pad) % 2
        place.append(jnp.where((row < group) & (slot < 8 * group_pad), owner * group + row, -1))
    place = jnp.broadcast_to(jnp.stack(place)[:, None].astype(jnp.int32), (2, ROWS, slot.shape[0]))
    attn_sums, ff_sums, rows, totals = backward_relay(
        w_attn, w_ff, g_last, norms, mask, place, ent, nrm, q, k, k1, v, v1, o, lse, up, hid, y, group_pad
    )
    totals = lax.dynamic_slice_in_dim(totals[:, :2], (ctx * 4 + shard) * group, group, 2)
    attn_sums = attn_sums[:, :group, :width].astype(f32)
    ff_sums = ff_sums[:, :group].astype(f32)
    return (
        rows[1][None, None],
        rows[0][None, None],
        jnp.concatenate([attn_sums[0], attn_sums[1], attn_sums[2]], axis=1)[None],
        attn_sums[3][None],
        jnp.concatenate([ff_sums[0], ff_sums[1]], axis=1)[None],
        jnp.concatenate([ff_sums[2].T, ff_sums[3].T], axis=0)[None],
        totals[:, 0][None],
        totals[:, 1][None],
    )


def passed_along(value, axis, steps):
    count = lax.axis_size(axis)
    initial, last = (max(0, -steps), min(count, count - steps))
    return lax.ppermute(value, axis, [(source, source + steps) for source in range(initial, last)])


def layer_norm(values, gain, shift):
    mean = jnp.mean(values, axis=-1, keepdims=True)
    centred = values - mean
    var = jnp.mean(centred * centred, axis=-1, keepdims=True)
    return centred * lax.rsqrt(var + eps_norm) * gain + shift


def gelu_tanh(values):
    return jax.nn.gelu(values, approximate=True)


def split_pair(key_value, head_count):
    block_len, seq_count, double = key_value.shape
    model_width = double // 2
    key_rows = key_value[..., :model_width].reshape(block_len, seq_count, head_count, HEAD)
    value_rows = key_value[..., model_width:].reshape(block_len, seq_count, head_count, HEAD)
    return (key_rows, value_rows)


def causal_mask(query_pos, key_pos):
    return (key_pos[None, :] <= query_pos[:, None])[None, :, None, :]


def forward_block(running, queries, query_pos, key_value, key_pos):
    row_max, row_sum, accum = running
    key_rows, value_rows = split_pair(key_value, queries.shape[2])
    scores = (
        jnp.einsum("sqhe,kshe->sqhk", queries, key_rows, preferred_element_type=jnp.float32)
        * score_scale
    )
    causal = causal_mask(query_pos, key_pos)
    new_max = jnp.maximum(row_max, jnp.max(jnp.where(causal, scores, -1e30), axis=-1))
    softmax_w = jnp.where(causal, jnp.exp(scores - new_max[..., None]), 0.0)
    factor = jnp.exp(row_max - new_max)
    row_sum = row_sum * factor + jnp.sum(softmax_w, axis=-1)
    accum = accum * factor[..., None] + jnp.einsum(
        "sqhk,kshe->sqhe",
        softmax_w.astype(jnp.bfloat16),
        value_rows,
        preferred_element_type=jnp.float32,
    )
    return (new_max, row_sum, accum)


def split_rows(whole):
    key_count = whole.shape[0]
    block_size = 512
    blocks = whole.reshape((key_count // block_size, block_size) + whole.shape[1:])
    offsets = jnp.arange(key_count // block_size, dtype=jnp.int32) * block_size
    return (blocks, offsets, block_size)


def fold_keys(running, piece, start, queries, query_pos, group_len):
    blocks, offsets, block_size = split_rows(piece)

    def fold_scan_step(inner, scan_item):
        block_rows, offset = scan_item
        for group_id in range(block_rows.shape[2]):
            key_pos = (
                group_id * group_len + start + offset + jnp.arange(block_size, dtype=jnp.int32)
            )
            inner = forward_block(inner, queries, query_pos, block_rows[:, :, group_id], key_pos)
        return (inner, None)

    result, _ = lax.scan(fold_scan_step, running, (blocks, offsets))
    return result


def pair_terms(d_scores, softmax_w, queries, d_attended, block_size):
    d_keys = (
        jnp.einsum("sqhk,sqhe->kshe", d_scores, queries, preferred_element_type=jnp.float32)
        * score_scale
    )
    d_values = jnp.einsum(
        "sqhk,sqhe->kshe",
        softmax_w.astype(jnp.bfloat16),
        d_attended,
        preferred_element_type=jnp.float32,
    )
    shape = (block_size, queries.shape[0], queries.shape[2] * queries.shape[3])
    return jnp.concatenate([d_keys.reshape(shape), d_values.reshape(shape)], axis=-1)


def score_grads(
    queries, query_pos, log_total, row_delta, d_attended, key_rows, value_rows, key_pos
):
    scores = (
        jnp.einsum("sqhe,kshe->sqhk", queries, key_rows, preferred_element_type=jnp.float32)
        * score_scale
    )
    causal = causal_mask(query_pos, key_pos)
    softmax_w = jnp.where(causal, jnp.exp(scores - log_total[..., None]), 0.0)
    d_probs = jnp.einsum(
        "sqhe,kshe->sqhk", d_attended, value_rows, preferred_element_type=jnp.float32
    )
    d_scores = (softmax_w * (d_probs - row_delta[..., None])).astype(jnp.bfloat16)
    return (softmax_w, d_scores)


def backward_keys(whole, queries, query_pos, log_total, row_delta, d_attended, group_len):
    blocks, offsets, block_size = split_rows(whole)

    def backward_scan_step(d_queries, scan_item):
        block_rows, offset = scan_item
        for group_id in range(block_rows.shape[2]):
            key_pos = group_id * group_len + offset + jnp.arange(block_size, dtype=jnp.int32)
            key_rows, value_rows = split_pair(block_rows[:, :, group_id], queries.shape[2])
            softmax_w, d_scores = score_grads(
                queries, query_pos, log_total, row_delta, d_attended, key_rows, value_rows, key_pos
            )
            d_queries = (
                d_queries
                + jnp.einsum(
                    "sqhk,kshe->sqhe", d_scores, key_rows, preferred_element_type=jnp.float32
                )
                * score_scale
            )
        return (d_queries, None)

    d_queries, terms = lax.scan(
        backward_scan_step, jnp.zeros(queries.shape, jnp.float32), (blocks, offsets)
    )
    return (d_queries, None)


def owner_terms(
    own_cache, all_queries, all_d_att, all_totals, all_deltas, micro_index, ctx_id, group_len
):
    block_len, seq_count, group_count, double = own_cache.shape
    head_count = all_queries.shape[2]
    query_rows = all_queries.shape[1]
    query_size = 512
    block_count = query_rows // query_size

    def loop_step(index, total):
        offset = index * query_size
        q_block = lax.dynamic_slice_in_dim(all_queries, offset, query_size, 1)
        d_block = lax.dynamic_slice_in_dim(all_d_att, offset, query_size, 1)
        t_block = lax.dynamic_slice_in_dim(all_totals, offset, query_size, 1)
        r_block = lax.dynamic_slice_in_dim(all_deltas, offset, query_size, 1)
        query_pos = micro_index * group_len + offset + jnp.arange(query_size, dtype=jnp.int32)
        pieces = []
        for group_id in range(group_count):
            key_pos = (
                group_id * group_len + ctx_id * block_len + jnp.arange(block_len, dtype=jnp.int32)
            )
            key_rows, value_rows = split_pair(own_cache[:, :, group_id], head_count)
            softmax_w, d_scores = score_grads(
                q_block, query_pos, t_block, r_block, d_block, key_rows, value_rows, key_pos
            )
            pieces.append(pair_terms(d_scores, softmax_w, q_block, d_block, block_len))
        return total + jnp.stack(pieces, axis=2)

    return lax.fori_loop(0, block_count, loop_step, jnp.zeros(own_cache.shape, jnp.float32))


def store_at(store, value, micro_index, active):
    updated = lax.dynamic_update_index_in_dim(store, value, micro_index, 0)
    return jnp.where(active, updated, store)


def shards(inputs, cotangent, qkv_weight, out_weight, up_weight, down_weight, norm_gain, norm_bias):
    section_id = lax.axis_index("section")
    ctx_count = lax.axis_size("ctx")
    ctx_id = lax.axis_index("ctx")
    seq_count, group_count, block_len, model_width = inputs.shape
    head_count = model_width // HEAD
    group_len = block_len * ctx_count
    row_count = seq_count * block_len
    w_qkv, w_out, w_up, w_down, gains, biases = (
        lax.all_gather(qkv_weight[0], "shard", axis=0, tiled=True),
        lax.all_gather(out_weight[0], "shard", axis=0, tiled=True),
        lax.all_gather(up_weight[0], "shard", axis=0, tiled=True),
        lax.all_gather(down_weight[0], "shard", axis=1, tiled=True),
        lax.all_gather(norm_gain[0], "shard", axis=1, tiled=True),
        lax.all_gather(norm_bias[0], "shard", axis=1, tiled=True),
    )
    gains = gains.astype(jnp.float32)
    biases = biases.astype(jnp.float32)
    ff_width = w_up.shape[1]
    cache = jnp.zeros((block_len, seq_count, group_count, 2 * model_width), jnp.bfloat16)
    in_store = jnp.zeros((group_count, seq_count, block_len, model_width), jnp.bfloat16)
    query_store = jnp.zeros((group_count, seq_count, block_len, head_count, HEAD), jnp.bfloat16)
    att_store = jnp.zeros((group_count, seq_count, block_len, head_count, HEAD), jnp.float32)
    total_store = jnp.zeros((group_count, seq_count, block_len, head_count), jnp.float32)
    middle_store = jnp.zeros((group_count, row_count, model_width), jnp.float32)
    upper_store = jnp.zeros((group_count, row_count, ff_width), jnp.float32)
    out_store = jnp.zeros((group_count, seq_count, block_len, model_width), jnp.bfloat16)
    received = jnp.zeros((seq_count, block_len, model_width), jnp.bfloat16)
    for tick_no in range(group_count + 1):
        micro = tick_no - section_id
        active = (micro >= 0) & (micro < group_count)
        micro_index = jnp.clip(micro, 0, group_count - 1)
        own_input = lax.dynamic_index_in_dim(inputs, micro_index, 1, keepdims=False)
        entering = jnp.where(section_id == 0, own_input, received)
        flat_rows = entering.reshape(row_count, model_width).astype(jnp.float32)
        normed = layer_norm(flat_rows, gains[0], biases[0]).astype(jnp.bfloat16)
        mixed = jnp.dot(normed, w_qkv, preferred_element_type=jnp.float32).astype(jnp.bfloat16)
        queries = mixed[:, :model_width].reshape(seq_count, block_len, head_count, HEAD)
        fresh = jnp.swapaxes(
            mixed[:, model_width:].reshape(seq_count, block_len, 2 * model_width), 0, 1
        )
        updated = lax.dynamic_update_index_in_dim(cache, fresh, micro_index, 2)
        cache = jnp.where(active, updated, cache)
        query_pos = (
            micro_index * group_len + ctx_id * block_len + jnp.arange(block_len, dtype=jnp.int32)
        )
        start_state = (
            jnp.full((seq_count, block_len, head_count), -1e30, jnp.float32),
            jnp.zeros((seq_count, block_len, head_count), jnp.float32),
            jnp.zeros((seq_count, block_len, head_count, HEAD), jnp.float32),
        )
        row_max, row_sum, accum = fold_keys(
            start_state,
            lax.all_gather(cache, "ctx", axis=0, tiled=True),
            jnp.int32(0),
            queries,
            query_pos,
            group_len,
        )
        attended = accum / row_sum[..., None]
        log_total = row_max + jnp.log(row_sum)
        att_low = attended.reshape(row_count, model_width).astype(jnp.bfloat16)
        middle = flat_rows + jnp.dot(att_low, w_out, preferred_element_type=jnp.float32)
        normed2 = layer_norm(middle, gains[1], biases[1]).astype(jnp.bfloat16)
        upper = jnp.dot(normed2, w_up, preferred_element_type=jnp.float32)
        hidden = gelu_tanh(upper).astype(jnp.bfloat16)
        leaving = (middle + jnp.dot(hidden, w_down, preferred_element_type=jnp.float32)).astype(
            jnp.bfloat16
        )
        leaving = leaving.reshape(seq_count, block_len, model_width)
        in_store = store_at(in_store, entering, micro_index, active)
        query_store = store_at(query_store, queries, micro_index, active)
        att_store = store_at(att_store, attended, micro_index, active)
        total_store = store_at(total_store, log_total, micro_index, active)
        middle_store = store_at(middle_store, middle, micro_index, active)
        upper_store = store_at(upper_store, upper, micro_index, active)
        out_store = store_at(out_store, leaving, micro_index, active)
        if tick_no < group_count:
            received = passed_along(leaving, "section", 1)
    key_acc = jnp.zeros((block_len, seq_count, group_count, 2 * model_width), jnp.float32)
    grad_qkv = jnp.zeros((model_width, 3 * model_width), jnp.float32)
    grad_out = jnp.zeros((model_width, model_width), jnp.float32)
    grad_up = jnp.zeros((model_width, ff_width), jnp.float32)
    grad_down = jnp.zeros((ff_width, model_width), jnp.float32)
    grad_gain = jnp.zeros((2, model_width), jnp.float32)
    grad_bias = jnp.zeros((2, model_width), jnp.float32)
    grad_store = jnp.zeros((group_count, seq_count, block_len, model_width), jnp.bfloat16)
    coming = jnp.zeros((seq_count, block_len, model_width), jnp.bfloat16)
    for tick_no in range(group_count + 1):
        micro = group_count - tick_no - section_id
        active = (micro >= 0) & (micro < group_count)
        active_weight = active.astype(jnp.float32)
        micro_index = jnp.clip(micro, 0, group_count - 1)
        own_cot = lax.dynamic_index_in_dim(cotangent, micro_index, 1, keepdims=False)
        d_out = (
            jnp.where(section_id == 1, own_cot, coming)
            .reshape(row_count, model_width)
            .astype(jnp.float32)
        )
        flat_rows = in_store[micro_index].reshape(row_count, model_width).astype(jnp.float32)
        queries = query_store[micro_index]
        attended = att_store[micro_index]
        log_total = total_store[micro_index]
        middle = middle_store[micro_index]
        upper = upper_store[micro_index]
        normed2_full, norm2_back = jax.vjp(
            lambda v, g, b: layer_norm(v, g, b), middle, gains[1], biases[1]
        )
        normed2 = normed2_full.astype(jnp.bfloat16)
        hidden_full, gelu_back = jax.vjp(gelu_tanh, upper)
        hidden = hidden_full.astype(jnp.bfloat16)
        d_branch = d_out.astype(jnp.bfloat16)
        grad_down = grad_down + active_weight * jnp.dot(
            hidden.T, d_branch, preferred_element_type=jnp.float32
        )
        d_hidden = jnp.dot(d_branch, w_down.T, preferred_element_type=jnp.float32)
        d_upper = gelu_back(d_hidden)[0].astype(jnp.bfloat16)
        grad_up = grad_up + active_weight * jnp.dot(
            normed2.T, d_upper, preferred_element_type=jnp.float32
        )
        d_normed2 = jnp.dot(d_upper, w_up.T, preferred_element_type=jnp.float32)
        d_mid_norm, d_gain2, d_bias2 = norm2_back(d_normed2)
        d_middle = d_out + d_mid_norm
        att_low = attended.reshape(row_count, model_width).astype(jnp.bfloat16)
        d_att = d_middle.astype(jnp.bfloat16)
        grad_out = grad_out + active_weight * jnp.dot(
            att_low.T, d_att, preferred_element_type=jnp.float32
        )
        d_attended = jnp.dot(d_att, w_out.T, preferred_element_type=jnp.float32).astype(
            jnp.bfloat16
        )
        d_attended = d_attended.reshape(seq_count, block_len, head_count, HEAD)
        row_delta = jnp.sum(d_attended.astype(jnp.float32) * attended, axis=-1)
        query_pos = (
            micro_index * group_len + ctx_id * block_len + jnp.arange(block_len, dtype=jnp.int32)
        )
        whole = lax.all_gather(cache, "ctx", axis=0, tiled=True)
        d_queries, unused = backward_keys(
            whole, queries, query_pos, log_total, row_delta, d_attended, group_len
        )
        all_queries, all_d_att = (
            lax.all_gather(queries, "ctx", axis=1, tiled=True),
            lax.all_gather(d_attended, "ctx", axis=1, tiled=True),
        )
        all_totals, all_deltas = (
            lax.all_gather(log_total, "ctx", axis=1, tiled=True),
            lax.all_gather(row_delta, "ctx", axis=1, tiled=True),
        )
        shares = owner_terms(
            cache, all_queries, all_d_att, all_totals, all_deltas, micro_index, ctx_id, group_len
        )
        key_acc = key_acc + active_weight * shares
        d_pair = jnp.swapaxes(
            lax.dynamic_index_in_dim(key_acc, micro_index, 2, keepdims=False), 0, 1
        )
        d_mixed = jnp.concatenate(
            [d_queries.reshape(row_count, model_width), d_pair.reshape(row_count, 2 * model_width)],
            axis=-1,
        ).astype(jnp.bfloat16)
        normed_full, norm1_back = jax.vjp(
            lambda v, g, b: layer_norm(v, g, b), flat_rows, gains[0], biases[0]
        )
        normed = normed_full.astype(jnp.bfloat16)
        grad_qkv = grad_qkv + active_weight * jnp.dot(
            normed.T, d_mixed, preferred_element_type=jnp.float32
        )
        d_normed = jnp.dot(d_mixed, w_qkv.T, preferred_element_type=jnp.float32)
        d_flat_norm, d_gain1, d_bias1 = norm1_back(d_normed)
        grad_gain = grad_gain + active_weight * jnp.stack([d_gain1, d_gain2])
        grad_bias = grad_bias + active_weight * jnp.stack([d_bias1, d_bias2])
        d_entering = (
            (d_middle + d_flat_norm).astype(jnp.bfloat16).reshape(seq_count, block_len, model_width)
        )
        grad_store = store_at(grad_store, d_entering, micro_index, active)
        if tick_no < group_count:
            coming = passed_along(d_entering, "section", -1)
    sums = (
        lax.psum_scatter(grad_qkv, ("ctx", "shard"), scatter_dimension=0, tiled=True),
        lax.psum_scatter(grad_out, ("ctx", "shard"), scatter_dimension=0, tiled=True),
        lax.psum_scatter(grad_up, ("ctx", "shard"), scatter_dimension=0, tiled=True),
        lax.psum_scatter(grad_down, ("ctx", "shard"), scatter_dimension=1, tiled=True),
        lax.psum_scatter(grad_gain, ("ctx", "shard"), scatter_dimension=1, tiled=True),
        lax.psum_scatter(grad_bias, ("ctx", "shard"), scatter_dimension=1, tiled=True),
    )
    layer_outputs = jnp.swapaxes(out_store, 0, 1)[None]
    input_grads = jnp.swapaxes(grad_store, 0, 1)[None]
    return (
        layer_outputs,
        input_grads,
        sums[0][None],
        sums[1][None],
        sums[2][None],
        sums[3][None],
        sums[4][None],
        sums[5][None],
    )


def solution(mesh):
    in_specs = (
        P("shard", None, "ctx", None),
        P("shard", None, "ctx", None),
        P("section", "shard", None),
        P("section", "shard", None),
        P("section", "shard", None),
        P("section", None, "shard"),
        P("section", None, "shard"),
        P("section", None, "shard"),
    )
    out_specs = (
        P("section", "shard", None, "ctx", None),
        P("section", "shard", None, "ctx", None),
        P("section", ("ctx", "shard"), None),
        P("section", ("ctx", "shard"), None),
        P("section", ("ctx", "shard"), None),
        P("section", None, ("ctx", "shard")),
        P("section", None, ("ctx", "shard")),
        P("section", None, ("ctx", "shard")),
    )
    relay = mesh.shape["section"] == 2 and mesh.shape["shard"] == 4 and mesh.shape["ctx"] == 4
    return jax.shard_map(chain if relay else shards, mesh=mesh, in_specs=in_specs, out_specs=out_specs, check_vma=False)
```

```python
import functools

import jax
import jax.numpy as jnp
from jax import lax
from jax.experimental import pallas as pl
from jax.experimental.pallas import tpu as pltpu
from jax.sharding import PartitionSpec as P

HEAD = 64
LANES = 128
ROWS = 8
NEG = -1e30
VMEM_BYTES = 66_900_000

eps_norm = 1e-05
score_scale = 0.125
f32 = jnp.float32
bf16 = jnp.bfloat16


def up_to(width, step):
    return -(-width // step) * step


def dot(a, b, dims):
    return lax.dot_general(a, b, (dims, ((), ())), preferred_element_type=f32)


def mm(a, b):
    return dot(a, b, ((1,), (0,)))


def mm_t(a, b):
    return dot(a, b, ((1,), (1,)))


def t_mm(a, b):
    return dot(a, b, ((0,), (0,)))


def attention_masks(core, half):
    row = lax.broadcasted_iota(jnp.int32, (2 * half, 2 * half), 0)
    col = lax.broadcasted_iota(jnp.int32, (2 * half, 2 * half), 1)
    row_slice, col_slice = row // half, col // half
    own = (col_slice < row_slice) | ((col_slice == row_slice) & (col <= row))
    other = (col_slice < row_slice) | ((col_slice == row_slice) & (core == 1))
    return jnp.where(jnp.stack([own, other]), 0.0, NEG).astype(f32)


def norm_backward(hat, scale, gain, grad):
    scaled = grad * gain
    mean = jnp.mean(scaled, axis=-1, keepdims=True)
    along = jnp.mean(scaled * hat, axis=-1, keepdims=True)
    return scale * (scaled - mean - hat * along)


ANY = pl.BlockSpec(memory_space=pl.ANY)


def remote(src, dst, send, recv, section, ctx, shard):
    return pltpu.make_async_remote_copy(
        src_ref=src,
        dst_ref=dst,
        send_sem=send,
        recv_sem=recv,
        device_id=(section, ctx, shard),
        device_id_type=pl.DeviceIdType.MESH,
    )


def normalised(values):
    mean = jnp.mean(values, axis=-1, keepdims=True)
    centred = values - mean
    var = jnp.mean(centred * centred, axis=-1, keepdims=True)
    scale = lax.rsqrt(var + eps_norm)
    return centred * scale, scale


def stack_heads(value, low):
    zero = jnp.zeros_like(value)
    return jnp.concatenate([jnp.where(low, value, zero), jnp.where(low, zero, value)], axis=0)


def unstack_heads(value, low):
    rows = value.shape[0] // 2
    return jnp.where(low, value[:rows], value[rows:])


def mask_last(scores, mask):
    width = mask.shape[1]
    last = scores[:, scores.shape[1] - width :] + mask
    if scores.shape[1] == width:
        return last
    return jnp.concatenate([scores[:, : scores.shape[1] - width], last], axis=1)


def attend_chunk(u, rows, mask_ref, q, k, k1, v, v1, o, lse):
    size = rows.size
    keys = pl.ds(0, (u + 1) * size)
    lane = lax.broadcasted_iota(jnp.int32, (size, LANES), 1)
    low = lane < HEAD

    @pl.loop(0, q.shape[1] // LANES, unroll=3)
    def _(pair):
        cols = pl.ds(pl.multiple_of(pair * LANES, LANES), LANES)
        q2 = stack_heads(q[rows, cols], low)
        scores = [mask_last(mm_t(q2, ref[keys, cols]), mask_ref[part]) for part, ref in enumerate((k, k1))]
        top = jnp.maximum(
            jnp.max(scores[0], axis=1, keepdims=True), jnp.max(scores[1], axis=1, keepdims=True)
        )
        total, acc = 0.0, 0.0
        for s, ref in zip(scores, (v, v1)):
            p = jnp.exp(s - top)
            total = total + jnp.sum(p, axis=1, keepdims=True)
            acc = acc + mm(p.astype(bf16), ref[keys, cols])
        o[rows, cols] = unstack_heads(acc / total, low)
        level = top + jnp.log(total)
        lse[rows, :] = jnp.where(
            lane == 2 * pair, level[:size], jnp.where(lane == 2 * pair + 1, level[size:], lse[rows, :])
        )


def near_ctx(c, step):
    return c + step - 2 * step * lax.rem(c // step, 2)


def add_into(total, term):
    total[...] = (total[...].astype(f32) + term[...].astype(f32)).astype(bf16)


def relay_kernel(
    attn_ref, ff_ref, x_ref, g_ref, norm_ref, mask_ref, place_ref,
    attn_out, ff_out, rows_out, sums_out,
    w, tokens, norm_all, norms, ent, nrm, lea, coming, slots, o, lse, da, big, sums, sums_in, spread, first, second, third,
    send, recv, token_send, token_recv, norm_send, norm_recv, far_send,
    up_send, up_recv, down_send, down_recv, pair_send, pair_recv, swap_send, swap_recv, rows_send, rows_recv, free,
    sums_send, sums_recv, first_send, first_recv, second_send, second_recv, third_send, third_recv, last_send, last_recv,
):
    section, ctx, shard = lax.axis_index("section"), lax.axis_index("ctx"), lax.axis_index("shard")
    kind = lax.rem(shard, 2)
    late = shard // 2
    far_core = 1 - late
    x_ctx, y_ctx = near_ctx(ctx, 1), near_ctx(ctx, 2)
    d_ctx = near_ctx(x_ctx, 2)
    width = ent.shape[1]
    wide = attn_ref.shape[1]
    size = da.shape[0]
    half = size // 2
    chunks = ent.shape[0] // size
    ff_half = ff_ref.shape[1]
    attn_cols = pl.ds(0, wide)
    ff_cols = pl.ds(0, ff_half)
    parts = ((0, wide), (wide, ff_half - wide))

    x_copy = remote(x_ref, tokens.at[ctx], token_send.at[0], token_recv.at[ctx], section, shard, 0)
    g_copy = remote(g_ref, tokens.at[ctx], token_send.at[1], token_recv.at[ctx], section, shard, 3)
    x_stays = (shard == 0) & (ctx == 0)
    g_stays = (shard == 3) & (ctx == 3)
    attn_copy = remote(
        attn_ref, w.at[ctx, shard, :, attn_cols], far_send.at[0], recv.at[ctx, shard], far_core, ctx, 2 * section
    )
    ff_copy = remote(
        ff_ref, w.at[ctx, shard, :, ff_cols], far_send.at[1], recv.at[ctx, shard], far_core, ctx, 2 * section + 1
    )
    norm_local = pltpu.make_async_copy(norm_ref, norm_all.at[shard], norm_recv.at[shard])

    def start_unless(stays, copy, src):
        @pl.when(stays)
        def _():
            pltpu.make_async_copy(src, tokens.at[ctx], token_recv.at[ctx]).start()

        @pl.when(jnp.logical_not(stays))
        def _():
            copy.start()

    attn_copy.start()
    start_unless(x_stays, x_copy, x_ref)
    norm_copies = []
    for core in range(2):
        for stage in range(2):
            copy = remote(
                norm_ref, norm_all.at[shard], norm_send.at[core * 2 + stage], norm_recv.at[shard],
                core, ctx, 2 * section + stage,
            )
            stays = (section == core) & (shard == 2 * section + stage)
            norm_copies.append((copy, stays))

            @pl.when(stays)
            def _():
                norm_local.start()

            @pl.when(jnp.logical_not(stays))
            def _():
                copy.start()

    ff_copy.start()
    start_unless(g_stays, g_copy, g_ref)

    def piece(cols, c, s, which, core, to_ctx):
        ref = w.at[c, s, :, cols]
        return remote(ref, ref, send.at[which], recv.at[c, s], core, to_ctx, shard)

    def collect(cols):
        here = lax.rem(section + late, 2)
        mine = [
            here * shard + (1 - here) * (2 - late),
            here * (shard + 1 - 2 * kind) + (1 - here) * (3 - 3 * late),
        ]
        started = []

        def go(c, s, core, to_ctx):
            copy = piece(cols, c, s, len(started), core, to_ctx)
            copy.start()
            started.append(copy)

        def arrived(c, s):
            piece(cols, c, s, 0, section, ctx).wait_recv()

        for s in mine:
            arrived(ctx, s)
            go(ctx, s, section, x_ctx)
            go(ctx, s, section, y_ctx)
            go(ctx, s, 1 - section, ctx)
        arrived(x_ctx, mine[0])
        go(x_ctx, mine[0], section, y_ctx)
        go(x_ctx, mine[0], 1 - section, ctx)
        arrived(y_ctx, mine[0])
        go(y_ctx, mine[0], 1 - section, ctx)
        arrived(y_ctx, mine[1])
        go(y_ctx, mine[1], section, x_ctx)
        go(y_ctx, mine[1], 1 - section, ctx)
        arrived(x_ctx, mine[1])
        go(x_ctx, mine[1], 1 - section, ctx)
        for s in mine:
            arrived(d_ctx, s)
            go(d_ctx, s, 1 - section, ctx)
        for c in (ctx, x_ctx, y_ctx, d_ctx):
            for j in range(2):
                arrived(c, 2 * section + j)
        for s in range(4):
            pltpu.make_async_copy(norm_ref, norm_all.at[s], norm_recv.at[s]).wait()
        norms[...] = (norm_all[0] + norm_all[1]) + (norm_all[2] + norm_all[3])
        return started

    def tokens_arrived():
        for c in range(4):
            pltpu.make_async_copy(x_ref, tokens.at[c], token_recv.at[c]).wait()

    def tokens_of(u):
        return tokens[pl.ds(2 * lax.rem(u, 2), 2), u // 2].reshape(size, width)

    def chunk_rows(u):
        return pl.ds(pl.multiple_of(u * size, size), size)

    def up_copy(u, stage):
        rows = chunk_rows(u)
        return remote(lea.at[rows], ent.at[rows], up_send.at[u], up_recv.at[u], section, ctx, stage)

    def down_copy(u, stage):
        rows = chunk_rows(u)
        return remote(ent.at[rows], coming.at[rows], down_send.at[u], down_recv.at[u], section, ctx, stage)

    def weight(c, start, columns):
        value = w[c, :, :, pl.ds(start, columns)]
        return value.reshape(value.shape[0] * value.shape[1], columns)

    def rows_copy(src, t, local):
        block, c = t // 4, lax.rem(t, 4)
        src = src.at[pl.ds(pl.multiple_of(t * half, half), half)]
        dst = rows_out.at[kind, block, pl.ds(pl.multiple_of(section * half, half), half)]
        recv = rows_recv.at[kind, section, block]
        if local:
            return pltpu.make_async_copy(src, dst, recv)
        return remote(src, dst, rows_send.at[t], recv, shard // 2, c, ctx)

    def rows_stay(t):
        return (section == shard // 2) & (ctx == lax.rem(t, 4)) & (ctx == shard)

    def rows_start(src, t):
        @pl.when(rows_stay(t))
        def _():
            rows_copy(src, t, True).start()

        @pl.when(jnp.logical_not(rows_stay(t)))
        def _():
            rows_copy(src, t, False).start()

    def rows_finish(src):
        @pl.loop(0, 2 * chunks)
        def _(t):

            @pl.when(jnp.logical_not(rows_stay(t)))
            def _():
                rows_copy(src, t, False).wait_send()

    def finish_chunk(rows, d_normed, gain):
        hat, scale = normalised(ent[rows].astype(f32))
        sums[0:1, :width] += jnp.sum(d_normed * hat, axis=0, keepdims=True)
        sums[1:2, :width] += jnp.sum(d_normed, axis=0, keepdims=True)
        total = coming[rows].astype(f32) + norm_backward(hat, scale, gain, d_normed)
        ent[rows] = total.astype(bf16)

    sums[...] = jnp.zeros_like(sums)

    def group_columns(index, ref):
        feature = lax.broadcasted_iota(jnp.int32, (LANES, width), 1)

        @pl.loop(0, 2)
        def _(side):
            @pl.loop(0, spread.shape[2] // LANES)
            def _(tile):
                at = pl.ds(pl.multiple_of(tile * LANES, LANES), LANES)
                chosen = jnp.where(feature == place_ref[side, at, 0:1], 1.0, 0.0).astype(bf16)
                spread[index, side, at, :] = mm_t(chosen, ref[...]).astype(bf16)

    def reduce(source, pieces, turn, out_ref, which):
        rows = first.shape[3]
        gap = up_to(rows, 16)
        count = out_ref.shape[0]
        lanes = lambda p: pl.ds(pieces[p][0], pieces[p][1])
        own = lambda a, p, c, j: w.at[a, c, pl.ds(gap * j, rows), lanes(p)]
        array = lambda a: lax.rem(a + turn, count)

        def first_copy(a, p, j):
            even = lax.rem(a, 2)
            return remote(
                w.at[2 * even + j, :, pl.ds(2 * gap, rows), lanes(p)], first.at[even, j, :, :, lanes(p)],
                first_send.at[a, p, j], first_recv.at[a, p, j], 1 - section, ctx, shard,
            )

        def second_copy(a, p, j, part):
            to = (x_ctx, y_ctx)[j]
            return remote(
                own(a, p, (to, d_ctx)[part], j), second.at[a, j, part, :, lanes(p)],
                second_send.at[a, p, j, part], second_recv.at[a, p, j, part], section, to, shard,
            )

        def third_copy(a, p, j):
            to = (y_ctx, x_ctx)[j]
            return remote(
                own(a, p, to, j), third.at[a, j, :, lanes(p)],
                third_send.at[a, p, j], third_recv.at[a, p, j], section, to, shard,
            )

        def last_copy(a, p, j):
            return remote(
                own(a, p, ctx, j), out_ref.at[array(a), :, lanes(p)],
                last_send.at[a, p, j], last_recv.at[which, array(a), p],
                shard // 2, ctx, 2 * (1 - section) + j,
            )

        def terms(a, p):
            @pl.loop(0, 2)
            def _(side):
                def emit(index, ref, columns):
                    def block(at, step):
                        value = mm(spread[index, side, pl.ds(0, 8 * rows), :], ref[:, pl.ds(at, step)])
                        cols = pl.ds(pl.multiple_of(pieces[p][0] + at, LANES), step)
                        for n in range(8):
                            lead = side * a + (1 - side) * (2 * lax.rem(a, 2) + n % 2)
                            row = pl.multiple_of(side * (gap * (n % 2)) + (1 - side) * 2 * gap, 16)
                            w[lead, n // 2, pl.ds(row, rows), cols] = value[n * rows : (n + 1) * rows].astype(bf16)

                    step = 2 * LANES

                    @pl.loop(0, columns // step)
                    def _(b):
                        block(pl.multiple_of(b * step, step), step)

                    if columns % step:
                        block(columns - columns % step, columns % step)

                source(a, p, side, emit)

                @pl.when(side == 0)
                def _():
                    for j in range(2):
                        first_copy(a, p, j).start()

        def stage_one(a, p):
            @pl.when(a >= 2)
            def _():
                for j in range(2):
                    first_copy(a - 2, p, j).wait_send()
                pl.semaphore_wait(free, 1)

            terms(a, p)
            for j in range(2):
                first_copy(a, p, j).wait_recv()

                @pl.loop(0, 4)
                def _(c):
                    add_into(own(a, p, c, j), first.at[lax.rem(a, 2), j, c, :, lanes(p)])

            @pl.when(a + 2 < count)
            def _():
                pl.semaphore_signal(
                    free, inc=1, device_id=(1 - section, ctx, shard), device_id_type=pl.DeviceIdType.MESH
                )

            for part in (1, 0):
                for j in range(2):
                    second_copy(a, p, j, part).start()

        def stage_two(a, p):
            for j in range(2):
                second_copy(a, p, j, 1).wait_recv()
                add_into(own(a, p, (y_ctx, x_ctx)[j], j), second.at[a, j, 1, :, lanes(p)])
                third_copy(a, p, j).start()
            for j in range(2):
                second_copy(a, p, j, 0).wait_recv()
                add_into(own(a, p, ctx, j), second.at[a, j, 0, :, lanes(p)])

        def stage_three(a, p):
            for j in range(2):
                third_copy(a, p, j).wait_recv()
                add_into(own(a, p, ctx, j), third.at[a, j, :, lanes(p)])
                last_copy(a, p, j).start()

        def sums_copy(step):
            to_core, to_ctx = ((1 - section, ctx), (section, x_ctx), (section, y_ctx))[step]
            return remote(sums, sums_in.at[step], sums_send.at[step], sums_recv.at[step], to_core, to_ctx, shard)

        def sums_last(j):
            return remote(
                sums, sums_out.at[which], sums_send.at[3 + j], sums_recv.at[3 + which],
                shard // 2, ctx, 2 * (1 - section) + j,
            )

        sums_copy(0).start()
        items = len(pieces)

        @pl.loop(0, count + 2)
        def _(a):
            for p in range(items):

                @pl.when(a < count)
                def _():
                    stage_one(a, p)

                back = [(-(-(d - p) // items), (p - d) % items) for d in (1, 2)]

                @pl.when((a >= back[0][0]) & (a < count + back[0][0]))
                def _():
                    stage_two(a - back[0][0], back[0][1])

                @pl.when((a >= back[1][0]) & (a < count + back[1][0]))
                def _():
                    stage_three(a - back[1][0], back[1][1])

            for step in range(3):

                @pl.when(a == step)
                def _():
                    sums_copy(step).wait()
                    sums[...] += sums_in[step]
                    if step < 2:
                        sums_copy(step + 1).start()
                    else:
                        for j in range(2):
                            sums_last(j).start()

        @pl.loop(0, count)
        def _(a):
            for p in range(items):
                for j in range(2):

                    @pl.when(a >= count - 2)
                    def _():
                        first_copy(a, p, j).wait_send()

                    for part in range(2):
                        second_copy(a, p, j, part).wait_send()
                    third_copy(a, p, j).wait_send()
                    last_copy(a, p, j).wait_send()

        for j in range(2):
            sums_last(j).wait_send()

    @pl.when(kind == 0)
    def _():
        started = collect(attn_cols)

        @pl.when(shard == 0)
        def _():
            tokens_arrived()

        lse[...] = jnp.zeros_like(lse)
        da[...] = jnp.zeros_like(da)
        gain, bias = norms[0:1, :width], norms[2:3, :width]

        def pair_copy(which, u):
            rows = chunk_rows(u)
            return remote(
                slots.at[1 + which, rows], slots.at[3 + which, rows], pair_send.at[which, u], pair_recv.at[which, u],
                1 - section, ctx, shard,
            )

        @pl.loop(0, chunks)
        def _(u):
            rows = chunk_rows(u)

            @pl.when(shard == 0)
            def _():
                ent[rows] = tokens_of(u)

            @pl.when(shard > 0)
            def _():
                up_copy(u, shard).wait_recv()

            hat, _ = normalised(ent[rows].astype(f32))
            normed = (hat * gain + bias).astype(bf16)
            nrm[rows] = normed

            @pl.loop(0, 3)
            def _(turn):
                index = lax.rem(turn + 1, 3)
                scale = jnp.where(turn == 2, score_scale, 1.0)
                slots[index, rows] = (mm(normed, weight(index, 0, wide)) * scale).astype(bf16)

                @pl.when(turn < 2)
                def _():
                    pair_copy(turn, u).start()

            for which in range(2):
                pair_copy(which, u).wait_recv()
            for index in range(chunks):

                @pl.when(u == index)
                def _():
                    attend_chunk(
                        index, pl.ds(index * size, size), mask_ref,
                        slots.at[0], slots.at[1], slots.at[3], slots.at[2], slots.at[4], o, lse,
                    )

            out = mm(o[rows, :width].astype(bf16), weight(3, 0, wide))[:, :width]
            lea[rows] = (ent[rows].astype(f32) + out).astype(bf16)
            up_copy(u, shard + 1).start()

        @pl.loop(0, chunks)
        def _(u):
            for which in range(2):
                pair_copy(which, u).wait_send()
            up_copy(u, shard + 1).wait_send()

        for copy in started:
            copy.wait_send()

        lane = lax.broadcasted_iota(jnp.int32, (size, LANES), 1)
        low = lane < HEAD

        def swap_copy(which, u):
            rows = chunk_rows(u)
            return remote(
                slots.at[3 + which, rows], slots.at[5 + which, rows], swap_send.at[which, u], swap_recv.at[which, u],
                1 - section, ctx, shard,
            )

        @pl.loop(0, chunks)
        def _(step):
            u = chunks - 1 - step
            rows_now = chunk_rows(u)
            down_copy(u, shard).wait_recv()
            da[:, :width] = mm_t(coming[rows_now], weight(3, 0, width)).astype(bf16)
            for index in range(chunks):

                @pl.when(u == index)
                def _():
                    rows = pl.ds(index * size, size)
                    keys = pl.ds(0, (index + 1) * size)

                    @pl.loop(0, wide // LANES, unroll=3)
                    def _(pair):
                        cols = pl.ds(pl.multiple_of(pair * LANES, LANES), LANES)
                        q2 = stack_heads(slots[0, rows, cols], low)
                        grad = da[:, cols]
                        a2 = stack_heads(grad, low)
                        level = lse[rows, :]
                        product = grad.astype(f32) * o[rows, cols]
                        column = lambda which: jnp.sum(jnp.where(lane == 2 * pair + which, level, 0.0), axis=1, keepdims=True)
                        level2 = jnp.concatenate([column(0), column(1)], axis=0)
                        delta2 = jnp.concatenate(
                            [
                                jnp.sum(jnp.where(low, product, 0.0), axis=1, keepdims=True),
                                jnp.sum(jnp.where(low, 0.0, product), axis=1, keepdims=True),
                            ],
                            axis=0,
                        )
                        dq2 = 0.0
                        for part in range(2):
                            keys_now, values_now = slots[1 + 2 * part, keys, cols], slots[2 + 2 * part, keys, cols]
                            p = jnp.exp(mask_last(mm_t(q2, keys_now), mask_ref[part]) - level2)
                            ds = (p * (mm_t(a2, values_now) - delta2)).astype(bf16)
                            dq2 = dq2 + mm(ds, keys_now)
                            d_keys, d_values = t_mm(ds, q2), t_mm(p.astype(bf16), a2)
                            if index == chunks - 1:
                                big[2 * part, keys, cols] = d_keys
                                big[2 * part + 1, keys, cols] = d_values
                            else:
                                big[2 * part, keys, cols] += d_keys
                                big[2 * part + 1, keys, cols] += d_values
                        slots[0, rows, cols] = (unstack_heads(dq2, low) * score_scale).astype(bf16)

            rows = rows_now
            for which in range(2):
                slots[3 + which, rows] = big[2 + which, rows].astype(bf16)
                swap_copy(which, u).start()

            def finish_part(which, total):
                swap_copy(which, u).wait_recv()
                slots[1 + which, rows] = (big[which, rows] + slots[5 + which, rows].astype(f32)).astype(bf16)
                return total + mm_t(slots[1 + which, rows], weight(1 + which, 0, wide))

            d_normed = lax.fori_loop(0, 2, finish_part, mm_t(slots[0, rows], weight(0, 0, wide)))
            finish_chunk(rows, d_normed, gain)

            @pl.when(shard > 0)
            def _():
                down_copy(u, shard - 1).start()

            for part in range(2):
                rows_start(ent, 2 * u + part)

        @pl.loop(0, chunks)
        def _(u):
            for which in range(2):
                swap_copy(which, u).wait_send()

        slots[3] = o[...].astype(bf16)
        group_columns(0, nrm)
        group_columns(1, slots.at[3, :, pl.ds(0, width)])

        def attn_source(a, p, side, emit):
            @pl.when(a == 0)
            def _():
                emit(1, coming, width)

            @pl.when(a > 0)
            def _():
                emit(0, slots.at[jnp.maximum(a - 1, 0)], wide)

        reduce(attn_source, ((0, wide),), 3, attn_out, 0)
        rows_finish(ent)

        @pl.loop(0, chunks)
        def _(u):

            @pl.when(shard > 0)
            def _():
                down_copy(u, shard - 1).wait_send()

    @pl.when(kind == 1)
    def _():
        started = collect(ff_cols)
        gain, bias = norms[1:2, :width], norms[3:4, :width]

        @pl.loop(0, chunks)
        def _(u):
            rows = chunk_rows(u)
            up_copy(u, shard).wait_recv()
            hat, _ = normalised(ent[rows].astype(f32))
            normed = (hat * gain + bias).astype(bf16)
            nrm[rows] = normed

            def add_half(i, total):
                for part, (start, columns) in enumerate(parts):
                    cols = pl.ds(0, columns)
                    upper = mm(normed, weight(i, start, columns))
                    big[2 * i + part, rows, cols] = upper
                    hidden = jax.nn.gelu(upper, approximate=True).astype(bf16)
                    slots[4 + 2 * i + part, rows, cols] = hidden
                    total = total + mm_t(hidden, weight(2 + i, start, columns))
                return total

            lea[rows] = lax.fori_loop(0, 2, add_half, ent[rows].astype(f32)).astype(bf16)

            @pl.when(shard < 3)
            def _():
                up_copy(u, shard + 1).start()

            for part in range(2):
                rows_start(lea, 2 * u + part)

        @pl.when(shard == 3)
        def _():
            tokens_arrived()

        @pl.loop(0, chunks)
        def _(step):
            u = chunks - 1 - step
            rows = chunk_rows(u)

            @pl.when(shard == 3)
            def _():
                coming[rows] = tokens_of(u)

            @pl.when(shard < 3)
            def _():
                down_copy(u, shard).wait_recv()

            grad = coming[rows]

            def back_half(i, total):
                for part, (start, columns) in enumerate(parts):
                    cols = pl.ds(0, columns)
                    d_hidden = mm(grad, weight(2 + i, start, columns))
                    _, back = jax.vjp(lambda value: jax.nn.gelu(value, approximate=True), big[2 * i + part, rows, cols])
                    d_upper = back(d_hidden)[0].astype(bf16)
                    slots[2 * i + part, rows, cols] = d_upper
                    total = total + mm_t(d_upper, weight(i, start, columns))
                return total

            finish_chunk(rows, lax.fori_loop(0, 2, back_half, jnp.zeros((size, width), f32)), gain)
            down_copy(u, shard - 1).start()

        for copy in started:
            copy.wait_send()
        group_columns(1, coming)
        group_columns(0, nrm)

        def ff_source(a, p, side, emit):
            emit(1 - a // 2, slots.at[lax.rem(2 * a + 4, 8) + p], parts[p][1])

        reduce(ff_source, parts, 2, ff_out, 1)
        rows_finish(lea)

        @pl.loop(0, chunks)
        def _(u):

            @pl.when(shard < 3)
            def _():
                up_copy(u, shard + 1).wait_send()

            down_copy(u, shard - 1).wait_send()

    @pl.loop(0, attn_out.shape[0])
    def _(index):
        arrivals = [(0, attn_out, 0, 0, wide)] + [(1, ff_out, p, start, columns) for p, (start, columns) in enumerate(parts)]
        for which, ref, p, start, columns in arrivals:
            ref = ref.at[index, :, pl.ds(start, columns)]
            remote(ref, ref, last_send.at[index, 0, 0], last_recv.at[which, index, p], section, ctx, shard).wait_recv()

    for which in range(2):
        remote(sums, sums_out.at[which], sums_send.at[3], sums_recv.at[3 + which], section, ctx, shard).wait_recv()
        for core in range(2):
            for block in range(2):
                ref = rows_out.at[which, block, pl.ds(core * half, half)]
                pltpu.make_async_copy(ref, ref, rows_recv.at[which, core, block]).wait()

    attn_copy.wait_send()
    ff_copy.wait_send()
    for copy, stays in norm_copies + [(x_copy, x_stays), (g_copy, g_stays)]:

        @pl.when(jnp.logical_not(stays))
        def _():
            copy.wait_send()


def relay(attn_piece, ff_piece, x_own, g_own, norm_own, mask, place, group_pad):
    share, ff_half = ff_piece.shape
    wide = attn_piece.shape[1]
    blocks, half, width = x_own.shape
    tokens = blocks * 4 * half
    size = 2 * half
    chunks = tokens // size
    dma = pltpu.SemaphoreType.DMA
    vmem = pl.BlockSpec(memory_space=pltpu.VMEM)
    narrow = ((tokens, width), bf16)
    outs = [
        ((4, group_pad, wide), bf16), ((4, group_pad, ff_half), bf16), ((2, blocks, size, width), bf16), ((2,) + norm_own.shape, f32),
    ]
    scratch = [
        ((4, 4, share, ff_half), bf16), ((4,) + x_own.shape, bf16), ((4,) + norm_own.shape, f32), (norm_own.shape, f32),
        narrow, narrow, narrow, narrow, ((8, tokens, wide), bf16),
        ((tokens, wide), f32), ((tokens, LANES), f32), ((size, wide), bf16), ((4, tokens, wide), f32),
        (norm_own.shape, f32), ((3,) + norm_own.shape, f32), ((2, 2, place.shape[1], tokens), bf16),
        ((2, 2, 4, group_pad, ff_half), bf16), ((4, 2, 2, group_pad, ff_half), bf16), ((4, 2, group_pad, ff_half), bf16),
    ]
    return pl.pallas_call(
        relay_kernel,
        in_specs=[ANY] * 5 + [vmem] * 2,
        out_specs=[ANY] * len(outs),
        out_shape=[jax.ShapeDtypeStruct(s, t) for s, t in outs],
        scratch_shapes=[pltpu.VMEM(s, t) for s, t in scratch]
        + [
            dma((14,)), dma((4, 4)), dma((2,)), dma((4,)), dma((4,)), dma((4,)), dma((2,)),
            dma((chunks,)), dma((chunks,)), dma((chunks,)), dma((chunks,)),
            dma((2, chunks)), dma((2, chunks)), dma((2, chunks)), dma((2, chunks)),
            dma((2 * chunks,)), dma((2, 2, 2)), pltpu.SemaphoreType.REGULAR,
            dma((5,)), dma((5,)), dma((4, 2, 2)), dma((4, 2, 2)), dma((4, 2, 2, 2)), dma((4, 2, 2, 2)),
            dma((4, 2, 2)), dma((4, 2, 2)), dma((4, 2, 2)), dma((2, 4, 2)),
        ],
        compiler_params=pltpu.CompilerParams(has_side_effects=True, vmem_limit_bytes=VMEM_BYTES),
        name="relay",
    )(attn_piece, ff_piece, x_own, g_own, norm_own, mask, place)


def chain(inputs, cotangent, qkv_weight, out_weight, up_weight, down_weight, norm_gain, norm_bias):
    section, ctx, shard = lax.axis_index("section"), lax.axis_index("ctx"), lax.axis_index("shard")
    seq_count, blocks, slice_len, width = inputs.shape
    half = slice_len // 2
    tokens = blocks * 4 * half
    share = width // 4
    group = share // 4
    group_pad = up_to(group, ROWS)
    wide = up_to(width, LANES)
    ff = up_weight.shape[2]
    is_attn = shard % 2 == 0

    pad = lambda w: jnp.pad(w, ((0, 0), (0, wide - width)))
    own_qkv, own_out = qkv_weight[0], out_weight[0]
    attn_src = jnp.stack([pad(own_qkv[:, i * width : (i + 1) * width]) for i in range(3)] + [pad(own_out)])
    down_t = down_weight[0].T
    up0 = up_weight[0]
    ff_src = jnp.stack([up0[:, : ff // 2], up0[:, ff // 2 :], down_t[:, : ff // 2], down_t[:, ff // 2 :]])
    norm_own = jnp.concatenate([norm_gain[0], norm_bias[0]], axis=0).astype(f32)
    norm_own = lax.dynamic_update_slice(
        jnp.zeros((ROWS, wide), f32), jnp.pad(norm_own, ((0, ROWS - 4), (0, 0))), (0, shard * share)
    )
    x_own = lax.dynamic_slice_in_dim(inputs[0], section * half, half, 1)
    g_own = lax.dynamic_slice_in_dim(cotangent[0], section * half, half, 1)
    mask = attention_masks(section, half)
    mask = jnp.concatenate([mask, mask], axis=1)
    slot = jnp.arange(up_to(8 * group_pad, LANES))
    row = slot % group_pad
    place = []
    for side in (section, 1 - section):
        owner = (slot // (2 * group_pad)) * 4 + 2 * side + (slot // group_pad) % 2
        place.append(jnp.where((row < group) & (slot < 8 * group_pad), owner * group + row, -1))
    place = jnp.broadcast_to(jnp.stack(place)[:, :, None].astype(jnp.int32), (2, slot.shape[0], LANES))
    attn_sums, ff_sums, rows, totals = relay(
        lax.dynamic_index_in_dim(attn_src, ctx, 0, keepdims=False),
        lax.dynamic_index_in_dim(ff_src, ctx, 0, keepdims=False),
        x_own, g_own, norm_own, mask, place, group_pad,
    )
    totals = lax.dynamic_slice_in_dim(totals[:, :2], (ctx * 4 + shard) * group, group, 2)
    attn_sums = attn_sums[:, :group, :width].astype(f32)
    ff_sums = ff_sums[:, :group].astype(f32)
    return (
        rows[1][None, None],
        rows[0][None, None],
        jnp.concatenate([attn_sums[0], attn_sums[1], attn_sums[2]], axis=1)[None],
        attn_sums[3][None],
        jnp.concatenate([ff_sums[0], ff_sums[1]], axis=1)[None],
        jnp.concatenate([ff_sums[2].T, ff_sums[3].T], axis=0)[None],
        totals[:, 0][None],
        totals[:, 1][None],
    )


def passed_along(value, axis, steps):
    count = lax.axis_size(axis)
    initial, last = (max(0, -steps), min(count, count - steps))
    return lax.ppermute(value, axis, [(source, source + steps) for source in range(initial, last)])


def layer_norm(values, gain, shift):
    mean = jnp.mean(values, axis=-1, keepdims=True)
    centred = values - mean
    var = jnp.mean(centred * centred, axis=-1, keepdims=True)
    return centred * lax.rsqrt(var + eps_norm) * gain + shift


def gelu_tanh(values):
    return jax.nn.gelu(values, approximate=True)


def split_pair(key_value, head_count):
    block_len, seq_count, double = key_value.shape
    model_width = double // 2
    key_rows = key_value[..., :model_width].reshape(block_len, seq_count, head_count, HEAD)
    value_rows = key_value[..., model_width:].reshape(block_len, seq_count, head_count, HEAD)
    return (key_rows, value_rows)


def causal_mask(query_pos, key_pos):
    return (key_pos[None, :] <= query_pos[:, None])[None, :, None, :]


def forward_block(running, queries, query_pos, key_value, key_pos):
    row_max, row_sum, accum = running
    key_rows, value_rows = split_pair(key_value, queries.shape[2])
    scores = (
        jnp.einsum("sqhe,kshe->sqhk", queries, key_rows, preferred_element_type=jnp.float32)
        * score_scale
    )
    causal = causal_mask(query_pos, key_pos)
    new_max = jnp.maximum(row_max, jnp.max(jnp.where(causal, scores, -1e30), axis=-1))
    softmax_w = jnp.where(causal, jnp.exp(scores - new_max[..., None]), 0.0)
    factor = jnp.exp(row_max - new_max)
    row_sum = row_sum * factor + jnp.sum(softmax_w, axis=-1)
    accum = accum * factor[..., None] + jnp.einsum(
        "sqhk,kshe->sqhe",
        softmax_w.astype(jnp.bfloat16),
        value_rows,
        preferred_element_type=jnp.float32,
    )
    return (new_max, row_sum, accum)


def split_rows(whole):
    key_count = whole.shape[0]
    block_size = 512
    blocks = whole.reshape((key_count // block_size, block_size) + whole.shape[1:])
    offsets = jnp.arange(key_count // block_size, dtype=jnp.int32) * block_size
    return (blocks, offsets, block_size)


def fold_keys(running, piece, start, queries, query_pos, group_len):
    blocks, offsets, block_size = split_rows(piece)

    def fold_scan_step(inner, scan_item):
        block_rows, offset = scan_item
        for group_id in range(block_rows.shape[2]):
            key_pos = (
                group_id * group_len + start + offset + jnp.arange(block_size, dtype=jnp.int32)
            )
            inner = forward_block(inner, queries, query_pos, block_rows[:, :, group_id], key_pos)
        return (inner, None)

    result, _ = lax.scan(fold_scan_step, running, (blocks, offsets))
    return result


def pair_terms(d_scores, softmax_w, queries, d_attended, block_size):
    d_keys = (
        jnp.einsum("sqhk,sqhe->kshe", d_scores, queries, preferred_element_type=jnp.float32)
        * score_scale
    )
    d_values = jnp.einsum(
        "sqhk,sqhe->kshe",
        softmax_w.astype(jnp.bfloat16),
        d_attended,
        preferred_element_type=jnp.float32,
    )
    shape = (block_size, queries.shape[0], queries.shape[2] * queries.shape[3])
    return jnp.concatenate([d_keys.reshape(shape), d_values.reshape(shape)], axis=-1)


def score_grads(
    queries, query_pos, log_total, row_delta, d_attended, key_rows, value_rows, key_pos
):
    scores = (
        jnp.einsum("sqhe,kshe->sqhk", queries, key_rows, preferred_element_type=jnp.float32)
        * score_scale
    )
    causal = causal_mask(query_pos, key_pos)
    softmax_w = jnp.where(causal, jnp.exp(scores - log_total[..., None]), 0.0)
    d_probs = jnp.einsum(
        "sqhe,kshe->sqhk", d_attended, value_rows, preferred_element_type=jnp.float32
    )
    d_scores = (softmax_w * (d_probs - row_delta[..., None])).astype(jnp.bfloat16)
    return (softmax_w, d_scores)


def backward_keys(whole, queries, query_pos, log_total, row_delta, d_attended, group_len):
    blocks, offsets, block_size = split_rows(whole)

    def backward_scan_step(d_queries, scan_item):
        block_rows, offset = scan_item
        for group_id in range(block_rows.shape[2]):
            key_pos = group_id * group_len + offset + jnp.arange(block_size, dtype=jnp.int32)
            key_rows, value_rows = split_pair(block_rows[:, :, group_id], queries.shape[2])
            softmax_w, d_scores = score_grads(
                queries, query_pos, log_total, row_delta, d_attended, key_rows, value_rows, key_pos
            )
            d_queries = (
                d_queries
                + jnp.einsum(
                    "sqhk,kshe->sqhe", d_scores, key_rows, preferred_element_type=jnp.float32
                )
                * score_scale
            )
        return (d_queries, None)

    d_queries, terms = lax.scan(
        backward_scan_step, jnp.zeros(queries.shape, jnp.float32), (blocks, offsets)
    )
    return (d_queries, None)


def owner_terms(
    own_cache, all_queries, all_d_att, all_totals, all_deltas, micro_index, ctx_id, group_len
):
    block_len, seq_count, group_count, double = own_cache.shape
    head_count = all_queries.shape[2]
    query_rows = all_queries.shape[1]
    query_size = 512
    block_count = query_rows // query_size

    def loop_step(index, total):
        offset = index * query_size
        q_block = lax.dynamic_slice_in_dim(all_queries, offset, query_size, 1)
        d_block = lax.dynamic_slice_in_dim(all_d_att, offset, query_size, 1)
        t_block = lax.dynamic_slice_in_dim(all_totals, offset, query_size, 1)
        r_block = lax.dynamic_slice_in_dim(all_deltas, offset, query_size, 1)
        query_pos = micro_index * group_len + offset + jnp.arange(query_size, dtype=jnp.int32)
        pieces = []
        for group_id in range(group_count):
            key_pos = (
                group_id * group_len + ctx_id * block_len + jnp.arange(block_len, dtype=jnp.int32)
            )
            key_rows, value_rows = split_pair(own_cache[:, :, group_id], head_count)
            softmax_w, d_scores = score_grads(
                q_block, query_pos, t_block, r_block, d_block, key_rows, value_rows, key_pos
            )
            pieces.append(pair_terms(d_scores, softmax_w, q_block, d_block, block_len))
        return total + jnp.stack(pieces, axis=2)

    return lax.fori_loop(0, block_count, loop_step, jnp.zeros(own_cache.shape, jnp.float32))


def store_at(store, value, micro_index, active):
    updated = lax.dynamic_update_index_in_dim(store, value, micro_index, 0)
    return jnp.where(active, updated, store)


def shards(inputs, cotangent, qkv_weight, out_weight, up_weight, down_weight, norm_gain, norm_bias):
    section_id = lax.axis_index("section")
    ctx_count = lax.axis_size("ctx")
    ctx_id = lax.axis_index("ctx")
    seq_count, group_count, block_len, model_width = inputs.shape
    head_count = model_width // HEAD
    group_len = block_len * ctx_count
    row_count = seq_count * block_len
    w_qkv, w_out, w_up, w_down, gains, biases = (
        lax.all_gather(qkv_weight[0], "shard", axis=0, tiled=True),
        lax.all_gather(out_weight[0], "shard", axis=0, tiled=True),
        lax.all_gather(up_weight[0], "shard", axis=0, tiled=True),
        lax.all_gather(down_weight[0], "shard", axis=1, tiled=True),
        lax.all_gather(norm_gain[0], "shard", axis=1, tiled=True),
        lax.all_gather(norm_bias[0], "shard", axis=1, tiled=True),
    )
    gains = gains.astype(jnp.float32)
    biases = biases.astype(jnp.float32)
    ff_width = w_up.shape[1]
    cache = jnp.zeros((block_len, seq_count, group_count, 2 * model_width), jnp.bfloat16)
    in_store = jnp.zeros((group_count, seq_count, block_len, model_width), jnp.bfloat16)
    query_store = jnp.zeros((group_count, seq_count, block_len, head_count, HEAD), jnp.bfloat16)
    att_store = jnp.zeros((group_count, seq_count, block_len, head_count, HEAD), jnp.float32)
    total_store = jnp.zeros((group_count, seq_count, block_len, head_count), jnp.float32)
    middle_store = jnp.zeros((group_count, row_count, model_width), jnp.float32)
    upper_store = jnp.zeros((group_count, row_count, ff_width), jnp.float32)
    out_store = jnp.zeros((group_count, seq_count, block_len, model_width), jnp.bfloat16)
    received = jnp.zeros((seq_count, block_len, model_width), jnp.bfloat16)
    for tick_no in range(group_count + 1):
        micro = tick_no - section_id
        active = (micro >= 0) & (micro < group_count)
        micro_index = jnp.clip(micro, 0, group_count - 1)
        own_input = lax.dynamic_index_in_dim(inputs, micro_index, 1, keepdims=False)
        entering = jnp.where(section_id == 0, own_input, received)
        flat_rows = entering.reshape(row_count, model_width).astype(jnp.float32)
        normed = layer_norm(flat_rows, gains[0], biases[0]).astype(jnp.bfloat16)
        mixed = jnp.dot(normed, w_qkv, preferred_element_type=jnp.float32).astype(jnp.bfloat16)
        queries = mixed[:, :model_width].reshape(seq_count, block_len, head_count, HEAD)
        fresh = jnp.swapaxes(
            mixed[:, model_width:].reshape(seq_count, block_len, 2 * model_width), 0, 1
        )
        updated = lax.dynamic_update_index_in_dim(cache, fresh, micro_index, 2)
        cache = jnp.where(active, updated, cache)
        query_pos = (
            micro_index * group_len + ctx_id * block_len + jnp.arange(block_len, dtype=jnp.int32)
        )
        start_state = (
            jnp.full((seq_count, block_len, head_count), -1e30, jnp.float32),
            jnp.zeros((seq_count, block_len, head_count), jnp.float32),
            jnp.zeros((seq_count, block_len, head_count, HEAD), jnp.float32),
        )
        row_max, row_sum, accum = fold_keys(
            start_state,
            lax.all_gather(cache, "ctx", axis=0, tiled=True),
            jnp.int32(0),
            queries,
            query_pos,
            group_len,
        )
        attended = accum / row_sum[..., None]
        log_total = row_max + jnp.log(row_sum)
        att_low = attended.reshape(row_count, model_width).astype(jnp.bfloat16)
        middle = flat_rows + jnp.dot(att_low, w_out, preferred_element_type=jnp.float32)
        normed2 = layer_norm(middle, gains[1], biases[1]).astype(jnp.bfloat16)
        upper = jnp.dot(normed2, w_up, preferred_element_type=jnp.float32)
        hidden = gelu_tanh(upper).astype(jnp.bfloat16)
        leaving = (middle + jnp.dot(hidden, w_down, preferred_element_type=jnp.float32)).astype(
            jnp.bfloat16
        )
        leaving = leaving.reshape(seq_count, block_len, model_width)
        in_store = store_at(in_store, entering, micro_index, active)
        query_store = store_at(query_store, queries, micro_index, active)
        att_store = store_at(att_store, attended, micro_index, active)
        total_store = store_at(total_store, log_total, micro_index, active)
        middle_store = store_at(middle_store, middle, micro_index, active)
        upper_store = store_at(upper_store, upper, micro_index, active)
        out_store = store_at(out_store, leaving, micro_index, active)
        if tick_no < group_count:
            received = passed_along(leaving, "section", 1)
    key_acc = jnp.zeros((block_len, seq_count, group_count, 2 * model_width), jnp.float32)
    grad_qkv = jnp.zeros((model_width, 3 * model_width), jnp.float32)
    grad_out = jnp.zeros((model_width, model_width), jnp.float32)
    grad_up = jnp.zeros((model_width, ff_width), jnp.float32)
    grad_down = jnp.zeros((ff_width, model_width), jnp.float32)
    grad_gain = jnp.zeros((2, model_width), jnp.float32)
    grad_bias = jnp.zeros((2, model_width), jnp.float32)
    grad_store = jnp.zeros((group_count, seq_count, block_len, model_width), jnp.bfloat16)
    coming = jnp.zeros((seq_count, block_len, model_width), jnp.bfloat16)
    for tick_no in range(group_count + 1):
        micro = group_count - tick_no - section_id
        active = (micro >= 0) & (micro < group_count)
        active_weight = active.astype(jnp.float32)
        micro_index = jnp.clip(micro, 0, group_count - 1)
        own_cot = lax.dynamic_index_in_dim(cotangent, micro_index, 1, keepdims=False)
        d_out = (
            jnp.where(section_id == 1, own_cot, coming)
            .reshape(row_count, model_width)
            .astype(jnp.float32)
        )
        flat_rows = in_store[micro_index].reshape(row_count, model_width).astype(jnp.float32)
        queries = query_store[micro_index]
        attended = att_store[micro_index]
        log_total = total_store[micro_index]
        middle = middle_store[micro_index]
        upper = upper_store[micro_index]
        normed2_full, norm2_back = jax.vjp(
            lambda v, g, b: layer_norm(v, g, b), middle, gains[1], biases[1]
        )
        normed2 = normed2_full.astype(jnp.bfloat16)
        hidden_full, gelu_back = jax.vjp(gelu_tanh, upper)
        hidden = hidden_full.astype(jnp.bfloat16)
        d_branch = d_out.astype(jnp.bfloat16)
        grad_down = grad_down + active_weight * jnp.dot(
            hidden.T, d_branch, preferred_element_type=jnp.float32
        )
        d_hidden = jnp.dot(d_branch, w_down.T, preferred_element_type=jnp.float32)
        d_upper = gelu_back(d_hidden)[0].astype(jnp.bfloat16)
        grad_up = grad_up + active_weight * jnp.dot(
            normed2.T, d_upper, preferred_element_type=jnp.float32
        )
        d_normed2 = jnp.dot(d_upper, w_up.T, preferred_element_type=jnp.float32)
        d_mid_norm, d_gain2, d_bias2 = norm2_back(d_normed2)
        d_middle = d_out + d_mid_norm
        att_low = attended.reshape(row_count, model_width).astype(jnp.bfloat16)
        d_att = d_middle.astype(jnp.bfloat16)
        grad_out = grad_out + active_weight * jnp.dot(
            att_low.T, d_att, preferred_element_type=jnp.float32
        )
        d_attended = jnp.dot(d_att, w_out.T, preferred_element_type=jnp.float32).astype(
            jnp.bfloat16
        )
        d_attended = d_attended.reshape(seq_count, block_len, head_count, HEAD)
        row_delta = jnp.sum(d_attended.astype(jnp.float32) * attended, axis=-1)
        query_pos = (
            micro_index * group_len + ctx_id * block_len + jnp.arange(block_len, dtype=jnp.int32)
        )
        whole = lax.all_gather(cache, "ctx", axis=0, tiled=True)
        d_queries, unused = backward_keys(
            whole, queries, query_pos, log_total, row_delta, d_attended, group_len
        )
        all_queries, all_d_att = (
            lax.all_gather(queries, "ctx", axis=1, tiled=True),
            lax.all_gather(d_attended, "ctx", axis=1, tiled=True),
        )
        all_totals, all_deltas = (
            lax.all_gather(log_total, "ctx", axis=1, tiled=True),
            lax.all_gather(row_delta, "ctx", axis=1, tiled=True),
        )
        shares = owner_terms(
            cache, all_queries, all_d_att, all_totals, all_deltas, micro_index, ctx_id, group_len
        )
        key_acc = key_acc + active_weight * shares
        d_pair = jnp.swapaxes(
            lax.dynamic_index_in_dim(key_acc, micro_index, 2, keepdims=False), 0, 1
        )
        d_mixed = jnp.concatenate(
            [d_queries.reshape(row_count, model_width), d_pair.reshape(row_count, 2 * model_width)],
            axis=-1,
        ).astype(jnp.bfloat16)
        normed_full, norm1_back = jax.vjp(
            lambda v, g, b: layer_norm(v, g, b), flat_rows, gains[0], biases[0]
        )
        normed = normed_full.astype(jnp.bfloat16)
        grad_qkv = grad_qkv + active_weight * jnp.dot(
            normed.T, d_mixed, preferred_element_type=jnp.float32
        )
        d_normed = jnp.dot(d_mixed, w_qkv.T, preferred_element_type=jnp.float32)
        d_flat_norm, d_gain1, d_bias1 = norm1_back(d_normed)
        grad_gain = grad_gain + active_weight * jnp.stack([d_gain1, d_gain2])
        grad_bias = grad_bias + active_weight * jnp.stack([d_bias1, d_bias2])
        d_entering = (
            (d_middle + d_flat_norm).astype(jnp.bfloat16).reshape(seq_count, block_len, model_width)
        )
        grad_store = store_at(grad_store, d_entering, micro_index, active)
        if tick_no < group_count:
            coming = passed_along(d_entering, "section", -1)
    sums = (
        lax.psum_scatter(grad_qkv, ("ctx", "shard"), scatter_dimension=0, tiled=True),
        lax.psum_scatter(grad_out, ("ctx", "shard"), scatter_dimension=0, tiled=True),
        lax.psum_scatter(grad_up, ("ctx", "shard"), scatter_dimension=0, tiled=True),
        lax.psum_scatter(grad_down, ("ctx", "shard"), scatter_dimension=1, tiled=True),
        lax.psum_scatter(grad_gain, ("ctx", "shard"), scatter_dimension=1, tiled=True),
        lax.psum_scatter(grad_bias, ("ctx", "shard"), scatter_dimension=1, tiled=True),
    )
    layer_outputs = jnp.swapaxes(out_store, 0, 1)[None]
    input_grads = jnp.swapaxes(grad_store, 0, 1)[None]
    return (
        layer_outputs,
        input_grads,
        sums[0][None],
        sums[1][None],
        sums[2][None],
        sums[3][None],
        sums[4][None],
        sums[5][None],
    )


def solution(mesh):
    in_specs = (
        P("shard", None, "ctx", None),
        P("shard", None, "ctx", None),
        P("section", "shard", None),
        P("section", "shard", None),
        P("section", "shard", None),
        P("section", None, "shard"),
        P("section", None, "shard"),
        P("section", None, "shard"),
    )
    out_specs = (
        P("section", "shard", None, "ctx", None),
        P("section", "shard", None, "ctx", None),
        P("section", ("ctx", "shard"), None),
        P("section", ("ctx", "shard"), None),
        P("section", ("ctx", "shard"), None),
        P("section", None, ("ctx", "shard")),
        P("section", None, ("ctx", "shard")),
        P("section", None, ("ctx", "shard")),
    )
    relay = mesh.shape["section"] == 2 and mesh.shape["shard"] == 4 and mesh.shape["ctx"] == 4
    return jax.shard_map(chain if relay else shards, mesh=mesh, in_specs=in_specs, out_specs=out_specs, check_vma=False)
```

```python
import functools

import jax
import jax.numpy as jnp
from jax import lax
from jax.experimental import pallas as pl
from jax.experimental.pallas import tpu as pltpu
from jax.sharding import PartitionSpec as P

HEAD = 64
LANES = 128
ROWS = 8
NEG = -1e30
VMEM_BYTES = 66_900_000

eps_norm = 1e-05
score_scale = 0.125
f32 = jnp.float32
bf16 = jnp.bfloat16


def up_to(width, step):
    return -(-width // step) * step


def dot(a, b, dims):
    return lax.dot_general(a, b, (dims, ((), ())), preferred_element_type=f32)


def mm(a, b):
    return dot(a, b, ((1,), (0,)))


def mm_t(a, b):
    return dot(a, b, ((1,), (1,)))


def t_mm(a, b):
    return dot(a, b, ((0,), (0,)))


def attention_masks(core, half):
    row = lax.broadcasted_iota(jnp.int32, (2 * half, 2 * half), 0)
    col = lax.broadcasted_iota(jnp.int32, (2 * half, 2 * half), 1)
    row_slice, col_slice = row // half, col // half
    own = (col_slice < row_slice) | ((col_slice == row_slice) & (col <= row))
    other = (col_slice < row_slice) | ((col_slice == row_slice) & (core == 1))
    return jnp.where(jnp.stack([own, other]), 0.0, NEG).astype(f32)


def norm_backward(hat, scale, gain, grad):
    scaled = grad * gain
    mean = jnp.mean(scaled, axis=-1, keepdims=True)
    along = jnp.mean(scaled * hat, axis=-1, keepdims=True)
    return scale * (scaled - mean - hat * along)


ANY = pl.BlockSpec(memory_space=pl.ANY)


def remote(src, dst, send, recv, section, ctx, shard):
    return pltpu.make_async_remote_copy(
        src_ref=src,
        dst_ref=dst,
        send_sem=send,
        recv_sem=recv,
        device_id=(section, ctx, shard),
        device_id_type=pl.DeviceIdType.MESH,
    )


def normalised(values):
    mean = jnp.mean(values, axis=-1, keepdims=True)
    centred = values - mean
    var = jnp.mean(centred * centred, axis=-1, keepdims=True)
    scale = lax.rsqrt(var + eps_norm)
    return centred * scale, scale


def stack_heads(value, low):
    zero = jnp.zeros_like(value)
    return jnp.concatenate([jnp.where(low, value, zero), jnp.where(low, zero, value)], axis=0)


def unstack_heads(value, low):
    rows = value.shape[0] // 2
    return jnp.where(low, value[:rows], value[rows:])


def mask_last(scores, mask):
    width = mask.shape[1]
    last = scores[:, scores.shape[1] - width :] + mask
    if scores.shape[1] == width:
        return last
    return jnp.concatenate([scores[:, : scores.shape[1] - width], last], axis=1)


def attend_chunk(u, rows, mask_ref, q, k, k1, v, v1, o, lse):
    size = rows.size
    keys = pl.ds(0, (u + 1) * size)
    lane = lax.broadcasted_iota(jnp.int32, (size, LANES), 1)
    low = lane < HEAD

    @pl.loop(0, q.shape[1] // LANES, unroll=3)
    def _(pair):
        cols = pl.ds(pl.multiple_of(pair * LANES, LANES), LANES)
        q2 = stack_heads(q[rows, cols], low)
        scores = [mask_last(mm_t(q2, ref[keys, cols]), mask_ref[part]) for part, ref in enumerate((k, k1))]
        top = jnp.maximum(
            jnp.max(scores[0], axis=1, keepdims=True), jnp.max(scores[1], axis=1, keepdims=True)
        )
        total, acc = 0.0, 0.0
        for s, ref in zip(scores, (v, v1)):
            p = jnp.exp(s - top)
            total = total + jnp.sum(p, axis=1, keepdims=True)
            acc = acc + mm(p.astype(bf16), ref[keys, cols])
        o[rows, cols] = unstack_heads(acc / total, low)
        level = top + jnp.log(total)
        lse[rows, :] = jnp.where(
            lane == 2 * pair, level[:size], jnp.where(lane == 2 * pair + 1, level[size:], lse[rows, :])
        )


def near_ctx(c, step):
    return c + step - 2 * step * lax.rem(c // step, 2)


def add_into(total, term):
    total[...] = (total[...].astype(f32) + term[...].astype(f32)).astype(bf16)


def relay_kernel(
    attn_ref, ff_ref, x_ref, g_ref, norm_ref, mask_ref, place_ref,
    attn_out, ff_out, rows_out, sums_out,
    w, tokens, norm_all, norms, ent, nrm, lea, coming, slots, o, lse, da, big, sums, sums_in, spread, first, second, third,
    send, recv, token_send, token_recv, norm_send, norm_recv, far_send,
    up_send, up_recv, down_send, down_recv, pair_send, pair_recv, swap_send, swap_recv, rows_send, rows_recv, free,
    sums_send, sums_recv, first_send, first_recv, second_send, second_recv, third_send, third_recv, last_send, last_recv,
):
    section, ctx, shard = lax.axis_index("section"), lax.axis_index("ctx"), lax.axis_index("shard")
    kind = lax.rem(shard, 2)
    late = shard // 2
    far_core = 1 - late
    x_ctx, y_ctx = near_ctx(ctx, 1), near_ctx(ctx, 2)
    d_ctx = near_ctx(x_ctx, 2)
    width = ent.shape[1]
    wide = attn_ref.shape[1]
    size = da.shape[0]
    half = size // 2
    chunks = ent.shape[0] // size
    ff_half = ff_ref.shape[1]
    attn_cols = pl.ds(0, wide)
    ff_cols = pl.ds(0, ff_half)
    parts = ((0, wide), (wide, ff_half - wide))

    def token_copy(which, block):
        src, stage = ((x_ref, 0), (g_ref, 3))[which]
        return remote(
            src.at[block], tokens.at[ctx, block], token_send.at[which, block], token_recv.at[ctx, block], section, shard, stage
        )

    x_stays = (shard == 0) & (ctx == 0)
    g_stays = (shard == 3) & (ctx == 3)
    attn_copy = remote(
        attn_ref, w.at[ctx, shard, :, attn_cols], far_send.at[0], recv.at[ctx, shard], far_core, ctx, 2 * section
    )
    ff_copy = remote(
        ff_ref, w.at[ctx, shard, :, ff_cols], far_send.at[1], recv.at[ctx, shard], far_core, ctx, 2 * section + 1
    )
    norm_local = pltpu.make_async_copy(norm_ref, norm_all.at[shard], norm_recv.at[shard])

    def token_start(which, block, stays):
        src = (x_ref, g_ref)[which]

        @pl.when(stays)
        def _():
            pltpu.make_async_copy(src.at[block], tokens.at[ctx, block], token_recv.at[ctx, block]).start()

        @pl.when(jnp.logical_not(stays))
        def _():
            token_copy(which, block).start()

    token_start(0, 0, x_stays)
    attn_copy.start()
    token_start(0, 1, x_stays)
    norm_copies = []
    for core in range(2):
        for stage in range(2):
            copy = remote(
                norm_ref, norm_all.at[shard], norm_send.at[core * 2 + stage], norm_recv.at[shard],
                core, ctx, 2 * section + stage,
            )
            stays = (section == core) & (shard == 2 * section + stage)
            norm_copies.append((copy, stays))

            @pl.when(stays)
            def _():
                norm_local.start()

            @pl.when(jnp.logical_not(stays))
            def _():
                copy.start()

    ff_copy.start()
    for block in (1, 0):
        token_start(1, block, g_stays)

    def piece(cols, c, s, which, core, to_ctx):
        ref = w.at[c, s, :, cols]
        return remote(ref, ref, send.at[which], recv.at[c, s], core, to_ctx, shard)

    def collect(cols):
        here = lax.rem(section + late, 2)
        mine = [
            here * shard + (1 - here) * (2 - late),
            here * (shard + 1 - 2 * kind) + (1 - here) * (3 - 3 * late),
        ]
        started = []

        def go(c, s, core, to_ctx):
            copy = piece(cols, c, s, len(started), core, to_ctx)
            copy.start()
            started.append(copy)

        def arrived(c, s):
            piece(cols, c, s, 0, section, ctx).wait_recv()

        for s in mine:
            arrived(ctx, s)
            go(ctx, s, section, x_ctx)
            go(ctx, s, section, y_ctx)
            go(ctx, s, 1 - section, ctx)
        arrived(x_ctx, mine[0])
        go(x_ctx, mine[0], section, y_ctx)
        go(x_ctx, mine[0], 1 - section, ctx)
        arrived(y_ctx, mine[0])
        go(y_ctx, mine[0], 1 - section, ctx)
        arrived(y_ctx, mine[1])
        go(y_ctx, mine[1], section, x_ctx)
        go(y_ctx, mine[1], 1 - section, ctx)
        arrived(x_ctx, mine[1])
        go(x_ctx, mine[1], 1 - section, ctx)
        for s in mine:
            arrived(d_ctx, s)
            go(d_ctx, s, 1 - section, ctx)
        for c in (ctx, x_ctx, y_ctx, d_ctx):
            for j in range(2):
                arrived(c, 2 * section + j)
        for s in range(4):
            pltpu.make_async_copy(norm_ref, norm_all.at[s], norm_recv.at[s]).wait()
        norms[...] = (norm_all[0] + norm_all[1]) + (norm_all[2] + norm_all[3])
        return started

    def tokens_arrived(u):
        for c in range(2):
            at = 2 * lax.rem(u, 2) + c
            pltpu.make_async_copy(x_ref.at[0], tokens.at[at, u // 2], token_recv.at[at, u // 2]).wait()

    def tokens_of(u):
        return tokens[pl.ds(2 * lax.rem(u, 2), 2), u // 2].reshape(size, width)

    def chunk_rows(u):
        return pl.ds(pl.multiple_of(u * size, size), size)

    def up_copy(u, stage):
        rows = chunk_rows(u)
        return remote(lea.at[rows], ent.at[rows], up_send.at[u], up_recv.at[u], section, ctx, stage)

    def down_copy(u, stage):
        rows = chunk_rows(u)
        return remote(ent.at[rows], coming.at[rows], down_send.at[u], down_recv.at[u], section, ctx, stage)

    def weight(c, start, columns):
        value = w[c, :, :, pl.ds(start, columns)]
        return value.reshape(value.shape[0] * value.shape[1], columns)

    def rows_copy(src, t, local):
        block, c = t // 4, lax.rem(t, 4)
        src = src.at[pl.ds(pl.multiple_of(t * half, half), half)]
        dst = rows_out.at[kind, block, pl.ds(pl.multiple_of(section * half, half), half)]
        recv = rows_recv.at[kind, section, block]
        if local:
            return pltpu.make_async_copy(src, dst, recv)
        return remote(src, dst, rows_send.at[t], recv, shard // 2, c, ctx)

    def rows_stay(t):
        return (section == shard // 2) & (ctx == lax.rem(t, 4)) & (ctx == shard)

    def rows_start(src, t):
        @pl.when(rows_stay(t))
        def _():
            rows_copy(src, t, True).start()

        @pl.when(jnp.logical_not(rows_stay(t)))
        def _():
            rows_copy(src, t, False).start()

    def rows_finish(src):
        @pl.loop(0, 2 * chunks)
        def _(t):

            @pl.when(jnp.logical_not(rows_stay(t)))
            def _():
                rows_copy(src, t, False).wait_send()

    def finish_chunk(rows, d_normed, gain):
        hat, scale = normalised(ent[rows].astype(f32))
        sums[0:1, :width] += jnp.sum(d_normed * hat, axis=0, keepdims=True)
        sums[1:2, :width] += jnp.sum(d_normed, axis=0, keepdims=True)
        total = coming[rows].astype(f32) + norm_backward(hat, scale, gain, d_normed)
        ent[rows] = total.astype(bf16)

    sums[...] = jnp.zeros_like(sums)

    def group_columns(index, ref):
        feature = lax.broadcasted_iota(jnp.int32, (LANES, width), 1)

        @pl.loop(0, 2)
        def _(side):
            @pl.loop(0, spread.shape[2] // LANES)
            def _(tile):
                at = pl.ds(pl.multiple_of(tile * LANES, LANES), LANES)
                chosen = jnp.where(feature == place_ref[side, at, 0:1], 1.0, 0.0).astype(bf16)
                spread[index, side, at, :] = mm_t(chosen, ref[...]).astype(bf16)

    def reduce(source, pieces, turn, out_ref, which):
        rows = first.shape[3]
        gap = up_to(rows, 16)
        count = out_ref.shape[0]
        lanes = lambda p: pl.ds(pieces[p][0], pieces[p][1])
        own = lambda a, p, c, j: w.at[a, c, pl.ds(gap * j, rows), lanes(p)]
        array = lambda a: lax.rem(a + turn, count)

        def first_copy(a, p, j):
            even = lax.rem(a, 2)
            return remote(
                w.at[2 * even + j, :, pl.ds(2 * gap, rows), lanes(p)], first.at[even, j, :, :, lanes(p)],
                first_send.at[a, p, j], first_recv.at[a, p, j], 1 - section, ctx, shard,
            )

        def second_copy(a, p, j, part):
            to = (x_ctx, y_ctx)[j]
            return remote(
                own(a, p, (to, d_ctx)[part], j), second.at[a, j, part, :, lanes(p)],
                second_send.at[a, p, j, part], second_recv.at[a, p, j, part], section, to, shard,
            )

        def third_copy(a, p, j):
            to = (y_ctx, x_ctx)[j]
            return remote(
                own(a, p, to, j), third.at[a, j, :, lanes(p)],
                third_send.at[a, p, j], third_recv.at[a, p, j], section, to, shard,
            )

        def last_copy(a, p, j):
            return remote(
                own(a, p, ctx, j), out_ref.at[array(a), :, lanes(p)],
                last_send.at[a, p, j], last_recv.at[which, array(a), p],
                shard // 2, ctx, 2 * (1 - section) + j,
            )

        def terms(a, p):
            @pl.loop(0, 2)
            def _(side):
                def emit(index, ref, columns):
                    def block(at, step):
                        value = mm(spread[index, side, pl.ds(0, 8 * rows), :], ref[:, pl.ds(at, step)])
                        cols = pl.ds(pl.multiple_of(pieces[p][0] + at, LANES), step)
                        for n in range(8):
                            lead = side * a + (1 - side) * (2 * lax.rem(a, 2) + n % 2)
                            row = pl.multiple_of(side * (gap * (n % 2)) + (1 - side) * 2 * gap, 16)
                            w[lead, n // 2, pl.ds(row, rows), cols] = value[n * rows : (n + 1) * rows].astype(bf16)

                    step = 2 * LANES

                    @pl.loop(0, columns // step)
                    def _(b):
                        block(pl.multiple_of(b * step, step), step)

                    if columns % step:
                        block(columns - columns % step, columns % step)

                source(a, p, side, emit)

                @pl.when(side == 0)
                def _():
                    for j in range(2):
                        first_copy(a, p, j).start()

        def stage_one(a, p):
            @pl.when(a >= 2)
            def _():
                for j in range(2):
                    first_copy(a - 2, p, j).wait_send()
                pl.semaphore_wait(free, 1)

            terms(a, p)
            for j in range(2):
                first_copy(a, p, j).wait_recv()

                @pl.loop(0, 4)
                def _(c):
                    add_into(own(a, p, c, j), first.at[lax.rem(a, 2), j, c, :, lanes(p)])

            @pl.when(a + 2 < count)
            def _():
                pl.semaphore_signal(
                    free, inc=1, device_id=(1 - section, ctx, shard), device_id_type=pl.DeviceIdType.MESH
                )

            for part in (1, 0):
                for j in range(2):
                    second_copy(a, p, j, part).start()

        def stage_two(a, p):
            for j in range(2):
                second_copy(a, p, j, 1).wait_recv()
                add_into(own(a, p, (y_ctx, x_ctx)[j], j), second.at[a, j, 1, :, lanes(p)])
                third_copy(a, p, j).start()
            for j in range(2):
                second_copy(a, p, j, 0).wait_recv()
                add_into(own(a, p, ctx, j), second.at[a, j, 0, :, lanes(p)])

        def stage_three(a, p):
            for j in range(2):
                third_copy(a, p, j).wait_recv()
                add_into(own(a, p, ctx, j), third.at[a, j, :, lanes(p)])
                last_copy(a, p, j).start()

        def sums_copy(step):
            to_core, to_ctx = ((1 - section, ctx), (section, x_ctx), (section, y_ctx))[step]
            return remote(sums, sums_in.at[step], sums_send.at[step], sums_recv.at[step], to_core, to_ctx, shard)

        def sums_last(j):
            return remote(
                sums, sums_out.at[which], sums_send.at[3 + j], sums_recv.at[3 + which],
                shard // 2, ctx, 2 * (1 - section) + j,
            )

        sums_copy(0).start()
        items = len(pieces)

        @pl.loop(0, count + 2)
        def _(a):
            for p in range(items):

                @pl.when(a < count)
                def _():
                    stage_one(a, p)

                back = [(-(-(d - p) // items), (p - d) % items) for d in (1, 2)]

                @pl.when((a >= back[0][0]) & (a < count + back[0][0]))
                def _():
                    stage_two(a - back[0][0], back[0][1])

                @pl.when((a >= back[1][0]) & (a < count + back[1][0]))
                def _():
                    stage_three(a - back[1][0], back[1][1])

            for step in range(3):

                @pl.when(a == step)
                def _():
                    sums_copy(step).wait()
                    sums[...] += sums_in[step]
                    if step < 2:
                        sums_copy(step + 1).start()
                    else:
                        for j in range(2):
                            sums_last(j).start()

        @pl.loop(0, count)
        def _(a):
            for p in range(items):
                for j in range(2):

                    @pl.when(a >= count - 2)
                    def _():
                        first_copy(a, p, j).wait_send()

                    for part in range(2):
                        second_copy(a, p, j, part).wait_send()
                    third_copy(a, p, j).wait_send()
                    last_copy(a, p, j).wait_send()

        for j in range(2):
            sums_last(j).wait_send()

    @pl.when(kind == 0)
    def _():
        started = collect(attn_cols)

        lse[...] = jnp.zeros_like(lse)
        da[...] = jnp.zeros_like(da)
        gain, bias = norms[0:1, :width], norms[2:3, :width]

        def pair_copy(which, u):
            rows = chunk_rows(u)
            return remote(
                slots.at[1 + which, rows], slots.at[3 + which, rows], pair_send.at[which, u], pair_recv.at[which, u],
                1 - section, ctx, shard,
            )

        @pl.loop(0, chunks)
        def _(u):
            rows = chunk_rows(u)

            @pl.when(shard == 0)
            def _():
                tokens_arrived(u)
                ent[rows] = tokens_of(u)

            @pl.when(shard > 0)
            def _():
                up_copy(u, shard).wait_recv()

            hat, _ = normalised(ent[rows].astype(f32))
            normed = (hat * gain + bias).astype(bf16)
            nrm[rows] = normed

            @pl.loop(0, 3)
            def _(turn):
                index = lax.rem(turn + 1, 3)
                scale = jnp.where(turn == 2, score_scale, 1.0)
                slots[index, rows] = (mm(normed, weight(index, 0, wide)) * scale).astype(bf16)

                @pl.when(turn < 2)
                def _():
                    pair_copy(turn, u).start()

            for which in range(2):
                pair_copy(which, u).wait_recv()
            for index in range(chunks):

                @pl.when(u == index)
                def _():
                    attend_chunk(
                        index, pl.ds(index * size, size), mask_ref,
                        slots.at[0], slots.at[1], slots.at[3], slots.at[2], slots.at[4], o, lse,
                    )

            out = mm(o[rows, :width].astype(bf16), weight(3, 0, wide))[:, :width]
            lea[rows] = (ent[rows].astype(f32) + out).astype(bf16)
            up_copy(u, shard + 1).start()

        @pl.loop(0, chunks)
        def _(u):
            for which in range(2):
                pair_copy(which, u).wait_send()
            up_copy(u, shard + 1).wait_send()

        for copy in started:
            copy.wait_send()

        slots[7] = o[...].astype(bf16)
        group_columns(0, nrm)
        group_columns(1, slots.at[7, :, pl.ds(0, width)])
        lane = lax.broadcasted_iota(jnp.int32, (size, LANES), 1)
        low = lane < HEAD

        def swap_copy(which, u):
            rows = chunk_rows(u)
            return remote(
                slots.at[3 + which, rows], slots.at[5 + which, rows], swap_send.at[which, u], swap_recv.at[which, u],
                1 - section, ctx, shard,
            )

        @pl.loop(0, chunks)
        def _(step):
            u = chunks - 1 - step
            rows_now = chunk_rows(u)
            down_copy(u, shard).wait_recv()
            da[:, :width] = mm_t(coming[rows_now], weight(3, 0, width)).astype(bf16)
            for index in range(chunks):

                @pl.when(u == index)
                def _():
                    rows = pl.ds(index * size, size)
                    keys = pl.ds(0, (index + 1) * size)

                    @pl.loop(0, wide // LANES, unroll=3)
                    def _(pair):
                        cols = pl.ds(pl.multiple_of(pair * LANES, LANES), LANES)
                        q2 = stack_heads(slots[0, rows, cols], low)
                        grad = da[:, cols]
                        a2 = stack_heads(grad, low)
                        level = lse[rows, :]
                        product = grad.astype(f32) * o[rows, cols]
                        column = lambda which: jnp.sum(jnp.where(lane == 2 * pair + which, level, 0.0), axis=1, keepdims=True)
                        level2 = jnp.concatenate([column(0), column(1)], axis=0)
                        delta2 = jnp.concatenate(
                            [
                                jnp.sum(jnp.where(low, product, 0.0), axis=1, keepdims=True),
                                jnp.sum(jnp.where(low, 0.0, product), axis=1, keepdims=True),
                            ],
                            axis=0,
                        )
                        dq2 = 0.0
                        for part in range(2):
                            keys_now, values_now = slots[1 + 2 * part, keys, cols], slots[2 + 2 * part, keys, cols]
                            p = jnp.exp(mask_last(mm_t(q2, keys_now), mask_ref[part]) - level2)
                            ds = (p * (mm_t(a2, values_now) - delta2)).astype(bf16)
                            dq2 = dq2 + mm(ds, keys_now)
                            d_keys, d_values = t_mm(ds, q2), t_mm(p.astype(bf16), a2)
                            if index == chunks - 1:
                                big[2 * part, keys, cols] = d_keys
                                big[2 * part + 1, keys, cols] = d_values
                            else:
                                big[2 * part, keys, cols] += d_keys
                                big[2 * part + 1, keys, cols] += d_values
                        slots[0, rows, cols] = (unstack_heads(dq2, low) * score_scale).astype(bf16)

            rows = rows_now
            for which in range(2):
                slots[3 + which, rows] = big[2 + which, rows].astype(bf16)
                swap_copy(which, u).start()

            def finish_part(which, total):
                swap_copy(which, u).wait_recv()
                slots[1 + which, rows] = (big[which, rows] + slots[5 + which, rows].astype(f32)).astype(bf16)
                return total + mm_t(slots[1 + which, rows], weight(1 + which, 0, wide))

            d_normed = lax.fori_loop(0, 2, finish_part, mm_t(slots[0, rows], weight(0, 0, wide)))
            finish_chunk(rows, d_normed, gain)

            @pl.when(shard > 0)
            def _():
                down_copy(u, shard - 1).start()

            for part in range(2):
                rows_start(ent, 2 * u + part)

        @pl.loop(0, chunks)
        def _(u):
            for which in range(2):
                swap_copy(which, u).wait_send()

        def attn_source(a, p, side, emit):
            @pl.when(a == 0)
            def _():
                emit(1, coming, width)

            @pl.when(a > 0)
            def _():
                emit(0, slots.at[jnp.maximum(a - 1, 0)], wide)

        reduce(attn_source, ((0, wide),), 3, attn_out, 0)
        rows_finish(ent)

        @pl.loop(0, chunks)
        def _(u):

            @pl.when(shard > 0)
            def _():
                down_copy(u, shard - 1).wait_send()

    @pl.when(kind == 1)
    def _():
        started = collect(ff_cols)
        gain, bias = norms[1:2, :width], norms[3:4, :width]

        @pl.loop(0, chunks)
        def _(u):
            rows = chunk_rows(u)
            up_copy(u, shard).wait_recv()
            hat, _ = normalised(ent[rows].astype(f32))
            normed = (hat * gain + bias).astype(bf16)
            nrm[rows] = normed

            def add_half(i, total):
                for part, (start, columns) in enumerate(parts):
                    cols = pl.ds(0, columns)
                    upper = mm(normed, weight(i, start, columns))
                    big[2 * i + part, rows, cols] = upper
                    hidden = jax.nn.gelu(upper, approximate=True).astype(bf16)
                    slots[4 + 2 * i + part, rows, cols] = hidden
                    total = total + mm_t(hidden, weight(2 + i, start, columns))
                return total

            lea[rows] = lax.fori_loop(0, 2, add_half, ent[rows].astype(f32)).astype(bf16)

            @pl.when(shard < 3)
            def _():
                up_copy(u, shard + 1).start()

            for part in range(2):
                rows_start(lea, 2 * u + part)

        @pl.when(shard < 3)
        def _():
            group_columns(0, nrm)

        @pl.loop(0, chunks)
        def _(step):
            u = chunks - 1 - step
            rows = chunk_rows(u)

            @pl.when(shard == 3)
            def _():
                tokens_arrived(u)
                coming[rows] = tokens_of(u)

            @pl.when(shard < 3)
            def _():
                down_copy(u, shard).wait_recv()

            grad = coming[rows]

            def back_half(i, total):
                for part, (start, columns) in enumerate(parts):
                    cols = pl.ds(0, columns)
                    d_hidden = mm(grad, weight(2 + i, start, columns))
                    _, back = jax.vjp(lambda value: jax.nn.gelu(value, approximate=True), big[2 * i + part, rows, cols])
                    d_upper = back(d_hidden)[0].astype(bf16)
                    slots[2 * i + part, rows, cols] = d_upper
                    total = total + mm_t(d_upper, weight(i, start, columns))
                return total

            finish_chunk(rows, lax.fori_loop(0, 2, back_half, jnp.zeros((size, width), f32)), gain)
            down_copy(u, shard - 1).start()

        for copy in started:
            copy.wait_send()

        @pl.when(shard == 3)
        def _():
            group_columns(0, nrm)

        def ff_source(a, p, side, emit):
            if p == 0:

                @pl.when((a == 2) & (side == 0))
                def _():
                    group_columns(1, coming)

            emit(a // 2, slots.at[2 * a + p], parts[p][1])

        reduce(ff_source, parts, 0, ff_out, 1)
        rows_finish(lea)

        @pl.loop(0, chunks)
        def _(u):

            @pl.when(shard < 3)
            def _():
                up_copy(u, shard + 1).wait_send()

            down_copy(u, shard - 1).wait_send()

    @pl.loop(0, attn_out.shape[0])
    def _(index):
        arrivals = [(0, attn_out, 0, 0, wide)] + [(1, ff_out, p, start, columns) for p, (start, columns) in enumerate(parts)]
        for which, ref, p, start, columns in arrivals:
            ref = ref.at[index, :, pl.ds(start, columns)]
            remote(ref, ref, last_send.at[index, 0, 0], last_recv.at[which, index, p], section, ctx, shard).wait_recv()

    for which in range(2):
        remote(sums, sums_out.at[which], sums_send.at[3], sums_recv.at[3 + which], section, ctx, shard).wait_recv()
        for core in range(2):
            for block in range(2):
                ref = rows_out.at[which, block, pl.ds(core * half, half)]
                pltpu.make_async_copy(ref, ref, rows_recv.at[which, core, block]).wait()

    attn_copy.wait_send()
    ff_copy.wait_send()
    for copy, stays in norm_copies + [
        (token_copy(which, block), stays) for which, stays in enumerate((x_stays, g_stays)) for block in range(2)
    ]:

        @pl.when(jnp.logical_not(stays))
        def _():
            copy.wait_send()


def relay(attn_piece, ff_piece, x_own, g_own, norm_own, mask, place, group_pad):
    share, ff_half = ff_piece.shape
    wide = attn_piece.shape[1]
    blocks, half, width = x_own.shape
    tokens = blocks * 4 * half
    size = 2 * half
    chunks = tokens // size
    dma = pltpu.SemaphoreType.DMA
    vmem = pl.BlockSpec(memory_space=pltpu.VMEM)
    narrow = ((tokens, width), bf16)
    outs = [
        ((4, group_pad, wide), bf16), ((4, group_pad, ff_half), bf16), ((2, blocks, size, width), bf16), ((2,) + norm_own.shape, f32),
    ]
    scratch = [
        ((4, 4, share, ff_half), bf16), ((4,) + x_own.shape, bf16), ((4,) + norm_own.shape, f32), (norm_own.shape, f32),
        narrow, narrow, narrow, narrow, ((8, tokens, wide), bf16),
        ((tokens, wide), f32), ((tokens, LANES), f32), ((size, wide), bf16), ((4, tokens, wide), f32),
        (norm_own.shape, f32), ((3,) + norm_own.shape, f32), ((2, 2, place.shape[1], tokens), bf16),
        ((2, 2, 4, group_pad, ff_half), bf16), ((4, 2, 2, group_pad, ff_half), bf16), ((4, 2, group_pad, ff_half), bf16),
    ]
    return pl.pallas_call(
        relay_kernel,
        in_specs=[ANY] * 5 + [vmem] * 2,
        out_specs=[ANY] * len(outs),
        out_shape=[jax.ShapeDtypeStruct(s, t) for s, t in outs],
        scratch_shapes=[pltpu.VMEM(s, t) for s, t in scratch]
        + [
            dma((14,)), dma((4, 4)), dma((2, 2)), dma((4, 2)), dma((4,)), dma((4,)), dma((2,)),
            dma((chunks,)), dma((chunks,)), dma((chunks,)), dma((chunks,)),
            dma((2, chunks)), dma((2, chunks)), dma((2, chunks)), dma((2, chunks)),
            dma((2 * chunks,)), dma((2, 2, 2)), pltpu.SemaphoreType.REGULAR,
            dma((5,)), dma((5,)), dma((4, 2, 2)), dma((4, 2, 2)), dma((4, 2, 2, 2)), dma((4, 2, 2, 2)),
            dma((4, 2, 2)), dma((4, 2, 2)), dma((4, 2, 2)), dma((2, 4, 2)),
        ],
        compiler_params=pltpu.CompilerParams(has_side_effects=True, vmem_limit_bytes=VMEM_BYTES),
        name="relay",
    )(attn_piece, ff_piece, x_own, g_own, norm_own, mask, place)


def chain(inputs, cotangent, qkv_weight, out_weight, up_weight, down_weight, norm_gain, norm_bias):
    section, ctx, shard = lax.axis_index("section"), lax.axis_index("ctx"), lax.axis_index("shard")
    seq_count, blocks, slice_len, width = inputs.shape
    half = slice_len // 2
    tokens = blocks * 4 * half
    share = width // 4
    group = share // 4
    group_pad = up_to(group, ROWS)
    wide = up_to(width, LANES)
    ff = up_weight.shape[2]
    is_attn = shard % 2 == 0

    pad = lambda w: jnp.pad(w, ((0, 0), (0, wide - width)))
    own_qkv, own_out = qkv_weight[0], out_weight[0]
    attn_src = jnp.stack([pad(own_qkv[:, i * width : (i + 1) * width]) for i in range(3)] + [pad(own_out)])
    down_t = down_weight[0].T
    up0 = up_weight[0]
    ff_src = jnp.stack([up0[:, : ff // 2], up0[:, ff // 2 :], down_t[:, : ff // 2], down_t[:, ff // 2 :]])
    norm_own = jnp.concatenate([norm_gain[0], norm_bias[0]], axis=0).astype(f32)
    norm_own = lax.dynamic_update_slice(
        jnp.zeros((ROWS, wide), f32), jnp.pad(norm_own, ((0, ROWS - 4), (0, 0))), (0, shard * share)
    )
    x_own = lax.dynamic_slice_in_dim(inputs[0], section * half, half, 1)
    g_own = lax.dynamic_slice_in_dim(cotangent[0], section * half, half, 1)
    mask = attention_masks(section, half)
    mask = jnp.concatenate([mask, mask], axis=1)
    slot = jnp.arange(up_to(8 * group_pad, LANES))
    row = slot % group_pad
    place = []
    for side in (section, 1 - section):
        owner = (slot // (2 * group_pad)) * 4 + 2 * side + (slot // group_pad) % 2
        place.append(jnp.where((row < group) & (slot < 8 * group_pad), owner * group + row, -1))
    place = jnp.broadcast_to(jnp.stack(place)[:, :, None].astype(jnp.int32), (2, slot.shape[0], LANES))
    attn_sums, ff_sums, rows, totals = relay(
        lax.dynamic_index_in_dim(attn_src, ctx, 0, keepdims=False),
        lax.dynamic_index_in_dim(ff_src, ctx, 0, keepdims=False),
        x_own, g_own, norm_own, mask, place, group_pad,
    )
    totals = lax.dynamic_slice_in_dim(totals[:, :2], (ctx * 4 + shard) * group, group, 2)
    attn_sums = attn_sums[:, :group, :width].astype(f32)
    ff_sums = ff_sums[:, :group].astype(f32)
    return (
        rows[1][None, None],
        rows[0][None, None],
        jnp.concatenate([attn_sums[0], attn_sums[1], attn_sums[2]], axis=1)[None],
        attn_sums[3][None],
        jnp.concatenate([ff_sums[0], ff_sums[1]], axis=1)[None],
        jnp.concatenate([ff_sums[2].T, ff_sums[3].T], axis=0)[None],
        totals[:, 0][None],
        totals[:, 1][None],
    )


def passed_along(value, axis, steps):
    count = lax.axis_size(axis)
    initial, last = (max(0, -steps), min(count, count - steps))
    return lax.ppermute(value, axis, [(source, source + steps) for source in range(initial, last)])


def layer_norm(values, gain, shift):
    mean = jnp.mean(values, axis=-1, keepdims=True)
    centred = values - mean
    var = jnp.mean(centred * centred, axis=-1, keepdims=True)
    return centred * lax.rsqrt(var + eps_norm) * gain + shift


def gelu_tanh(values):
    return jax.nn.gelu(values, approximate=True)


def split_pair(key_value, head_count):
    block_len, seq_count, double = key_value.shape
    model_width = double // 2
    key_rows = key_value[..., :model_width].reshape(block_len, seq_count, head_count, HEAD)
    value_rows = key_value[..., model_width:].reshape(block_len, seq_count, head_count, HEAD)
    return (key_rows, value_rows)


def causal_mask(query_pos, key_pos):
    return (key_pos[None, :] <= query_pos[:, None])[None, :, None, :]


def forward_block(running, queries, query_pos, key_value, key_pos):
    row_max, row_sum, accum = running
    key_rows, value_rows = split_pair(key_value, queries.shape[2])
    scores = (
        jnp.einsum("sqhe,kshe->sqhk", queries, key_rows, preferred_element_type=jnp.float32)
        * score_scale
    )
    causal = causal_mask(query_pos, key_pos)
    new_max = jnp.maximum(row_max, jnp.max(jnp.where(causal, scores, -1e30), axis=-1))
    softmax_w = jnp.where(causal, jnp.exp(scores - new_max[..., None]), 0.0)
    factor = jnp.exp(row_max - new_max)
    row_sum = row_sum * factor + jnp.sum(softmax_w, axis=-1)
    accum = accum * factor[..., None] + jnp.einsum(
        "sqhk,kshe->sqhe",
        softmax_w.astype(jnp.bfloat16),
        value_rows,
        preferred_element_type=jnp.float32,
    )
    return (new_max, row_sum, accum)


def split_rows(whole):
    key_count = whole.shape[0]
    block_size = 512
    blocks = whole.reshape((key_count // block_size, block_size) + whole.shape[1:])
    offsets = jnp.arange(key_count // block_size, dtype=jnp.int32) * block_size
    return (blocks, offsets, block_size)


def fold_keys(running, piece, start, queries, query_pos, group_len):
    blocks, offsets, block_size = split_rows(piece)

    def fold_scan_step(inner, scan_item):
        block_rows, offset = scan_item
        for group_id in range(block_rows.shape[2]):
            key_pos = (
                group_id * group_len + start + offset + jnp.arange(block_size, dtype=jnp.int32)
            )
            inner = forward_block(inner, queries, query_pos, block_rows[:, :, group_id], key_pos)
        return (inner, None)

    result, _ = lax.scan(fold_scan_step, running, (blocks, offsets))
    return result


def pair_terms(d_scores, softmax_w, queries, d_attended, block_size):
    d_keys = (
        jnp.einsum("sqhk,sqhe->kshe", d_scores, queries, preferred_element_type=jnp.float32)
        * score_scale
    )
    d_values = jnp.einsum(
        "sqhk,sqhe->kshe",
        softmax_w.astype(jnp.bfloat16),
        d_attended,
        preferred_element_type=jnp.float32,
    )
    shape = (block_size, queries.shape[0], queries.shape[2] * queries.shape[3])
    return jnp.concatenate([d_keys.reshape(shape), d_values.reshape(shape)], axis=-1)


def score_grads(
    queries, query_pos, log_total, row_delta, d_attended, key_rows, value_rows, key_pos
):
    scores = (
        jnp.einsum("sqhe,kshe->sqhk", queries, key_rows, preferred_element_type=jnp.float32)
        * score_scale
    )
    causal = causal_mask(query_pos, key_pos)
    softmax_w = jnp.where(causal, jnp.exp(scores - log_total[..., None]), 0.0)
    d_probs = jnp.einsum(
        "sqhe,kshe->sqhk", d_attended, value_rows, preferred_element_type=jnp.float32
    )
    d_scores = (softmax_w * (d_probs - row_delta[..., None])).astype(jnp.bfloat16)
    return (softmax_w, d_scores)


def backward_keys(whole, queries, query_pos, log_total, row_delta, d_attended, group_len):
    blocks, offsets, block_size = split_rows(whole)

    def backward_scan_step(d_queries, scan_item):
        block_rows, offset = scan_item
        for group_id in range(block_rows.shape[2]):
            key_pos = group_id * group_len + offset + jnp.arange(block_size, dtype=jnp.int32)
            key_rows, value_rows = split_pair(block_rows[:, :, group_id], queries.shape[2])
            softmax_w, d_scores = score_grads(
                queries, query_pos, log_total, row_delta, d_attended, key_rows, value_rows, key_pos
            )
            d_queries = (
                d_queries
                + jnp.einsum(
                    "sqhk,kshe->sqhe", d_scores, key_rows, preferred_element_type=jnp.float32
                )
                * score_scale
            )
        return (d_queries, None)

    d_queries, terms = lax.scan(
        backward_scan_step, jnp.zeros(queries.shape, jnp.float32), (blocks, offsets)
    )
    return (d_queries, None)


def owner_terms(
    own_cache, all_queries, all_d_att, all_totals, all_deltas, micro_index, ctx_id, group_len
):
    block_len, seq_count, group_count, double = own_cache.shape
    head_count = all_queries.shape[2]
    query_rows = all_queries.shape[1]
    query_size = 512
    block_count = query_rows // query_size

    def loop_step(index, total):
        offset = index * query_size
        q_block = lax.dynamic_slice_in_dim(all_queries, offset, query_size, 1)
        d_block = lax.dynamic_slice_in_dim(all_d_att, offset, query_size, 1)
        t_block = lax.dynamic_slice_in_dim(all_totals, offset, query_size, 1)
        r_block = lax.dynamic_slice_in_dim(all_deltas, offset, query_size, 1)
        query_pos = micro_index * group_len + offset + jnp.arange(query_size, dtype=jnp.int32)
        pieces = []
        for group_id in range(group_count):
            key_pos = (
                group_id * group_len + ctx_id * block_len + jnp.arange(block_len, dtype=jnp.int32)
            )
            key_rows, value_rows = split_pair(own_cache[:, :, group_id], head_count)
            softmax_w, d_scores = score_grads(
                q_block, query_pos, t_block, r_block, d_block, key_rows, value_rows, key_pos
            )
            pieces.append(pair_terms(d_scores, softmax_w, q_block, d_block, block_len))
        return total + jnp.stack(pieces, axis=2)

    return lax.fori_loop(0, block_count, loop_step, jnp.zeros(own_cache.shape, jnp.float32))


def store_at(store, value, micro_index, active):
    updated = lax.dynamic_update_index_in_dim(store, value, micro_index, 0)
    return jnp.where(active, updated, store)


def shards(inputs, cotangent, qkv_weight, out_weight, up_weight, down_weight, norm_gain, norm_bias):
    section_id = lax.axis_index("section")
    ctx_count = lax.axis_size("ctx")
    ctx_id = lax.axis_index("ctx")
    seq_count, group_count, block_len, model_width = inputs.shape
    head_count = model_width // HEAD
    group_len = block_len * ctx_count
    row_count = seq_count * block_len
    w_qkv, w_out, w_up, w_down, gains, biases = (
        lax.all_gather(qkv_weight[0], "shard", axis=0, tiled=True),
        lax.all_gather(out_weight[0], "shard", axis=0, tiled=True),
        lax.all_gather(up_weight[0], "shard", axis=0, tiled=True),
        lax.all_gather(down_weight[0], "shard", axis=1, tiled=True),
        lax.all_gather(norm_gain[0], "shard", axis=1, tiled=True),
        lax.all_gather(norm_bias[0], "shard", axis=1, tiled=True),
    )
    gains = gains.astype(jnp.float32)
    biases = biases.astype(jnp.float32)
    ff_width = w_up.shape[1]
    cache = jnp.zeros((block_len, seq_count, group_count, 2 * model_width), jnp.bfloat16)
    in_store = jnp.zeros((group_count, seq_count, block_len, model_width), jnp.bfloat16)
    query_store = jnp.zeros((group_count, seq_count, block_len, head_count, HEAD), jnp.bfloat16)
    att_store = jnp.zeros((group_count, seq_count, block_len, head_count, HEAD), jnp.float32)
    total_store = jnp.zeros((group_count, seq_count, block_len, head_count), jnp.float32)
    middle_store = jnp.zeros((group_count, row_count, model_width), jnp.float32)
    upper_store = jnp.zeros((group_count, row_count, ff_width), jnp.float32)
    out_store = jnp.zeros((group_count, seq_count, block_len, model_width), jnp.bfloat16)
    received = jnp.zeros((seq_count, block_len, model_width), jnp.bfloat16)
    for tick_no in range(group_count + 1):
        micro = tick_no - section_id
        active = (micro >= 0) & (micro < group_count)
        micro_index = jnp.clip(micro, 0, group_count - 1)
        own_input = lax.dynamic_index_in_dim(inputs, micro_index, 1, keepdims=False)
        entering = jnp.where(section_id == 0, own_input, received)
        flat_rows = entering.reshape(row_count, model_width).astype(jnp.float32)
        normed = layer_norm(flat_rows, gains[0], biases[0]).astype(jnp.bfloat16)
        mixed = jnp.dot(normed, w_qkv, preferred_element_type=jnp.float32).astype(jnp.bfloat16)
        queries = mixed[:, :model_width].reshape(seq_count, block_len, head_count, HEAD)
        fresh = jnp.swapaxes(
            mixed[:, model_width:].reshape(seq_count, block_len, 2 * model_width), 0, 1
        )
        updated = lax.dynamic_update_index_in_dim(cache, fresh, micro_index, 2)
        cache = jnp.where(active, updated, cache)
        query_pos = (
            micro_index * group_len + ctx_id * block_len + jnp.arange(block_len, dtype=jnp.int32)
        )
        start_state = (
            jnp.full((seq_count, block_len, head_count), -1e30, jnp.float32),
            jnp.zeros((seq_count, block_len, head_count), jnp.float32),
            jnp.zeros((seq_count, block_len, head_count, HEAD), jnp.float32),
        )
        row_max, row_sum, accum = fold_keys(
            start_state,
            lax.all_gather(cache, "ctx", axis=0, tiled=True),
            jnp.int32(0),
            queries,
            query_pos,
            group_len,
        )
        attended = accum / row_sum[..., None]
        log_total = row_max + jnp.log(row_sum)
        att_low = attended.reshape(row_count, model_width).astype(jnp.bfloat16)
        middle = flat_rows + jnp.dot(att_low, w_out, preferred_element_type=jnp.float32)
        normed2 = layer_norm(middle, gains[1], biases[1]).astype(jnp.bfloat16)
        upper = jnp.dot(normed2, w_up, preferred_element_type=jnp.float32)
        hidden = gelu_tanh(upper).astype(jnp.bfloat16)
        leaving = (middle + jnp.dot(hidden, w_down, preferred_element_type=jnp.float32)).astype(
            jnp.bfloat16
        )
        leaving = leaving.reshape(seq_count, block_len, model_width)
        in_store = store_at(in_store, entering, micro_index, active)
        query_store = store_at(query_store, queries, micro_index, active)
        att_store = store_at(att_store, attended, micro_index, active)
        total_store = store_at(total_store, log_total, micro_index, active)
        middle_store = store_at(middle_store, middle, micro_index, active)
        upper_store = store_at(upper_store, upper, micro_index, active)
        out_store = store_at(out_store, leaving, micro_index, active)
        if tick_no < group_count:
            received = passed_along(leaving, "section", 1)
    key_acc = jnp.zeros((block_len, seq_count, group_count, 2 * model_width), jnp.float32)
    grad_qkv = jnp.zeros((model_width, 3 * model_width), jnp.float32)
    grad_out = jnp.zeros((model_width, model_width), jnp.float32)
    grad_up = jnp.zeros((model_width, ff_width), jnp.float32)
    grad_down = jnp.zeros((ff_width, model_width), jnp.float32)
    grad_gain = jnp.zeros((2, model_width), jnp.float32)
    grad_bias = jnp.zeros((2, model_width), jnp.float32)
    grad_store = jnp.zeros((group_count, seq_count, block_len, model_width), jnp.bfloat16)
    coming = jnp.zeros((seq_count, block_len, model_width), jnp.bfloat16)
    for tick_no in range(group_count + 1):
        micro = group_count - tick_no - section_id
        active = (micro >= 0) & (micro < group_count)
        active_weight = active.astype(jnp.float32)
        micro_index = jnp.clip(micro, 0, group_count - 1)
        own_cot = lax.dynamic_index_in_dim(cotangent, micro_index, 1, keepdims=False)
        d_out = (
            jnp.where(section_id == 1, own_cot, coming)
            .reshape(row_count, model_width)
            .astype(jnp.float32)
        )
        flat_rows = in_store[micro_index].reshape(row_count, model_width).astype(jnp.float32)
        queries = query_store[micro_index]
        attended = att_store[micro_index]
        log_total = total_store[micro_index]
        middle = middle_store[micro_index]
        upper = upper_store[micro_index]
        normed2_full, norm2_back = jax.vjp(
            lambda v, g, b: layer_norm(v, g, b), middle, gains[1], biases[1]
        )
        normed2 = normed2_full.astype(jnp.bfloat16)
        hidden_full, gelu_back = jax.vjp(gelu_tanh, upper)
        hidden = hidden_full.astype(jnp.bfloat16)
        d_branch = d_out.astype(jnp.bfloat16)
        grad_down = grad_down + active_weight * jnp.dot(
            hidden.T, d_branch, preferred_element_type=jnp.float32
        )
        d_hidden = jnp.dot(d_branch, w_down.T, preferred_element_type=jnp.float32)
        d_upper = gelu_back(d_hidden)[0].astype(jnp.bfloat16)
        grad_up = grad_up + active_weight * jnp.dot(
            normed2.T, d_upper, preferred_element_type=jnp.float32
        )
        d_normed2 = jnp.dot(d_upper, w_up.T, preferred_element_type=jnp.float32)
        d_mid_norm, d_gain2, d_bias2 = norm2_back(d_normed2)
        d_middle = d_out + d_mid_norm
        att_low = attended.reshape(row_count, model_width).astype(jnp.bfloat16)
        d_att = d_middle.astype(jnp.bfloat16)
        grad_out = grad_out + active_weight * jnp.dot(
            att_low.T, d_att, preferred_element_type=jnp.float32
        )
        d_attended = jnp.dot(d_att, w_out.T, preferred_element_type=jnp.float32).astype(
            jnp.bfloat16
        )
        d_attended = d_attended.reshape(seq_count, block_len, head_count, HEAD)
        row_delta = jnp.sum(d_attended.astype(jnp.float32) * attended, axis=-1)
        query_pos = (
            micro_index * group_len + ctx_id * block_len + jnp.arange(block_len, dtype=jnp.int32)
        )
        whole = lax.all_gather(cache, "ctx", axis=0, tiled=True)
        d_queries, unused = backward_keys(
            whole, queries, query_pos, log_total, row_delta, d_attended, group_len
        )
        all_queries, all_d_att = (
            lax.all_gather(queries, "ctx", axis=1, tiled=True),
            lax.all_gather(d_attended, "ctx", axis=1, tiled=True),
        )
        all_totals, all_deltas = (
            lax.all_gather(log_total, "ctx", axis=1, tiled=True),
            lax.all_gather(row_delta, "ctx", axis=1, tiled=True),
        )
        shares = owner_terms(
            cache, all_queries, all_d_att, all_totals, all_deltas, micro_index, ctx_id, group_len
        )
        key_acc = key_acc + active_weight * shares
        d_pair = jnp.swapaxes(
            lax.dynamic_index_in_dim(key_acc, micro_index, 2, keepdims=False), 0, 1
        )
        d_mixed = jnp.concatenate(
            [d_queries.reshape(row_count, model_width), d_pair.reshape(row_count, 2 * model_width)],
            axis=-1,
        ).astype(jnp.bfloat16)
        normed_full, norm1_back = jax.vjp(
            lambda v, g, b: layer_norm(v, g, b), flat_rows, gains[0], biases[0]
        )
        normed = normed_full.astype(jnp.bfloat16)
        grad_qkv = grad_qkv + active_weight * jnp.dot(
            normed.T, d_mixed, preferred_element_type=jnp.float32
        )
        d_normed = jnp.dot(d_mixed, w_qkv.T, preferred_element_type=jnp.float32)
        d_flat_norm, d_gain1, d_bias1 = norm1_back(d_normed)
        grad_gain = grad_gain + active_weight * jnp.stack([d_gain1, d_gain2])
        grad_bias = grad_bias + active_weight * jnp.stack([d_bias1, d_bias2])
        d_entering = (
            (d_middle + d_flat_norm).astype(jnp.bfloat16).reshape(seq_count, block_len, model_width)
        )
        grad_store = store_at(grad_store, d_entering, micro_index, active)
        if tick_no < group_count:
            coming = passed_along(d_entering, "section", -1)
    sums = (
        lax.psum_scatter(grad_qkv, ("ctx", "shard"), scatter_dimension=0, tiled=True),
        lax.psum_scatter(grad_out, ("ctx", "shard"), scatter_dimension=0, tiled=True),
        lax.psum_scatter(grad_up, ("ctx", "shard"), scatter_dimension=0, tiled=True),
        lax.psum_scatter(grad_down, ("ctx", "shard"), scatter_dimension=1, tiled=True),
        lax.psum_scatter(grad_gain, ("ctx", "shard"), scatter_dimension=1, tiled=True),
        lax.psum_scatter(grad_bias, ("ctx", "shard"), scatter_dimension=1, tiled=True),
    )
    layer_outputs = jnp.swapaxes(out_store, 0, 1)[None]
    input_grads = jnp.swapaxes(grad_store, 0, 1)[None]
    return (
        layer_outputs,
        input_grads,
        sums[0][None],
        sums[1][None],
        sums[2][None],
        sums[3][None],
        sums[4][None],
        sums[5][None],
    )


def solution(mesh):
    in_specs = (
        P("shard", None, "ctx", None),
        P("shard", None, "ctx", None),
        P("section", "shard", None),
        P("section", "shard", None),
        P("section", "shard", None),
        P("section", None, "shard"),
        P("section", None, "shard"),
        P("section", None, "shard"),
    )
    out_specs = (
        P("section", "shard", None, "ctx", None),
        P("section", "shard", None, "ctx", None),
        P("section", ("ctx", "shard"), None),
        P("section", ("ctx", "shard"), None),
        P("section", ("ctx", "shard"), None),
        P("section", None, ("ctx", "shard")),
        P("section", None, ("ctx", "shard")),
        P("section", None, ("ctx", "shard")),
    )
    relay = mesh.shape["section"] == 2 and mesh.shape["shard"] == 4 and mesh.shape["ctx"] == 4
    return jax.shard_map(chain if relay else shards, mesh=mesh, in_specs=in_specs, out_specs=out_specs, check_vma=False)
```

```python
import functools

import jax
import jax.numpy as jnp
from jax import lax
from jax.experimental import pallas as pl
from jax.experimental.pallas import tpu as pltpu
from jax.sharding import PartitionSpec as P

HEAD = 64
LANES = 128
ROWS = 8
NEG = -1e30
VMEM_BYTES = 66_900_000

eps_norm = 1e-05
score_scale = 0.125
f32 = jnp.float32
bf16 = jnp.bfloat16


def up_to(width, step):
    return -(-width // step) * step


def dot(a, b, dims):
    return lax.dot_general(a, b, (dims, ((), ())), preferred_element_type=f32)


def mm(a, b):
    return dot(a, b, ((1,), (0,)))


def mm_t(a, b):
    return dot(a, b, ((1,), (1,)))


def t_mm(a, b):
    return dot(a, b, ((0,), (0,)))


def attention_masks(core, half):
    row = lax.broadcasted_iota(jnp.int32, (2 * half, 2 * half), 0)
    col = lax.broadcasted_iota(jnp.int32, (2 * half, 2 * half), 1)
    row_slice, col_slice = row // half, col // half
    own = (col_slice < row_slice) | ((col_slice == row_slice) & (col <= row))
    other = (col_slice < row_slice) | ((col_slice == row_slice) & (core == 1))
    return jnp.where(jnp.stack([own, other]), 0.0, NEG).astype(f32)


def norm_backward(hat, scale, gain, grad):
    scaled = grad * gain
    mean = jnp.mean(scaled, axis=-1, keepdims=True)
    along = jnp.mean(scaled * hat, axis=-1, keepdims=True)
    return scale * (scaled - mean - hat * along)


ANY = pl.BlockSpec(memory_space=pl.ANY)


def remote(src, dst, send, recv, section, ctx, shard):
    return pltpu.make_async_remote_copy(
        src_ref=src,
        dst_ref=dst,
        send_sem=send,
        recv_sem=recv,
        device_id=(section, ctx, shard),
        device_id_type=pl.DeviceIdType.MESH,
    )


def normalised(values):
    mean = jnp.mean(values, axis=-1, keepdims=True)
    centred = values - mean
    var = jnp.mean(centred * centred, axis=-1, keepdims=True)
    scale = lax.rsqrt(var + eps_norm)
    return centred * scale, scale


def stack_heads(value, low):
    zero = jnp.zeros_like(value)
    return jnp.concatenate([jnp.where(low, value, zero), jnp.where(low, zero, value)], axis=0)


def unstack_heads(value, low):
    rows = value.shape[0] // 2
    return jnp.where(low, value[:rows], value[rows:])


def mask_last(scores, mask):
    width = mask.shape[1]
    last = scores[:, scores.shape[1] - width :] + mask
    if scores.shape[1] == width:
        return last
    return jnp.concatenate([scores[:, : scores.shape[1] - width], last], axis=1)


def attend_chunk(u, rows, mask_ref, q, k, k1, v, v1, o, lse):
    size = rows.size
    keys = pl.ds(0, (u + 1) * size)
    lane = lax.broadcasted_iota(jnp.int32, (size, LANES), 1)
    low = lane < HEAD

    @pl.loop(0, q.shape[1] // LANES, unroll=3)
    def _(pair):
        cols = pl.ds(pl.multiple_of(pair * LANES, LANES), LANES)
        q2 = stack_heads(q[rows, cols], low)
        scores = [mask_last(mm_t(q2, ref[keys, cols]), mask_ref[part]) for part, ref in enumerate((k, k1))]
        top = jnp.maximum(
            jnp.max(scores[0], axis=1, keepdims=True), jnp.max(scores[1], axis=1, keepdims=True)
        )
        total, acc = 0.0, 0.0
        for s, ref in zip(scores, (v, v1)):
            p = jnp.exp(s - top)
            total = total + jnp.sum(p, axis=1, keepdims=True)
            acc = acc + mm(p.astype(bf16), ref[keys, cols])
        o[rows, cols] = unstack_heads(acc / total, low)
        level = top + jnp.log(total)
        lse[rows, :] = jnp.where(
            lane == 2 * pair, level[:size], jnp.where(lane == 2 * pair + 1, level[size:], lse[rows, :])
        )


def near_ctx(c, step):
    return c + step - 2 * step * lax.rem(c // step, 2)


def add_into(total, term):
    total[...] = (total[...].astype(f32) + term[...].astype(f32)).astype(bf16)


def relay_kernel(
    attn_ref, ff_ref, x_ref, g_ref, norm_ref, mask_ref, place_ref,
    attn_out, ff_out, rows_out, sums_out,
    w, staged, norm_all, norms, ent, nrm, lea, coming, slots, o, lse, da, big, sums, sums_in, spread, first, second, third,
    send, recv, token_send, token_recv, norm_send, norm_recv, far_send,
    up_send, up_recv, down_send, down_recv, pair_send, pair_recv, swap_send, swap_recv, rows_send, rows_recv, free,
    sums_send, sums_recv, first_send, first_recv, second_send, second_recv, third_send, third_recv, last_send, last_recv,
    staged_recv, pass_send,
):
    section, ctx, shard = lax.axis_index("section"), lax.axis_index("ctx"), lax.axis_index("shard")
    kind = lax.rem(shard, 2)
    late = shard // 2
    far_core = 1 - late
    x_ctx, y_ctx = near_ctx(ctx, 1), near_ctx(ctx, 2)
    d_ctx = near_ctx(x_ctx, 2)
    width = ent.shape[1]
    wide = attn_ref.shape[1]
    size = da.shape[0]
    half = size // 2
    chunks = ent.shape[0] // size
    ff_half = ff_ref.shape[1]
    attn_cols = pl.ds(0, wide)
    ff_cols = pl.ds(0, ff_half)
    parts = ((0, wide), (wide, ff_half - wide))

    def token_rows(ref, c, block):
        return ref.at[pl.ds(pl.multiple_of((block * 4 + c) * half, half), half)]

    def x_copy(block, straight):
        index = jnp.maximum(shard - 1, 0)
        dst = token_rows(ent, ctx, block) if straight else staged.at[index, block]
        arrived = token_recv.at[ctx, block] if straight else staged_recv.at[index, block]
        return remote(
            x_ref.at[block], dst, token_send.at[0, block], arrived, section, ctx * jnp.minimum(shard, 1), 0
        )

    def g_copy(block):
        return remote(
            g_ref.at[block], token_rows(coming, ctx, block), token_send.at[1, block], token_recv.at[ctx, block], section, shard, 3
        )

    def pass_copy(s, block):
        return remote(
            staged.at[s - 1, block], token_rows(ent, ctx, block), pass_send.at[s - 1, block], token_recv.at[ctx, block],
            section, s, 0,
        )

    x_straight = (shard == 0) | (ctx == shard)
    x_stays = (shard == 0) & (ctx == 0)
    g_stays = (shard == 3) & (ctx == 3)
    attn_copy = remote(
        attn_ref, w.at[ctx, shard, :, attn_cols], far_send.at[0], recv.at[ctx, shard], far_core, ctx, 2 * section
    )
    ff_copy = remote(
        ff_ref, w.at[ctx, shard, :, ff_cols], far_send.at[1], recv.at[ctx, shard], far_core, ctx, 2 * section + 1
    )
    norm_local = pltpu.make_async_copy(norm_ref, norm_all.at[shard], norm_recv.at[shard])

    def stay_copy(src, dst, block):
        return pltpu.make_async_copy(src.at[block], token_rows(dst, ctx, block), token_recv.at[ctx, block])

    def x_start(block):
        @pl.when(x_stays)
        def _():
            stay_copy(x_ref, ent, block).start()

        @pl.when(x_straight & jnp.logical_not(x_stays))
        def _():
            x_copy(block, True).start()

        @pl.when(jnp.logical_not(x_straight))
        def _():
            x_copy(block, False).start()

    def pass_on(block):
        for s in range(1, 4):

            @pl.when((shard == 0) & (ctx != s))
            def _():
                ref = staged.at[s - 1, block]
                pltpu.make_async_copy(ref, ref, staged_recv.at[s - 1, block]).wait()
                pass_copy(s, block).start()

    x_start(0)
    attn_copy.start()
    x_start(1)
    norm_copies = []
    for core in range(2):
        for stage in range(2):
            copy = remote(
                norm_ref, norm_all.at[shard], norm_send.at[core * 2 + stage], norm_recv.at[shard],
                core, ctx, 2 * section + stage,
            )
            stays = (section == core) & (shard == 2 * section + stage)
            norm_copies.append((copy, stays))

            @pl.when(stays)
            def _():
                norm_local.start()

            @pl.when(jnp.logical_not(stays))
            def _():
                copy.start()

    ff_copy.start()
    for block in (1, 0):

        @pl.when(g_stays)
        def _():
            stay_copy(g_ref, coming, block).start()

        @pl.when(jnp.logical_not(g_stays))
        def _():
            g_copy(block).start()


    def piece(cols, c, s, which, core, to_ctx):
        ref = w.at[c, s, :, cols]
        return remote(ref, ref, send.at[which], recv.at[c, s], core, to_ctx, shard)

    def collect(cols):
        here = lax.rem(section + late, 2)
        mine = [
            here * shard + (1 - here) * (2 - late),
            here * (shard + 1 - 2 * kind) + (1 - here) * (3 - 3 * late),
        ]
        started = []

        def go(c, s, core, to_ctx):
            copy = piece(cols, c, s, len(started), core, to_ctx)
            copy.start()
            started.append(copy)

        def arrived(c, s):
            piece(cols, c, s, 0, section, ctx).wait_recv()

        for turn, s in enumerate(mine):
            arrived(ctx, s)
            go(ctx, s, section, x_ctx)
            go(ctx, s, section, y_ctx)
            go(ctx, s, 1 - section, ctx)
            if cols is attn_cols:
                pass_on(turn)
        arrived(x_ctx, mine[0])
        go(x_ctx, mine[0], section, y_ctx)
        go(x_ctx, mine[0], 1 - section, ctx)
        arrived(y_ctx, mine[0])
        go(y_ctx, mine[0], 1 - section, ctx)
        arrived(y_ctx, mine[1])
        go(y_ctx, mine[1], section, x_ctx)
        go(y_ctx, mine[1], 1 - section, ctx)
        arrived(x_ctx, mine[1])
        go(x_ctx, mine[1], 1 - section, ctx)
        for s in mine:
            arrived(d_ctx, s)
            go(d_ctx, s, 1 - section, ctx)
        for c in (ctx, x_ctx, y_ctx, d_ctx):
            for j in range(2):
                arrived(c, 2 * section + j)
        for s in range(4):
            pltpu.make_async_copy(norm_ref, norm_all.at[s], norm_recv.at[s]).wait()
        norms[...] = (norm_all[0] + norm_all[1]) + (norm_all[2] + norm_all[3])
        return started

    def tokens_arrived(u, ref):
        for c in range(2):
            at = 2 * lax.rem(u, 2) + c
            dst = token_rows(ref, at, u // 2)
            pltpu.make_async_copy(dst, dst, token_recv.at[at, u // 2]).wait()

    def chunk_rows(u):
        return pl.ds(pl.multiple_of(u * size, size), size)

    def up_copy(u, stage):
        rows = chunk_rows(u)
        return remote(lea.at[rows], ent.at[rows], up_send.at[u], up_recv.at[u], section, ctx, stage)

    def down_copy(u, stage):
        rows = chunk_rows(u)
        return remote(ent.at[rows], coming.at[rows], down_send.at[u], down_recv.at[u], section, ctx, stage)

    def weight(c, start, columns):
        value = w[c, :, :, pl.ds(start, columns)]
        return value.reshape(value.shape[0] * value.shape[1], columns)

    def rows_copy(src, t, local):
        block, c = t // 4, lax.rem(t, 4)
        src = src.at[pl.ds(pl.multiple_of(t * half, half), half)]
        dst = rows_out.at[kind, block, pl.ds(pl.multiple_of(section * half, half), half)]
        recv = rows_recv.at[kind, section, block]
        if local:
            return pltpu.make_async_copy(src, dst, recv)
        return remote(src, dst, rows_send.at[t], recv, shard // 2, c, ctx)

    def rows_stay(t):
        return (section == shard // 2) & (ctx == lax.rem(t, 4)) & (ctx == shard)

    def rows_start(src, t):
        @pl.when(rows_stay(t))
        def _():
            rows_copy(src, t, True).start()

        @pl.when(jnp.logical_not(rows_stay(t)))
        def _():
            rows_copy(src, t, False).start()

    def rows_finish(src):
        @pl.loop(0, 2 * chunks)
        def _(t):

            @pl.when(jnp.logical_not(rows_stay(t)))
            def _():
                rows_copy(src, t, False).wait_send()

    def finish_chunk(rows, d_normed, gain):
        hat, scale = normalised(ent[rows].astype(f32))
        sums[0:1, :width] += jnp.sum(d_normed * hat, axis=0, keepdims=True)
        sums[1:2, :width] += jnp.sum(d_normed, axis=0, keepdims=True)
        total = coming[rows].astype(f32) + norm_backward(hat, scale, gain, d_normed)
        ent[rows] = total.astype(bf16)

    sums[...] = jnp.zeros_like(sums)

    def group_columns(index, ref):
        feature = lax.broadcasted_iota(jnp.int32, (LANES, width), 1)

        @pl.loop(0, 2)
        def _(side):
            @pl.loop(0, spread.shape[2] // LANES)
            def _(tile):
                at = pl.ds(pl.multiple_of(tile * LANES, LANES), LANES)
                chosen = jnp.where(feature == place_ref[side, at, 0:1], 1.0, 0.0).astype(bf16)
                spread[index, side, at, :] = mm_t(chosen, ref[...]).astype(bf16)

    def reduce(source, pieces, turn, out_ref, which):
        rows = first.shape[3]
        gap = up_to(rows, 16)
        count = out_ref.shape[0]
        lanes = lambda p: pl.ds(pieces[p][0], pieces[p][1])
        own = lambda a, p, c, j: w.at[a, c, pl.ds(pl.multiple_of(gap * j, 16), rows), lanes(p)]
        x_or_y = lambda j: x_ctx + j * (y_ctx - x_ctx)
        array = lambda a: lax.rem(a + turn, count)

        def first_copy(a, p, j):
            even = lax.rem(a, 2)
            return remote(
                w.at[2 * even + j, :, pl.ds(2 * gap, rows), lanes(p)], first.at[even, j, :, :, lanes(p)],
                first_send.at[a, p, j], first_recv.at[a, p, j], 1 - section, ctx, shard,
            )

        def second_copy(a, p, j, part):
            to = x_or_y(j)
            return remote(
                own(a, p, (to, d_ctx)[part], j), second.at[a, j, part, :, lanes(p)],
                second_send.at[a, p, j, part], second_recv.at[a, p, j, part], section, to, shard,
            )

        def third_copy(a, p, j):
            to = x_or_y(1 - j)
            return remote(
                own(a, p, to, j), third.at[a, j, :, lanes(p)],
                third_send.at[a, p, j], third_recv.at[a, p, j], section, to, shard,
            )

        def last_copy(a, p, j):
            return remote(
                own(a, p, ctx, j), out_ref.at[array(a), :, lanes(p)],
                last_send.at[a, p, j], last_recv.at[which, array(a), p],
                shard // 2, ctx, 2 * (1 - section) + j,
            )

        def terms(a, p):
            @pl.loop(0, 2)
            def _(side):
                def emit(index, ref, columns):
                    def block(at, step):
                        value = mm(spread[index, side, pl.ds(0, 8 * rows), :], ref[:, pl.ds(at, step)])
                        cols = pl.ds(pl.multiple_of(pieces[p][0] + at, LANES), step)
                        for n in range(8):
                            lead = side * a + (1 - side) * (2 * lax.rem(a, 2) + n % 2)
                            row = pl.multiple_of(side * (gap * (n % 2)) + (1 - side) * 2 * gap, 16)
                            w[lead, n // 2, pl.ds(row, rows), cols] = value[n * rows : (n + 1) * rows].astype(bf16)

                    step = 2 * LANES

                    @pl.loop(0, columns // step)
                    def _(b):
                        block(pl.multiple_of(b * step, step), step)

                    if columns % step:
                        block(columns - columns % step, columns % step)

                source(a, p, side, emit)

                @pl.when(side == 0)
                def _():
                    for j in range(2):
                        first_copy(a, p, j).start()

        def stage_one(a, p):
            @pl.when(a >= 2)
            def _():
                for j in range(2):
                    first_copy(a - 2, p, j).wait_send()
                pl.semaphore_wait(free, 1)

            terms(a, p)

            @pl.loop(0, 2)
            def _(j):
                first_copy(a, p, j).wait_recv()

                @pl.loop(0, 4)
                def _(c):
                    add_into(own(a, p, c, j), first.at[lax.rem(a, 2), j, c, :, lanes(p)])

            @pl.when(a + 2 < count)
            def _():
                pl.semaphore_signal(
                    free, inc=1, device_id=(1 - section, ctx, shard), device_id_type=pl.DeviceIdType.MESH
                )

            for part in (1, 0):
                for j in range(2):
                    second_copy(a, p, j, part).start()

        def stage_two(a, p):
            @pl.loop(0, 2)
            def _(j):
                second_copy(a, p, j, 1).wait_recv()
                add_into(own(a, p, x_or_y(1 - j), j), second.at[a, j, 1, :, lanes(p)])
                third_copy(a, p, j).start()

            @pl.loop(0, 2)
            def _(j):
                second_copy(a, p, j, 0).wait_recv()
                add_into(own(a, p, ctx, j), second.at[a, j, 0, :, lanes(p)])

        def stage_three(a, p):
            @pl.loop(0, 2)
            def _(j):
                third_copy(a, p, j).wait_recv()
                add_into(own(a, p, ctx, j), third.at[a, j, :, lanes(p)])
                last_copy(a, p, j).start()

        def sums_copy(step):
            to_core, to_ctx = ((1 - section, ctx), (section, x_ctx), (section, y_ctx))[step]
            return remote(sums, sums_in.at[step], sums_send.at[step], sums_recv.at[step], to_core, to_ctx, shard)

        def sums_last(j):
            return remote(
                sums, sums_out.at[which], sums_send.at[3 + j], sums_recv.at[3 + which],
                shard // 2, ctx, 2 * (1 - section) + j,
            )

        sums_copy(0).start()
        items = len(pieces)

        @pl.loop(0, count + 2)
        def _(a):
            for p in range(items):

                @pl.when(a < count)
                def _():
                    stage_one(a, p)

                back = [(-(-(d - p) // items), (p - d) % items) for d in (1, 2)]

                @pl.when((a >= back[0][0]) & (a < count + back[0][0]))
                def _():
                    stage_two(a - back[0][0], back[0][1])

                @pl.when((a >= back[1][0]) & (a < count + back[1][0]))
                def _():
                    stage_three(a - back[1][0], back[1][1])

            for step in range(3):

                @pl.when(a == step)
                def _():
                    sums_copy(step).wait()
                    sums[...] += sums_in[step]
                    if step < 2:
                        sums_copy(step + 1).start()
                    else:
                        for j in range(2):
                            sums_last(j).start()

        @pl.loop(0, count)
        def _(a):
            for p in range(items):
                for j in range(2):

                    @pl.when(a >= count - 2)
                    def _():
                        first_copy(a, p, j).wait_send()

                    for part in range(2):
                        second_copy(a, p, j, part).wait_send()
                    third_copy(a, p, j).wait_send()
                    last_copy(a, p, j).wait_send()

        for j in range(2):
            sums_last(j).wait_send()

    @pl.when(kind == 0)
    def _():
        started = collect(attn_cols)

        lse[...] = jnp.zeros_like(lse)
        da[...] = jnp.zeros_like(da)
        gain, bias = norms[0:1, :width], norms[2:3, :width]

        def pair_copy(which, u):
            rows = chunk_rows(u)
            return remote(
                slots.at[1 + which, rows], slots.at[3 + which, rows], pair_send.at[which, u], pair_recv.at[which, u],
                1 - section, ctx, shard,
            )

        @pl.loop(0, chunks)
        def _(u):
            rows = chunk_rows(u)

            @pl.when(shard == 0)
            def _():
                tokens_arrived(u, ent)

            @pl.when(shard > 0)
            def _():
                up_copy(u, shard).wait_recv()

            hat, _ = normalised(ent[rows].astype(f32))
            normed = (hat * gain + bias).astype(bf16)
            nrm[rows] = normed

            @pl.loop(0, 3)
            def _(turn):
                index = lax.rem(turn + 1, 3)
                scale = jnp.where(turn == 2, score_scale, 1.0)
                slots[index, rows] = (mm(normed, weight(index, 0, wide)) * scale).astype(bf16)

                @pl.when(turn < 2)
                def _():
                    pair_copy(turn, u).start()

            for which in range(2):
                pair_copy(which, u).wait_recv()
            for index in range(chunks):

                @pl.when(u == index)
                def _():
                    attend_chunk(
                        index, pl.ds(index * size, size), mask_ref,
                        slots.at[0], slots.at[1], slots.at[3], slots.at[2], slots.at[4], o, lse,
                    )

            out = mm(o[rows, :width].astype(bf16), weight(3, 0, wide))[:, :width]
            lea[rows] = (ent[rows].astype(f32) + out).astype(bf16)
            up_copy(u, shard + 1).start()

        @pl.loop(0, chunks)
        def _(u):
            for which in range(2):
                pair_copy(which, u).wait_send()
            up_copy(u, shard + 1).wait_send()

        for copy in started:
            copy.wait_send()

        slots[7] = o[...].astype(bf16)
        group_columns(0, nrm)
        group_columns(1, slots.at[7, :, pl.ds(0, width)])
        lane = lax.broadcasted_iota(jnp.int32, (size, LANES), 1)
        low = lane < HEAD

        def swap_copy(which, u):
            rows = chunk_rows(u)
            return remote(
                slots.at[3 + which, rows], slots.at[5 + which, rows], swap_send.at[which, u], swap_recv.at[which, u],
                1 - section, ctx, shard,
            )

        @pl.loop(0, chunks)
        def _(step):
            u = chunks - 1 - step
            rows_now = chunk_rows(u)
            down_copy(u, shard).wait_recv()
            da[:, :width] = mm_t(coming[rows_now], weight(3, 0, width)).astype(bf16)
            for index in range(chunks):

                @pl.when(u == index)
                def _():
                    rows = pl.ds(index * size, size)
                    keys = pl.ds(0, (index + 1) * size)

                    @pl.loop(0, wide // LANES, unroll=3)
                    def _(pair):
                        cols = pl.ds(pl.multiple_of(pair * LANES, LANES), LANES)
                        q2 = stack_heads(slots[0, rows, cols], low)
                        grad = da[:, cols]
                        a2 = stack_heads(grad, low)
                        level = lse[rows, :]
                        product = grad.astype(f32) * o[rows, cols]
                        column = lambda which: jnp.sum(jnp.where(lane == 2 * pair + which, level, 0.0), axis=1, keepdims=True)
                        level2 = jnp.concatenate([column(0), column(1)], axis=0)
                        delta2 = jnp.concatenate(
                            [
                                jnp.sum(jnp.where(low, product, 0.0), axis=1, keepdims=True),
                                jnp.sum(jnp.where(low, 0.0, product), axis=1, keepdims=True),
                            ],
                            axis=0,
                        )
                        dq2 = 0.0
                        for part in range(2):
                            keys_now, values_now = slots[1 + 2 * part, keys, cols], slots[2 + 2 * part, keys, cols]
                            p = jnp.exp(mask_last(mm_t(q2, keys_now), mask_ref[part]) - level2)
                            ds = (p * (mm_t(a2, values_now) - delta2)).astype(bf16)
                            dq2 = dq2 + mm(ds, keys_now)
                            d_keys, d_values = t_mm(ds, q2), t_mm(p.astype(bf16), a2)
                            if index == chunks - 1:
                                big[2 * part, keys, cols] = d_keys
                                big[2 * part + 1, keys, cols] = d_values
                            else:
                                big[2 * part, keys, cols] += d_keys
                                big[2 * part + 1, keys, cols] += d_values
                        slots[0, rows, cols] = (unstack_heads(dq2, low) * score_scale).astype(bf16)

            rows = rows_now
            for which in range(2):
                slots[3 + which, rows] = big[2 + which, rows].astype(bf16)
                swap_copy(which, u).start()

            def finish_part(which, total):
                swap_copy(which, u).wait_recv()
                slots[1 + which, rows] = (big[which, rows] + slots[5 + which, rows].astype(f32)).astype(bf16)
                return total + mm_t(slots[1 + which, rows], weight(1 + which, 0, wide))

            d_normed = lax.fori_loop(0, 2, finish_part, mm_t(slots[0, rows], weight(0, 0, wide)))
            finish_chunk(rows, d_normed, gain)

            @pl.when(shard > 0)
            def _():
                down_copy(u, shard - 1).start()

            for part in range(2):
                rows_start(ent, 2 * u + part)

        @pl.loop(0, chunks)
        def _(u):
            for which in range(2):
                swap_copy(which, u).wait_send()

        def attn_source(a, p, side, emit):
            @pl.when(a == 0)
            def _():
                emit(1, coming, width)

            @pl.when(a > 0)
            def _():
                emit(0, slots.at[jnp.maximum(a - 1, 0)], wide)

        reduce(attn_source, ((0, wide),), 3, attn_out, 0)
        rows_finish(ent)

        @pl.loop(0, chunks)
        def _(u):

            @pl.when(shard > 0)
            def _():
                down_copy(u, shard - 1).wait_send()

    @pl.when(kind == 1)
    def _():
        started = collect(ff_cols)
        gain, bias = norms[1:2, :width], norms[3:4, :width]

        @pl.loop(0, chunks)
        def _(u):
            rows = chunk_rows(u)
            up_copy(u, shard).wait_recv()
            hat, _ = normalised(ent[rows].astype(f32))
            normed = (hat * gain + bias).astype(bf16)
            nrm[rows] = normed

            def add_half(i, total):
                for part, (start, columns) in enumerate(parts):
                    cols = pl.ds(0, columns)
                    upper = mm(normed, weight(i, start, columns))
                    big[2 * i + part, rows, cols] = upper
                    hidden = jax.nn.gelu(upper, approximate=True).astype(bf16)
                    slots[4 + 2 * i + part, rows, cols] = hidden
                    total = total + mm_t(hidden, weight(2 + i, start, columns))
                return total

            lea[rows] = lax.fori_loop(0, 2, add_half, ent[rows].astype(f32)).astype(bf16)

            @pl.when(shard < 3)
            def _():
                up_copy(u, shard + 1).start()

            for part in range(2):
                rows_start(lea, 2 * u + part)

        @pl.when(shard < 3)
        def _():
            group_columns(0, nrm)

        @pl.loop(0, chunks)
        def _(step):
            u = chunks - 1 - step
            rows = chunk_rows(u)

            @pl.when(shard == 3)
            def _():
                tokens_arrived(u, coming)

            @pl.when(shard < 3)
            def _():
                down_copy(u, shard).wait_recv()

            grad = coming[rows]

            def back_half(i, total):
                for part, (start, columns) in enumerate(parts):
                    cols = pl.ds(0, columns)
                    d_hidden = mm(grad, weight(2 + i, start, columns))
                    _, back = jax.vjp(lambda value: jax.nn.gelu(value, approximate=True), big[2 * i + part, rows, cols])
                    d_upper = back(d_hidden)[0].astype(bf16)
                    slots[2 * i + part, rows, cols] = d_upper
                    total = total + mm_t(d_upper, weight(i, start, columns))
                return total

            finish_chunk(rows, lax.fori_loop(0, 2, back_half, jnp.zeros((size, width), f32)), gain)
            down_copy(u, shard - 1).start()

        for copy in started:
            copy.wait_send()

        @pl.when(shard == 3)
        def _():
            group_columns(0, nrm)

        def ff_source(a, p, side, emit):
            if p == 0:

                @pl.when((a == 2) & (side == 0))
                def _():
                    group_columns(1, coming)

            emit(a // 2, slots.at[2 * a + p], parts[p][1])

        reduce(ff_source, parts, 0, ff_out, 1)
        rows_finish(lea)

        @pl.loop(0, chunks)
        def _(u):

            @pl.when(shard < 3)
            def _():
                up_copy(u, shard + 1).wait_send()

            down_copy(u, shard - 1).wait_send()

    @pl.loop(0, attn_out.shape[0])
    def _(index):
        arrivals = [(0, attn_out, 0, 0, wide)] + [(1, ff_out, p, start, columns) for p, (start, columns) in enumerate(parts)]
        for which, ref, p, start, columns in arrivals:
            ref = ref.at[index, :, pl.ds(start, columns)]
            remote(ref, ref, last_send.at[index, 0, 0], last_recv.at[which, index, p], section, ctx, shard).wait_recv()

    for which in range(2):
        remote(sums, sums_out.at[which], sums_send.at[3], sums_recv.at[3 + which], section, ctx, shard).wait_recv()
        for core in range(2):
            for block in range(2):
                ref = rows_out.at[which, block, pl.ds(core * half, half)]
                pltpu.make_async_copy(ref, ref, rows_recv.at[which, core, block]).wait()

    attn_copy.wait_send()
    ff_copy.wait_send()
    for block in range(2):

        @pl.when(jnp.logical_not(x_stays))
        def _():
            x_copy(block, True).wait_send()

        for s in range(1, 4):

            @pl.when((shard == 0) & (ctx != s))
            def _():
                pass_copy(s, block).wait_send()

    for copy, stays in norm_copies + [(g_copy(block), g_stays) for block in range(2)]:

        @pl.when(jnp.logical_not(stays))
        def _():
            copy.wait_send()


def relay(attn_piece, ff_piece, x_own, g_own, norm_own, mask, place, group_pad):
    share, ff_half = ff_piece.shape
    wide = attn_piece.shape[1]
    blocks, half, width = x_own.shape
    tokens = blocks * 4 * half
    size = 2 * half
    chunks = tokens // size
    dma = pltpu.SemaphoreType.DMA
    vmem = pl.BlockSpec(memory_space=pltpu.VMEM)
    narrow = ((tokens, width), bf16)
    outs = [
        ((4, group_pad, wide), bf16), ((4, group_pad, ff_half), bf16), ((2, blocks, size, width), bf16), ((2,) + norm_own.shape, f32),
    ]
    scratch = [
        ((4, 4, share, ff_half), bf16), ((3,) + x_own.shape, bf16), ((4,) + norm_own.shape, f32), (norm_own.shape, f32),
        narrow, narrow, narrow, narrow, ((8, tokens, wide), bf16),
        ((tokens, wide), f32), ((tokens, LANES), f32), ((size, wide), bf16), ((4, tokens, wide), f32),
        (norm_own.shape, f32), ((3,) + norm_own.shape, f32), ((2, 2, place.shape[1], tokens), bf16),
        ((2, 2, 4, group_pad, ff_half), bf16), ((4, 2, 2, group_pad, ff_half), bf16), ((4, 2, group_pad, ff_half), bf16),
    ]
    return pl.pallas_call(
        relay_kernel,
        in_specs=[ANY] * 5 + [vmem] * 2,
        out_specs=[ANY] * len(outs),
        out_shape=[jax.ShapeDtypeStruct(s, t) for s, t in outs],
        scratch_shapes=[pltpu.VMEM(s, t) for s, t in scratch]
        + [
            dma((14,)), dma((4, 4)), dma((2, 2)), dma((4, 2)), dma((4,)), dma((4,)), dma((2,)),
            dma((chunks,)), dma((chunks,)), dma((chunks,)), dma((chunks,)),
            dma((2, chunks)), dma((2, chunks)), dma((2, chunks)), dma((2, chunks)),
            dma((2 * chunks,)), dma((2, 2, 2)), pltpu.SemaphoreType.REGULAR,
            dma((5,)), dma((5,)), dma((4, 2, 2)), dma((4, 2, 2)), dma((4, 2, 2, 2)), dma((4, 2, 2, 2)),
            dma((4, 2, 2)), dma((4, 2, 2)), dma((4, 2, 2)), dma((2, 4, 2)), dma((3, 2)), dma((3, 2)),
        ],
        compiler_params=pltpu.CompilerParams(has_side_effects=True, vmem_limit_bytes=VMEM_BYTES),
        name="relay",
    )(attn_piece, ff_piece, x_own, g_own, norm_own, mask, place)


def chain(inputs, cotangent, qkv_weight, out_weight, up_weight, down_weight, norm_gain, norm_bias):
    section, ctx, shard = lax.axis_index("section"), lax.axis_index("ctx"), lax.axis_index("shard")
    seq_count, blocks, slice_len, width = inputs.shape
    half = slice_len // 2
    tokens = blocks * 4 * half
    share = width // 4
    group = share // 4
    group_pad = up_to(group, ROWS)
    wide = up_to(width, LANES)
    ff = up_weight.shape[2]
    is_attn = shard % 2 == 0

    pad = lambda w: jnp.pad(w, ((0, 0), (0, wide - width)))
    own_qkv, own_out = qkv_weight[0], out_weight[0]
    attn_src = jnp.stack([pad(own_qkv[:, i * width : (i + 1) * width]) for i in range(3)] + [pad(own_out)])
    down_t = down_weight[0].T
    up0 = up_weight[0]
    ff_src = jnp.stack([up0[:, : ff // 2], up0[:, ff // 2 :], down_t[:, : ff // 2], down_t[:, ff // 2 :]])
    norm_own = jnp.concatenate([norm_gain[0], norm_bias[0]], axis=0).astype(f32)
    norm_own = lax.dynamic_update_slice(
        jnp.zeros((ROWS, wide), f32), jnp.pad(norm_own, ((0, ROWS - 4), (0, 0))), (0, shard * share)
    )
    x_own = lax.dynamic_slice_in_dim(inputs[0], section * half, half, 1)
    g_own = lax.dynamic_slice_in_dim(cotangent[0], section * half, half, 1)
    mask = attention_masks(section, half)
    mask = jnp.concatenate([mask, mask], axis=1)
    slot = jnp.arange(up_to(8 * group_pad, LANES))
    row = slot % group_pad
    place = []
    for side in (section, 1 - section):
        owner = (slot // (2 * group_pad)) * 4 + 2 * side + (slot // group_pad) % 2
        place.append(jnp.where((row < group) & (slot < 8 * group_pad), owner * group + row, -1))
    place = jnp.broadcast_to(jnp.stack(place)[:, :, None].astype(jnp.int32), (2, slot.shape[0], LANES))
    attn_sums, ff_sums, rows, totals = relay(
        lax.dynamic_index_in_dim(attn_src, ctx, 0, keepdims=False),
        lax.dynamic_index_in_dim(ff_src, ctx, 0, keepdims=False),
        x_own, g_own, norm_own, mask, place, group_pad,
    )
    totals = lax.dynamic_slice_in_dim(totals[:, :2], (ctx * 4 + shard) * group, group, 2)
    attn_sums = attn_sums[:, :group, :width].astype(f32)
    ff_sums = ff_sums[:, :group].astype(f32)
    return (
        rows[1][None, None],
        rows[0][None, None],
        jnp.concatenate([attn_sums[0], attn_sums[1], attn_sums[2]], axis=1)[None],
        attn_sums[3][None],
        jnp.concatenate([ff_sums[0], ff_sums[1]], axis=1)[None],
        jnp.concatenate([ff_sums[2].T, ff_sums[3].T], axis=0)[None],
        totals[:, 0][None],
        totals[:, 1][None],
    )


def passed_along(value, axis, steps):
    count = lax.axis_size(axis)
    initial, last = (max(0, -steps), min(count, count - steps))
    return lax.ppermute(value, axis, [(source, source + steps) for source in range(initial, last)])


def layer_norm(values, gain, shift):
    mean = jnp.mean(values, axis=-1, keepdims=True)
    centred = values - mean
    var = jnp.mean(centred * centred, axis=-1, keepdims=True)
    return centred * lax.rsqrt(var + eps_norm) * gain + shift


def gelu_tanh(values):
    return jax.nn.gelu(values, approximate=True)


def split_pair(key_value, head_count):
    block_len, seq_count, double = key_value.shape
    model_width = double // 2
    key_rows = key_value[..., :model_width].reshape(block_len, seq_count, head_count, HEAD)
    value_rows = key_value[..., model_width:].reshape(block_len, seq_count, head_count, HEAD)
    return (key_rows, value_rows)


def causal_mask(query_pos, key_pos):
    return (key_pos[None, :] <= query_pos[:, None])[None, :, None, :]


def forward_block(running, queries, query_pos, key_value, key_pos):
    row_max, row_sum, accum = running
    key_rows, value_rows = split_pair(key_value, queries.shape[2])
    scores = (
        jnp.einsum("sqhe,kshe->sqhk", queries, key_rows, preferred_element_type=jnp.float32)
        * score_scale
    )
    causal = causal_mask(query_pos, key_pos)
    new_max = jnp.maximum(row_max, jnp.max(jnp.where(causal, scores, -1e30), axis=-1))
    softmax_w = jnp.where(causal, jnp.exp(scores - new_max[..., None]), 0.0)
    factor = jnp.exp(row_max - new_max)
    row_sum = row_sum * factor + jnp.sum(softmax_w, axis=-1)
    accum = accum * factor[..., None] + jnp.einsum(
        "sqhk,kshe->sqhe",
        softmax_w.astype(jnp.bfloat16),
        value_rows,
        preferred_element_type=jnp.float32,
    )
    return (new_max, row_sum, accum)


def split_rows(whole):
    key_count = whole.shape[0]
    block_size = 512
    blocks = whole.reshape((key_count // block_size, block_size) + whole.shape[1:])
    offsets = jnp.arange(key_count // block_size, dtype=jnp.int32) * block_size
    return (blocks, offsets, block_size)


def fold_keys(running, piece, start, queries, query_pos, group_len):
    blocks, offsets, block_size = split_rows(piece)

    def fold_scan_step(inner, scan_item):
        block_rows, offset = scan_item
        for group_id in range(block_rows.shape[2]):
            key_pos = (
                group_id * group_len + start + offset + jnp.arange(block_size, dtype=jnp.int32)
            )
            inner = forward_block(inner, queries, query_pos, block_rows[:, :, group_id], key_pos)
        return (inner, None)

    result, _ = lax.scan(fold_scan_step, running, (blocks, offsets))
    return result


def pair_terms(d_scores, softmax_w, queries, d_attended, block_size):
    d_keys = (
        jnp.einsum("sqhk,sqhe->kshe", d_scores, queries, preferred_element_type=jnp.float32)
        * score_scale
    )
    d_values = jnp.einsum(
        "sqhk,sqhe->kshe",
        softmax_w.astype(jnp.bfloat16),
        d_attended,
        preferred_element_type=jnp.float32,
    )
    shape = (block_size, queries.shape[0], queries.shape[2] * queries.shape[3])
    return jnp.concatenate([d_keys.reshape(shape), d_values.reshape(shape)], axis=-1)


def score_grads(
    queries, query_pos, log_total, row_delta, d_attended, key_rows, value_rows, key_pos
):
    scores = (
        jnp.einsum("sqhe,kshe->sqhk", queries, key_rows, preferred_element_type=jnp.float32)
        * score_scale
    )
    causal = causal_mask(query_pos, key_pos)
    softmax_w = jnp.where(causal, jnp.exp(scores - log_total[..., None]), 0.0)
    d_probs = jnp.einsum(
        "sqhe,kshe->sqhk", d_attended, value_rows, preferred_element_type=jnp.float32
    )
    d_scores = (softmax_w * (d_probs - row_delta[..., None])).astype(jnp.bfloat16)
    return (softmax_w, d_scores)


def backward_keys(whole, queries, query_pos, log_total, row_delta, d_attended, group_len):
    blocks, offsets, block_size = split_rows(whole)

    def backward_scan_step(d_queries, scan_item):
        block_rows, offset = scan_item
        for group_id in range(block_rows.shape[2]):
            key_pos = group_id * group_len + offset + jnp.arange(block_size, dtype=jnp.int32)
            key_rows, value_rows = split_pair(block_rows[:, :, group_id], queries.shape[2])
            softmax_w, d_scores = score_grads(
                queries, query_pos, log_total, row_delta, d_attended, key_rows, value_rows, key_pos
            )
            d_queries = (
                d_queries
                + jnp.einsum(
                    "sqhk,kshe->sqhe", d_scores, key_rows, preferred_element_type=jnp.float32
                )
                * score_scale
            )
        return (d_queries, None)

    d_queries, terms = lax.scan(
        backward_scan_step, jnp.zeros(queries.shape, jnp.float32), (blocks, offsets)
    )
    return (d_queries, None)


def owner_terms(
    own_cache, all_queries, all_d_att, all_totals, all_deltas, micro_index, ctx_id, group_len
):
    block_len, seq_count, group_count, double = own_cache.shape
    head_count = all_queries.shape[2]
    query_rows = all_queries.shape[1]
    query_size = 512
    block_count = query_rows // query_size

    def loop_step(index, total):
        offset = index * query_size
        q_block = lax.dynamic_slice_in_dim(all_queries, offset, query_size, 1)
        d_block = lax.dynamic_slice_in_dim(all_d_att, offset, query_size, 1)
        t_block = lax.dynamic_slice_in_dim(all_totals, offset, query_size, 1)
        r_block = lax.dynamic_slice_in_dim(all_deltas, offset, query_size, 1)
        query_pos = micro_index * group_len + offset + jnp.arange(query_size, dtype=jnp.int32)
        pieces = []
        for group_id in range(group_count):
            key_pos = (
                group_id * group_len + ctx_id * block_len + jnp.arange(block_len, dtype=jnp.int32)
            )
            key_rows, value_rows = split_pair(own_cache[:, :, group_id], head_count)
            softmax_w, d_scores = score_grads(
                q_block, query_pos, t_block, r_block, d_block, key_rows, value_rows, key_pos
            )
            pieces.append(pair_terms(d_scores, softmax_w, q_block, d_block, block_len))
        return total + jnp.stack(pieces, axis=2)

    return lax.fori_loop(0, block_count, loop_step, jnp.zeros(own_cache.shape, jnp.float32))


def store_at(store, value, micro_index, active):
    updated = lax.dynamic_update_index_in_dim(store, value, micro_index, 0)
    return jnp.where(active, updated, store)


def shards(inputs, cotangent, qkv_weight, out_weight, up_weight, down_weight, norm_gain, norm_bias):
    section_id = lax.axis_index("section")
    ctx_count = lax.axis_size("ctx")
    ctx_id = lax.axis_index("ctx")
    seq_count, group_count, block_len, model_width = inputs.shape
    head_count = model_width // HEAD
    group_len = block_len * ctx_count
    row_count = seq_count * block_len
    w_qkv, w_out, w_up, w_down, gains, biases = (
        lax.all_gather(qkv_weight[0], "shard", axis=0, tiled=True),
        lax.all_gather(out_weight[0], "shard", axis=0, tiled=True),
        lax.all_gather(up_weight[0], "shard", axis=0, tiled=True),
        lax.all_gather(down_weight[0], "shard", axis=1, tiled=True),
        lax.all_gather(norm_gain[0], "shard", axis=1, tiled=True),
        lax.all_gather(norm_bias[0], "shard", axis=1, tiled=True),
    )
    gains = gains.astype(jnp.float32)
    biases = biases.astype(jnp.float32)
    ff_width = w_up.shape[1]
    cache = jnp.zeros((block_len, seq_count, group_count, 2 * model_width), jnp.bfloat16)
    in_store = jnp.zeros((group_count, seq_count, block_len, model_width), jnp.bfloat16)
    query_store = jnp.zeros((group_count, seq_count, block_len, head_count, HEAD), jnp.bfloat16)
    att_store = jnp.zeros((group_count, seq_count, block_len, head_count, HEAD), jnp.float32)
    total_store = jnp.zeros((group_count, seq_count, block_len, head_count), jnp.float32)
    middle_store = jnp.zeros((group_count, row_count, model_width), jnp.float32)
    upper_store = jnp.zeros((group_count, row_count, ff_width), jnp.float32)
    out_store = jnp.zeros((group_count, seq_count, block_len, model_width), jnp.bfloat16)
    received = jnp.zeros((seq_count, block_len, model_width), jnp.bfloat16)
    for tick_no in range(group_count + 1):
        micro = tick_no - section_id
        active = (micro >= 0) & (micro < group_count)
        micro_index = jnp.clip(micro, 0, group_count - 1)
        own_input = lax.dynamic_index_in_dim(inputs, micro_index, 1, keepdims=False)
        entering = jnp.where(section_id == 0, own_input, received)
        flat_rows = entering.reshape(row_count, model_width).astype(jnp.float32)
        normed = layer_norm(flat_rows, gains[0], biases[0]).astype(jnp.bfloat16)
        mixed = jnp.dot(normed, w_qkv, preferred_element_type=jnp.float32).astype(jnp.bfloat16)
        queries = mixed[:, :model_width].reshape(seq_count, block_len, head_count, HEAD)
        fresh = jnp.swapaxes(
            mixed[:, model_width:].reshape(seq_count, block_len, 2 * model_width), 0, 1
        )
        updated = lax.dynamic_update_index_in_dim(cache, fresh, micro_index, 2)
        cache = jnp.where(active, updated, cache)
        query_pos = (
            micro_index * group_len + ctx_id * block_len + jnp.arange(block_len, dtype=jnp.int32)
        )
        start_state = (
            jnp.full((seq_count, block_len, head_count), -1e30, jnp.float32),
            jnp.zeros((seq_count, block_len, head_count), jnp.float32),
            jnp.zeros((seq_count, block_len, head_count, HEAD), jnp.float32),
        )
        row_max, row_sum, accum = fold_keys(
            start_state,
            lax.all_gather(cache, "ctx", axis=0, tiled=True),
            jnp.int32(0),
            queries,
            query_pos,
            group_len,
        )
        attended = accum / row_sum[..., None]
        log_total = row_max + jnp.log(row_sum)
        att_low = attended.reshape(row_count, model_width).astype(jnp.bfloat16)
        middle = flat_rows + jnp.dot(att_low, w_out, preferred_element_type=jnp.float32)
        normed2 = layer_norm(middle, gains[1], biases[1]).astype(jnp.bfloat16)
        upper = jnp.dot(normed2, w_up, preferred_element_type=jnp.float32)
        hidden = gelu_tanh(upper).astype(jnp.bfloat16)
        leaving = (middle + jnp.dot(hidden, w_down, preferred_element_type=jnp.float32)).astype(
            jnp.bfloat16
        )
        leaving = leaving.reshape(seq_count, block_len, model_width)
        in_store = store_at(in_store, entering, micro_index, active)
        query_store = store_at(query_store, queries, micro_index, active)
        att_store = store_at(att_store, attended, micro_index, active)
        total_store = store_at(total_store, log_total, micro_index, active)
        middle_store = store_at(middle_store, middle, micro_index, active)
        upper_store = store_at(upper_store, upper, micro_index, active)
        out_store = store_at(out_store, leaving, micro_index, active)
        if tick_no < group_count:
            received = passed_along(leaving, "section", 1)
    key_acc = jnp.zeros((block_len, seq_count, group_count, 2 * model_width), jnp.float32)
    grad_qkv = jnp.zeros((model_width, 3 * model_width), jnp.float32)
    grad_out = jnp.zeros((model_width, model_width), jnp.float32)
    grad_up = jnp.zeros((model_width, ff_width), jnp.float32)
    grad_down = jnp.zeros((ff_width, model_width), jnp.float32)
    grad_gain = jnp.zeros((2, model_width), jnp.float32)
    grad_bias = jnp.zeros((2, model_width), jnp.float32)
    grad_store = jnp.zeros((group_count, seq_count, block_len, model_width), jnp.bfloat16)
    coming = jnp.zeros((seq_count, block_len, model_width), jnp.bfloat16)
    for tick_no in range(group_count + 1):
        micro = group_count - tick_no - section_id
        active = (micro >= 0) & (micro < group_count)
        active_weight = active.astype(jnp.float32)
        micro_index = jnp.clip(micro, 0, group_count - 1)
        own_cot = lax.dynamic_index_in_dim(cotangent, micro_index, 1, keepdims=False)
        d_out = (
            jnp.where(section_id == 1, own_cot, coming)
            .reshape(row_count, model_width)
            .astype(jnp.float32)
        )
        flat_rows = in_store[micro_index].reshape(row_count, model_width).astype(jnp.float32)
        queries = query_store[micro_index]
        attended = att_store[micro_index]
        log_total = total_store[micro_index]
        middle = middle_store[micro_index]
        upper = upper_store[micro_index]
        normed2_full, norm2_back = jax.vjp(
            lambda v, g, b: layer_norm(v, g, b), middle, gains[1], biases[1]
        )
        normed2 = normed2_full.astype(jnp.bfloat16)
        hidden_full, gelu_back = jax.vjp(gelu_tanh, upper)
        hidden = hidden_full.astype(jnp.bfloat16)
        d_branch = d_out.astype(jnp.bfloat16)
        grad_down = grad_down + active_weight * jnp.dot(
            hidden.T, d_branch, preferred_element_type=jnp.float32
        )
        d_hidden = jnp.dot(d_branch, w_down.T, preferred_element_type=jnp.float32)
        d_upper = gelu_back(d_hidden)[0].astype(jnp.bfloat16)
        grad_up = grad_up + active_weight * jnp.dot(
            normed2.T, d_upper, preferred_element_type=jnp.float32
        )
        d_normed2 = jnp.dot(d_upper, w_up.T, preferred_element_type=jnp.float32)
        d_mid_norm, d_gain2, d_bias2 = norm2_back(d_normed2)
        d_middle = d_out + d_mid_norm
        att_low = attended.reshape(row_count, model_width).astype(jnp.bfloat16)
        d_att = d_middle.astype(jnp.bfloat16)
        grad_out = grad_out + active_weight * jnp.dot(
            att_low.T, d_att, preferred_element_type=jnp.float32
        )
        d_attended = jnp.dot(d_att, w_out.T, preferred_element_type=jnp.float32).astype(
            jnp.bfloat16
        )
        d_attended = d_attended.reshape(seq_count, block_len, head_count, HEAD)
        row_delta = jnp.sum(d_attended.astype(jnp.float32) * attended, axis=-1)
        query_pos = (
            micro_index * group_len + ctx_id * block_len + jnp.arange(block_len, dtype=jnp.int32)
        )
        whole = lax.all_gather(cache, "ctx", axis=0, tiled=True)
        d_queries, unused = backward_keys(
            whole, queries, query_pos, log_total, row_delta, d_attended, group_len
        )
        all_queries, all_d_att = (
            lax.all_gather(queries, "ctx", axis=1, tiled=True),
            lax.all_gather(d_attended, "ctx", axis=1, tiled=True),
        )
        all_totals, all_deltas = (
            lax.all_gather(log_total, "ctx", axis=1, tiled=True),
            lax.all_gather(row_delta, "ctx", axis=1, tiled=True),
        )
        shares = owner_terms(
            cache, all_queries, all_d_att, all_totals, all_deltas, micro_index, ctx_id, group_len
        )
        key_acc = key_acc + active_weight * shares
        d_pair = jnp.swapaxes(
            lax.dynamic_index_in_dim(key_acc, micro_index, 2, keepdims=False), 0, 1
        )
        d_mixed = jnp.concatenate(
            [d_queries.reshape(row_count, model_width), d_pair.reshape(row_count, 2 * model_width)],
            axis=-1,
        ).astype(jnp.bfloat16)
        normed_full, norm1_back = jax.vjp(
            lambda v, g, b: layer_norm(v, g, b), flat_rows, gains[0], biases[0]
        )
        normed = normed_full.astype(jnp.bfloat16)
        grad_qkv = grad_qkv + active_weight * jnp.dot(
            normed.T, d_mixed, preferred_element_type=jnp.float32
        )
        d_normed = jnp.dot(d_mixed, w_qkv.T, preferred_element_type=jnp.float32)
        d_flat_norm, d_gain1, d_bias1 = norm1_back(d_normed)
        grad_gain = grad_gain + active_weight * jnp.stack([d_gain1, d_gain2])
        grad_bias = grad_bias + active_weight * jnp.stack([d_bias1, d_bias2])
        d_entering = (
            (d_middle + d_flat_norm).astype(jnp.bfloat16).reshape(seq_count, block_len, model_width)
        )
        grad_store = store_at(grad_store, d_entering, micro_index, active)
        if tick_no < group_count:
            coming = passed_along(d_entering, "section", -1)
    sums = (
        lax.psum_scatter(grad_qkv, ("ctx", "shard"), scatter_dimension=0, tiled=True),
        lax.psum_scatter(grad_out, ("ctx", "shard"), scatter_dimension=0, tiled=True),
        lax.psum_scatter(grad_up, ("ctx", "shard"), scatter_dimension=0, tiled=True),
        lax.psum_scatter(grad_down, ("ctx", "shard"), scatter_dimension=1, tiled=True),
        lax.psum_scatter(grad_gain, ("ctx", "shard"), scatter_dimension=1, tiled=True),
        lax.psum_scatter(grad_bias, ("ctx", "shard"), scatter_dimension=1, tiled=True),
    )
    layer_outputs = jnp.swapaxes(out_store, 0, 1)[None]
    input_grads = jnp.swapaxes(grad_store, 0, 1)[None]
    return (
        layer_outputs,
        input_grads,
        sums[0][None],
        sums[1][None],
        sums[2][None],
        sums[3][None],
        sums[4][None],
        sums[5][None],
    )


def solution(mesh):
    in_specs = (
        P("shard", None, "ctx", None),
        P("shard", None, "ctx", None),
        P("section", "shard", None),
        P("section", "shard", None),
        P("section", "shard", None),
        P("section", None, "shard"),
        P("section", None, "shard"),
        P("section", None, "shard"),
    )
    out_specs = (
        P("section", "shard", None, "ctx", None),
        P("section", "shard", None, "ctx", None),
        P("section", ("ctx", "shard"), None),
        P("section", ("ctx", "shard"), None),
        P("section", ("ctx", "shard"), None),
        P("section", None, ("ctx", "shard")),
        P("section", None, ("ctx", "shard")),
        P("section", None, ("ctx", "shard")),
    )
    relay = mesh.shape["section"] == 2 and mesh.shape["shard"] == 4 and mesh.shape["ctx"] == 4
    return jax.shard_map(chain if relay else shards, mesh=mesh, in_specs=in_specs, out_specs=out_specs, check_vma=False)
```

```python
import functools

import jax
import jax.numpy as jnp
from jax import lax
from jax.experimental import pallas as pl
from jax.experimental.pallas import tpu as pltpu
from jax.sharding import PartitionSpec as P

HEAD = 64
LANES = 128
ROWS = 8
NEG = -1e30
VMEM_BYTES = 66_900_000

eps_norm = 1e-05
score_scale = 0.125
f32 = jnp.float32
bf16 = jnp.bfloat16


def up_to(width, step):
    return -(-width // step) * step


def dot(a, b, dims):
    return lax.dot_general(a, b, (dims, ((), ())), preferred_element_type=f32)


def mm(a, b):
    return dot(a, b, ((1,), (0,)))


def mm_t(a, b):
    return dot(a, b, ((1,), (1,)))


def t_mm(a, b):
    return dot(a, b, ((0,), (0,)))


def attention_masks(core, half):
    row = lax.broadcasted_iota(jnp.int32, (2 * half, 2 * half), 0)
    col = lax.broadcasted_iota(jnp.int32, (2 * half, 2 * half), 1)
    row_slice, col_slice = row // half, col // half
    own = (col_slice < row_slice) | ((col_slice == row_slice) & (col <= row))
    other = (col_slice < row_slice) | ((col_slice == row_slice) & (core == 1))
    return jnp.where(jnp.stack([own, other]), 0.0, NEG).astype(f32)


def norm_backward(hat, scale, gain, grad):
    scaled = grad * gain
    mean = jnp.mean(scaled, axis=-1, keepdims=True)
    along = jnp.mean(scaled * hat, axis=-1, keepdims=True)
    return scale * (scaled - mean - hat * along)


ANY = pl.BlockSpec(memory_space=pl.ANY)


def remote(src, dst, send, recv, section, ctx, shard):
    return pltpu.make_async_remote_copy(
        src_ref=src,
        dst_ref=dst,
        send_sem=send,
        recv_sem=recv,
        device_id=(section, ctx, shard),
        device_id_type=pl.DeviceIdType.MESH,
    )


def normalised(values):
    mean = jnp.mean(values, axis=-1, keepdims=True)
    centred = values - mean
    var = jnp.mean(centred * centred, axis=-1, keepdims=True)
    scale = lax.rsqrt(var + eps_norm)
    return centred * scale, scale


def stack_heads(value, low):
    zero = jnp.zeros_like(value)
    return jnp.concatenate([jnp.where(low, value, zero), jnp.where(low, zero, value)], axis=0)


def unstack_heads(value, low):
    rows = value.shape[0] // 2
    return jnp.where(low, value[:rows], value[rows:])


def mask_last(scores, mask):
    width = mask.shape[1]
    last = scores[:, scores.shape[1] - width :] + mask
    if scores.shape[1] == width:
        return last
    return jnp.concatenate([scores[:, : scores.shape[1] - width], last], axis=1)


def attend_chunk(u, rows, mask_ref, q, k, k1, v, v1, o, lse):
    size = rows.size
    keys = pl.ds(0, (u + 1) * size)
    lane = lax.broadcasted_iota(jnp.int32, (size, LANES), 1)
    low = lane < HEAD

    @pl.loop(0, q.shape[1] // LANES, unroll=3)
    def _(pair):
        cols = pl.ds(pl.multiple_of(pair * LANES, LANES), LANES)
        q2 = stack_heads(q[rows, cols], low)
        scores = [mask_last(mm_t(q2, ref[keys, cols]), mask_ref[part]) for part, ref in enumerate((k, k1))]
        top = jnp.maximum(
            jnp.max(scores[0], axis=1, keepdims=True), jnp.max(scores[1], axis=1, keepdims=True)
        )
        total, acc = 0.0, 0.0
        for s, ref in zip(scores, (v, v1)):
            p = jnp.exp(s - top)
            total = total + jnp.sum(p, axis=1, keepdims=True)
            acc = acc + mm(p.astype(bf16), ref[keys, cols])
        o[rows, cols] = unstack_heads(acc / total, low)
        level = top + jnp.log(total)
        lse[rows, :] = jnp.where(
            lane == 2 * pair, level[:size], jnp.where(lane == 2 * pair + 1, level[size:], lse[rows, :])
        )


def near_ctx(c, step):
    return c + step - 2 * step * lax.rem(c // step, 2)


def add_into(total, term):
    total[...] = (total[...].astype(f32) + term[...].astype(f32)).astype(bf16)


def relay_kernel(
    attn_ref, ff_ref, x_ref, g_ref, norm_ref, mask_ref, place_ref,
    attn_out, ff_out, rows_out, sums_out,
    w, staged, norm_all, norms, ent, nrm, lea, coming, slots, o, lse, da, big, sums, sums_in, spread, first, second, third,
    send, recv, token_send, token_recv, norm_send, norm_recv, far_send,
    up_send, up_recv, down_send, down_recv, pair_send, pair_recv, swap_send, swap_recv, rows_send, rows_recv, free,
    sums_send, sums_recv, first_send, first_recv, second_send, second_recv, third_send, third_recv, last_send, last_recv,
    staged_recv, pass_send,
):
    section, ctx, shard = lax.axis_index("section"), lax.axis_index("ctx"), lax.axis_index("shard")
    kind = lax.rem(shard, 2)
    late = shard // 2
    far_core = 1 - late
    x_ctx, y_ctx = near_ctx(ctx, 1), near_ctx(ctx, 2)
    d_ctx = near_ctx(x_ctx, 2)
    width = ent.shape[1]
    wide = attn_ref.shape[1]
    size = da.shape[0]
    half = size // 2
    chunks = ent.shape[0] // size
    ff_half = ff_ref.shape[1]
    attn_cols = pl.ds(0, wide)
    ff_cols = pl.ds(0, ff_half)
    parts = ((0, wide), (wide, ff_half - wide))

    def token_rows(ref, c, block):
        return ref.at[pl.ds(pl.multiple_of((block * 4 + c) * half, half), half)]

    def own_rows(ref, block):
        return ref.at[block, pl.ds(pl.multiple_of(section * half, half), half)]

    def x_copy(block, straight):
        index = jnp.maximum(shard - 1, 0)
        dst = token_rows(ent, ctx, block) if straight else staged.at[index, block]
        arrived = token_recv.at[ctx, block] if straight else staged_recv.at[index, block]
        return remote(
            own_rows(x_ref, block), dst, token_send.at[0, block], arrived, section, ctx * jnp.minimum(shard, 1), 0
        )

    def g_copy(block):
        return remote(
            own_rows(g_ref, block), token_rows(coming, ctx, block), token_send.at[1, block], token_recv.at[ctx, block], section, shard, 3
        )

    def pass_copy(s, block):
        return remote(
            staged.at[s - 1, block], token_rows(ent, ctx, block), pass_send.at[s - 1, block], token_recv.at[ctx, block],
            section, s, 0,
        )

    x_straight = (shard == 0) | (ctx == shard)
    x_stays = (shard == 0) & (ctx == 0)
    g_stays = (shard == 3) & (ctx == 3)
    attn_copy = remote(
        attn_ref, w.at[ctx, shard, :, attn_cols], far_send.at[0], recv.at[ctx, shard], far_core, ctx, 2 * section
    )
    ff_copy = remote(
        ff_ref, w.at[ctx, shard, :, ff_cols], far_send.at[1], recv.at[ctx, shard], far_core, ctx, 2 * section + 1
    )
    norm_local = pltpu.make_async_copy(norm_ref, norm_all.at[shard], norm_recv.at[shard])

    def stay_copy(src, dst, block):
        return pltpu.make_async_copy(own_rows(src, block), token_rows(dst, ctx, block), token_recv.at[ctx, block])

    def x_start(block):
        @pl.when(x_stays)
        def _():
            stay_copy(x_ref, ent, block).start()

        @pl.when(x_straight & jnp.logical_not(x_stays))
        def _():
            x_copy(block, True).start()

        @pl.when(jnp.logical_not(x_straight))
        def _():
            x_copy(block, False).start()

    def pass_on(block):
        for s in range(1, 4):

            @pl.when((shard == 0) & (ctx != s))
            def _():
                ref = staged.at[s - 1, block]
                pltpu.make_async_copy(ref, ref, staged_recv.at[s - 1, block]).wait()
                pass_copy(s, block).start()

    attn_copy.start()
    norm_copies = []
    for core in range(2):
        for stage in range(2):
            copy = remote(
                norm_ref, norm_all.at[shard], norm_send.at[core * 2 + stage], norm_recv.at[shard],
                core, ctx, 2 * section + stage,
            )
            stays = (section == core) & (shard == 2 * section + stage)
            norm_copies.append((copy, stays))

            @pl.when(stays)
            def _():
                norm_local.start()

            @pl.when(jnp.logical_not(stays))
            def _():
                copy.start()

    ff_copy.start()
    x_start(0)
    x_start(1)
    def g_start():
        for block in (1, 0):

            @pl.when(g_stays)
            def _():
                stay_copy(g_ref, coming, block).start()

            @pl.when(jnp.logical_not(g_stays))
            def _():
                g_copy(block).start()

    g_start()

    def piece(cols, c, s, which, core, to_ctx):
        ref = w.at[c, s, :, cols]
        return remote(ref, ref, send.at[which], recv.at[c, s], core, to_ctx, shard)

    def collect(cols):
        here = lax.rem(section + late, 2)
        mine = [
            here * shard + (1 - here) * (2 - late),
            here * (shard + 1 - 2 * kind) + (1 - here) * (3 - 3 * late),
        ]
        started = []

        def go(c, s, core, to_ctx):
            copy = piece(cols, c, s, len(started), core, to_ctx)
            copy.start()
            started.append(copy)

        def arrived(c, s):
            piece(cols, c, s, 0, section, ctx).wait_recv()

        for turn, s in enumerate(mine):
            arrived(ctx, s)
            go(ctx, s, section, x_ctx)
            go(ctx, s, section, y_ctx)
            go(ctx, s, 1 - section, ctx)
            if cols is attn_cols:
                pass_on(turn)
        arrived(x_ctx, mine[0])
        go(x_ctx, mine[0], section, y_ctx)
        go(x_ctx, mine[0], 1 - section, ctx)
        arrived(y_ctx, mine[0])
        go(y_ctx, mine[0], 1 - section, ctx)
        arrived(y_ctx, mine[1])
        go(y_ctx, mine[1], section, x_ctx)
        go(y_ctx, mine[1], 1 - section, ctx)
        arrived(x_ctx, mine[1])
        go(x_ctx, mine[1], 1 - section, ctx)
        for s in mine:
            arrived(d_ctx, s)
            go(d_ctx, s, 1 - section, ctx)
        for c in (ctx, x_ctx, y_ctx, d_ctx):
            for j in range(2):
                arrived(c, 2 * section + j)
        for s in range(4):
            pltpu.make_async_copy(norm_ref, norm_all.at[s], norm_recv.at[s]).wait()
        norms[...] = (norm_all[0] + norm_all[1]) + (norm_all[2] + norm_all[3])
        return started

    def tokens_arrived(u, ref):
        for c in range(2):
            at = 2 * lax.rem(u, 2) + c
            dst = token_rows(ref, at, u // 2)
            pltpu.make_async_copy(dst, dst, token_recv.at[at, u // 2]).wait()

    def chunk_rows(u):
        return pl.ds(pl.multiple_of(u * size, size), size)

    def up_copy(u, stage):
        rows = chunk_rows(u)
        return remote(lea.at[rows], ent.at[rows], up_send.at[u], up_recv.at[u], section, ctx, stage)

    def down_copy(u, stage):
        rows = chunk_rows(u)
        return remote(ent.at[rows], coming.at[rows], down_send.at[u], down_recv.at[u], section, ctx, stage)

    def weight(c, start, columns):
        value = w[c, :, :, pl.ds(start, columns)]
        return value.reshape(value.shape[0] * value.shape[1], columns)

    def rows_copy(src, t, local):
        block, c = t // 4, lax.rem(t, 4)
        src = src.at[pl.ds(pl.multiple_of(t * half, half), half)]
        dst = rows_out.at[kind, block, pl.ds(pl.multiple_of(section * half, half), half)]
        recv = rows_recv.at[kind, section, block]
        if local:
            return pltpu.make_async_copy(src, dst, recv)
        return remote(src, dst, rows_send.at[t], recv, shard // 2, c, ctx)

    def rows_stay(t):
        return (section == shard // 2) & (ctx == lax.rem(t, 4)) & (ctx == shard)

    def rows_start(src, t):
        @pl.when(rows_stay(t))
        def _():
            rows_copy(src, t, True).start()

        @pl.when(jnp.logical_not(rows_stay(t)))
        def _():
            rows_copy(src, t, False).start()

    def rows_finish(src):
        @pl.loop(0, 2 * chunks)
        def _(t):

            @pl.when(jnp.logical_not(rows_stay(t)))
            def _():
                rows_copy(src, t, False).wait_send()

    def finish_chunk(rows, d_normed, gain):
        hat, scale = normalised(ent[rows].astype(f32))
        sums[0:1, :width] += jnp.sum(d_normed * hat, axis=0, keepdims=True)
        sums[1:2, :width] += jnp.sum(d_normed, axis=0, keepdims=True)
        total = coming[rows].astype(f32) + norm_backward(hat, scale, gain, d_normed)
        ent[rows] = total.astype(bf16)

    sums[...] = jnp.zeros_like(sums)

    def group_columns(index, ref):
        feature = lax.broadcasted_iota(jnp.int32, (LANES, width), 1)

        @pl.loop(0, 2)
        def _(side):
            @pl.loop(0, spread.shape[2] // LANES)
            def _(tile):
                at = pl.ds(pl.multiple_of(tile * LANES, LANES), LANES)
                chosen = jnp.where(feature == place_ref[side, at, 0:1], 1.0, 0.0).astype(bf16)
                spread[index, side, at, :] = mm_t(chosen, ref[...]).astype(bf16)

    def reduce(source, pieces, turn, out_ref, which):
        rows = first.shape[3]
        gap = up_to(rows, 16)
        count = out_ref.shape[0]
        lanes = lambda p: pl.ds(pieces[p][0], pieces[p][1])
        own = lambda a, p, c, j: w.at[a, c, pl.ds(pl.multiple_of(gap * j, 16), rows), lanes(p)]
        x_or_y = lambda j: x_ctx + j * (y_ctx - x_ctx)
        array = lambda a: lax.rem(a + turn, count)

        def first_copy(a, p, j):
            even = lax.rem(a, 2)
            return remote(
                w.at[2 * even + j, :, pl.ds(2 * gap, rows), lanes(p)], first.at[even, j, :, :, lanes(p)],
                first_send.at[a, p, j], first_recv.at[a, p, j], 1 - section, ctx, shard,
            )

        def second_copy(a, p, j, part):
            to = x_or_y(j)
            return remote(
                own(a, p, (to, d_ctx)[part], j), second.at[a, j, part, :, lanes(p)],
                second_send.at[a, p, j, part], second_recv.at[a, p, j, part], section, to, shard,
            )

        def third_copy(a, p, j):
            to = x_or_y(1 - j)
            return remote(
                own(a, p, to, j), third.at[a, j, :, lanes(p)],
                third_send.at[a, p, j], third_recv.at[a, p, j], section, to, shard,
            )

        def last_copy(a, p, j):
            return remote(
                own(a, p, ctx, j), out_ref.at[array(a), :, lanes(p)],
                last_send.at[a, p, j], last_recv.at[which, array(a), p],
                shard // 2, ctx, 2 * (1 - section) + j,
            )

        def terms(a, p):
            @pl.loop(0, 2)
            def _(side):
                def emit(index, ref, columns):
                    def block(at, step):
                        value = mm(spread[index, side, pl.ds(0, 8 * rows), :], ref[:, pl.ds(at, step)])
                        cols = pl.ds(pl.multiple_of(pieces[p][0] + at, LANES), step)
                        for n in range(8):
                            lead = side * a + (1 - side) * (2 * lax.rem(a, 2) + n % 2)
                            row = pl.multiple_of(side * (gap * (n % 2)) + (1 - side) * 2 * gap, 16)
                            w[lead, n // 2, pl.ds(row, rows), cols] = value[n * rows : (n + 1) * rows].astype(bf16)

                    step = 2 * LANES

                    @pl.loop(0, columns // step)
                    def _(b):
                        block(pl.multiple_of(b * step, step), step)

                    if columns % step:
                        block(columns - columns % step, columns % step)

                source(a, p, side, emit)

                @pl.when(side == 0)
                def _():
                    for j in range(2):
                        first_copy(a, p, j).start()

        def stage_one(a, p):
            @pl.when(a >= 2)
            def _():
                for j in range(2):
                    first_copy(a - 2, p, j).wait_send()
                pl.semaphore_wait(free, 1)

            terms(a, p)

            @pl.loop(0, 2)
            def _(j):
                first_copy(a, p, j).wait_recv()

                @pl.loop(0, 4)
                def _(c):
                    add_into(own(a, p, c, j), first.at[lax.rem(a, 2), j, c, :, lanes(p)])

            @pl.when(a + 2 < count)
            def _():
                pl.semaphore_signal(
                    free, inc=1, device_id=(1 - section, ctx, shard), device_id_type=pl.DeviceIdType.MESH
                )

            for part in (1, 0):
                for j in range(2):
                    second_copy(a, p, j, part).start()

        def stage_two(a, p):
            @pl.loop(0, 2)
            def _(j):
                second_copy(a, p, j, 1).wait_recv()
                add_into(own(a, p, x_or_y(1 - j), j), second.at[a, j, 1, :, lanes(p)])
                third_copy(a, p, j).start()

            @pl.loop(0, 2)
            def _(j):
                second_copy(a, p, j, 0).wait_recv()
                add_into(own(a, p, ctx, j), second.at[a, j, 0, :, lanes(p)])

        def stage_three(a, p):
            @pl.loop(0, 2)
            def _(j):
                third_copy(a, p, j).wait_recv()
                add_into(own(a, p, ctx, j), third.at[a, j, :, lanes(p)])
                last_copy(a, p, j).start()

        def sums_copy(step):
            to_core, to_ctx = ((1 - section, ctx), (section, x_ctx), (section, y_ctx))[step]
            return remote(sums, sums_in.at[step], sums_send.at[step], sums_recv.at[step], to_core, to_ctx, shard)

        def sums_last(j):
            return remote(
                sums, sums_out.at[which], sums_send.at[3 + j], sums_recv.at[3 + which],
                shard // 2, ctx, 2 * (1 - section) + j,
            )

        sums_copy(0).start()
        items = len(pieces)

        @pl.loop(0, count + 2)
        def _(a):
            for p in range(items):

                @pl.when(a < count)
                def _():
                    stage_one(a, p)

                back = [(-(-(d - p) // items), (p - d) % items) for d in (1, 2)]

                @pl.when((a >= back[0][0]) & (a < count + back[0][0]))
                def _():
                    stage_two(a - back[0][0], back[0][1])

                @pl.when((a >= back[1][0]) & (a < count + back[1][0]))
                def _():
                    stage_three(a - back[1][0], back[1][1])

            for step in range(3):

                @pl.when(a == step)
                def _():
                    sums_copy(step).wait()
                    sums[...] += sums_in[step]
                    if step < 2:
                        sums_copy(step + 1).start()
                    else:
                        for j in range(2):
                            sums_last(j).start()

        @pl.loop(0, count)
        def _(a):
            for p in range(items):
                for j in range(2):

                    @pl.when(a >= count - 2)
                    def _():
                        first_copy(a, p, j).wait_send()

                    for part in range(2):
                        second_copy(a, p, j, part).wait_send()
                    third_copy(a, p, j).wait_send()
                    last_copy(a, p, j).wait_send()

        for j in range(2):
            sums_last(j).wait_send()

    @pl.when(kind == 0)
    def _():
        started = collect(attn_cols)

        lse[...] = jnp.zeros_like(lse)
        da[...] = jnp.zeros_like(da)
        gain, bias = norms[0:1, :width], norms[2:3, :width]

        def pair_copy(which, u):
            rows = chunk_rows(u)
            return remote(
                slots.at[1 + which, rows], slots.at[3 + which, rows], pair_send.at[which, u], pair_recv.at[which, u],
                1 - section, ctx, shard,
            )

        @pl.loop(0, chunks)
        def _(u):
            rows = chunk_rows(u)

            @pl.when(shard == 0)
            def _():
                tokens_arrived(u, ent)

            @pl.when(shard > 0)
            def _():
                up_copy(u, shard).wait_recv()

            hat, _ = normalised(ent[rows].astype(f32))
            normed = (hat * gain + bias).astype(bf16)
            nrm[rows] = normed

            @pl.loop(0, 3)
            def _(turn):
                index = lax.rem(turn + 1, 3)
                scale = jnp.where(turn == 2, score_scale, 1.0)
                slots[index, rows] = (mm(normed, weight(index, 0, wide)) * scale).astype(bf16)

                @pl.when(turn < 2)
                def _():
                    pair_copy(turn, u).start()

            for which in range(2):
                pair_copy(which, u).wait_recv()
            for index in range(chunks):

                @pl.when(u == index)
                def _():
                    attend_chunk(
                        index, pl.ds(index * size, size), mask_ref,
                        slots.at[0], slots.at[1], slots.at[3], slots.at[2], slots.at[4], o, lse,
                    )

            out = mm(o[rows, :width].astype(bf16), weight(3, 0, wide))[:, :width]
            lea[rows] = (ent[rows].astype(f32) + out).astype(bf16)
            up_copy(u, shard + 1).start()

        @pl.loop(0, chunks)
        def _(u):
            for which in range(2):
                pair_copy(which, u).wait_send()
            up_copy(u, shard + 1).wait_send()

        for copy in started:
            copy.wait_send()

        slots[7] = o[...].astype(bf16)
        group_columns(0, nrm)
        group_columns(1, slots.at[7, :, pl.ds(0, width)])
        lane = lax.broadcasted_iota(jnp.int32, (size, LANES), 1)
        low = lane < HEAD

        def swap_copy(which, u):
            rows = chunk_rows(u)
            return remote(
                slots.at[3 + which, rows], slots.at[5 + which, rows], swap_send.at[which, u], swap_recv.at[which, u],
                1 - section, ctx, shard,
            )

        @pl.loop(0, chunks)
        def _(step):
            u = chunks - 1 - step
            rows_now = chunk_rows(u)
            down_copy(u, shard).wait_recv()
            da[:, :width] = mm_t(coming[rows_now], weight(3, 0, width)).astype(bf16)
            for index in range(chunks):

                @pl.when(u == index)
                def _():
                    rows = pl.ds(index * size, size)
                    keys = pl.ds(0, (index + 1) * size)

                    @pl.loop(0, wide // LANES, unroll=3)
                    def _(pair):
                        cols = pl.ds(pl.multiple_of(pair * LANES, LANES), LANES)
                        q2 = stack_heads(slots[0, rows, cols], low)
                        grad = da[:, cols]
                        a2 = stack_heads(grad, low)
                        level = lse[rows, :]
                        product = grad.astype(f32) * o[rows, cols]
                        column = lambda which: jnp.sum(jnp.where(lane == 2 * pair + which, level, 0.0), axis=1, keepdims=True)
                        level2 = jnp.concatenate([column(0), column(1)], axis=0)
                        delta2 = jnp.concatenate(
                            [
                                jnp.sum(jnp.where(low, product, 0.0), axis=1, keepdims=True),
                                jnp.sum(jnp.where(low, 0.0, product), axis=1, keepdims=True),
                            ],
                            axis=0,
                        )
                        dq2 = 0.0
                        for part in range(2):
                            keys_now, values_now = slots[1 + 2 * part, keys, cols], slots[2 + 2 * part, keys, cols]
                            p = jnp.exp(mask_last(mm_t(q2, keys_now), mask_ref[part]) - level2)
                            ds = (p * (mm_t(a2, values_now) - delta2)).astype(bf16)
                            dq2 = dq2 + mm(ds, keys_now)
                            d_keys, d_values = t_mm(ds, q2), t_mm(p.astype(bf16), a2)
                            if index == chunks - 1:
                                big[2 * part, keys, cols] = d_keys
                                big[2 * part + 1, keys, cols] = d_values
                            else:
                                big[2 * part, keys, cols] += d_keys
                                big[2 * part + 1, keys, cols] += d_values
                        slots[0, rows, cols] = (unstack_heads(dq2, low) * score_scale).astype(bf16)

            rows = rows_now
            for which in range(2):
                slots[3 + which, rows] = big[2 + which, rows].astype(bf16)
                swap_copy(which, u).start()

            def finish_part(which, total):
                swap_copy(which, u).wait_recv()
                slots[1 + which, rows] = (big[which, rows] + slots[5 + which, rows].astype(f32)).astype(bf16)
                return total + mm_t(slots[1 + which, rows], weight(1 + which, 0, wide))

            d_normed = lax.fori_loop(0, 2, finish_part, mm_t(slots[0, rows], weight(0, 0, wide)))
            finish_chunk(rows, d_normed, gain)

            @pl.when(shard > 0)
            def _():
                down_copy(u, shard - 1).start()

            for part in range(2):
                rows_start(ent, 2 * u + part)

        @pl.loop(0, chunks)
        def _(u):
            for which in range(2):
                swap_copy(which, u).wait_send()

        def attn_source(a, p, side, emit):
            @pl.when(a == 0)
            def _():
                emit(1, coming, width)

            @pl.when(a > 0)
            def _():
                emit(0, slots.at[jnp.maximum(a - 1, 0)], wide)

        reduce(attn_source, ((0, wide),), 3, attn_out, 0)
        rows_finish(ent)

        @pl.loop(0, chunks)
        def _(u):

            @pl.when(shard > 0)
            def _():
                down_copy(u, shard - 1).wait_send()

    @pl.when(kind == 1)
    def _():
        started = collect(ff_cols)
        gain, bias = norms[1:2, :width], norms[3:4, :width]

        @pl.loop(0, chunks)
        def _(u):
            rows = chunk_rows(u)
            up_copy(u, shard).wait_recv()
            hat, _ = normalised(ent[rows].astype(f32))
            normed = (hat * gain + bias).astype(bf16)
            nrm[rows] = normed

            def add_half(i, total):
                for part, (start, columns) in enumerate(parts):
                    cols = pl.ds(0, columns)
                    upper = mm(normed, weight(i, start, columns))
                    big[2 * i + part, rows, cols] = upper
                    hidden = jax.nn.gelu(upper, approximate=True).astype(bf16)
                    slots[4 + 2 * i + part, rows, cols] = hidden
                    total = total + mm_t(hidden, weight(2 + i, start, columns))
                return total

            lea[rows] = lax.fori_loop(0, 2, add_half, ent[rows].astype(f32)).astype(bf16)

            @pl.when(shard < 3)
            def _():
                up_copy(u, shard + 1).start()

            for part in range(2):
                rows_start(lea, 2 * u + part)

        @pl.when(shard < 3)
        def _():
            group_columns(0, nrm)

        @pl.loop(0, chunks)
        def _(step):
            u = chunks - 1 - step
            rows = chunk_rows(u)

            @pl.when(shard == 3)
            def _():
                tokens_arrived(u, coming)

            @pl.when(shard < 3)
            def _():
                down_copy(u, shard).wait_recv()

            grad = coming[rows]

            def back_half(i, total):
                for part, (start, columns) in enumerate(parts):
                    cols = pl.ds(0, columns)
                    d_hidden = mm(grad, weight(2 + i, start, columns))
                    _, back = jax.vjp(lambda value: jax.nn.gelu(value, approximate=True), big[2 * i + part, rows, cols])
                    d_upper = back(d_hidden)[0].astype(bf16)
                    slots[2 * i + part, rows, cols] = d_upper
                    total = total + mm_t(d_upper, weight(i, start, columns))
                return total

            finish_chunk(rows, lax.fori_loop(0, 2, back_half, jnp.zeros((size, width), f32)), gain)
            down_copy(u, shard - 1).start()

        for copy in started:
            copy.wait_send()

        @pl.when(shard == 3)
        def _():
            group_columns(0, nrm)

        def ff_source(a, p, side, emit):
            if p == 0:

                @pl.when((a == 2) & (side == 0))
                def _():
                    group_columns(1, coming)

            emit(a // 2, slots.at[2 * a + p], parts[p][1])

        reduce(ff_source, parts, 0, ff_out, 1)
        rows_finish(lea)

        @pl.loop(0, chunks)
        def _(u):

            @pl.when(shard < 3)
            def _():
                up_copy(u, shard + 1).wait_send()

            down_copy(u, shard - 1).wait_send()

    @pl.loop(0, attn_out.shape[0])
    def _(index):
        arrivals = [(0, attn_out, 0, 0, wide)] + [(1, ff_out, p, start, columns) for p, (start, columns) in enumerate(parts)]
        for which, ref, p, start, columns in arrivals:
            ref = ref.at[index, :, pl.ds(start, columns)]
            remote(ref, ref, last_send.at[index, 0, 0], last_recv.at[which, index, p], section, ctx, shard).wait_recv()

    for which in range(2):
        remote(sums, sums_out.at[which], sums_send.at[3], sums_recv.at[3 + which], section, ctx, shard).wait_recv()
        for core in range(2):
            for block in range(2):
                ref = rows_out.at[which, block, pl.ds(core * half, half)]
                pltpu.make_async_copy(ref, ref, rows_recv.at[which, core, block]).wait()

    attn_copy.wait_send()
    ff_copy.wait_send()
    for block in range(2):

        @pl.when(jnp.logical_not(x_stays))
        def _():
            x_copy(block, True).wait_send()

        for s in range(1, 4):

            @pl.when((shard == 0) & (ctx != s))
            def _():
                pass_copy(s, block).wait_send()

    for copy, stays in norm_copies + [(g_copy(block), g_stays) for block in range(2)]:

        @pl.when(jnp.logical_not(stays))
        def _():
            copy.wait_send()


def relay(attn_piece, ff_piece, x_own, g_own, norm_own, mask, place, group_pad):
    share, ff_half = ff_piece.shape
    wide = attn_piece.shape[1]
    blocks, size, width = x_own.shape
    half = size // 2
    tokens = blocks * 4 * half
    chunks = tokens // size
    dma = pltpu.SemaphoreType.DMA
    vmem = pl.BlockSpec(memory_space=pltpu.VMEM)
    narrow = ((tokens, width), bf16)
    outs = [
        ((4, group_pad, wide), bf16), ((4, group_pad, ff_half), bf16), ((2, blocks, size, width), bf16), ((2,) + norm_own.shape, f32),
    ]
    scratch = [
        ((4, 4, share, ff_half), bf16), ((3, blocks, half, width), bf16), ((4,) + norm_own.shape, f32), (norm_own.shape, f32),
        narrow, narrow, narrow, narrow, ((8, tokens, wide), bf16),
        ((tokens, wide), f32), ((tokens, LANES), f32), ((size, wide), bf16), ((4, tokens, wide), f32),
        (norm_own.shape, f32), ((3,) + norm_own.shape, f32), ((2, 2, place.shape[1], tokens), bf16),
        ((2, 2, 4, group_pad, ff_half), bf16), ((4, 2, 2, group_pad, ff_half), bf16), ((4, 2, group_pad, ff_half), bf16),
    ]
    return pl.pallas_call(
        relay_kernel,
        in_specs=[ANY] * 5 + [vmem] * 2,
        out_specs=[ANY] * len(outs),
        out_shape=[jax.ShapeDtypeStruct(s, t) for s, t in outs],
        scratch_shapes=[pltpu.VMEM(s, t) for s, t in scratch]
        + [
            dma((14,)), dma((4, 4)), dma((2, 2)), dma((4, 2)), dma((4,)), dma((4,)), dma((2,)),
            dma((chunks,)), dma((chunks,)), dma((chunks,)), dma((chunks,)),
            dma((2, chunks)), dma((2, chunks)), dma((2, chunks)), dma((2, chunks)),
            dma((2 * chunks,)), dma((2, 2, 2)), pltpu.SemaphoreType.REGULAR,
            dma((5,)), dma((5,)), dma((4, 2, 2)), dma((4, 2, 2)), dma((4, 2, 2, 2)), dma((4, 2, 2, 2)),
            dma((4, 2, 2)), dma((4, 2, 2)), dma((4, 2, 2)), dma((2, 4, 2)), dma((3, 2)), dma((3, 2)),
        ],
        compiler_params=pltpu.CompilerParams(has_side_effects=True, vmem_limit_bytes=VMEM_BYTES),
        name="relay",
    )(attn_piece, ff_piece, x_own, g_own, norm_own, mask, place)


def chain(inputs, cotangent, qkv_weight, out_weight, up_weight, down_weight, norm_gain, norm_bias):
    section, ctx, shard = lax.axis_index("section"), lax.axis_index("ctx"), lax.axis_index("shard")
    seq_count, blocks, slice_len, width = inputs.shape
    half = slice_len // 2
    tokens = blocks * 4 * half
    share = width // 4
    group = share // 4
    group_pad = up_to(group, ROWS)
    wide = up_to(width, LANES)
    ff = up_weight.shape[2]
    is_attn = shard % 2 == 0

    pad = lambda w: jnp.pad(w, ((0, 0), (0, wide - width)))
    own_qkv, own_out = qkv_weight[0], out_weight[0]
    attn_src = jnp.stack([pad(own_qkv[:, i * width : (i + 1) * width]) for i in range(3)] + [pad(own_out)])
    down_t = down_weight[0].T
    up0 = up_weight[0]
    ff_src = jnp.stack([up0[:, : ff // 2], up0[:, ff // 2 :], down_t[:, : ff // 2], down_t[:, ff // 2 :]])
    norm_own = jnp.concatenate([norm_gain[0], norm_bias[0]], axis=0).astype(f32)
    norm_own = lax.dynamic_update_slice(
        jnp.zeros((ROWS, wide), f32), jnp.pad(norm_own, ((0, ROWS - 4), (0, 0))), (0, shard * share)
    )
    mask = attention_masks(section, half)
    mask = jnp.concatenate([mask, mask], axis=1)
    slot = jnp.arange(up_to(8 * group_pad, LANES))
    row = slot % group_pad
    place = []
    for side in (section, 1 - section):
        owner = (slot // (2 * group_pad)) * 4 + 2 * side + (slot // group_pad) % 2
        place.append(jnp.where((row < group) & (slot < 8 * group_pad), owner * group + row, -1))
    place = jnp.broadcast_to(jnp.stack(place)[:, :, None].astype(jnp.int32), (2, slot.shape[0], LANES))
    attn_sums, ff_sums, rows, totals = relay(
        lax.dynamic_index_in_dim(attn_src, ctx, 0, keepdims=False),
        lax.dynamic_index_in_dim(ff_src, ctx, 0, keepdims=False),
        inputs[0], cotangent[0], norm_own, mask, place, group_pad,
    )
    totals = lax.dynamic_slice_in_dim(totals[:, :2], (ctx * 4 + shard) * group, group, 2)
    attn_sums = attn_sums[:, :group, :width].astype(f32)
    ff_sums = ff_sums[:, :group].astype(f32)
    return (
        rows[1][None, None],
        rows[0][None, None],
        jnp.concatenate([attn_sums[0], attn_sums[1], attn_sums[2]], axis=1)[None],
        attn_sums[3][None],
        jnp.concatenate([ff_sums[0], ff_sums[1]], axis=1)[None],
        jnp.concatenate([ff_sums[2].T, ff_sums[3].T], axis=0)[None],
        totals[:, 0][None],
        totals[:, 1][None],
    )


def passed_along(value, axis, steps):
    count = lax.axis_size(axis)
    initial, last = (max(0, -steps), min(count, count - steps))
    return lax.ppermute(value, axis, [(source, source + steps) for source in range(initial, last)])


def layer_norm(values, gain, shift):
    mean = jnp.mean(values, axis=-1, keepdims=True)
    centred = values - mean
    var = jnp.mean(centred * centred, axis=-1, keepdims=True)
    return centred * lax.rsqrt(var + eps_norm) * gain + shift


def gelu_tanh(values):
    return jax.nn.gelu(values, approximate=True)


def split_pair(key_value, head_count):
    block_len, seq_count, double = key_value.shape
    model_width = double // 2
    key_rows = key_value[..., :model_width].reshape(block_len, seq_count, head_count, HEAD)
    value_rows = key_value[..., model_width:].reshape(block_len, seq_count, head_count, HEAD)
    return (key_rows, value_rows)


def causal_mask(query_pos, key_pos):
    return (key_pos[None, :] <= query_pos[:, None])[None, :, None, :]


def forward_block(running, queries, query_pos, key_value, key_pos):
    row_max, row_sum, accum = running
    key_rows, value_rows = split_pair(key_value, queries.shape[2])
    scores = (
        jnp.einsum("sqhe,kshe->sqhk", queries, key_rows, preferred_element_type=jnp.float32)
        * score_scale
    )
    causal = causal_mask(query_pos, key_pos)
    new_max = jnp.maximum(row_max, jnp.max(jnp.where(causal, scores, -1e30), axis=-1))
    softmax_w = jnp.where(causal, jnp.exp(scores - new_max[..., None]), 0.0)
    factor = jnp.exp(row_max - new_max)
    row_sum = row_sum * factor + jnp.sum(softmax_w, axis=-1)
    accum = accum * factor[..., None] + jnp.einsum(
        "sqhk,kshe->sqhe",
        softmax_w.astype(jnp.bfloat16),
        value_rows,
        preferred_element_type=jnp.float32,
    )
    return (new_max, row_sum, accum)


def split_rows(whole):
    key_count = whole.shape[0]
    block_size = 512
    blocks = whole.reshape((key_count // block_size, block_size) + whole.shape[1:])
    offsets = jnp.arange(key_count // block_size, dtype=jnp.int32) * block_size
    return (blocks, offsets, block_size)


def fold_keys(running, piece, start, queries, query_pos, group_len):
    blocks, offsets, block_size = split_rows(piece)

    def fold_scan_step(inner, scan_item):
        block_rows, offset = scan_item
        for group_id in range(block_rows.shape[2]):
            key_pos = (
                group_id * group_len + start + offset + jnp.arange(block_size, dtype=jnp.int32)
            )
            inner = forward_block(inner, queries, query_pos, block_rows[:, :, group_id], key_pos)
        return (inner, None)

    result, _ = lax.scan(fold_scan_step, running, (blocks, offsets))
    return result


def pair_terms(d_scores, softmax_w, queries, d_attended, block_size):
    d_keys = (
        jnp.einsum("sqhk,sqhe->kshe", d_scores, queries, preferred_element_type=jnp.float32)
        * score_scale
    )
    d_values = jnp.einsum(
        "sqhk,sqhe->kshe",
        softmax_w.astype(jnp.bfloat16),
        d_attended,
        preferred_element_type=jnp.float32,
    )
    shape = (block_size, queries.shape[0], queries.shape[2] * queries.shape[3])
    return jnp.concatenate([d_keys.reshape(shape), d_values.reshape(shape)], axis=-1)


def score_grads(
    queries, query_pos, log_total, row_delta, d_attended, key_rows, value_rows, key_pos
):
    scores = (
        jnp.einsum("sqhe,kshe->sqhk", queries, key_rows, preferred_element_type=jnp.float32)
        * score_scale
    )
    causal = causal_mask(query_pos, key_pos)
    softmax_w = jnp.where(causal, jnp.exp(scores - log_total[..., None]), 0.0)
    d_probs = jnp.einsum(
        "sqhe,kshe->sqhk", d_attended, value_rows, preferred_element_type=jnp.float32
    )
    d_scores = (softmax_w * (d_probs - row_delta[..., None])).astype(jnp.bfloat16)
    return (softmax_w, d_scores)


def backward_keys(whole, queries, query_pos, log_total, row_delta, d_attended, group_len):
    blocks, offsets, block_size = split_rows(whole)

    def backward_scan_step(d_queries, scan_item):
        block_rows, offset = scan_item
        for group_id in range(block_rows.shape[2]):
            key_pos = group_id * group_len + offset + jnp.arange(block_size, dtype=jnp.int32)
            key_rows, value_rows = split_pair(block_rows[:, :, group_id], queries.shape[2])
            softmax_w, d_scores = score_grads(
                queries, query_pos, log_total, row_delta, d_attended, key_rows, value_rows, key_pos
            )
            d_queries = (
                d_queries
                + jnp.einsum(
                    "sqhk,kshe->sqhe", d_scores, key_rows, preferred_element_type=jnp.float32
                )
                * score_scale
            )
        return (d_queries, None)

    d_queries, terms = lax.scan(
        backward_scan_step, jnp.zeros(queries.shape, jnp.float32), (blocks, offsets)
    )
    return (d_queries, None)


def owner_terms(
    own_cache, all_queries, all_d_att, all_totals, all_deltas, micro_index, ctx_id, group_len
):
    block_len, seq_count, group_count, double = own_cache.shape
    head_count = all_queries.shape[2]
    query_rows = all_queries.shape[1]
    query_size = 512
    block_count = query_rows // query_size

    def loop_step(index, total):
        offset = index * query_size
        q_block = lax.dynamic_slice_in_dim(all_queries, offset, query_size, 1)
        d_block = lax.dynamic_slice_in_dim(all_d_att, offset, query_size, 1)
        t_block = lax.dynamic_slice_in_dim(all_totals, offset, query_size, 1)
        r_block = lax.dynamic_slice_in_dim(all_deltas, offset, query_size, 1)
        query_pos = micro_index * group_len + offset + jnp.arange(query_size, dtype=jnp.int32)
        pieces = []
        for group_id in range(group_count):
            key_pos = (
                group_id * group_len + ctx_id * block_len + jnp.arange(block_len, dtype=jnp.int32)
            )
            key_rows, value_rows = split_pair(own_cache[:, :, group_id], head_count)
            softmax_w, d_scores = score_grads(
                q_block, query_pos, t_block, r_block, d_block, key_rows, value_rows, key_pos
            )
            pieces.append(pair_terms(d_scores, softmax_w, q_block, d_block, block_len))
        return total + jnp.stack(pieces, axis=2)

    return lax.fori_loop(0, block_count, loop_step, jnp.zeros(own_cache.shape, jnp.float32))


def store_at(store, value, micro_index, active):
    updated = lax.dynamic_update_index_in_dim(store, value, micro_index, 0)
    return jnp.where(active, updated, store)


def shards(inputs, cotangent, qkv_weight, out_weight, up_weight, down_weight, norm_gain, norm_bias):
    section_id = lax.axis_index("section")
    ctx_count = lax.axis_size("ctx")
    ctx_id = lax.axis_index("ctx")
    seq_count, group_count, block_len, model_width = inputs.shape
    head_count = model_width // HEAD
    group_len = block_len * ctx_count
    row_count = seq_count * block_len
    w_qkv, w_out, w_up, w_down, gains, biases = (
        lax.all_gather(qkv_weight[0], "shard", axis=0, tiled=True),
        lax.all_gather(out_weight[0], "shard", axis=0, tiled=True),
        lax.all_gather(up_weight[0], "shard", axis=0, tiled=True),
        lax.all_gather(down_weight[0], "shard", axis=1, tiled=True),
        lax.all_gather(norm_gain[0], "shard", axis=1, tiled=True),
        lax.all_gather(norm_bias[0], "shard", axis=1, tiled=True),
    )
    gains = gains.astype(jnp.float32)
    biases = biases.astype(jnp.float32)
    ff_width = w_up.shape[1]
    cache = jnp.zeros((block_len, seq_count, group_count, 2 * model_width), jnp.bfloat16)
    in_store = jnp.zeros((group_count, seq_count, block_len, model_width), jnp.bfloat16)
    query_store = jnp.zeros((group_count, seq_count, block_len, head_count, HEAD), jnp.bfloat16)
    att_store = jnp.zeros((group_count, seq_count, block_len, head_count, HEAD), jnp.float32)
    total_store = jnp.zeros((group_count, seq_count, block_len, head_count), jnp.float32)
    middle_store = jnp.zeros((group_count, row_count, model_width), jnp.float32)
    upper_store = jnp.zeros((group_count, row_count, ff_width), jnp.float32)
    out_store = jnp.zeros((group_count, seq_count, block_len, model_width), jnp.bfloat16)
    received = jnp.zeros((seq_count, block_len, model_width), jnp.bfloat16)
    for tick_no in range(group_count + 1):
        micro = tick_no - section_id
        active = (micro >= 0) & (micro < group_count)
        micro_index = jnp.clip(micro, 0, group_count - 1)
        own_input = lax.dynamic_index_in_dim(inputs, micro_index, 1, keepdims=False)
        entering = jnp.where(section_id == 0, own_input, received)
        flat_rows = entering.reshape(row_count, model_width).astype(jnp.float32)
        normed = layer_norm(flat_rows, gains[0], biases[0]).astype(jnp.bfloat16)
        mixed = jnp.dot(normed, w_qkv, preferred_element_type=jnp.float32).astype(jnp.bfloat16)
        queries = mixed[:, :model_width].reshape(seq_count, block_len, head_count, HEAD)
        fresh = jnp.swapaxes(
            mixed[:, model_width:].reshape(seq_count, block_len, 2 * model_width), 0, 1
        )
        updated = lax.dynamic_update_index_in_dim(cache, fresh, micro_index, 2)
        cache = jnp.where(active, updated, cache)
        query_pos = (
            micro_index * group_len + ctx_id * block_len + jnp.arange(block_len, dtype=jnp.int32)
        )
        start_state = (
            jnp.full((seq_count, block_len, head_count), -1e30, jnp.float32),
            jnp.zeros((seq_count, block_len, head_count), jnp.float32),
            jnp.zeros((seq_count, block_len, head_count, HEAD), jnp.float32),
        )
        row_max, row_sum, accum = fold_keys(
            start_state,
            lax.all_gather(cache, "ctx", axis=0, tiled=True),
            jnp.int32(0),
            queries,
            query_pos,
            group_len,
        )
        attended = accum / row_sum[..., None]
        log_total = row_max + jnp.log(row_sum)
        att_low = attended.reshape(row_count, model_width).astype(jnp.bfloat16)
        middle = flat_rows + jnp.dot(att_low, w_out, preferred_element_type=jnp.float32)
        normed2 = layer_norm(middle, gains[1], biases[1]).astype(jnp.bfloat16)
        upper = jnp.dot(normed2, w_up, preferred_element_type=jnp.float32)
        hidden = gelu_tanh(upper).astype(jnp.bfloat16)
        leaving = (middle + jnp.dot(hidden, w_down, preferred_element_type=jnp.float32)).astype(
            jnp.bfloat16
        )
        leaving = leaving.reshape(seq_count, block_len, model_width)
        in_store = store_at(in_store, entering, micro_index, active)
        query_store = store_at(query_store, queries, micro_index, active)
        att_store = store_at(att_store, attended, micro_index, active)
        total_store = store_at(total_store, log_total, micro_index, active)
        middle_store = store_at(middle_store, middle, micro_index, active)
        upper_store = store_at(upper_store, upper, micro_index, active)
        out_store = store_at(out_store, leaving, micro_index, active)
        if tick_no < group_count:
            received = passed_along(leaving, "section", 1)
    key_acc = jnp.zeros((block_len, seq_count, group_count, 2 * model_width), jnp.float32)
    grad_qkv = jnp.zeros((model_width, 3 * model_width), jnp.float32)
    grad_out = jnp.zeros((model_width, model_width), jnp.float32)
    grad_up = jnp.zeros((model_width, ff_width), jnp.float32)
    grad_down = jnp.zeros((ff_width, model_width), jnp.float32)
    grad_gain = jnp.zeros((2, model_width), jnp.float32)
    grad_bias = jnp.zeros((2, model_width), jnp.float32)
    grad_store = jnp.zeros((group_count, seq_count, block_len, model_width), jnp.bfloat16)
    coming = jnp.zeros((seq_count, block_len, model_width), jnp.bfloat16)
    for tick_no in range(group_count + 1):
        micro = group_count - tick_no - section_id
        active = (micro >= 0) & (micro < group_count)
        active_weight = active.astype(jnp.float32)
        micro_index = jnp.clip(micro, 0, group_count - 1)
        own_cot = lax.dynamic_index_in_dim(cotangent, micro_index, 1, keepdims=False)
        d_out = (
            jnp.where(section_id == 1, own_cot, coming)
            .reshape(row_count, model_width)
            .astype(jnp.float32)
        )
        flat_rows = in_store[micro_index].reshape(row_count, model_width).astype(jnp.float32)
        queries = query_store[micro_index]
        attended = att_store[micro_index]
        log_total = total_store[micro_index]
        middle = middle_store[micro_index]
        upper = upper_store[micro_index]
        normed2_full, norm2_back = jax.vjp(
            lambda v, g, b: layer_norm(v, g, b), middle, gains[1], biases[1]
        )
        normed2 = normed2_full.astype(jnp.bfloat16)
        hidden_full, gelu_back = jax.vjp(gelu_tanh, upper)
        hidden = hidden_full.astype(jnp.bfloat16)
        d_branch = d_out.astype(jnp.bfloat16)
        grad_down = grad_down + active_weight * jnp.dot(
            hidden.T, d_branch, preferred_element_type=jnp.float32
        )
        d_hidden = jnp.dot(d_branch, w_down.T, preferred_element_type=jnp.float32)
        d_upper = gelu_back(d_hidden)[0].astype(jnp.bfloat16)
        grad_up = grad_up + active_weight * jnp.dot(
            normed2.T, d_upper, preferred_element_type=jnp.float32
        )
        d_normed2 = jnp.dot(d_upper, w_up.T, preferred_element_type=jnp.float32)
        d_mid_norm, d_gain2, d_bias2 = norm2_back(d_normed2)
        d_middle = d_out + d_mid_norm
        att_low = attended.reshape(row_count, model_width).astype(jnp.bfloat16)
        d_att = d_middle.astype(jnp.bfloat16)
        grad_out = grad_out + active_weight * jnp.dot(
            att_low.T, d_att, preferred_element_type=jnp.float32
        )
        d_attended = jnp.dot(d_att, w_out.T, preferred_element_type=jnp.float32).astype(
            jnp.bfloat16
        )
        d_attended = d_attended.reshape(seq_count, block_len, head_count, HEAD)
        row_delta = jnp.sum(d_attended.astype(jnp.float32) * attended, axis=-1)
        query_pos = (
            micro_index * group_len + ctx_id * block_len + jnp.arange(block_len, dtype=jnp.int32)
        )
        whole = lax.all_gather(cache, "ctx", axis=0, tiled=True)
        d_queries, unused = backward_keys(
            whole, queries, query_pos, log_total, row_delta, d_attended, group_len
        )
        all_queries, all_d_att = (
            lax.all_gather(queries, "ctx", axis=1, tiled=True),
            lax.all_gather(d_attended, "ctx", axis=1, tiled=True),
        )
        all_totals, all_deltas = (
            lax.all_gather(log_total, "ctx", axis=1, tiled=True),
            lax.all_gather(row_delta, "ctx", axis=1, tiled=True),
        )
        shares = owner_terms(
            cache, all_queries, all_d_att, all_totals, all_deltas, micro_index, ctx_id, group_len
        )
        key_acc = key_acc + active_weight * shares
        d_pair = jnp.swapaxes(
            lax.dynamic_index_in_dim(key_acc, micro_index, 2, keepdims=False), 0, 1
        )
        d_mixed = jnp.concatenate(
            [d_queries.reshape(row_count, model_width), d_pair.reshape(row_count, 2 * model_width)],
            axis=-1,
        ).astype(jnp.bfloat16)
        normed_full, norm1_back = jax.vjp(
            lambda v, g, b: layer_norm(v, g, b), flat_rows, gains[0], biases[0]
        )
        normed = normed_full.astype(jnp.bfloat16)
        grad_qkv = grad_qkv + active_weight * jnp.dot(
            normed.T, d_mixed, preferred_element_type=jnp.float32
        )
        d_normed = jnp.dot(d_mixed, w_qkv.T, preferred_element_type=jnp.float32)
        d_flat_norm, d_gain1, d_bias1 = norm1_back(d_normed)
        grad_gain = grad_gain + active_weight * jnp.stack([d_gain1, d_gain2])
        grad_bias = grad_bias + active_weight * jnp.stack([d_bias1, d_bias2])
        d_entering = (
            (d_middle + d_flat_norm).astype(jnp.bfloat16).reshape(seq_count, block_len, model_width)
        )
        grad_store = store_at(grad_store, d_entering, micro_index, active)
        if tick_no < group_count:
            coming = passed_along(d_entering, "section", -1)
    sums = (
        lax.psum_scatter(grad_qkv, ("ctx", "shard"), scatter_dimension=0, tiled=True),
        lax.psum_scatter(grad_out, ("ctx", "shard"), scatter_dimension=0, tiled=True),
        lax.psum_scatter(grad_up, ("ctx", "shard"), scatter_dimension=0, tiled=True),
        lax.psum_scatter(grad_down, ("ctx", "shard"), scatter_dimension=1, tiled=True),
        lax.psum_scatter(grad_gain, ("ctx", "shard"), scatter_dimension=1, tiled=True),
        lax.psum_scatter(grad_bias, ("ctx", "shard"), scatter_dimension=1, tiled=True),
    )
    layer_outputs = jnp.swapaxes(out_store, 0, 1)[None]
    input_grads = jnp.swapaxes(grad_store, 0, 1)[None]
    return (
        layer_outputs,
        input_grads,
        sums[0][None],
        sums[1][None],
        sums[2][None],
        sums[3][None],
        sums[4][None],
        sums[5][None],
    )


def solution(mesh):
    in_specs = (
        P("shard", None, "ctx", None),
        P("shard", None, "ctx", None),
        P("section", "shard", None),
        P("section", "shard", None),
        P("section", "shard", None),
        P("section", None, "shard"),
        P("section", None, "shard"),
        P("section", None, "shard"),
    )
    out_specs = (
        P("section", "shard", None, "ctx", None),
        P("section", "shard", None, "ctx", None),
        P("section", ("ctx", "shard"), None),
        P("section", ("ctx", "shard"), None),
        P("section", ("ctx", "shard"), None),
        P("section", None, ("ctx", "shard")),
        P("section", None, ("ctx", "shard")),
        P("section", None, ("ctx", "shard")),
    )
    relay = mesh.shape["section"] == 2 and mesh.shape["shard"] == 4 and mesh.shape["ctx"] == 4
    return jax.shard_map(chain if relay else shards, mesh=mesh, in_specs=in_specs, out_specs=out_specs, check_vma=False)
```

```python
import functools

import jax
import jax.numpy as jnp
from jax import lax
from jax.experimental import pallas as pl
from jax.experimental.pallas import tpu as pltpu
from jax.sharding import PartitionSpec as P

HEAD = 64
LANES = 128
ROWS = 8
NEG = -1e30
VMEM_BYTES = 66_900_000

eps_norm = 1e-05
score_scale = 0.125
f32 = jnp.float32
bf16 = jnp.bfloat16


def up_to(width, step):
    return -(-width // step) * step


def dot(a, b, dims):
    return lax.dot_general(a, b, (dims, ((), ())), preferred_element_type=f32)


def mm(a, b):
    return dot(a, b, ((1,), (0,)))


def mm_t(a, b):
    return dot(a, b, ((1,), (1,)))


def t_mm(a, b):
    return dot(a, b, ((0,), (0,)))


def attention_masks(core, half):
    row = lax.broadcasted_iota(jnp.int32, (2 * half, 2 * half), 0)
    col = lax.broadcasted_iota(jnp.int32, (2 * half, 2 * half), 1)
    row_slice, col_slice = row // half, col // half
    own = (col_slice < row_slice) | ((col_slice == row_slice) & (col <= row))
    other = (col_slice < row_slice) | ((col_slice == row_slice) & (core == 1))
    return jnp.where(jnp.stack([own, other]), 0.0, NEG).astype(f32)


def norm_backward(hat, scale, gain, grad):
    scaled = grad * gain
    mean = jnp.mean(scaled, axis=-1, keepdims=True)
    along = jnp.mean(scaled * hat, axis=-1, keepdims=True)
    return scale * (scaled - mean - hat * along)


ANY = pl.BlockSpec(memory_space=pl.ANY)


def remote(src, dst, send, recv, section, ctx, shard):
    return pltpu.make_async_remote_copy(
        src_ref=src,
        dst_ref=dst,
        send_sem=send,
        recv_sem=recv,
        device_id=(section, ctx, shard),
        device_id_type=pl.DeviceIdType.MESH,
    )


def normalised(values):
    mean = jnp.mean(values, axis=-1, keepdims=True)
    centred = values - mean
    var = jnp.mean(centred * centred, axis=-1, keepdims=True)
    scale = lax.rsqrt(var + eps_norm)
    return centred * scale, scale


def stack_heads(value, low):
    zero = jnp.zeros_like(value)
    return jnp.concatenate([jnp.where(low, value, zero), jnp.where(low, zero, value)], axis=0)


def unstack_heads(value, low):
    rows = value.shape[0] // 2
    return jnp.where(low, value[:rows], value[rows:])


def mask_last(scores, mask):
    width = mask.shape[1]
    last = scores[:, scores.shape[1] - width :] + mask
    if scores.shape[1] == width:
        return last
    return jnp.concatenate([scores[:, : scores.shape[1] - width], last], axis=1)


def attend_chunk(u, rows, mask_ref, q, k, k1, v, v1, o, lse):
    size = rows.size
    keys = pl.ds(0, (u + 1) * size)
    lane = lax.broadcasted_iota(jnp.int32, (size, LANES), 1)
    low = lane < HEAD

    @pl.loop(0, q.shape[1] // LANES, unroll=3)
    def _(pair):
        cols = pl.ds(pl.multiple_of(pair * LANES, LANES), LANES)
        q2 = stack_heads(q[rows, cols], low)
        scores = [mask_last(mm_t(q2, ref[keys, cols]), mask_ref[part]) for part, ref in enumerate((k, k1))]
        top = jnp.maximum(
            jnp.max(scores[0], axis=1, keepdims=True), jnp.max(scores[1], axis=1, keepdims=True)
        )
        total, acc = 0.0, 0.0
        for s, ref in zip(scores, (v, v1)):
            p = jnp.exp(s - top)
            total = total + jnp.sum(p, axis=1, keepdims=True)
            acc = acc + mm(p.astype(bf16), ref[keys, cols])
        o[rows, cols] = unstack_heads(acc / total, low)
        level = top + jnp.log(total)
        lse[rows, :] = jnp.where(
            lane == 2 * pair, level[:size], jnp.where(lane == 2 * pair + 1, level[size:], lse[rows, :])
        )


def near_ctx(c, step):
    return c + step - 2 * step * lax.rem(c // step, 2)


def add_into(total, term):
    total[...] = (total[...].astype(f32) + term[...].astype(f32)).astype(bf16)


def relay_kernel(
    attn_ref, ff_ref, x_ref, g_ref, norm_ref, mask_ref, place_ref,
    attn_out, ff_out, rows_out, sums_out,
    w, staged, norm_all, norms, ent, nrm, lea, coming, slots, o, lse, da, big, sums, sums_in, spread, first, second, third,
    send, recv, token_send, token_recv, norm_send, norm_recv, far_send,
    up_send, up_recv, down_send, down_recv, pair_send, pair_recv, swap_send, swap_recv, rows_send, rows_recv, free,
    sums_send, sums_recv, first_send, first_recv, second_send, second_recv, third_send, third_recv, last_send, last_recv,
    staged_recv, pass_send,
):
    section, ctx, shard = lax.axis_index("section"), lax.axis_index("ctx"), lax.axis_index("shard")
    kind = lax.rem(shard, 2)
    late = shard // 2
    far_core = 1 - late
    x_ctx, y_ctx = near_ctx(ctx, 1), near_ctx(ctx, 2)
    d_ctx = near_ctx(x_ctx, 2)
    width = ent.shape[1]
    wide = attn_ref.shape[1]
    size = da.shape[0]
    half = size // 2
    chunks = ent.shape[0] // size
    ff_half = ff_ref.shape[1]
    attn_cols = pl.ds(0, wide)
    ff_cols = pl.ds(0, ff_half)
    parts = ((0, wide), (wide, ff_half - wide))

    def token_rows(ref, c, block):
        return ref.at[pl.ds(pl.multiple_of((block * 4 + c) * half, half), half)]

    def own_rows(ref, block):
        return ref.at[block, pl.ds(pl.multiple_of(section * half, half), half)]

    def x_copy(block, straight):
        index = jnp.maximum(shard - 1, 0)
        dst = token_rows(ent, ctx, block) if straight else staged.at[index, block]
        arrived = token_recv.at[ctx, block] if straight else staged_recv.at[index, block]
        return remote(
            own_rows(x_ref, block), dst, token_send.at[0, block], arrived, section, ctx * jnp.minimum(shard, 1), 0
        )

    def g_copy(block):
        return remote(
            own_rows(g_ref, block), token_rows(coming, ctx, block), token_send.at[1, block], token_recv.at[ctx, block], section, shard, 3
        )

    def pass_copy(s, block):
        return remote(
            staged.at[s - 1, block], token_rows(ent, ctx, block), pass_send.at[s - 1, block], token_recv.at[ctx, block],
            section, s, 0,
        )

    x_straight = (shard == 0) | (ctx == shard)
    x_stays = (shard == 0) & (ctx == 0)
    g_stays = (shard == 3) & (ctx == 3)
    attn_copy = remote(
        attn_ref, w.at[ctx, shard, :, attn_cols], far_send.at[0], recv.at[ctx, shard], far_core, ctx, 2 * section
    )
    ff_copy = remote(
        ff_ref, w.at[ctx, shard, :, ff_cols], far_send.at[1], recv.at[ctx, shard], far_core, ctx, 2 * section + 1
    )
    norm_local = pltpu.make_async_copy(norm_ref, norm_all.at[shard], norm_recv.at[shard])

    def stay_copy(src, dst, block):
        return pltpu.make_async_copy(own_rows(src, block), token_rows(dst, ctx, block), token_recv.at[ctx, block])

    def x_start(block):
        @pl.when(x_stays)
        def _():
            stay_copy(x_ref, ent, block).start()

        @pl.when(x_straight & jnp.logical_not(x_stays))
        def _():
            x_copy(block, True).start()

        @pl.when(jnp.logical_not(x_straight))
        def _():
            x_copy(block, False).start()

    def pass_on(block):
        for s in range(1, 4):

            @pl.when((shard == 0) & (ctx != s))
            def _():
                ref = staged.at[s - 1, block]
                pltpu.make_async_copy(ref, ref, staged_recv.at[s - 1, block]).wait()
                pass_copy(s, block).start()

    attn_copy.start()
    ff_copy.start()
    norm_copies = []
    for core in range(2):
        for stage in range(2):
            copy = remote(
                norm_ref, norm_all.at[shard], norm_send.at[core * 2 + stage], norm_recv.at[shard],
                core, ctx, 2 * section + stage,
            )
            stays = (section == core) & (shard == 2 * section + stage)
            norm_copies.append((copy, stays))

            @pl.when(stays)
            def _():
                norm_local.start()

            @pl.when(jnp.logical_not(stays))
            def _():
                copy.start()

    x_start(0)
    x_start(1)
    def g_start():
        for block in (1, 0):

            @pl.when(g_stays)
            def _():
                stay_copy(g_ref, coming, block).start()

            @pl.when(jnp.logical_not(g_stays))
            def _():
                g_copy(block).start()

    g_start()

    def piece(cols, c, s, which, core, to_ctx):
        ref = w.at[c, s, :, cols]
        return remote(ref, ref, send.at[which], recv.at[c, s], core, to_ctx, shard)

    def collect(cols):
        here = lax.rem(section + late, 2)
        mine = [
            here * shard + (1 - here) * (2 - late),
            here * (shard + 1 - 2 * kind) + (1 - here) * (3 - 3 * late),
        ]
        started = []

        def go(c, s, core, to_ctx):
            copy = piece(cols, c, s, len(started), core, to_ctx)
            copy.start()
            started.append(copy)

        def arrived(c, s):
            piece(cols, c, s, 0, section, ctx).wait_recv()

        for turn, s in enumerate(mine):
            arrived(ctx, s)
            go(ctx, s, section, x_ctx)
            go(ctx, s, section, y_ctx)
            go(ctx, s, 1 - section, ctx)
            if cols is attn_cols:
                pass_on(turn)
        arrived(x_ctx, mine[0])
        go(x_ctx, mine[0], section, y_ctx)
        go(x_ctx, mine[0], 1 - section, ctx)
        arrived(y_ctx, mine[0])
        go(y_ctx, mine[0], 1 - section, ctx)
        arrived(y_ctx, mine[1])
        go(y_ctx, mine[1], section, x_ctx)
        go(y_ctx, mine[1], 1 - section, ctx)
        arrived(x_ctx, mine[1])
        go(x_ctx, mine[1], 1 - section, ctx)
        for s in mine:
            arrived(d_ctx, s)
            go(d_ctx, s, 1 - section, ctx)
        for c in (ctx, x_ctx, y_ctx, d_ctx):
            for j in range(2):
                arrived(c, 2 * section + j)
        for s in range(4):
            pltpu.make_async_copy(norm_ref, norm_all.at[s], norm_recv.at[s]).wait()
        norms[...] = (norm_all[0] + norm_all[1]) + (norm_all[2] + norm_all[3])
        return started

    def tokens_arrived(u, ref):
        for c in range(2):
            at = 2 * lax.rem(u, 2) + c
            dst = token_rows(ref, at, u // 2)
            pltpu.make_async_copy(dst, dst, token_recv.at[at, u // 2]).wait()

    def chunk_rows(u):
        return pl.ds(pl.multiple_of(u * size, size), size)

    def up_copy(u, stage):
        rows = chunk_rows(u)
        return remote(lea.at[rows], ent.at[rows], up_send.at[u], up_recv.at[u], section, ctx, stage)

    def down_copy(u, stage):
        rows = chunk_rows(u)
        return remote(ent.at[rows], coming.at[rows], down_send.at[u], down_recv.at[u], section, ctx, stage)

    def weight(c, start, columns):
        value = w[c, :, :, pl.ds(start, columns)]
        return value.reshape(value.shape[0] * value.shape[1], columns)

    def rows_copy(src, t, local):
        block, c = t // 4, lax.rem(t, 4)
        src = src.at[pl.ds(pl.multiple_of(t * half, half), half)]
        dst = rows_out.at[kind, block, pl.ds(pl.multiple_of(section * half, half), half)]
        recv = rows_recv.at[kind, section, block]
        if local:
            return pltpu.make_async_copy(src, dst, recv)
        return remote(src, dst, rows_send.at[t], recv, shard // 2, c, ctx)

    def rows_stay(t):
        return (section == shard // 2) & (ctx == lax.rem(t, 4)) & (ctx == shard)

    def rows_start(src, t):
        @pl.when(rows_stay(t))
        def _():
            rows_copy(src, t, True).start()

        @pl.when(jnp.logical_not(rows_stay(t)))
        def _():
            rows_copy(src, t, False).start()

    def rows_finish(src):
        @pl.loop(0, 2 * chunks)
        def _(t):

            @pl.when(jnp.logical_not(rows_stay(t)))
            def _():
                rows_copy(src, t, False).wait_send()

    def finish_chunk(rows, d_normed, gain):
        hat, scale = normalised(ent[rows].astype(f32))
        sums[0:1, :width] += jnp.sum(d_normed * hat, axis=0, keepdims=True)
        sums[1:2, :width] += jnp.sum(d_normed, axis=0, keepdims=True)
        total = coming[rows].astype(f32) + norm_backward(hat, scale, gain, d_normed)
        ent[rows] = total.astype(bf16)

    sums[...] = jnp.zeros_like(sums)

    def group_columns(index, ref):
        feature = lax.broadcasted_iota(jnp.int32, (LANES, width), 1)

        @pl.loop(0, 2)
        def _(side):
            @pl.loop(0, spread.shape[2] // LANES)
            def _(tile):
                at = pl.ds(pl.multiple_of(tile * LANES, LANES), LANES)
                chosen = jnp.where(feature == place_ref[side, at, 0:1], 1.0, 0.0).astype(bf16)
                spread[index, side, at, :] = mm_t(chosen, ref[...]).astype(bf16)

    def reduce(source, pieces, turn, out_ref, which):
        rows = first.shape[3]
        gap = up_to(rows, 16)
        count = out_ref.shape[0]
        lanes = lambda p: pl.ds(pieces[p][0], pieces[p][1])
        own = lambda a, p, c, j: w.at[a, c, pl.ds(pl.multiple_of(gap * j, 16), rows), lanes(p)]
        x_or_y = lambda j: x_ctx + j * (y_ctx - x_ctx)
        array = lambda a: lax.rem(a + turn, count)

        def first_copy(a, p, j):
            even = lax.rem(a, 2)
            return remote(
                w.at[2 * even + j, :, pl.ds(2 * gap, rows), lanes(p)], first.at[even, j, :, :, lanes(p)],
                first_send.at[a, p, j], first_recv.at[a, p, j], 1 - section, ctx, shard,
            )

        def second_copy(a, p, j, part):
            to = x_or_y(j)
            return remote(
                own(a, p, (to, d_ctx)[part], j), second.at[a, j, part, :, lanes(p)],
                second_send.at[a, p, j, part], second_recv.at[a, p, j, part], section, to, shard,
            )

        def third_copy(a, p, j):
            to = x_or_y(1 - j)
            return remote(
                own(a, p, to, j), third.at[a, j, :, lanes(p)],
                third_send.at[a, p, j], third_recv.at[a, p, j], section, to, shard,
            )

        def last_copy(a, p, j):
            return remote(
                own(a, p, ctx, j), out_ref.at[array(a), :, lanes(p)],
                last_send.at[a, p, j], last_recv.at[which, array(a), p],
                shard // 2, ctx, 2 * (1 - section) + j,
            )

        def terms(a, p):
            @pl.loop(0, 2)
            def _(side):
                def emit(index, ref, columns):
                    def block(at, step):
                        value = mm(spread[index, side, pl.ds(0, 8 * rows), :], ref[:, pl.ds(at, step)])
                        cols = pl.ds(pl.multiple_of(pieces[p][0] + at, LANES), step)
                        for n in range(8):
                            lead = side * a + (1 - side) * (2 * lax.rem(a, 2) + n % 2)
                            row = pl.multiple_of(side * (gap * (n % 2)) + (1 - side) * 2 * gap, 16)
                            w[lead, n // 2, pl.ds(row, rows), cols] = value[n * rows : (n + 1) * rows].astype(bf16)

                    step = 2 * LANES

                    @pl.loop(0, columns // step)
                    def _(b):
                        block(pl.multiple_of(b * step, step), step)

                    if columns % step:
                        block(columns - columns % step, columns % step)

                source(a, p, side, emit)

                @pl.when(side == 0)
                def _():
                    for j in range(2):
                        first_copy(a, p, j).start()

        def stage_one(a, p):
            @pl.when(a >= 2)
            def _():
                for j in range(2):
                    first_copy(a - 2, p, j).wait_send()
                pl.semaphore_wait(free, 1)

            terms(a, p)

            @pl.loop(0, 2)
            def _(j):
                first_copy(a, p, j).wait_recv()

                @pl.loop(0, 4)
                def _(c):
                    add_into(own(a, p, c, j), first.at[lax.rem(a, 2), j, c, :, lanes(p)])

            @pl.when(a + 2 < count)
            def _():
                pl.semaphore_signal(
                    free, inc=1, device_id=(1 - section, ctx, shard), device_id_type=pl.DeviceIdType.MESH
                )

            for part in (1, 0):
                for j in range(2):
                    second_copy(a, p, j, part).start()

        def stage_two(a, p):
            @pl.loop(0, 2)
            def _(j):
                second_copy(a, p, j, 1).wait_recv()
                add_into(own(a, p, x_or_y(1 - j), j), second.at[a, j, 1, :, lanes(p)])
                third_copy(a, p, j).start()

            @pl.loop(0, 2)
            def _(j):
                second_copy(a, p, j, 0).wait_recv()
                add_into(own(a, p, ctx, j), second.at[a, j, 0, :, lanes(p)])

        def stage_three(a, p):
            @pl.loop(0, 2)
            def _(j):
                third_copy(a, p, j).wait_recv()
                add_into(own(a, p, ctx, j), third.at[a, j, :, lanes(p)])
                last_copy(a, p, j).start()

        def sums_copy(step):
            to_core, to_ctx = ((1 - section, ctx), (section, x_ctx), (section, y_ctx))[step]
            return remote(sums, sums_in.at[step], sums_send.at[step], sums_recv.at[step], to_core, to_ctx, shard)

        def sums_last(j):
            return remote(
                sums, sums_out.at[which], sums_send.at[3 + j], sums_recv.at[3 + which],
                shard // 2, ctx, 2 * (1 - section) + j,
            )

        sums_copy(0).start()
        items = len(pieces)

        @pl.loop(0, count + 2)
        def _(a):
            for p in range(items):

                @pl.when(a < count)
                def _():
                    stage_one(a, p)

                back = [(-(-(d - p) // items), (p - d) % items) for d in (1, 2)]

                @pl.when((a >= back[0][0]) & (a < count + back[0][0]))
                def _():
                    stage_two(a - back[0][0], back[0][1])

                @pl.when((a >= back[1][0]) & (a < count + back[1][0]))
                def _():
                    stage_three(a - back[1][0], back[1][1])

            for step in range(3):

                @pl.when(a == step)
                def _():
                    sums_copy(step).wait()
                    sums[...] += sums_in[step]
                    if step < 2:
                        sums_copy(step + 1).start()
                    else:
                        for j in range(2):
                            sums_last(j).start()

        @pl.loop(0, count)
        def _(a):
            for p in range(items):
                for j in range(2):

                    @pl.when(a >= count - 2)
                    def _():
                        first_copy(a, p, j).wait_send()

                    for part in range(2):
                        second_copy(a, p, j, part).wait_send()
                    third_copy(a, p, j).wait_send()
                    last_copy(a, p, j).wait_send()

        for j in range(2):
            sums_last(j).wait_send()

    @pl.when(kind == 0)
    def _():
        started = collect(attn_cols)

        lse[...] = jnp.zeros_like(lse)
        da[...] = jnp.zeros_like(da)
        gain, bias = norms[0:1, :width], norms[2:3, :width]

        def pair_copy(which, u):
            rows = chunk_rows(u)
            return remote(
                slots.at[1 + which, rows], slots.at[3 + which, rows], pair_send.at[which, u], pair_recv.at[which, u],
                1 - section, ctx, shard,
            )

        @pl.loop(0, chunks)
        def _(u):
            rows = chunk_rows(u)

            @pl.when(shard == 0)
            def _():
                tokens_arrived(u, ent)

            @pl.when(shard > 0)
            def _():
                up_copy(u, shard).wait_recv()

            hat, _ = normalised(ent[rows].astype(f32))
            normed = (hat * gain + bias).astype(bf16)
            nrm[rows] = normed

            @pl.loop(0, 3)
            def _(turn):
                index = lax.rem(turn + 1, 3)
                scale = jnp.where(turn == 2, score_scale, 1.0)
                slots[index, rows] = (mm(normed, weight(index, 0, wide)) * scale).astype(bf16)

                @pl.when(turn < 2)
                def _():
                    pair_copy(turn, u).start()

            for which in range(2):
                pair_copy(which, u).wait_recv()
            for index in range(chunks):

                @pl.when(u == index)
                def _():
                    attend_chunk(
                        index, pl.ds(index * size, size), mask_ref,
                        slots.at[0], slots.at[1], slots.at[3], slots.at[2], slots.at[4], o, lse,
                    )

            out = mm(o[rows, :width].astype(bf16), weight(3, 0, wide))[:, :width]
            lea[rows] = (ent[rows].astype(f32) + out).astype(bf16)
            up_copy(u, shard + 1).start()

        @pl.loop(0, chunks)
        def _(u):
            for which in range(2):
                pair_copy(which, u).wait_send()
            up_copy(u, shard + 1).wait_send()

        for copy in started:
            copy.wait_send()

        slots[7] = o[...].astype(bf16)
        group_columns(0, nrm)
        group_columns(1, slots.at[7, :, pl.ds(0, width)])
        lane = lax.broadcasted_iota(jnp.int32, (size, LANES), 1)
        low = lane < HEAD

        def swap_copy(which, u):
            rows = chunk_rows(u)
            return remote(
                slots.at[3 + which, rows], slots.at[5 + which, rows], swap_send.at[which, u], swap_recv.at[which, u],
                1 - section, ctx, shard,
            )

        @pl.loop(0, chunks)
        def _(step):
            u = chunks - 1 - step
            rows_now = chunk_rows(u)
            down_copy(u, shard).wait_recv()
            da[:, :width] = mm_t(coming[rows_now], weight(3, 0, width)).astype(bf16)
            for index in range(chunks):

                @pl.when(u == index)
                def _():
                    rows = pl.ds(index * size, size)
                    keys = pl.ds(0, (index + 1) * size)

                    @pl.loop(0, wide // LANES, unroll=3)
                    def _(pair):
                        cols = pl.ds(pl.multiple_of(pair * LANES, LANES), LANES)
                        q2 = stack_heads(slots[0, rows, cols], low)
                        grad = da[:, cols]
                        a2 = stack_heads(grad, low)
                        level = lse[rows, :]
                        product = grad.astype(f32) * o[rows, cols]
                        column = lambda which: jnp.sum(jnp.where(lane == 2 * pair + which, level, 0.0), axis=1, keepdims=True)
                        level2 = jnp.concatenate([column(0), column(1)], axis=0)
                        delta2 = jnp.concatenate(
                            [
                                jnp.sum(jnp.where(low, product, 0.0), axis=1, keepdims=True),
                                jnp.sum(jnp.where(low, 0.0, product), axis=1, keepdims=True),
                            ],
                            axis=0,
                        )
                        dq2 = 0.0
                        for part in range(2):
                            keys_now, values_now = slots[1 + 2 * part, keys, cols], slots[2 + 2 * part, keys, cols]
                            p = jnp.exp(mask_last(mm_t(q2, keys_now), mask_ref[part]) - level2)
                            ds = (p * (mm_t(a2, values_now) - delta2)).astype(bf16)
                            dq2 = dq2 + mm(ds, keys_now)
                            d_keys, d_values = t_mm(ds, q2), t_mm(p.astype(bf16), a2)
                            if index == chunks - 1:
                                big[2 * part, keys, cols] = d_keys
                                big[2 * part + 1, keys, cols] = d_values
                            else:
                                big[2 * part, keys, cols] += d_keys
                                big[2 * part + 1, keys, cols] += d_values
                        slots[0, rows, cols] = (unstack_heads(dq2, low) * score_scale).astype(bf16)

            rows = rows_now
            for which in range(2):
                slots[3 + which, rows] = big[2 + which, rows].astype(bf16)
                swap_copy(which, u).start()

            def finish_part(which, total):
                swap_copy(which, u).wait_recv()
                slots[1 + which, rows] = (big[which, rows] + slots[5 + which, rows].astype(f32)).astype(bf16)
                return total + mm_t(slots[1 + which, rows], weight(1 + which, 0, wide))

            d_normed = lax.fori_loop(0, 2, finish_part, mm_t(slots[0, rows], weight(0, 0, wide)))
            finish_chunk(rows, d_normed, gain)

            @pl.when(shard > 0)
            def _():
                down_copy(u, shard - 1).start()

            for part in range(2):
                rows_start(ent, 2 * u + part)

        @pl.loop(0, chunks)
        def _(u):
            for which in range(2):
                swap_copy(which, u).wait_send()

        def attn_source(a, p, side, emit):
            @pl.when(a == 0)
            def _():
                emit(1, coming, width)

            @pl.when(a > 0)
            def _():
                emit(0, slots.at[jnp.maximum(a - 1, 0)], wide)

        reduce(attn_source, ((0, wide),), 3, attn_out, 0)
        rows_finish(ent)

        @pl.loop(0, chunks)
        def _(u):

            @pl.when(shard > 0)
            def _():
                down_copy(u, shard - 1).wait_send()

    @pl.when(kind == 1)
    def _():
        started = collect(ff_cols)
        gain, bias = norms[1:2, :width], norms[3:4, :width]

        @pl.loop(0, chunks)
        def _(u):
            rows = chunk_rows(u)
            up_copy(u, shard).wait_recv()
            hat, _ = normalised(ent[rows].astype(f32))
            normed = (hat * gain + bias).astype(bf16)
            nrm[rows] = normed

            def add_half(i, total):
                for part, (start, columns) in enumerate(parts):
                    cols = pl.ds(0, columns)
                    upper = mm(normed, weight(i, start, columns))
                    big[2 * i + part, rows, cols] = upper
                    hidden = jax.nn.gelu(upper, approximate=True).astype(bf16)
                    slots[4 + 2 * i + part, rows, cols] = hidden
                    total = total + mm_t(hidden, weight(2 + i, start, columns))
                return total

            lea[rows] = lax.fori_loop(0, 2, add_half, ent[rows].astype(f32)).astype(bf16)

            @pl.when(shard < 3)
            def _():
                up_copy(u, shard + 1).start()

            for part in range(2):
                rows_start(lea, 2 * u + part)

        @pl.when(shard < 3)
        def _():
            group_columns(0, nrm)

        @pl.loop(0, chunks)
        def _(step):
            u = chunks - 1 - step
            rows = chunk_rows(u)

            @pl.when(shard == 3)
            def _():
                tokens_arrived(u, coming)

            @pl.when(shard < 3)
            def _():
                down_copy(u, shard).wait_recv()

            grad = coming[rows]

            def back_half(i, total):
                for part, (start, columns) in enumerate(parts):
                    cols = pl.ds(0, columns)
                    d_hidden = mm(grad, weight(2 + i, start, columns))
                    _, back = jax.vjp(lambda value: jax.nn.gelu(value, approximate=True), big[2 * i + part, rows, cols])
                    d_upper = back(d_hidden)[0].astype(bf16)
                    slots[2 * i + part, rows, cols] = d_upper
                    total = total + mm_t(d_upper, weight(i, start, columns))
                return total

            finish_chunk(rows, lax.fori_loop(0, 2, back_half, jnp.zeros((size, width), f32)), gain)
            down_copy(u, shard - 1).start()

        for copy in started:
            copy.wait_send()

        @pl.when(shard == 3)
        def _():
            group_columns(0, nrm)

        def ff_source(a, p, side, emit):
            if p == 0:

                @pl.when((a == 2) & (side == 0))
                def _():
                    group_columns(1, coming)

            emit(a // 2, slots.at[2 * a + p], parts[p][1])

        reduce(ff_source, parts, 0, ff_out, 1)
        rows_finish(lea)

        @pl.loop(0, chunks)
        def _(u):

            @pl.when(shard < 3)
            def _():
                up_copy(u, shard + 1).wait_send()

            down_copy(u, shard - 1).wait_send()

    @pl.loop(0, attn_out.shape[0])
    def _(index):
        arrivals = [(0, attn_out, 0, 0, wide)] + [(1, ff_out, p, start, columns) for p, (start, columns) in enumerate(parts)]
        for which, ref, p, start, columns in arrivals:
            ref = ref.at[index, :, pl.ds(start, columns)]
            remote(ref, ref, last_send.at[index, 0, 0], last_recv.at[which, index, p], section, ctx, shard).wait_recv()

    for which in range(2):
        remote(sums, sums_out.at[which], sums_send.at[3], sums_recv.at[3 + which], section, ctx, shard).wait_recv()
        for core in range(2):
            for block in range(2):
                ref = rows_out.at[which, block, pl.ds(core * half, half)]
                pltpu.make_async_copy(ref, ref, rows_recv.at[which, core, block]).wait()

    attn_copy.wait_send()
    ff_copy.wait_send()
    for block in range(2):

        @pl.when(jnp.logical_not(x_stays))
        def _():
            x_copy(block, True).wait_send()

        for s in range(1, 4):

            @pl.when((shard == 0) & (ctx != s))
            def _():
                pass_copy(s, block).wait_send()

    for copy, stays in norm_copies + [(g_copy(block), g_stays) for block in range(2)]:

        @pl.when(jnp.logical_not(stays))
        def _():
            copy.wait_send()


def relay(attn_piece, ff_piece, x_own, g_own, norm_own, mask, place, group_pad):
    share, ff_half = ff_piece.shape
    wide = attn_piece.shape[1]
    blocks, size, width = x_own.shape
    half = size // 2
    tokens = blocks * 4 * half
    chunks = tokens // size
    dma = pltpu.SemaphoreType.DMA
    vmem = pl.BlockSpec(memory_space=pltpu.VMEM)
    narrow = ((tokens, width), bf16)
    outs = [
        ((4, group_pad, wide), bf16), ((4, group_pad, ff_half), bf16), ((2, blocks, size, width), bf16), ((2,) + norm_own.shape, f32),
    ]
    scratch = [
        ((4, 4, share, ff_half), bf16), ((3, blocks, half, width), bf16), ((4,) + norm_own.shape, f32), (norm_own.shape, f32),
        narrow, narrow, narrow, narrow, ((8, tokens, wide), bf16),
        ((tokens, wide), f32), ((tokens, LANES), f32), ((size, wide), bf16), ((4, tokens, wide), f32),
        (norm_own.shape, f32), ((3,) + norm_own.shape, f32), ((2, 2, place.shape[1], tokens), bf16),
        ((2, 2, 4, group_pad, ff_half), bf16), ((4, 2, 2, group_pad, ff_half), bf16), ((4, 2, group_pad, ff_half), bf16),
    ]
    return pl.pallas_call(
        relay_kernel,
        in_specs=[ANY] * 5 + [vmem] * 2,
        out_specs=[ANY] * len(outs),
        out_shape=[jax.ShapeDtypeStruct(s, t) for s, t in outs],
        scratch_shapes=[pltpu.VMEM(s, t) for s, t in scratch]
        + [
            dma((14,)), dma((4, 4)), dma((2, 2)), dma((4, 2)), dma((4,)), dma((4,)), dma((2,)),
            dma((chunks,)), dma((chunks,)), dma((chunks,)), dma((chunks,)),
            dma((2, chunks)), dma((2, chunks)), dma((2, chunks)), dma((2, chunks)),
            dma((2 * chunks,)), dma((2, 2, 2)), pltpu.SemaphoreType.REGULAR,
            dma((5,)), dma((5,)), dma((4, 2, 2)), dma((4, 2, 2)), dma((4, 2, 2, 2)), dma((4, 2, 2, 2)),
            dma((4, 2, 2)), dma((4, 2, 2)), dma((4, 2, 2)), dma((2, 4, 2)), dma((3, 2)), dma((3, 2)),
        ],
        compiler_params=pltpu.CompilerParams(has_side_effects=True, vmem_limit_bytes=VMEM_BYTES),
        name="relay",
    )(attn_piece, ff_piece, x_own, g_own, norm_own, mask, place)


def chain(inputs, cotangent, qkv_weight, out_weight, up_weight, down_weight, norm_gain, norm_bias):
    section, ctx, shard = lax.axis_index("section"), lax.axis_index("ctx"), lax.axis_index("shard")
    seq_count, blocks, slice_len, width = inputs.shape
    half = slice_len // 2
    tokens = blocks * 4 * half
    share = width // 4
    group = share // 4
    group_pad = up_to(group, ROWS)
    wide = up_to(width, LANES)
    ff = up_weight.shape[2]
    is_attn = shard % 2 == 0

    pad = lambda w: jnp.pad(w, ((0, 0), (0, wide - width)))
    own_qkv, own_out = qkv_weight[0], out_weight[0]
    attn_src = jnp.stack([pad(own_qkv[:, i * width : (i + 1) * width]) for i in range(3)] + [pad(own_out)])
    down_t = down_weight[0].T
    up0 = up_weight[0]
    ff_src = jnp.stack([up0[:, : ff // 2], up0[:, ff // 2 :], down_t[:, : ff // 2], down_t[:, ff // 2 :]])
    norm_own = jnp.concatenate([norm_gain[0], norm_bias[0]], axis=0).astype(f32)
    norm_own = lax.dynamic_update_slice(
        jnp.zeros((ROWS, wide), f32), jnp.pad(norm_own, ((0, ROWS - 4), (0, 0))), (0, shard * share)
    )
    mask = attention_masks(section, half)
    mask = jnp.concatenate([mask, mask], axis=1)
    slot = jnp.arange(up_to(8 * group_pad, LANES))
    row = slot % group_pad
    place = []
    for side in (section, 1 - section):
        owner = (slot // (2 * group_pad)) * 4 + 2 * side + (slot // group_pad) % 2
        place.append(jnp.where((row < group) & (slot < 8 * group_pad), owner * group + row, -1))
    place = jnp.broadcast_to(jnp.stack(place)[:, :, None].astype(jnp.int32), (2, slot.shape[0], LANES))
    attn_sums, ff_sums, rows, totals = relay(
        lax.dynamic_index_in_dim(attn_src, ctx, 0, keepdims=False),
        lax.dynamic_index_in_dim(ff_src, ctx, 0, keepdims=False),
        inputs[0], cotangent[0], norm_own, mask, place, group_pad,
    )
    totals = lax.dynamic_slice_in_dim(totals[:, :2], (ctx * 4 + shard) * group, group, 2)
    attn_sums = attn_sums[:, :group, :width].astype(f32)
    ff_sums = ff_sums[:, :group].astype(f32)
    return (
        rows[1][None, None],
        rows[0][None, None],
        jnp.concatenate([attn_sums[0], attn_sums[1], attn_sums[2]], axis=1)[None],
        attn_sums[3][None],
        jnp.concatenate([ff_sums[0], ff_sums[1]], axis=1)[None],
        jnp.concatenate([ff_sums[2].T, ff_sums[3].T], axis=0)[None],
        totals[:, 0][None],
        totals[:, 1][None],
    )


def passed_along(value, axis, steps):
    count = lax.axis_size(axis)
    initial, last = (max(0, -steps), min(count, count - steps))
    return lax.ppermute(value, axis, [(source, source + steps) for source in range(initial, last)])


def layer_norm(values, gain, shift):
    mean = jnp.mean(values, axis=-1, keepdims=True)
    centred = values - mean
    var = jnp.mean(centred * centred, axis=-1, keepdims=True)
    return centred * lax.rsqrt(var + eps_norm) * gain + shift


def gelu_tanh(values):
    return jax.nn.gelu(values, approximate=True)


def split_pair(key_value, head_count):
    block_len, seq_count, double = key_value.shape
    model_width = double // 2
    key_rows = key_value[..., :model_width].reshape(block_len, seq_count, head_count, HEAD)
    value_rows = key_value[..., model_width:].reshape(block_len, seq_count, head_count, HEAD)
    return (key_rows, value_rows)


def causal_mask(query_pos, key_pos):
    return (key_pos[None, :] <= query_pos[:, None])[None, :, None, :]


def forward_block(running, queries, query_pos, key_value, key_pos):
    row_max, row_sum, accum = running
    key_rows, value_rows = split_pair(key_value, queries.shape[2])
    scores = (
        jnp.einsum("sqhe,kshe->sqhk", queries, key_rows, preferred_element_type=jnp.float32)
        * score_scale
    )
    causal = causal_mask(query_pos, key_pos)
    new_max = jnp.maximum(row_max, jnp.max(jnp.where(causal, scores, -1e30), axis=-1))
    softmax_w = jnp.where(causal, jnp.exp(scores - new_max[..., None]), 0.0)
    factor = jnp.exp(row_max - new_max)
    row_sum = row_sum * factor + jnp.sum(softmax_w, axis=-1)
    accum = accum * factor[..., None] + jnp.einsum(
        "sqhk,kshe->sqhe",
        softmax_w.astype(jnp.bfloat16),
        value_rows,
        preferred_element_type=jnp.float32,
    )
    return (new_max, row_sum, accum)


def split_rows(whole):
    key_count = whole.shape[0]
    block_size = 512
    blocks = whole.reshape((key_count // block_size, block_size) + whole.shape[1:])
    offsets = jnp.arange(key_count // block_size, dtype=jnp.int32) * block_size
    return (blocks, offsets, block_size)


def fold_keys(running, piece, start, queries, query_pos, group_len):
    blocks, offsets, block_size = split_rows(piece)

    def fold_scan_step(inner, scan_item):
        block_rows, offset = scan_item
        for group_id in range(block_rows.shape[2]):
            key_pos = (
                group_id * group_len + start + offset + jnp.arange(block_size, dtype=jnp.int32)
            )
            inner = forward_block(inner, queries, query_pos, block_rows[:, :, group_id], key_pos)
        return (inner, None)

    result, _ = lax.scan(fold_scan_step, running, (blocks, offsets))
    return result


def pair_terms(d_scores, softmax_w, queries, d_attended, block_size):
    d_keys = (
        jnp.einsum("sqhk,sqhe->kshe", d_scores, queries, preferred_element_type=jnp.float32)
        * score_scale
    )
    d_values = jnp.einsum(
        "sqhk,sqhe->kshe",
        softmax_w.astype(jnp.bfloat16),
        d_attended,
        preferred_element_type=jnp.float32,
    )
    shape = (block_size, queries.shape[0], queries.shape[2] * queries.shape[3])
    return jnp.concatenate([d_keys.reshape(shape), d_values.reshape(shape)], axis=-1)


def score_grads(
    queries, query_pos, log_total, row_delta, d_attended, key_rows, value_rows, key_pos
):
    scores = (
        jnp.einsum("sqhe,kshe->sqhk", queries, key_rows, preferred_element_type=jnp.float32)
        * score_scale
    )
    causal = causal_mask(query_pos, key_pos)
    softmax_w = jnp.where(causal, jnp.exp(scores - log_total[..., None]), 0.0)
    d_probs = jnp.einsum(
        "sqhe,kshe->sqhk", d_attended, value_rows, preferred_element_type=jnp.float32
    )
    d_scores = (softmax_w * (d_probs - row_delta[..., None])).astype(jnp.bfloat16)
    return (softmax_w, d_scores)


def backward_keys(whole, queries, query_pos, log_total, row_delta, d_attended, group_len):
    blocks, offsets, block_size = split_rows(whole)

    def backward_scan_step(d_queries, scan_item):
        block_rows, offset = scan_item
        for group_id in range(block_rows.shape[2]):
            key_pos = group_id * group_len + offset + jnp.arange(block_size, dtype=jnp.int32)
            key_rows, value_rows = split_pair(block_rows[:, :, group_id], queries.shape[2])
            softmax_w, d_scores = score_grads(
                queries, query_pos, log_total, row_delta, d_attended, key_rows, value_rows, key_pos
            )
            d_queries = (
                d_queries
                + jnp.einsum(
                    "sqhk,kshe->sqhe", d_scores, key_rows, preferred_element_type=jnp.float32
                )
                * score_scale
            )
        return (d_queries, None)

    d_queries, terms = lax.scan(
        backward_scan_step, jnp.zeros(queries.shape, jnp.float32), (blocks, offsets)
    )
    return (d_queries, None)


def owner_terms(
    own_cache, all_queries, all_d_att, all_totals, all_deltas, micro_index, ctx_id, group_len
):
    block_len, seq_count, group_count, double = own_cache.shape
    head_count = all_queries.shape[2]
    query_rows = all_queries.shape[1]
    query_size = 512
    block_count = query_rows // query_size

    def loop_step(index, total):
        offset = index * query_size
        q_block = lax.dynamic_slice_in_dim(all_queries, offset, query_size, 1)
        d_block = lax.dynamic_slice_in_dim(all_d_att, offset, query_size, 1)
        t_block = lax.dynamic_slice_in_dim(all_totals, offset, query_size, 1)
        r_block = lax.dynamic_slice_in_dim(all_deltas, offset, query_size, 1)
        query_pos = micro_index * group_len + offset + jnp.arange(query_size, dtype=jnp.int32)
        pieces = []
        for group_id in range(group_count):
            key_pos = (
                group_id * group_len + ctx_id * block_len + jnp.arange(block_len, dtype=jnp.int32)
            )
            key_rows, value_rows = split_pair(own_cache[:, :, group_id], head_count)
            softmax_w, d_scores = score_grads(
                q_block, query_pos, t_block, r_block, d_block, key_rows, value_rows, key_pos
            )
            pieces.append(pair_terms(d_scores, softmax_w, q_block, d_block, block_len))
        return total + jnp.stack(pieces, axis=2)

    return lax.fori_loop(0, block_count, loop_step, jnp.zeros(own_cache.shape, jnp.float32))


def store_at(store, value, micro_index, active):
    updated = lax.dynamic_update_index_in_dim(store, value, micro_index, 0)
    return jnp.where(active, updated, store)


def shards(inputs, cotangent, qkv_weight, out_weight, up_weight, down_weight, norm_gain, norm_bias):
    section_id = lax.axis_index("section")
    ctx_count = lax.axis_size("ctx")
    ctx_id = lax.axis_index("ctx")
    seq_count, group_count, block_len, model_width = inputs.shape
    head_count = model_width // HEAD
    group_len = block_len * ctx_count
    row_count = seq_count * block_len
    w_qkv, w_out, w_up, w_down, gains, biases = (
        lax.all_gather(qkv_weight[0], "shard", axis=0, tiled=True),
        lax.all_gather(out_weight[0], "shard", axis=0, tiled=True),
        lax.all_gather(up_weight[0], "shard", axis=0, tiled=True),
        lax.all_gather(down_weight[0], "shard", axis=1, tiled=True),
        lax.all_gather(norm_gain[0], "shard", axis=1, tiled=True),
        lax.all_gather(norm_bias[0], "shard", axis=1, tiled=True),
    )
    gains = gains.astype(jnp.float32)
    biases = biases.astype(jnp.float32)
    ff_width = w_up.shape[1]
    cache = jnp.zeros((block_len, seq_count, group_count, 2 * model_width), jnp.bfloat16)
    in_store = jnp.zeros((group_count, seq_count, block_len, model_width), jnp.bfloat16)
    query_store = jnp.zeros((group_count, seq_count, block_len, head_count, HEAD), jnp.bfloat16)
    att_store = jnp.zeros((group_count, seq_count, block_len, head_count, HEAD), jnp.float32)
    total_store = jnp.zeros((group_count, seq_count, block_len, head_count), jnp.float32)
    middle_store = jnp.zeros((group_count, row_count, model_width), jnp.float32)
    upper_store = jnp.zeros((group_count, row_count, ff_width), jnp.float32)
    out_store = jnp.zeros((group_count, seq_count, block_len, model_width), jnp.bfloat16)
    received = jnp.zeros((seq_count, block_len, model_width), jnp.bfloat16)
    for tick_no in range(group_count + 1):
        micro = tick_no - section_id
        active = (micro >= 0) & (micro < group_count)
        micro_index = jnp.clip(micro, 0, group_count - 1)
        own_input = lax.dynamic_index_in_dim(inputs, micro_index, 1, keepdims=False)
        entering = jnp.where(section_id == 0, own_input, received)
        flat_rows = entering.reshape(row_count, model_width).astype(jnp.float32)
        normed = layer_norm(flat_rows, gains[0], biases[0]).astype(jnp.bfloat16)
        mixed = jnp.dot(normed, w_qkv, preferred_element_type=jnp.float32).astype(jnp.bfloat16)
        queries = mixed[:, :model_width].reshape(seq_count, block_len, head_count, HEAD)
        fresh = jnp.swapaxes(
            mixed[:, model_width:].reshape(seq_count, block_len, 2 * model_width), 0, 1
        )
        updated = lax.dynamic_update_index_in_dim(cache, fresh, micro_index, 2)
        cache = jnp.where(active, updated, cache)
        query_pos = (
            micro_index * group_len + ctx_id * block_len + jnp.arange(block_len, dtype=jnp.int32)
        )
        start_state = (
            jnp.full((seq_count, block_len, head_count), -1e30, jnp.float32),
            jnp.zeros((seq_count, block_len, head_count), jnp.float32),
            jnp.zeros((seq_count, block_len, head_count, HEAD), jnp.float32),
        )
        row_max, row_sum, accum = fold_keys(
            start_state,
            lax.all_gather(cache, "ctx", axis=0, tiled=True),
            jnp.int32(0),
            queries,
            query_pos,
            group_len,
        )
        attended = accum / row_sum[..., None]
        log_total = row_max + jnp.log(row_sum)
        att_low = attended.reshape(row_count, model_width).astype(jnp.bfloat16)
        middle = flat_rows + jnp.dot(att_low, w_out, preferred_element_type=jnp.float32)
        normed2 = layer_norm(middle, gains[1], biases[1]).astype(jnp.bfloat16)
        upper = jnp.dot(normed2, w_up, preferred_element_type=jnp.float32)
        hidden = gelu_tanh(upper).astype(jnp.bfloat16)
        leaving = (middle + jnp.dot(hidden, w_down, preferred_element_type=jnp.float32)).astype(
            jnp.bfloat16
        )
        leaving = leaving.reshape(seq_count, block_len, model_width)
        in_store = store_at(in_store, entering, micro_index, active)
        query_store = store_at(query_store, queries, micro_index, active)
        att_store = store_at(att_store, attended, micro_index, active)
        total_store = store_at(total_store, log_total, micro_index, active)
        middle_store = store_at(middle_store, middle, micro_index, active)
        upper_store = store_at(upper_store, upper, micro_index, active)
        out_store = store_at(out_store, leaving, micro_index, active)
        if tick_no < group_count:
            received = passed_along(leaving, "section", 1)
    key_acc = jnp.zeros((block_len, seq_count, group_count, 2 * model_width), jnp.float32)
    grad_qkv = jnp.zeros((model_width, 3 * model_width), jnp.float32)
    grad_out = jnp.zeros((model_width, model_width), jnp.float32)
    grad_up = jnp.zeros((model_width, ff_width), jnp.float32)
    grad_down = jnp.zeros((ff_width, model_width), jnp.float32)
    grad_gain = jnp.zeros((2, model_width), jnp.float32)
    grad_bias = jnp.zeros((2, model_width), jnp.float32)
    grad_store = jnp.zeros((group_count, seq_count, block_len, model_width), jnp.bfloat16)
    coming = jnp.zeros((seq_count, block_len, model_width), jnp.bfloat16)
    for tick_no in range(group_count + 1):
        micro = group_count - tick_no - section_id
        active = (micro >= 0) & (micro < group_count)
        active_weight = active.astype(jnp.float32)
        micro_index = jnp.clip(micro, 0, group_count - 1)
        own_cot = lax.dynamic_index_in_dim(cotangent, micro_index, 1, keepdims=False)
        d_out = (
            jnp.where(section_id == 1, own_cot, coming)
            .reshape(row_count, model_width)
            .astype(jnp.float32)
        )
        flat_rows = in_store[micro_index].reshape(row_count, model_width).astype(jnp.float32)
        queries = query_store[micro_index]
        attended = att_store[micro_index]
        log_total = total_store[micro_index]
        middle = middle_store[micro_index]
        upper = upper_store[micro_index]
        normed2_full, norm2_back = jax.vjp(
            lambda v, g, b: layer_norm(v, g, b), middle, gains[1], biases[1]
        )
        normed2 = normed2_full.astype(jnp.bfloat16)
        hidden_full, gelu_back = jax.vjp(gelu_tanh, upper)
        hidden = hidden_full.astype(jnp.bfloat16)
        d_branch = d_out.astype(jnp.bfloat16)
        grad_down = grad_down + active_weight * jnp.dot(
            hidden.T, d_branch, preferred_element_type=jnp.float32
        )
        d_hidden = jnp.dot(d_branch, w_down.T, preferred_element_type=jnp.float32)
        d_upper = gelu_back(d_hidden)[0].astype(jnp.bfloat16)
        grad_up = grad_up + active_weight * jnp.dot(
            normed2.T, d_upper, preferred_element_type=jnp.float32
        )
        d_normed2 = jnp.dot(d_upper, w_up.T, preferred_element_type=jnp.float32)
        d_mid_norm, d_gain2, d_bias2 = norm2_back(d_normed2)
        d_middle = d_out + d_mid_norm
        att_low = attended.reshape(row_count, model_width).astype(jnp.bfloat16)
        d_att = d_middle.astype(jnp.bfloat16)
        grad_out = grad_out + active_weight * jnp.dot(
            att_low.T, d_att, preferred_element_type=jnp.float32
        )
        d_attended = jnp.dot(d_att, w_out.T, preferred_element_type=jnp.float32).astype(
            jnp.bfloat16
        )
        d_attended = d_attended.reshape(seq_count, block_len, head_count, HEAD)
        row_delta = jnp.sum(d_attended.astype(jnp.float32) * attended, axis=-1)
        query_pos = (
            micro_index * group_len + ctx_id * block_len + jnp.arange(block_len, dtype=jnp.int32)
        )
        whole = lax.all_gather(cache, "ctx", axis=0, tiled=True)
        d_queries, unused = backward_keys(
            whole, queries, query_pos, log_total, row_delta, d_attended, group_len
        )
        all_queries, all_d_att = (
            lax.all_gather(queries, "ctx", axis=1, tiled=True),
            lax.all_gather(d_attended, "ctx", axis=1, tiled=True),
        )
        all_totals, all_deltas = (
            lax.all_gather(log_total, "ctx", axis=1, tiled=True),
            lax.all_gather(row_delta, "ctx", axis=1, tiled=True),
        )
        shares = owner_terms(
            cache, all_queries, all_d_att, all_totals, all_deltas, micro_index, ctx_id, group_len
        )
        key_acc = key_acc + active_weight * shares
        d_pair = jnp.swapaxes(
            lax.dynamic_index_in_dim(key_acc, micro_index, 2, keepdims=False), 0, 1
        )
        d_mixed = jnp.concatenate(
            [d_queries.reshape(row_count, model_width), d_pair.reshape(row_count, 2 * model_width)],
            axis=-1,
        ).astype(jnp.bfloat16)
        normed_full, norm1_back = jax.vjp(
            lambda v, g, b: layer_norm(v, g, b), flat_rows, gains[0], biases[0]
        )
        normed = normed_full.astype(jnp.bfloat16)
        grad_qkv = grad_qkv + active_weight * jnp.dot(
            normed.T, d_mixed, preferred_element_type=jnp.float32
        )
        d_normed = jnp.dot(d_mixed, w_qkv.T, preferred_element_type=jnp.float32)
        d_flat_norm, d_gain1, d_bias1 = norm1_back(d_normed)
        grad_gain = grad_gain + active_weight * jnp.stack([d_gain1, d_gain2])
        grad_bias = grad_bias + active_weight * jnp.stack([d_bias1, d_bias2])
        d_entering = (
            (d_middle + d_flat_norm).astype(jnp.bfloat16).reshape(seq_count, block_len, model_width)
        )
        grad_store = store_at(grad_store, d_entering, micro_index, active)
        if tick_no < group_count:
            coming = passed_along(d_entering, "section", -1)
    sums = (
        lax.psum_scatter(grad_qkv, ("ctx", "shard"), scatter_dimension=0, tiled=True),
        lax.psum_scatter(grad_out, ("ctx", "shard"), scatter_dimension=0, tiled=True),
        lax.psum_scatter(grad_up, ("ctx", "shard"), scatter_dimension=0, tiled=True),
        lax.psum_scatter(grad_down, ("ctx", "shard"), scatter_dimension=1, tiled=True),
        lax.psum_scatter(grad_gain, ("ctx", "shard"), scatter_dimension=1, tiled=True),
        lax.psum_scatter(grad_bias, ("ctx", "shard"), scatter_dimension=1, tiled=True),
    )
    layer_outputs = jnp.swapaxes(out_store, 0, 1)[None]
    input_grads = jnp.swapaxes(grad_store, 0, 1)[None]
    return (
        layer_outputs,
        input_grads,
        sums[0][None],
        sums[1][None],
        sums[2][None],
        sums[3][None],
        sums[4][None],
        sums[5][None],
    )


def solution(mesh):
    in_specs = (
        P("shard", None, "ctx", None),
        P("shard", None, "ctx", None),
        P("section", "shard", None),
        P("section", "shard", None),
        P("section", "shard", None),
        P("section", None, "shard"),
        P("section", None, "shard"),
        P("section", None, "shard"),
    )
    out_specs = (
        P("section", "shard", None, "ctx", None),
        P("section", "shard", None, "ctx", None),
        P("section", ("ctx", "shard"), None),
        P("section", ("ctx", "shard"), None),
        P("section", ("ctx", "shard"), None),
        P("section", None, ("ctx", "shard")),
        P("section", None, ("ctx", "shard")),
        P("section", None, ("ctx", "shard")),
    )
    relay = mesh.shape["section"] == 2 and mesh.shape["shard"] == 4 and mesh.shape["ctx"] == 4
    return jax.shard_map(chain if relay else shards, mesh=mesh, in_specs=in_specs, out_specs=out_specs, check_vma=False)
```
